32 devices in a mesh: fsdp: 2 (over x), blk: 4 (over y, core), uly: 4 (over z).
Axes of the slice: x: 2, y: 2, z: 4, core: 2. Of those that a mesh axis runs over, the one named last changes fastest.
Arguments:
- inputs: bfloat16 [4, 1024, 1024], P('fsdp', ('blk', 'uly')), may hold values from -36 to 36
- segments: int32 [4, 1024], P('fsdp'), may hold values from 0 to 3, never falling along the last dimension, each value on 1 to 512 neighbouring positions
- attn_gain: bfloat16 [1024], P(('fsdp', 'blk', 'uly')), may hold values from 0.5 to 1.5
- head_gains: bfloat16 [2, 128], replicated, may hold values from 0.5 to 1.5
- query_weight: bfloat16 [1024, 2048], P(('fsdp', 'blk', 'uly')), may hold values from -0.1875 to 0.1875
- key_matrix: bfloat16 [1024, 1024], P(('fsdp', 'blk', 'uly')), may hold values from -0.1875 to 0.1875
- value_matrix: bfloat16 [1024, 1024], P(('fsdp', 'blk', 'uly')), may hold values from -0.1875 to 0.1875
- out_weight: bfloat16 [2048, 1024], P(('fsdp', 'blk', 'uly')), may hold values from -1.5 to 1.5
- ffn_gain: bfloat16 [1024], P(('fsdp', 'blk', 'uly')), may hold values from 0.5 to 1.5
- gate_weight: bfloat16 [1024, 3072], P(('fsdp', 'blk', 'uly')), may hold values from -0.1875 to 0.1875
- up_weight: bfloat16 [1024, 3072], P(('fsdp', 'blk', 'uly')), may hold values from -0.1875 to 0.1875
- down_weight: bfloat16 [3072, 1024], P(('fsdp', 'blk', 'uly')), may hold values from -0.109375 to 0.109375
- cotangent: bfloat16 [4, 1024, 1024], P('fsdp', ('blk', 'uly')), may hold values from -6 to 6
Outputs:
- outputs: bfloat16 [4, 1024, 1024], P('fsdp', ('blk', 'uly'))
- grad_inputs: bfloat16 [4, 1024, 1024], P('fsdp', ('blk', 'uly'))
- grad_attn_gain: float32 [1024], P(('fsdp', 'blk', 'uly'))
- grad_head_gains: float32 [2, 128], P(None, ('fsdp', 'blk', 'uly'))
- grad_query_weight: float32 [1024, 2048], P(('fsdp', 'blk', 'uly'))
- grad_key_weight: float32 [1024, 1024], P(('fsdp', 'blk', 'uly'))
- grad_value_weight: float32 [1024, 1024], P(('fsdp', 'blk', 'uly'))
- grad_out_weight: float32 [2048, 1024], P(('fsdp', 'blk', 'uly'))
- grad_ffn_gain: float32 [1024], P(('fsdp', 'blk', 'uly'))
- grad_gate_weight: float32 [1024, 3072], P(('fsdp', 'blk', 'uly'))
- grad_up_weight: float32 [1024, 3072], P(('fsdp', 'blk', 'uly'))
- grad_down_weight: float32 [3072, 1024], P(('fsdp', 'blk', 'uly'))
The draws below stay inside these ranges and needn't reach their ends.
Inputs may be any that keep to these rules, and one draw needn't show every extreme that they name: `segments`: document numbers never fall along a sequence; every document has 1 to 512 tokens, and one of each sequence has exactly 512.
All inputs are finite; a program needn't handle non-finite values.
Results may differ from the reference program's by a relative error of at most 0.017.
Values may be sent and summed in bfloat16 or wider, within the bound.
A program may use at most 192 MiB of HBM per device.

```python
import math
import jax
import jax.numpy as jnp
import numpy as np
from jax import lax

MODEL_SIZE = 1024
QUERY_HEADS = 16
KEY_VALUE_HEADS = 8
HEAD_SIZE = 128
FF = 3072
DOCS = 4
ROWS = 4
SEQUENCE_LENGTH = 1024


def draw_inputs(key, part):
    key_base, key_rows, key_cols = jax.random.split(key, 3)
    low_end = math.log(0.3)
    high_end = math.log(3.0)
    row_scale = jnp.exp(jax.random.uniform(key_rows, (ROWS, SEQUENCE_LENGTH, 1), jnp.float32, low_end, high_end))
    col_scale = jnp.exp(jax.random.uniform(key_cols, (1, 1, MODEL_SIZE), jnp.float32, low_end, high_end))
    base_values = jnp.clip(jax.random.normal(key_base, (ROWS, SEQUENCE_LENGTH, MODEL_SIZE), jnp.float32), -4.0, 4.0)
    return (base_values * row_scale * col_scale).astype(jnp.bfloat16)


def level_of(own_key, shape, cuts, least, largest):
    level = 1.0
    for dim, shards_of in cuts:
        heights = jax.random.uniform(jax.random.fold_in(jax.random.fold_in(own_key, 6), dim), (shards_of,), jnp.float32, least / len(cuts), largest / len(cuts))
        level = level * jnp.repeat(jnp.exp(heights), shape[dim] // shards_of).reshape((-1,) + (1,) * (len(shape) - 1 - dim))
    return level


def profile(number_of, total, reach, slope):
    loads = [(1 << 20) // math.isqrt(rank ** slope) + 1 for rank in range(2, number_of + 1)]
    spare, given = total - reach - (number_of - 1), [1] * (number_of - 1)
    while spare > 0:
        movable = [i for i in range(number_of - 1) if given[i] < reach]
        pool, left = sum([loads[i] for i in movable]), spare
        for i in movable:
            more = min(reach - given[i], max(1, left * loads[i] // pool), spare)
            given[i] = given[i] + more
            spare = spare - more
    return np.array([reach] + given)


def ragged_sizes(own_key, amount, total, most, skew):
    if amount == 2:
        one = jax.random.randint(own_key, (), max(1, total - most), min(most, total - 1) + 1)
        return jnp.stack([one, total - one])
    tallies = jnp.asarray(profile(amount, total, most, skew), jnp.int32)
    pairs = (amount - 1) // 2
    giver, taker = tallies[1:1 + 2 * pairs:2], tallies[2:2 + 2 * pairs:2]
    slack = jnp.minimum(giver - 1, most - taker)
    moved = jax.random.randint(jax.random.fold_in(own_key, 1), (pairs,), 0, 1 << 20) % (slack + 1)
    tallies = tallies.at[1:1 + 2 * pairs:2].set(giver - moved).at[2:2 + 2 * pairs:2].set(taker + moved)
    return tallies[jax.random.permutation(jax.random.fold_in(own_key, 2), amount)]


def normal_values(own_key, dims, spread, most, cuts=(), kind=jnp.bfloat16):
    factor_of = level_of(own_key, dims, cuts, -0.22, 0.18) if cuts else 1.0
    values = jax.random.normal(own_key, dims, jnp.float32) * spread * factor_of
    return jnp.minimum(jnp.maximum(values, -most), most).astype(kind)


def setup_inputs(seed: int = 0) -> dict:
    arg_keys = jax.random.split(jax.random.key(seed), 14)
    return {
        "inputs": draw_inputs(jax.random.fold_in(arg_keys[13], 71), 0),
        "segments": jax.vmap(lambda own: jnp.searchsorted(jnp.cumsum(ragged_sizes(own, DOCS, SEQUENCE_LENGTH, SEQUENCE_LENGTH // 2, 1)), jnp.arange(SEQUENCE_LENGTH), side="right"))(jax.random.split(arg_keys[1], ROWS)).reshape((ROWS, SEQUENCE_LENGTH)).astype(jnp.int32),
        "attn_gain": jnp.clip(1.0 + 0.1 * jax.random.normal(arg_keys[2], (MODEL_SIZE,), jnp.float32), 0.5, 1.5).astype(jnp.bfloat16),
        "head_gains": jnp.clip(1.0 + 0.1 * jax.random.normal(arg_keys[3], (2, HEAD_SIZE), jnp.float32), 0.5, 1.5).astype(jnp.bfloat16),
        "query_weight": normal_values(arg_keys[4], (MODEL_SIZE, QUERY_HEADS * HEAD_SIZE), MODEL_SIZE ** -0.5, 0.1875, ((0, 32),)),
        "key_matrix": normal_values(arg_keys[5], (MODEL_SIZE, KEY_VALUE_HEADS * HEAD_SIZE), MODEL_SIZE ** -0.5, 0.1875, ((0, 32),)),
        "value_matrix": normal_values(arg_keys[6], (MODEL_SIZE, KEY_VALUE_HEADS * HEAD_SIZE), MODEL_SIZE ** -0.5, 0.1875, ((0, 32),)),
        "out_weight": normal_values(arg_keys[7], (QUERY_HEADS * HEAD_SIZE, MODEL_SIZE), (max(1, QUERY_HEADS * HEAD_SIZE * 8 // SEQUENCE_LENGTH)) ** -0.5, 1.5, ((0, 32),)),
        "ffn_gain": jnp.clip(1.0 + 0.1 * jax.random.normal(arg_keys[8], (MODEL_SIZE,), jnp.float32), 0.5, 1.5).astype(jnp.bfloat16),
        "gate_weight": normal_values(arg_keys[9], (MODEL_SIZE, FF), MODEL_SIZE ** -0.5, 0.1875, ((0, 32),)),
        "up_weight": normal_values(arg_keys[10], (MODEL_SIZE, FF), MODEL_SIZE ** -0.5, 0.1875, ((0, 32),)),
        "down_weight": normal_values(arg_keys[11], (FF, MODEL_SIZE), FF ** -0.5, 0.109375, ((0, 32),)),
        "cotangent": normal_values(arg_keys[12], (ROWS, SEQUENCE_LENGTH, MODEL_SIZE), 1.0, 6.0, ((0, 2), (1, 16))),
    }


EPSILON = 1e-06
THETA = 1000000.0
TOP_PRECISION = lax.Precision.HIGHEST

@jax.custom_vjp
def low(v):
    return lax.optimization_barrier(v.astype(jnp.bfloat16)).astype(jnp.float32)

@jax.custom_vjp
def low_back(v):
    return v

def low_keep(v):
    return (low(v), None)

def low_pass(kept, grad):
    return (grad,)

def back_keep(v):
    return (v, None)

def back_low(kept, grad):
    return (low(grad),)
low.defvjp(low_keep, low_pass)
low_back.defvjp(back_keep, back_low)

def rms_norm(vector, weight):
    mean_square = lax.optimization_barrier(jnp.mean(vector * vector, axis=-1, keepdims=True))
    return vector * lax.rsqrt(mean_square + EPSILON) * weight

def rotate(vector, cosine, sine_table):
    half_width = vector.shape[-1] // 2
    turned = jnp.concatenate([-vector[..., half_width:], vector[..., :half_width]], axis=-1)
    return vector * cosine + turned * sine_table

def rope_tables(seg_row):
    token_index = jnp.arange(SEQUENCE_LENGTH, dtype=jnp.int32)
    doc_ids = jnp.arange(DOCS, dtype=jnp.int32)
    starts = lax.optimization_barrier(jnp.sum((seg_row[None, :] < doc_ids[:, None]).astype(jnp.int32), axis=1))
    doc_start = lax.optimization_barrier(jnp.sum(jnp.where(seg_row[:, None] == doc_ids[None, :], starts[None, :], 0), axis=1))
    token_place = (token_index - doc_start).astype(jnp.float32)
    inverse = jnp.exp(jnp.arange(HEAD_SIZE // 2, dtype=jnp.float32) * (-2.0 * math.log(THETA) / HEAD_SIZE))
    angles = token_place[:, None] * inverse[None, :]
    cosine = jnp.concatenate([jnp.cos(angles), jnp.cos(angles)], axis=-1)
    sine_table = jnp.concatenate([jnp.sin(angles), jnp.sin(angles)], axis=-1)
    return (cosine, sine_table)

def attention(query_matrix_rows, keys, values, seg_row, bound):
    rows_per_block = math.gcd(SEQUENCE_LENGTH, 512)
    heads_per_group = QUERY_HEADS // KEY_VALUE_HEADS
    block_split = query_matrix_rows.reshape(SEQUENCE_LENGTH // rows_per_block, rows_per_block, KEY_VALUE_HEADS, heads_per_group, HEAD_SIZE)
    key_index = jnp.arange(SEQUENCE_LENGTH, dtype=jnp.int32)
    offsets = jnp.arange(SEQUENCE_LENGTH // rows_per_block, dtype=jnp.int32) * rows_per_block

    def one_block(operands):
        query_block, offset = operands
        query_index = offset + jnp.arange(rows_per_block, dtype=jnp.int32)
        query_segment = lax.dynamic_slice_in_dim(seg_row, offset, rows_per_block)
        allowed = (key_index[None, :] <= query_index[:, None]) & (seg_row[None, :] == query_segment[:, None])
        scores = jnp.einsum('qhgd,khd->hgqk', query_block, keys, precision=TOP_PRECISION) * HEAD_SIZE ** (-0.5)
        scores = low_back(scores)
        weights = jnp.where(allowed[None, None], jnp.exp(scores - bound), 0.0)
        totals = lax.optimization_barrier(jnp.sum(weights, axis=-1))
        mixed = jnp.einsum('hgqk,khd->qhgd', low(weights), values, precision=TOP_PRECISION)
        return mixed / jnp.transpose(totals, (2, 0, 1))[..., None]
    mixed_all = lax.map(jax.checkpoint(one_block), (block_split, offsets))
    return mixed_all.reshape(SEQUENCE_LENGTH, QUERY_HEADS, HEAD_SIZE)

def layer_forward(rows_in, params, seg_row, cosine, sine_table, bound):
    attn_gain, head_gains, query_weight, key_matrix, value_matrix, out_weight, ffn_gain, gate_weight, up_weight, down_weight = params
    normalized_input = low(rms_norm(rows_in, attn_gain))
    query_pre = low_back(jnp.dot(normalized_input, query_weight, precision=TOP_PRECISION)).reshape(SEQUENCE_LENGTH, QUERY_HEADS, HEAD_SIZE)
    key_before_rotate = low_back(jnp.dot(normalized_input, key_matrix, precision=TOP_PRECISION)).reshape(SEQUENCE_LENGTH, KEY_VALUE_HEADS, HEAD_SIZE)
    rows_of_value = low_back(low(jnp.dot(normalized_input, value_matrix, precision=TOP_PRECISION))).reshape(SEQUENCE_LENGTH, KEY_VALUE_HEADS, HEAD_SIZE)
    cos_heads = cosine[:, None, :]
    sin_heads = sine_table[:, None, :]
    query_rows = low_back(low(rotate(rms_norm(query_pre, head_gains[0]), cos_heads, sin_heads)))
    key_rows = low_back(low(rotate(rms_norm(key_before_rotate, head_gains[1]), cos_heads, sin_heads)))
    attended = attention(query_rows, key_rows, rows_of_value, seg_row, bound)
    attended = low_back(low(attended)).reshape(SEQUENCE_LENGTH, QUERY_HEADS * HEAD_SIZE)
    middle = rows_in + low_back(jnp.dot(attended, out_weight, precision=TOP_PRECISION))
    normed_two = low(rms_norm(middle, ffn_gain))
    gate_rows = low_back(jnp.dot(normed_two, gate_weight, precision=TOP_PRECISION))
    up_rows = low_back(jnp.dot(normed_two, up_weight, precision=TOP_PRECISION))
    hidden = low(jax.nn.silu(gate_rows) * up_rows)
    return middle + low_back(jnp.dot(hidden, down_weight, precision=TOP_PRECISION))

def reference(inputs, segments, attn_gain, head_gains, query_weight, key_matrix, value_matrix, out_weight, ffn_gain, gate_weight, up_weight, down_weight, cotangent):
    params = tuple((matrix.astype(jnp.float32) for matrix in (attn_gain, head_gains, query_weight, key_matrix, value_matrix, out_weight, ffn_gain, gate_weight, up_weight, down_weight)))
    gains_float = params[1]
    bound = math.sqrt(HEAD_SIZE) * jnp.max(jnp.abs(gains_float[0])) * jnp.max(jnp.abs(gains_float[1]))

    def per_sequence(running, operands):
        rows_in, seg_row, cot_row = operands
        cosine, sine_table = rope_tables(seg_row)

        def forward(rows_arg, *weights):
            return layer_forward(rows_arg, weights, seg_row, cosine, sine_table, bound)
        output, pullback = jax.vjp(forward, rows_in, *params)
        gradients = pullback(cot_row)
        running = tuple((total + gradient for total, gradient in zip(running, gradients[1:])))
        return (running, (output.astype(jnp.bfloat16), gradients[0].astype(jnp.bfloat16)))
    initial = tuple((jnp.zeros(matrix.shape, jnp.float32) for matrix in params))
    running, (outputs, input_grads) = lax.scan(per_sequence, initial, (inputs.astype(jnp.float32), segments, cotangent.astype(jnp.float32)))
    return (outputs, input_grads, running[0], running[1], running[2], running[3], running[4], running[5], running[6], running[7], running[8], running[9])
```

```python
import functools
import math

import jax
import jax.numpy as jnp
from jax import lax
from jax.experimental import pallas as pl
from jax.experimental.pallas import tpu as pltpu
from jax.sharding import PartitionSpec as P

DOCS = 4


EPSILON = 1e-06
THETA = 1000000.0


def passed_along(value, axis, steps):
    count = lax.axis_size(axis)
    first, last = (max(0, -steps), min(count, count - steps))
    return lax.ppermute(value, axis, [(source, source + steps) for source in range(first, last)])


def from_behind(value, axis, steps):
    count = lax.axis_size(axis)
    pairs = [(source, (source + steps) % count) for source in range(count)]
    return lax.ppermute(value, axis, pairs)


def rms_norm(vector, weight):
    mean_square = jnp.mean(vector * vector, axis=-1, keepdims=True)
    return vector * lax.rsqrt(mean_square + EPSILON) * weight


def rotate(vector, cosine, sine_table):
    half_width = vector.shape[-1] // 2
    turned = jnp.concatenate([-vector[..., half_width:], vector[..., :half_width]], axis=-1)
    return vector * cosine + turned * sine_table


def prepare(query_pre, key_before_rotate, gains, cosine, sine_table):
    cos_heads = cosine[:, :, None, :]
    sin_heads = sine_table[:, :, None, :]
    query_rot = rotate(rms_norm(query_pre, gains[0]), cos_heads, sin_heads)
    key_rot = rotate(rms_norm(key_before_rotate, gains[1]), cos_heads, sin_heads)
    return (query_rot, key_rot)


def swiglu(gate_rows, up_rows):
    return jax.nn.silu(gate_rows) * up_rows


def fetch_attention(attn_gain, query_weight, key_matrix, value_matrix, out_weight):
    return (
        lax.all_gather(attn_gain, ("fsdp", "blk", "uly"), axis=0, tiled=True),
        lax.all_gather(query_weight, ("fsdp", "blk", "uly"), axis=0, tiled=True),
        lax.all_gather(key_matrix, ("fsdp", "blk", "uly"), axis=0, tiled=True),
        lax.all_gather(value_matrix, ("fsdp", "blk", "uly"), axis=0, tiled=True),
        lax.all_gather(out_weight, ("fsdp", "blk", "uly"), axis=0, tiled=True),
    )


def fetch_feedforward(ffn_gain, gate_weight, up_weight, down_weight):
    return (
        lax.all_gather(ffn_gain, ("fsdp", "blk", "uly"), axis=0, tiled=True),
        lax.all_gather(gate_weight, ("fsdp", "blk", "uly"), axis=0, tiled=True),
        lax.all_gather(up_weight, ("fsdp", "blk", "uly"), axis=0, tiled=True),
        lax.all_gather(down_weight, ("fsdp", "blk", "uly"), axis=0, tiled=True),
    )


def body(
    inputs,
    segments,
    attn_gain,
    head_gains,
    query_weight,
    key_matrix,
    value_matrix,
    out_weight,
    ffn_gain,
    gate_weight,
    up_weight,
    down_weight,
    cotangent,
):
    seq_count, tok_count, model_width = inputs.shape
    head_dim = head_gains.shape[1]
    query_heads = query_weight.shape[1] // head_dim
    value_heads = key_matrix.shape[1] // head_dim
    heads_per_group = query_heads // value_heads
    uly_size = lax.axis_size("uly")
    blk_size = lax.axis_size("blk")
    blk_index = lax.axis_index("blk")
    uly_index = lax.axis_index("uly")
    offset = (blk_index * uly_size + uly_index) * tok_count
    doc_ids = jnp.arange(DOCS, dtype=jnp.int32)
    starts = jnp.sum((segments[:, None, :] < doc_ids[None, :, None]).astype(jnp.int32), axis=2)
    local_segs = lax.dynamic_slice_in_dim(segments, offset, tok_count, 1)
    doc_start = jnp.sum(
        jnp.where(local_segs[:, :, None] == doc_ids[None, None, :], starts[:, None, :], 0), axis=2
    )
    token_place = (offset + jnp.arange(tok_count, dtype=jnp.int32)[None, :] - doc_start).astype(
        jnp.float32
    )
    inverse = jnp.exp(
        jnp.arange(head_dim // 2, dtype=jnp.float32) * (-2.0 * math.log(THETA) / head_dim)
    )
    angles = token_place[..., None] * inverse
    cosine = jnp.concatenate([jnp.cos(angles), jnp.cos(angles)], axis=-1)
    sine_table = jnp.concatenate([jnp.sin(angles), jnp.sin(angles)], axis=-1)
    floats = inputs.astype(jnp.float32)
    gain_one, query_full, key_full, value_full, out_full = fetch_attention(
        attn_gain, query_weight, key_matrix, value_matrix, out_weight
    )
    normed_float, norm_pull_one = jax.vjp(rms_norm, floats, gain_one.astype(jnp.float32))
    normalized_input = normed_float.astype(jnp.bfloat16)
    query_pre = jnp.einsum(
        "std,de->ste", normalized_input, query_full, preferred_element_type=jnp.float32
    ).reshape(seq_count, tok_count, query_heads, head_dim)
    key_before_rotate = jnp.einsum(
        "std,de->ste", normalized_input, key_full, preferred_element_type=jnp.float32
    ).reshape(seq_count, tok_count, value_heads, head_dim)
    rows_of_value = (
        jnp.einsum("std,de->ste", normalized_input, value_full, preferred_element_type=jnp.float32)
        .astype(jnp.bfloat16)
        .reshape(seq_count, tok_count, value_heads, head_dim)
    )
    head_float = head_gains.astype(jnp.float32)

    def prepare_local(query_arg, key_arg, gains_arg):
        return prepare(query_arg, key_arg, gains_arg, cosine, sine_table)

    (query_rot, key_rot), prep_pull = jax.vjp(
        prepare_local, query_pre, key_before_rotate, head_float
    )
    query_local, key_local, value_local = (
        lax.all_to_all(
            query_rot.astype(jnp.bfloat16), "uly", split_axis=2, concat_axis=1, tiled=True
        ),
        lax.all_to_all(
            key_rot.astype(jnp.bfloat16), "uly", split_axis=2, concat_axis=1, tiled=True
        ),
        lax.all_to_all(rows_of_value, "uly", split_axis=2, concat_axis=1, tiled=True),
    )
    block_len = query_local.shape[1]
    local_kv = key_local.shape[2]
    query_group = query_local.reshape(seq_count, block_len, local_kv, heads_per_group, head_dim)
    bound = math.sqrt(head_dim) * jnp.max(jnp.abs(head_float[0])) * jnp.max(jnp.abs(head_float[1]))
    scale = head_dim ** (-0.5)
    query_index = blk_index * block_len + jnp.arange(block_len, dtype=jnp.int32)
    query_segs = lax.dynamic_slice_in_dim(segments, blk_index * block_len, block_len, 1)

    def block_weights(keys_in, source):
        key_index = source * block_len + jnp.arange(block_len, dtype=jnp.int32)
        key_segs = lax.dynamic_slice_in_dim(segments, source * block_len, block_len, 1)
        allowed = (key_index[None, None, :] <= query_index[None, :, None]) & (
            key_segs[:, None, :] == query_segs[:, :, None]
        )
        scores = (
            jnp.einsum(
                "sqhgd,skhd->shgqk", query_group, keys_in, preferred_element_type=jnp.float32
            )
            * scale
        )
        return jnp.where(allowed[:, None, None], jnp.exp(scores - bound), 0.0)

    def absorb(stats, key_value, source):
        row_sums, summed = stats
        weights = block_weights(key_value[0], source)
        row_sums = row_sums + jnp.sum(weights, axis=-1)
        summed = summed + jnp.einsum(
            "shgqk,skhd->sqhgd",
            weights.astype(jnp.bfloat16),
            key_value[1],
            preferred_element_type=jnp.float32,
        )
        return (row_sums, summed)

    own_pair = jnp.stack([key_local, value_local])
    start_stats = (
        jnp.zeros((seq_count, local_kv, heads_per_group, block_len), jnp.float32),
        jnp.zeros((seq_count, block_len, local_kv, heads_per_group, head_dim), jnp.float32),
    )
    first_stats = absorb(start_stats, own_pair, blk_index)

    def forward_turn(turn_index, carry):
        key_value, stats_in = carry
        key_value = passed_along(key_value, "blk", 1)
        stats_in = lax.cond(
            turn_index <= blk_index,
            lambda holding: absorb(holding, key_value, blk_index - turn_index),
            lambda holding: holding,
            stats_in,
        )
        return (key_value, stats_in)

    moved_pair, (row_totals, summed_all) = lax.fori_loop(
        1, blk_size, forward_turn, (own_pair, first_stats)
    )
    attended = summed_all / jnp.transpose(row_totals, (0, 3, 1, 2))[..., None]
    attended_tok = lax.all_to_all(
        attended.reshape(seq_count, block_len, local_kv * heads_per_group, head_dim).astype(
            jnp.bfloat16
        ),
        "uly",
        split_axis=1,
        concat_axis=2,
        tiled=True,
    ).reshape(seq_count, tok_count, query_heads * head_dim)
    middle = floats + jnp.einsum(
        "ste,ed->std", attended_tok, out_full, preferred_element_type=jnp.float32
    )
    gain_two, gate_full, up_full, down_full = fetch_feedforward(
        ffn_gain, gate_weight, up_weight, down_weight
    )
    normed_two_float, norm_pull_two = jax.vjp(rms_norm, middle, gain_two.astype(jnp.float32))
    normed_two = normed_two_float.astype(jnp.bfloat16)
    gate_rows = jnp.einsum("std,df->stf", normed_two, gate_full, preferred_element_type=jnp.float32)
    up_rows = jnp.einsum("std,df->stf", normed_two, up_full, preferred_element_type=jnp.float32)
    hidden_float, swiglu_pull = jax.vjp(swiglu, gate_rows, up_rows)
    hidden = hidden_float.astype(jnp.bfloat16)
    outputs = (
        middle + jnp.einsum("stf,fd->std", hidden, down_full, preferred_element_type=jnp.float32)
    ).astype(jnp.bfloat16)
    refetched = fetch_feedforward(ffn_gain, gate_weight, up_weight, down_weight)
    gate_back, up_back, down_back = (refetched[1], refetched[2], refetched[3])
    grad_out = cotangent.astype(jnp.float32)
    down_grad = jnp.einsum("stf,std->fd", hidden, cotangent, preferred_element_type=jnp.float32)
    grad_hidden = jnp.einsum(
        "std,fd->stf", cotangent, down_back, preferred_element_type=jnp.float32
    )
    grad_gate, grad_up = swiglu_pull(grad_hidden)
    grad_gate = grad_gate.astype(jnp.bfloat16)
    grad_up = grad_up.astype(jnp.bfloat16)
    gate_grad = jnp.einsum("std,stf->df", normed_two, grad_gate, preferred_element_type=jnp.float32)
    up_grad = jnp.einsum("std,stf->df", normed_two, grad_up, preferred_element_type=jnp.float32)
    grad_normed_two = jnp.einsum(
        "stf,df->std", grad_gate, gate_back, preferred_element_type=jnp.float32
    ) + jnp.einsum("stf,df->std", grad_up, up_back, preferred_element_type=jnp.float32)
    middle_part, gain_two_grad = norm_pull_two(grad_normed_two)
    grad_middle = grad_out + middle_part
    ffn_shares = (
        lax.psum_scatter(gain_two_grad, ("fsdp", "blk", "uly"), scatter_dimension=0, tiled=True),
        lax.psum_scatter(gate_grad, ("fsdp", "blk", "uly"), scatter_dimension=0, tiled=True),
        lax.psum_scatter(up_grad, ("fsdp", "blk", "uly"), scatter_dimension=0, tiled=True),
        lax.psum_scatter(down_grad, ("fsdp", "blk", "uly"), scatter_dimension=0, tiled=True),
    )
    fetched_again = fetch_attention(attn_gain, query_weight, key_matrix, value_matrix, out_weight)
    query_back, key_back, value_back, out_back = (
        fetched_again[1],
        fetched_again[2],
        fetched_again[3],
        fetched_again[4],
    )
    grad_middle_low = grad_middle.astype(jnp.bfloat16)
    out_grad = jnp.einsum(
        "ste,std->ed", attended_tok, grad_middle_low, preferred_element_type=jnp.float32
    )
    grad_att_tok = (
        jnp.einsum("std,ed->ste", grad_middle_low, out_back, preferred_element_type=jnp.float32)
        .astype(jnp.bfloat16)
        .reshape(seq_count, tok_count, query_heads, head_dim)
    )
    grad_att = lax.all_to_all(grad_att_tok, "uly", split_axis=2, concat_axis=1, tiled=True).reshape(
        seq_count, block_len, local_kv, heads_per_group, head_dim
    )
    delta = jnp.transpose(jnp.sum(grad_att.astype(jnp.float32) * attended, axis=-1), (0, 2, 3, 1))

    def block_grads(key_value, source):
        keys_in = key_value[0]
        values_in = key_value[1]
        probs = block_weights(keys_in, source) / row_totals[..., None]
        grad_probs = jnp.einsum(
            "sqhgd,skhd->shgqk", grad_att, values_in, preferred_element_type=jnp.float32
        )
        grad_scores = (probs * (grad_probs - delta[..., None])).astype(jnp.bfloat16)
        grad_query = (
            jnp.einsum(
                "shgqk,skhd->sqhgd", grad_scores, keys_in, preferred_element_type=jnp.float32
            )
            * scale
        )
        grad_keys = (
            jnp.einsum(
                "shgqk,sqhgd->skhd", grad_scores, query_group, preferred_element_type=jnp.float32
            )
            * scale
        )
        grad_values = jnp.einsum(
            "shgqk,sqhgd->skhd",
            probs.astype(jnp.bfloat16),
            grad_att,
            preferred_element_type=jnp.float32,
        )
        return (grad_query, jnp.stack([grad_keys, grad_values]))

    def pass_grads(moving):
        return from_behind(moving.astype(jnp.bfloat16), "blk", 1).astype(moving.dtype)

    query_start, pair_start = block_grads(own_pair, blk_index)

    def backward_turn(turn_index, carry):
        key_value, query_acc, pair_acc = carry
        key_value = passed_along(key_value, "blk", 1)
        pair_acc = pass_grads(pair_acc)

        def accumulate(holding):
            part_query, part_pair = block_grads(key_value, blk_index - turn_index)
            return (holding[0] + part_query, holding[1] + part_pair)

        query_acc, pair_acc = lax.cond(
            turn_index <= blk_index, accumulate, lambda holding: holding, (query_acc, pair_acc)
        )
        return (key_value, query_acc, pair_acc)

    spent_pair, query_total, pair_total = lax.fori_loop(
        1, blk_size, backward_turn, (own_pair, query_start, pair_start)
    )
    pair_total = pass_grads(pair_total)
    grad_query_low = query_total.reshape(
        seq_count, block_len, local_kv * heads_per_group, head_dim
    ).astype(jnp.bfloat16)
    grad_query_tok, grad_key_tok, grad_value_tok = (
        lax.all_to_all(grad_query_low, "uly", split_axis=1, concat_axis=2, tiled=True),
        lax.all_to_all(
            pair_total[0].astype(jnp.bfloat16), "uly", split_axis=1, concat_axis=2, tiled=True
        ),
        lax.all_to_all(
            pair_total[1].astype(jnp.bfloat16), "uly", split_axis=1, concat_axis=2, tiled=True
        ),
    )
    grad_query_pre, grad_key_pre, heads_grad = prep_pull(
        (grad_query_tok.astype(jnp.float32), grad_key_tok.astype(jnp.float32))
    )
    grad_query_flat = grad_query_pre.astype(jnp.bfloat16).reshape(
        seq_count, tok_count, query_heads * head_dim
    )
    grad_key_flat = grad_key_pre.astype(jnp.bfloat16).reshape(
        seq_count, tok_count, value_heads * head_dim
    )
    grad_value_flat = grad_value_tok.reshape(seq_count, tok_count, value_heads * head_dim)
    query_grad = jnp.einsum(
        "std,ste->de", normalized_input, grad_query_flat, preferred_element_type=jnp.float32
    )
    key_grad = jnp.einsum(
        "std,ste->de", normalized_input, grad_key_flat, preferred_element_type=jnp.float32
    )
    value_grad = jnp.einsum(
        "std,ste->de", normalized_input, grad_value_flat, preferred_element_type=jnp.float32
    )
    grad_normed = jnp.einsum(
        "ste,de->std", grad_query_flat, query_back, preferred_element_type=jnp.float32
    )
    grad_normed = grad_normed + jnp.einsum(
        "ste,de->std", grad_key_flat, key_back, preferred_element_type=jnp.float32
    )
    grad_normed = grad_normed + jnp.einsum(
        "ste,de->std", grad_value_flat, value_back, preferred_element_type=jnp.float32
    )
    input_part, gain_one_grad = norm_pull_one(grad_normed)
    input_grad = (grad_middle + input_part).astype(jnp.bfloat16)
    attn_shares = (
        lax.psum_scatter(gain_one_grad, ("fsdp", "blk", "uly"), scatter_dimension=0, tiled=True),
        lax.psum_scatter(heads_grad, ("fsdp", "blk", "uly"), scatter_dimension=1, tiled=True),
        lax.psum_scatter(query_grad, ("fsdp", "blk", "uly"), scatter_dimension=0, tiled=True),
        lax.psum_scatter(key_grad, ("fsdp", "blk", "uly"), scatter_dimension=0, tiled=True),
        lax.psum_scatter(value_grad, ("fsdp", "blk", "uly"), scatter_dimension=0, tiled=True),
        lax.psum_scatter(out_grad, ("fsdp", "blk", "uly"), scatter_dimension=0, tiled=True),
    )
    return (
        outputs,
        input_grad,
        attn_shares[0],
        attn_shares[1],
        attn_shares[2],
        attn_shares[3],
        attn_shares[4],
        attn_shares[5],
        ffn_shares[0],
        ffn_shares[1],
        ffn_shares[2],
        ffn_shares[3],
    )


MESH = pl.DeviceIdType.MESH
ANY = pl.BlockSpec(memory_space=pl.ANY)
VMEM = pl.BlockSpec(memory_space=pltpu.VMEM)
PLANE = [(dx, dy, dc) for dx in (0, 1) for dy in (0, 1) for dc in (0, 1)]
FAR = [(1, 1, 0), (1, 0, 0), (0, 1, 0)]
TURNS = (1, 2, 3)
SEM = pltpu.SemaphoreType.DMA


class Place:
    def __init__(self):
        self.x = lax.axis_index("fsdp")
        self.block = lax.axis_index("blk")
        self.z = lax.axis_index("uly")
        self.y, self.c = (self.block // 2, self.block % 2)
        self.head = 4 * self.x + self.block
        self.here = (self.x, self.block, self.z)

    def coords(self, dx, dy, dc):
        return ((self.x + dx) % 2, (self.y + dy) % 2, (self.c + dc) % 2)

    def peer(self, dx, dy, dc):
        x, y, c = self.coords(dx, dy, dc)
        return (x, 2 * y + c, self.z)

    def index(self, dx, dy, dc):
        x, y, c = self.coords(dx, dy, dc)
        return 4 * x + 2 * y + c

    def shard(self, ref, dx=0, dy=0, dc=0):
        x, y, c = self.coords(dx, dy, dc)
        return ref.at[2 * y + c, :, x]

    def behind(self, turn):
        return (self.z + 4 - turn) % 4

    def ahead(self, turn):
        return (self.z + turn) % 4

    def line(self, turn):
        return (self.x, self.block, self.ahead(turn))


def remote(src, dst, send_sem, recv_sem, device):
    return pltpu.make_async_remote_copy(
        src_ref=src,
        dst_ref=dst,
        send_sem=send_sem,
        recv_sem=recv_sem,
        device_id=device,
        device_id_type=MESH,
    )


def arrived(ref, sem):
    pltpu.make_async_copy(ref, ref, sem).wait()


def meet(peers):
    barrier = pltpu.get_barrier_semaphore()
    for peer in peers:
        pl.semaphore_signal(barrier, inc=1, device_id=peer, device_id_type=MESH)
    pl.semaphore_wait(barrier, len(peers))


class Sends:
    def __init__(self):
        self.pending = []

    def go(self, *args):
        copy = remote(*args)
        copy.start()
        self.pending.append(copy)

    def drain(self):
        for copy in self.pending:
            copy.wait_send()


def spread_start(me, sends, src, full, send_sems, recv_sems):
    for i, d in enumerate(FAR + [(0, 0, 1)]):
        sends.go(src, me.shard(full), send_sems.at[i], recv_sems.at[i], me.peer(*d))


def spread_forward(me, sends, full, send_sems, recv_sems):
    for i in (1, 2, 0):
        part = me.shard(full, *FAR[i])
        arrived(part, recv_sems.at[i])
        sends.go(part, part, send_sems.at[4 + i], recv_sems.at[4 + i], me.peer(0, 0, 1))


def spread_finish(me, full, recv_sems):
    for i, (dx, dy, _) in enumerate([(0, 0, 0)] + FAR):
        arrived(me.shard(full, dx, dy, 1), recv_sems.at[3 + i])


def gather_kernel(
    x_ref, cot_ref, seg_ref, q_ref, k_ref, v_ref, g_ref, u_ref, gain_ref,
    xf_ref, cf_ref, segf_ref, w_ref, gu_ref, gains_ref,
    ps, pr, as_, ar, ws, wr, zs, zr, us, ur, gs, gr, ls,
):
    me = Place()
    x, z, p = (me.x, me.z, me.head)
    across = [((x + 1) % 2, me.block, me.ahead(turn)) for turn in TURNS]
    meet([me.peer(*d) for d in PLANE[1:]] + [me.line(turn) for turn in TURNS] + across)
    sends = Sends()
    half = x_ref.shape[1] // 2
    own_gain = pltpu.make_async_copy(gain_ref, gains_ref.at[p, z], ls.at[0])
    own_gain.start()
    own_seg = pltpu.make_async_copy(seg_ref, segf_ref.at[x], ls.at[1])
    own_seg.start()
    sends.go(seg_ref, segf_ref.at[x], ls.at[2], ls.at[3], me.peer(1, 0, 0))
    for turn in TURNS:
        sends.go(gain_ref, gains_ref.at[p, z], gs.at[turn], gr.at[turn], me.line(turn))

    def permute(src_ref, full_ref, o, wait=False):
        for j in (0, 1):
            for to in (0, 1):
                src = src_ref.at[j, pl.ds(half * to, half)]
                dst = full_ref.at[me.block, z, to]
                target = (to, me.block, 2 * x + j)
                mine = jnp.logical_and(x == to, z == 2 * x + j)
                copy = remote(src, dst, ps.at[o + 2 * j + to], pr.at[o + z], target)

                @pl.when(jnp.logical_not(mine))
                def _():
                    if wait:
                        copy.wait_send()
                    else:
                        copy.start()

                if not wait:

                    @pl.when(mine)
                    def _():
                        pltpu.make_async_copy(src, dst, pr.at[o + z]).start()

    def permuted(full_ref, o):
        for k in range(4):
            arrived(full_ref.at[me.block, k, x], pr.at[o + k])

    permute(x_ref, xf_ref, 0)
    wide, narrow = (q_ref.shape[1] // 8, k_ref.shape[1] // 8)
    cuts = ((q_ref, wide, 0), (k_ref, narrow, wide), (v_ref, narrow, wide + narrow))
    for i, d in enumerate(PLANE):
        t = me.index(*d)
        for n, (ref, width, off) in enumerate(cuts):
            src = ref.at[:, pl.ds(pl.multiple_of(t * width, 128), width)]
            dst = w_ref.at[p, z, :, pl.ds(off, width)]
            if i == 0:
                pltpu.make_async_copy(src, dst, wr.at[n]).start()
            else:
                sends.go(src, dst, ws.at[3 * i + n], wr.at[3 * i + n], me.peer(*d))
    permute(cot_ref, cf_ref, 4)
    permuted(xf_ref, 0)
    spread_start(me, sends, me.shard(xf_ref), xf_ref, as_, ar)
    for i, d in enumerate(PLANE):
        t = me.index(*d)
        for n, (ref, width, off) in enumerate(cuts):
            arrived(w_ref.at[t, z, :, pl.ds(off, width)], wr.at[3 * i + n])
        for turn in TURNS:
            s = 3 * i + turn - 1
            sends.go(w_ref.at[t, z], w_ref.at[t, z], zs.at[s], zr.at[s], me.line(turn))
    width = g_ref.shape[1] // 8
    for i, d in enumerate(PLANE):
        t = me.index(*d)
        for n, ref in enumerate((g_ref, u_ref)):
            src = ref.at[:, pl.ds(pl.multiple_of(t * width, 128), width)]
            dst = gu_ref.at[p, :, pl.ds(n * width, width)]
            if i == 0:
                pltpu.make_async_copy(src, dst, ur.at[n]).start()
            else:
                sends.go(src, dst, us.at[2 * i + n], ur.at[2 * i + n], me.peer(*d))
    permuted(cf_ref, 4)
    spread_start(me, sends, me.shard(cf_ref), cf_ref, as_.at[pl.ds(7, 7)], ar.at[pl.ds(7, 7)])
    own_gain.wait()
    own_seg.wait()
    arrived(segf_ref.at[(x + 1) % 2], ls.at[3])
    for turn in TURNS:
        arrived(gains_ref.at[p, me.behind(turn)], gr.at[turn])
    for i, d in enumerate(PLANE[1:]):
        sends.go(gains_ref.at[p], gains_ref.at[p], gs.at[4 + i], gr.at[4 + i], me.peer(*d))
    spread_forward(me, sends, xf_ref, as_, ar)
    spread_finish(me, xf_ref, ar)
    for i, d in enumerate(PLANE[1:]):
        arrived(gains_ref.at[me.index(*d)], gr.at[4 + i])
    for i, d in enumerate(PLANE):
        for turn in TURNS:
            arrived(w_ref.at[me.index(*d), me.behind(turn)], zr.at[3 * i + turn - 1])
    for i, d in enumerate(PLANE):
        for n in (0, 1):
            arrived(gu_ref.at[me.index(*d), :, pl.ds(n * width, width)], ur.at[2 * i + n])
    spread_forward(me, sends, cf_ref, as_.at[pl.ds(7, 7)], ar.at[pl.ds(7, 7)])
    spread_finish(me, cf_ref, ar.at[pl.ds(7, 7)])
    permute(x_ref, xf_ref, 0, wait=True)
    permute(cot_ref, cf_ref, 4, wait=True)
    sends.drain()


def full_shape(tokens, width):
    return (4, 4, 2, tokens // 32, width)


def gather_all(x, cot, seg, q, k, v, g, u, gain):
    tokens, width = (16 * x.shape[1], x.shape[2])
    rows = q.shape[0]
    cols = (q.shape[1] + 2 * k.shape[1]) // 8
    full = jax.ShapeDtypeStruct(full_shape(tokens, width), jnp.bfloat16)
    return pl.pallas_call(
        gather_kernel,
        name="gather_all",
        out_shape=(
            full,
            full,
            jax.ShapeDtypeStruct((2,) + seg.shape, seg.dtype),
            jax.ShapeDtypeStruct((8, 4, rows, cols), jnp.bfloat16),
            jax.ShapeDtypeStruct((8, rows, g.shape[1] // 4), jnp.bfloat16),
            jax.ShapeDtypeStruct((8, 4, 8, 128), jnp.float32),
        ),
        in_specs=[ANY] * 9,
        out_specs=(ANY,) * 6,
        scratch_shapes=[SEM((8,)), SEM((8,)), SEM((14,)), SEM((14,))]
        + [SEM((24,))] * 4
        + [SEM((16,))] * 2
        + [SEM((11,))] * 2
        + [SEM((4,))],
        compiler_params=pltpu.CompilerParams(collective_id=0, has_side_effects=True),
    )(x, cot, seg, q, k, v, g, u, gain)


def half_start(me, sends, part, kept, sibling, keep_sems, send_sems, recv_sems):
    for i, (dx, dy, _) in enumerate(FAR + [(0, 0, 0)]):
        src = me.shard(part, dx, dy, 1)
        sends.go(src, sibling.at[i], send_sems.at[i], recv_sems.at[i], me.peer(0, 0, 1))
        pltpu.make_async_copy(me.shard(part, dx, dy, 0), kept.at[i], keep_sems.at[i]).start()


def half_send(me, sends, kept, sibling, out, came, keep_sems, send_sems, recv_sems):
    for i, d in enumerate(FAR):
        arrived(kept.at[i], keep_sems.at[i])
        arrived(sibling.at[i], recv_sems.at[i])
        out[i] = (
            kept[i].astype(jnp.float32) + sibling[i].astype(jnp.float32)
        ).astype(jnp.bfloat16)
        sends.go(out.at[i], came.at[i], send_sems.at[4 + i], recv_sems.at[4 + i], me.peer(*d))


def half_sum(kept, sibling, came, keep_sems, recv_sems):
    arrived(kept.at[3], keep_sems.at[3])
    arrived(sibling.at[3], recv_sems.at[3])
    total = kept[3].astype(jnp.float32) + sibling[3].astype(jnp.float32)
    for i in (1, 2, 0):
        arrived(came.at[i], recv_sems.at[4 + i])
        total = total + came[i].astype(jnp.float32)
    return total


def quarter_scratch(tokens, width):
    piece = (4, tokens // 32, width)
    return [
        pltpu.VMEM((4,) + piece, jnp.bfloat16),
        pltpu.VMEM((4,) + piece, jnp.bfloat16),
        pltpu.VMEM((3,) + piece, jnp.bfloat16),
        pltpu.VMEM((3,) + piece, jnp.bfloat16),
        SEM((4,)),
        SEM((7,)),
        SEM((7,)),
    ]


def near(me):
    return [me.peer(*d) for d in FAR + [(0, 0, 1)]]


def middle_kernel(
    part_ref, xf_ref, gain_ref, mid_ref, nf_ref,
    kept, sibling, out, came, ks, ss, rs, xs_ref, n_ref, as_, ar, ls,
):
    me = Place()
    meet(near(me))
    sends = Sends()
    half_start(me, sends, part_ref, kept, sibling, ks, ss, rs)
    own_x = pltpu.make_async_copy(me.shard(xf_ref), xs_ref, ls.at[0])
    own_x.start()
    half_send(me, sends, kept, sibling, out, came, ks, ss, rs)
    own_x.wait()
    middle = xs_ref[...].astype(jnp.float32) + half_sum(kept, sibling, came, ks, rs)
    mid_ref[...] = middle
    scale = lax.rsqrt(jnp.mean(middle * middle, axis=-1, keepdims=True) + EPSILON)
    n_ref[...] = (middle * scale * gain_ref[...]).astype(jnp.bfloat16)
    own_n = pltpu.make_async_copy(n_ref, me.shard(nf_ref), ls.at[1])
    own_n.start()
    spread_start(me, sends, n_ref, nf_ref, as_, ar)
    spread_forward(me, sends, nf_ref, as_, ar)
    spread_finish(me, nf_ref, ar)
    own_n.wait()
    sends.drain()


def middle_step(part, xf, gain):
    tokens, width = (part.shape[0], part.shape[1])
    piece = (4, tokens // 32, width)
    return pl.pallas_call(
        middle_kernel,
        name="middle_step",
        out_shape=(
            jax.ShapeDtypeStruct(piece, jnp.float32),
            jax.ShapeDtypeStruct(full_shape(tokens, width), jnp.bfloat16),
        ),
        in_specs=[ANY, ANY, VMEM],
        out_specs=(VMEM, ANY),
        scratch_shapes=quarter_scratch(tokens, width)
        + [pltpu.VMEM(piece, jnp.bfloat16)] * 2
        + [SEM((7,)), SEM((7,)), SEM((2,))],
        compiler_params=pltpu.CompilerParams(collective_id=1, has_side_effects=True),
    )(part.reshape(full_shape(tokens, width)), xf, gain)


def norm_back(grad, vector, gain, scale):
    weighted = grad * gain
    inner = jnp.mean(weighted * vector, axis=-1, keepdims=True)
    return scale * weighted - vector * (scale * scale * scale * inner)


def turn_kernel(
    part_ref, down_ref, cf_ref, mid_ref, gain_ref, gmid_ref, gf_ref, out_ref, gg_ref,
    kept, sibling, out, came, ks, ss, rs, kept2, sibling2, out2, came2, ks2, ss2, rs2,
    cs_ref, n_ref, as_, ar, ls,
):
    me = Place()
    meet(near(me))
    sends = Sends()
    half_start(me, sends, part_ref, kept, sibling, ks, ss, rs)
    own_c = pltpu.make_async_copy(me.shard(cf_ref), cs_ref, ls.at[0])
    own_c.start()
    half_start(me, sends, down_ref, kept2, sibling2, ks2, ss2, rs2)
    half_send(me, sends, kept, sibling, out, came, ks, ss, rs)
    half_send(me, sends, kept2, sibling2, out2, came2, ks2, ss2, rs2)
    own_c.wait()
    grad = half_sum(kept, sibling, came, ks, rs)
    middle = mid_ref[...]
    scale = lax.rsqrt(jnp.mean(middle * middle, axis=-1, keepdims=True) + EPSILON)
    total = cs_ref[...].astype(jnp.float32) + norm_back(grad, middle, gain_ref[...], scale)
    gmid_ref[...] = total
    n_ref[...] = total.astype(jnp.bfloat16)
    own_n = pltpu.make_async_copy(n_ref, me.shard(gf_ref), ls.at[1])
    own_n.start()
    spread_start(me, sends, n_ref, gf_ref, as_, ar)
    share = grad * middle * scale
    gg_ref[...] = jnp.sum(jnp.sum(share, axis=0), axis=0, keepdims=True)
    out_ref[...] = (middle + half_sum(kept2, sibling2, came2, ks2, rs2)).astype(jnp.bfloat16)
    spread_forward(me, sends, gf_ref, as_, ar)
    spread_finish(me, gf_ref, ar)
    own_n.wait()
    sends.drain()


def turn_step(part, down, cf, middle, gain):
    tokens, width = (part.shape[0], part.shape[1])
    piece = (4, tokens // 32, width)
    full = full_shape(tokens, width)
    return pl.pallas_call(
        turn_kernel,
        name="turn_step",
        out_shape=(
            jax.ShapeDtypeStruct(piece, jnp.float32),
            jax.ShapeDtypeStruct(full, jnp.bfloat16),
            jax.ShapeDtypeStruct(piece, jnp.bfloat16),
            jax.ShapeDtypeStruct((1, width), jnp.float32),
        ),
        in_specs=[ANY, ANY, ANY, VMEM, VMEM],
        out_specs=(VMEM, ANY, VMEM, VMEM),
        scratch_shapes=quarter_scratch(tokens, width) * 2
        + [pltpu.VMEM(piece, jnp.bfloat16)] * 2
        + [SEM((7,)), SEM((7,)), SEM((2,))],
        compiler_params=pltpu.CompilerParams(collective_id=2, has_side_effects=True),
    )(part.reshape(full), down.reshape(full), cf, middle, gain)


def last_kernel(
    part_ref, xf_ref, gmid_ref, out_ref, gain_ref, small_ref, dw_ref, dgu_ref,
    y_ref, gx_ref, q_ref, k_ref, v_ref, g_ref, u_ref, sums_ref,
    kept, sibling, out, came, ks, ss, rs, xs_ref, gi_ref, ps, pr, ls,
    wown, wcame, wsum, zs, zr, ws, wr, us, ur, pack, packs, lines, gs, gr,
):
    me = Place()
    x, z, p = (me.x, me.z, me.head)
    across = [((x + 1) % 2, me.block, me.ahead(turn)) for turn in TURNS]
    meet([me.peer(*d) for d in PLANE[1:]] + [me.line(turn) for turn in TURNS] + across)
    sends = Sends()
    half_start(me, sends, part_ref, kept, sibling, ks, ss, rs)
    for turn in TURNS:
        sends.go(
            dw_ref.at[:, me.ahead(turn)], wcame.at[turn - 1],
            zs.at[turn - 1], zr.at[turn - 1], me.line(turn),
        )
    own_w = pltpu.make_async_copy(dw_ref.at[:, z], wown, ls.at[2])
    own_w.start()
    own_x = pltpu.make_async_copy(me.shard(xf_ref), xs_ref, ls.at[0])
    own_x.start()
    half_send(me, sends, kept, sibling, out, came, ks, ss, rs)
    half = y_ref.shape[1] // 2

    def permute(src_ref, dst_ref, o, wait=False):
        for k in range(4):
            dst = dst_ref.at[z % 2, pl.ds(half * x, half)]
            src = src_ref.at[k]
            mine = jnp.logical_and(x == z // 2, z == k)
            copy = remote(src, dst, ps.at[o + k], pr.at[o + 2 * (z % 2) + x], (z // 2, me.block, k))

            @pl.when(jnp.logical_not(mine))
            def _():
                if wait:
                    copy.wait_send()
                else:
                    copy.start()

            if not wait:

                @pl.when(mine)
                def _():
                    pltpu.make_async_copy(src, dst, pr.at[o + 2 * (z % 2) + x]).start()

    def permuted(dst_ref, o):
        for j in (0, 1):
            for to in (0, 1):
                arrived(dst_ref.at[j, pl.ds(half * to, half)], pr.at[o + 2 * j + to])

    permute(out_ref, y_ref, 0)
    width = g_ref.shape[1] // 8
    for i, d in enumerate(PLANE):
        t = me.index(*d)
        for n, ref in enumerate((g_ref, u_ref)):
            src = dgu_ref.at[t, :, pl.ds(n * width, width)]
            dst = ref.at[:, pl.ds(pl.multiple_of(p * width, 128), width)]
            if i == 0:
                pltpu.make_async_copy(src, dst, ur.at[n]).start()
            else:
                sends.go(src, dst, us.at[2 * i + n], ur.at[2 * i + n], me.peer(*d))
    own_x.wait()
    grad = half_sum(kept, sibling, came, ks, rs)
    rows = xs_ref[...].astype(jnp.float32)
    scale = lax.rsqrt(jnp.mean(rows * rows, axis=-1, keepdims=True) + EPSILON)
    gi_ref[...] = (gmid_ref[...] + norm_back(grad, rows, gain_ref[...], scale)).astype(jnp.bfloat16)
    permute(gi_ref, gx_ref, 4)
    share = jnp.sum(jnp.sum(grad * rows * scale, axis=0), axis=0, keepdims=True)
    for i in range(8):
        pack[pl.ds(i, 1)] = share[:, 128 * i : 128 * i + 128]
    pack[pl.ds(8, 16)] = small_ref[...]
    for i, d in enumerate(PLANE[1:]):
        sends.go(pack, packs.at[i], gs.at[i], gr.at[i], me.peer(*d))
    own_w.wait()
    for turn in TURNS:
        arrived(wcame.at[turn - 1], zr.at[turn - 1])
    wsum[...] = (
        wown[...].astype(jnp.float32)
        + wcame[0].astype(jnp.float32)
        + wcame[1].astype(jnp.float32)
        + wcame[2].astype(jnp.float32)
    ).astype(jnp.bfloat16)
    wide, narrow = (q_ref.shape[1] // 8, k_ref.shape[1] // 8)
    cuts = ((q_ref, wide, 0), (k_ref, narrow, wide), (v_ref, narrow, wide + narrow))
    for i, d in enumerate(PLANE):
        t = me.index(*d)
        for n, (ref, cols, off) in enumerate(cuts):
            src = wsum.at[t, :, pl.ds(off, cols)]
            dst = ref.at[:, pl.ds(pl.multiple_of(p * cols, 128), cols)]
            if i == 0:
                pltpu.make_async_copy(src, dst, wr.at[n]).start()
            else:
                sends.go(src, dst, ws.at[3 * i + n], wr.at[3 * i + n], me.peer(*d))
    total = pack[...]
    for i in range(7):
        arrived(packs.at[i], gr.at[i])
        total = total + packs[i]
    sums_ref[...] = total
    packs[7] = total
    for turn in TURNS:
        sends.go(packs.at[7], lines.at[turn - 1], gs.at[6 + turn], gr.at[6 + turn], me.line(turn))
    for turn in TURNS:
        arrived(lines.at[turn - 1], gr.at[6 + turn])
    sums_ref[...] = ((sums_ref[...] + lines[0]) + lines[1]) + lines[2]
    for i, d in enumerate(PLANE):
        t = me.index(*d)
        for n, ref in enumerate((g_ref, u_ref)):
            arrived(ref.at[:, pl.ds(pl.multiple_of(t * width, 128), width)], ur.at[2 * i + n])
        for n, (ref, cols, off) in enumerate(cuts):
            arrived(ref.at[:, pl.ds(pl.multiple_of(t * cols, 128), cols)], wr.at[3 * i + n])
    permuted(y_ref, 0)
    permuted(gx_ref, 4)
    permute(out_ref, y_ref, 0, wait=True)
    permute(gi_ref, gx_ref, 4, wait=True)
    sends.drain()


def last_step(part, xf, gmid, out, gain, small, dw, dgu, per_device):
    tokens, width = (part.shape[0], part.shape[1])
    piece = (4, tokens // 32, width)
    rows, cols = (dw.shape[2], dw.shape[3])
    token_shape, q_cols, k_cols, f_cols = per_device
    back = jax.ShapeDtypeStruct(token_shape, jnp.bfloat16)
    weights = [jax.ShapeDtypeStruct((rows, n), jnp.bfloat16) for n in (q_cols, k_cols, k_cols, f_cols, f_cols)]
    return pl.pallas_call(
        last_kernel,
        name="last_step",
        out_shape=(back, back, *weights, jax.ShapeDtypeStruct((24, 128), jnp.float32)),
        in_specs=[ANY, ANY, VMEM, ANY, VMEM, VMEM, ANY, ANY],
        out_specs=(ANY,) * 7 + (VMEM,),
        scratch_shapes=quarter_scratch(tokens, width)
        + [pltpu.VMEM(piece, jnp.bfloat16)] * 2
        + [SEM((8,)), SEM((8,)), SEM((3,))]
        + [
            pltpu.VMEM((8, rows, cols), jnp.bfloat16),
            pltpu.VMEM((3, 8, rows, cols), jnp.bfloat16),
            pltpu.VMEM((8, rows, cols), jnp.bfloat16),
            SEM((3,)), SEM((3,)), SEM((24,)), SEM((24,)), SEM((16,)), SEM((16,)),
            pltpu.VMEM((24, 128), jnp.float32),
            pltpu.VMEM((8, 24, 128), jnp.float32),
            pltpu.VMEM((3, 24, 128), jnp.float32),
            SEM((10,)), SEM((10,)),
        ],
        compiler_params=pltpu.CompilerParams(collective_id=3, has_side_effects=True),
    )(part.reshape(full_shape(tokens, width)), xf, gmid, out, gain, small, dw, dgu)


def rope_tables(segs, head_dim):
    count = segs.shape[0]
    doc_ids = jnp.arange(DOCS, dtype=jnp.int32)
    starts = jnp.sum((segs[None, :] < doc_ids[:, None]).astype(jnp.int32), axis=1)
    inverse = jnp.exp(
        jnp.arange(head_dim // 2, dtype=jnp.float32) * (-2.0 * math.log(THETA) / head_dim)
    )
    inverse = jnp.concatenate([inverse, inverse])
    low = jnp.arange(32, dtype=jnp.float32)[:, None] * inverse
    high = jnp.arange(count // 32, dtype=jnp.float32)[:, None] * (32.0 * inverse)
    first = starts.astype(jnp.float32)[:, None] * inverse
    cl, sl, ch, sh, cf, sf = (
        f(v) for v in (low, high, first) for f in (jnp.cos, jnp.sin)
    )
    cos_at = (ch[:, None] * cl - sh[:, None] * sl).reshape(count, head_dim)
    sin_at = (sh[:, None] * cl + ch[:, None] * sl).reshape(count, head_dim)
    chosen_cos = jnp.broadcast_to(cf[0], (count, head_dim))
    chosen_sin = jnp.broadcast_to(sf[0], (count, head_dim))
    for doc in range(1, DOCS):
        here = (segs == doc)[:, None]
        chosen_cos = jnp.where(here, cf[doc], chosen_cos)
        chosen_sin = jnp.where(here, sf[doc], chosen_sin)
    return (
        cos_at * chosen_cos + sin_at * chosen_sin,
        sin_at * chosen_cos - cos_at * chosen_sin,
    )


def dot(a, b, kind=jnp.float32):
    return jnp.dot(a, b, preferred_element_type=jnp.float32).astype(kind)


def dot_left(a, b, kind=jnp.float32):
    return lax.dot_general(
        a, b, (((0,), (0,)), ((), ())), preferred_element_type=jnp.float32
    ).astype(kind)


def dot_right(a, b, kind=jnp.float32):
    return lax.dot_general(
        a, b, (((1,), (1,)), ((), ())), preferred_element_type=jnp.float32
    ).astype(kind)


def plane_body(
    inputs, segments, attn_gain, head_gains, query_weight, key_matrix, value_matrix, out_weight,
    ffn_gain, gate_weight, up_weight, down_weight, cotangent,
):
    low = jnp.bfloat16
    width = inputs.shape[2]
    head_dim = head_gains.shape[1]
    z = lax.axis_index("uly")
    head = 4 * lax.axis_index("fsdp") + lax.axis_index("blk")
    out_full = lax.all_gather(out_weight, "uly", axis=0, tiled=True)
    down_full = lax.all_gather(down_weight, "uly", axis=0, tiled=True)
    piece = attn_gain.shape[0]
    gains_own = jnp.zeros((8, 128), jnp.float32)
    gains_own = gains_own.at[0, :piece].set(attn_gain.astype(jnp.float32))
    gains_own = gains_own.at[1, :piece].set(ffn_gain.astype(jnp.float32))
    xf, cf, segf, w_qkv, gu_part, gains = gather_all(
        inputs, cotangent, segments, query_weight, key_matrix, value_matrix, gate_weight,
        up_weight, gains_own,
    )
    gate_up = lax.all_gather(gu_part, "uly", axis=1, tiled=False)
    gate_up = gate_up.reshape(width, gu_part.shape[2])
    w_qkv = w_qkv.reshape(width, w_qkv.shape[3])
    gain_one = gains[:, :, 0, :piece].reshape(1, width)
    gain_two = gains[:, :, 1, :piece].reshape(1, width)
    tokens = xf.shape[0] * xf.shape[1] * xf.shape[2] * xf.shape[3]
    x_all = xf.reshape(tokens, width)
    cot_all = cf.reshape(tokens, width)
    segs = lax.dynamic_index_in_dim(segf.reshape(-1, tokens), z, 0, keepdims=False)
    normed = rms_norm(x_all.astype(jnp.float32), gain_one).astype(low)
    pre = dot(normed, w_qkv).reshape(tokens, -1, head_dim)
    groups = pre.shape[1] - 2
    cosine, sine = rope_tables(segs, head_dim)
    head_float = head_gains.astype(jnp.float32)

    def prepare_local(query_arg, key_arg, gains_arg):
        return prepare(query_arg[None], key_arg[None], gains_arg, cosine[None], sine[None])

    (query_rot, key_rot), prep_pull = jax.vjp(
        prepare_local, pre[:, :groups], pre[:, groups : groups + 1], head_float
    )
    query = query_rot[0].astype(low)
    key = key_rot[0, :, 0].astype(low)
    value = pre[:, groups + 1].astype(low)
    bound = math.sqrt(head_dim) * jnp.max(jnp.abs(head_float[0])) * jnp.max(jnp.abs(head_float[1]))
    scale = head_dim ** (-0.5)
    index = jnp.arange(tokens, dtype=jnp.int32)
    allowed = (index[None, :] <= index[:, None]) & (segs[None, :] == segs[:, None])
    scores = jnp.einsum("qgd,kd->gqk", query, key, preferred_element_type=jnp.float32) * scale
    weights = jnp.where(allowed[None], jnp.exp(scores - bound), 0.0)
    totals = jnp.sum(weights, axis=-1)
    mixed = jnp.einsum("gqk,kd->qgd", weights.astype(low), value, preferred_element_type=jnp.float32)
    attended = mixed / jnp.transpose(totals)[..., None]
    attended_low = attended.astype(low).reshape(tokens, groups * head_dim)
    middle, nf = middle_step(dot(attended_low, out_full, low), xf, gain_two)
    normed_two = nf.reshape(tokens, width)
    hidden_width = gate_up.shape[1] // 2
    both = dot(normed_two, gate_up)
    gate_rows, up_rows = (both[:, :hidden_width], both[:, hidden_width:])
    hidden_float, swiglu_pull = jax.vjp(swiglu, gate_rows, up_rows)
    hidden = hidden_float.astype(low)
    down_part = dot(hidden, down_full, low)
    grad_hidden = dot_right(cot_all, down_full)
    grad_gate, grad_up = swiglu_pull(grad_hidden)
    grad_both = jnp.concatenate([grad_gate.astype(low), grad_up.astype(low)], axis=1)
    gmid, gf, out_own, gain_two_grad = turn_step(
        dot_right(grad_both, gate_up, low), down_part, cf, middle, gain_two
    )
    down_grad = lax.psum_scatter(
        dot_left(hidden, cot_all, low), "uly", scatter_dimension=0, tiled=True
    )
    both_grad = dot_left(normed_two, grad_both, low).reshape(8, 4, -1, 2 * hidden_width)
    both_grad = lax.psum_scatter(both_grad, "uly", scatter_dimension=1, tiled=False)
    grad_mid = gf.reshape(tokens, width)
    out_grad = lax.psum_scatter(
        dot_left(attended_low, grad_mid, low), "uly", scatter_dimension=0, tiled=True
    )
    grad_att = dot_right(grad_mid, out_full, low).reshape(tokens, groups, head_dim)
    delta = jnp.transpose(jnp.sum(grad_att.astype(jnp.float32) * attended, axis=-1))
    probs = weights / totals[..., None]
    grad_probs = jnp.einsum("qgd,kd->gqk", grad_att, value, preferred_element_type=jnp.float32)
    grad_scores = (probs * (grad_probs - delta[..., None])).astype(low)
    grad_query = (
        jnp.einsum("gqk,kd->qgd", grad_scores, key, preferred_element_type=jnp.float32) * scale
    )
    grad_key = (
        jnp.einsum("gqk,qgd->kd", grad_scores, query, preferred_element_type=jnp.float32) * scale
    )
    grad_value = jnp.einsum(
        "gqk,qgd->kd", probs.astype(low), grad_att, preferred_element_type=jnp.float32
    )
    grad_query_pre, grad_key_pre, heads_grad = prep_pull(
        (
            grad_query.astype(low).astype(jnp.float32)[None],
            grad_key.astype(low).astype(jnp.float32)[None, :, None],
        )
    )
    grad_pre = jnp.concatenate(
        [
            grad_query_pre.astype(low).reshape(tokens, groups * head_dim),
            grad_key_pre.astype(low).reshape(tokens, head_dim),
            grad_value.astype(low),
        ],
        axis=1,
    )
    dw = dot_left(normed, grad_pre, low).reshape(8, 4, -1, grad_pre.shape[1])
    small = jnp.concatenate(
        [gain_two_grad.reshape(8, 128), heads_grad, jnp.zeros((6, 128), jnp.float32)], axis=0
    )
    per_device = (inputs.shape, query_weight.shape[1], key_matrix.shape[1], gate_weight.shape[1])
    outputs, grad_inputs, q_grad, k_grad, v_grad, g_grad, u_grad, sums = last_step(
        dot_right(grad_pre, w_qkv, low), xf, gmid, out_own, gain_one, small, dw, both_grad, per_device
    )
    floats = lambda v: v.astype(jnp.float32)
    attn_gain_grad = lax.dynamic_slice(sums, (head, z * piece), (1, piece))[0]
    ffn_gain_grad = lax.dynamic_slice(sums, (8 + head, z * piece), (1, piece))[0]
    share = head_dim // 32
    head_gain_grad = lax.dynamic_slice(sums, (16, (4 * head + z) * share), (2, share))
    return (
        outputs, grad_inputs, attn_gain_grad, head_gain_grad, floats(q_grad), floats(k_grad),
        floats(v_grad), floats(out_grad), ffn_gain_grad, floats(g_grad), floats(u_grad),
        floats(down_grad),
    )


def fits_plane(mesh, seq_count, heads):
    shape = mesh.shape
    return (shape["fsdp"], shape["blk"], shape["uly"]) == (2, 4, 4) and seq_count == 4 and heads == 8


def solution(mesh):
    def step(*arrays):
        seq_count = arrays[0].shape[0]
        heads = arrays[5].shape[1] // arrays[3].shape[1]
        chosen = plane_body if fits_plane(mesh, seq_count, heads) else body
        return mapped(chosen)(*arrays)

    mapped = functools.partial(
        jax.shard_map,
        mesh=mesh,
        in_specs=(
            P("fsdp", ("blk", "uly"), None),
            P("fsdp", None),
            P(("fsdp", "blk", "uly")),
            P(),
            P(("fsdp", "blk", "uly"), None),
            P(("fsdp", "blk", "uly"), None),
            P(("fsdp", "blk", "uly"), None),
            P(("fsdp", "blk", "uly"), None),
            P(("fsdp", "blk", "uly")),
            P(("fsdp", "blk", "uly"), None),
            P(("fsdp", "blk", "uly"), None),
            P(("fsdp", "blk", "uly"), None),
            P("fsdp", ("blk", "uly"), None),
        ),
        out_specs=(
            P("fsdp", ("blk", "uly"), None),
            P("fsdp", ("blk", "uly"), None),
            P(("fsdp", "blk", "uly")),
            P(None, ("fsdp", "blk", "uly")),
            P(("fsdp", "blk", "uly"), None),
            P(("fsdp", "blk", "uly"), None),
            P(("fsdp", "blk", "uly"), None),
            P(("fsdp", "blk", "uly"), None),
            P(("fsdp", "blk", "uly")),
            P(("fsdp", "blk", "uly"), None),
            P(("fsdp", "blk", "uly"), None),
            P(("fsdp", "blk", "uly"), None),
        ),
        check_vma=False,
    )
    return step
```

```python
import functools
import math

import jax
import jax.numpy as jnp
from jax import lax
from jax.experimental import pallas as pl
from jax.experimental.pallas import tpu as pltpu
from jax.sharding import PartitionSpec as P

DOCS = 4


EPSILON = 1e-06
THETA = 1000000.0


def passed_along(value, axis, steps):
    count = lax.axis_size(axis)
    first, last = (max(0, -steps), min(count, count - steps))
    return lax.ppermute(value, axis, [(source, source + steps) for source in range(first, last)])


def from_behind(value, axis, steps):
    count = lax.axis_size(axis)
    pairs = [(source, (source + steps) % count) for source in range(count)]
    return lax.ppermute(value, axis, pairs)


def rms_norm(vector, weight):
    mean_square = jnp.mean(vector * vector, axis=-1, keepdims=True)
    return vector * lax.rsqrt(mean_square + EPSILON) * weight


def rotate(vector, cosine, sine_table):
    half_width = vector.shape[-1] // 2
    turned = jnp.concatenate([-vector[..., half_width:], vector[..., :half_width]], axis=-1)
    return vector * cosine + turned * sine_table


def prepare(query_pre, key_before_rotate, gains, cosine, sine_table):
    cos_heads = cosine[:, :, None, :]
    sin_heads = sine_table[:, :, None, :]
    query_rot = rotate(rms_norm(query_pre, gains[0]), cos_heads, sin_heads)
    key_rot = rotate(rms_norm(key_before_rotate, gains[1]), cos_heads, sin_heads)
    return (query_rot, key_rot)


def swiglu(gate_rows, up_rows):
    return jax.nn.silu(gate_rows) * up_rows


def fetch_attention(attn_gain, query_weight, key_matrix, value_matrix, out_weight):
    return (
        lax.all_gather(attn_gain, ("fsdp", "blk", "uly"), axis=0, tiled=True),
        lax.all_gather(query_weight, ("fsdp", "blk", "uly"), axis=0, tiled=True),
        lax.all_gather(key_matrix, ("fsdp", "blk", "uly"), axis=0, tiled=True),
        lax.all_gather(value_matrix, ("fsdp", "blk", "uly"), axis=0, tiled=True),
        lax.all_gather(out_weight, ("fsdp", "blk", "uly"), axis=0, tiled=True),
    )


def fetch_feedforward(ffn_gain, gate_weight, up_weight, down_weight):
    return (
        lax.all_gather(ffn_gain, ("fsdp", "blk", "uly"), axis=0, tiled=True),
        lax.all_gather(gate_weight, ("fsdp", "blk", "uly"), axis=0, tiled=True),
        lax.all_gather(up_weight, ("fsdp", "blk", "uly"), axis=0, tiled=True),
        lax.all_gather(down_weight, ("fsdp", "blk", "uly"), axis=0, tiled=True),
    )


def body(
    inputs,
    segments,
    attn_gain,
    head_gains,
    query_weight,
    key_matrix,
    value_matrix,
    out_weight,
    ffn_gain,
    gate_weight,
    up_weight,
    down_weight,
    cotangent,
):
    seq_count, tok_count, model_width = inputs.shape
    head_dim = head_gains.shape[1]
    query_heads = query_weight.shape[1] // head_dim
    value_heads = key_matrix.shape[1] // head_dim
    heads_per_group = query_heads // value_heads
    uly_size = lax.axis_size("uly")
    blk_size = lax.axis_size("blk")
    blk_index = lax.axis_index("blk")
    uly_index = lax.axis_index("uly")
    offset = (blk_index * uly_size + uly_index) * tok_count
    doc_ids = jnp.arange(DOCS, dtype=jnp.int32)
    starts = jnp.sum((segments[:, None, :] < doc_ids[None, :, None]).astype(jnp.int32), axis=2)
    local_segs = lax.dynamic_slice_in_dim(segments, offset, tok_count, 1)
    doc_start = jnp.sum(
        jnp.where(local_segs[:, :, None] == doc_ids[None, None, :], starts[:, None, :], 0), axis=2
    )
    token_place = (offset + jnp.arange(tok_count, dtype=jnp.int32)[None, :] - doc_start).astype(
        jnp.float32
    )
    inverse = jnp.exp(
        jnp.arange(head_dim // 2, dtype=jnp.float32) * (-2.0 * math.log(THETA) / head_dim)
    )
    angles = token_place[..., None] * inverse
    cosine = jnp.concatenate([jnp.cos(angles), jnp.cos(angles)], axis=-1)
    sine_table = jnp.concatenate([jnp.sin(angles), jnp.sin(angles)], axis=-1)
    floats = inputs.astype(jnp.float32)
    gain_one, query_full, key_full, value_full, out_full = fetch_attention(
        attn_gain, query_weight, key_matrix, value_matrix, out_weight
    )
    normed_float, norm_pull_one = jax.vjp(rms_norm, floats, gain_one.astype(jnp.float32))
    normalized_input = normed_float.astype(jnp.bfloat16)
    query_pre = jnp.einsum(
        "std,de->ste", normalized_input, query_full, preferred_element_type=jnp.float32
    ).reshape(seq_count, tok_count, query_heads, head_dim)
    key_before_rotate = jnp.einsum(
        "std,de->ste", normalized_input, key_full, preferred_element_type=jnp.float32
    ).reshape(seq_count, tok_count, value_heads, head_dim)
    rows_of_value = (
        jnp.einsum("std,de->ste", normalized_input, value_full, preferred_element_type=jnp.float32)
        .astype(jnp.bfloat16)
        .reshape(seq_count, tok_count, value_heads, head_dim)
    )
    head_float = head_gains.astype(jnp.float32)

    def prepare_local(query_arg, key_arg, gains_arg):
        return prepare(query_arg, key_arg, gains_arg, cosine, sine_table)

    (query_rot, key_rot), prep_pull = jax.vjp(
        prepare_local, query_pre, key_before_rotate, head_float
    )
    query_local, key_local, value_local = (
        lax.all_to_all(
            query_rot.astype(jnp.bfloat16), "uly", split_axis=2, concat_axis=1, tiled=True
        ),
        lax.all_to_all(
            key_rot.astype(jnp.bfloat16), "uly", split_axis=2, concat_axis=1, tiled=True
        ),
        lax.all_to_all(rows_of_value, "uly", split_axis=2, concat_axis=1, tiled=True),
    )
    block_len = query_local.shape[1]
    local_kv = key_local.shape[2]
    query_group = query_local.reshape(seq_count, block_len, local_kv, heads_per_group, head_dim)
    bound = math.sqrt(head_dim) * jnp.max(jnp.abs(head_float[0])) * jnp.max(jnp.abs(head_float[1]))
    scale = head_dim ** (-0.5)
    query_index = blk_index * block_len + jnp.arange(block_len, dtype=jnp.int32)
    query_segs = lax.dynamic_slice_in_dim(segments, blk_index * block_len, block_len, 1)

    def block_weights(keys_in, source):
        key_index = source * block_len + jnp.arange(block_len, dtype=jnp.int32)
        key_segs = lax.dynamic_slice_in_dim(segments, source * block_len, block_len, 1)
        allowed = (key_index[None, None, :] <= query_index[None, :, None]) & (
            key_segs[:, None, :] == query_segs[:, :, None]
        )
        scores = (
            jnp.einsum(
                "sqhgd,skhd->shgqk", query_group, keys_in, preferred_element_type=jnp.float32
            )
            * scale
        )
        return jnp.where(allowed[:, None, None], jnp.exp(scores - bound), 0.0)

    def absorb(stats, key_value, source):
        row_sums, summed = stats
        weights = block_weights(key_value[0], source)
        row_sums = row_sums + jnp.sum(weights, axis=-1)
        summed = summed + jnp.einsum(
            "shgqk,skhd->sqhgd",
            weights.astype(jnp.bfloat16),
            key_value[1],
            preferred_element_type=jnp.float32,
        )
        return (row_sums, summed)

    own_pair = jnp.stack([key_local, value_local])
    start_stats = (
        jnp.zeros((seq_count, local_kv, heads_per_group, block_len), jnp.float32),
        jnp.zeros((seq_count, block_len, local_kv, heads_per_group, head_dim), jnp.float32),
    )
    first_stats = absorb(start_stats, own_pair, blk_index)

    def forward_turn(turn_index, carry):
        key_value, stats_in = carry
        key_value = passed_along(key_value, "blk", 1)
        stats_in = lax.cond(
            turn_index <= blk_index,
            lambda holding: absorb(holding, key_value, blk_index - turn_index),
            lambda holding: holding,
            stats_in,
        )
        return (key_value, stats_in)

    moved_pair, (row_totals, summed_all) = lax.fori_loop(
        1, blk_size, forward_turn, (own_pair, first_stats)
    )
    attended = summed_all / jnp.transpose(row_totals, (0, 3, 1, 2))[..., None]
    attended_tok = lax.all_to_all(
        attended.reshape(seq_count, block_len, local_kv * heads_per_group, head_dim).astype(
            jnp.bfloat16
        ),
        "uly",
        split_axis=1,
        concat_axis=2,
        tiled=True,
    ).reshape(seq_count, tok_count, query_heads * head_dim)
    middle = floats + jnp.einsum(
        "ste,ed->std", attended_tok, out_full, preferred_element_type=jnp.float32
    )
    gain_two, gate_full, up_full, down_full = fetch_feedforward(
        ffn_gain, gate_weight, up_weight, down_weight
    )
    normed_two_float, norm_pull_two = jax.vjp(rms_norm, middle, gain_two.astype(jnp.float32))
    normed_two = normed_two_float.astype(jnp.bfloat16)
    gate_rows = jnp.einsum("std,df->stf", normed_two, gate_full, preferred_element_type=jnp.float32)
    up_rows = jnp.einsum("std,df->stf", normed_two, up_full, preferred_element_type=jnp.float32)
    hidden_float, swiglu_pull = jax.vjp(swiglu, gate_rows, up_rows)
    hidden = hidden_float.astype(jnp.bfloat16)
    outputs = (
        middle + jnp.einsum("stf,fd->std", hidden, down_full, preferred_element_type=jnp.float32)
    ).astype(jnp.bfloat16)
    refetched = fetch_feedforward(ffn_gain, gate_weight, up_weight, down_weight)
    gate_back, up_back, down_back = (refetched[1], refetched[2], refetched[3])
    grad_out = cotangent.astype(jnp.float32)
    down_grad = jnp.einsum("stf,std->fd", hidden, cotangent, preferred_element_type=jnp.float32)
    grad_hidden = jnp.einsum(
        "std,fd->stf", cotangent, down_back, preferred_element_type=jnp.float32
    )
    grad_gate, grad_up = swiglu_pull(grad_hidden)
    grad_gate = grad_gate.astype(jnp.bfloat16)
    grad_up = grad_up.astype(jnp.bfloat16)
    gate_grad = jnp.einsum("std,stf->df", normed_two, grad_gate, preferred_element_type=jnp.float32)
    up_grad = jnp.einsum("std,stf->df", normed_two, grad_up, preferred_element_type=jnp.float32)
    grad_normed_two = jnp.einsum(
        "stf,df->std", grad_gate, gate_back, preferred_element_type=jnp.float32
    ) + jnp.einsum("stf,df->std", grad_up, up_back, preferred_element_type=jnp.float32)
    middle_part, gain_two_grad = norm_pull_two(grad_normed_two)
    grad_middle = grad_out + middle_part
    ffn_shares = (
        lax.psum_scatter(gain_two_grad, ("fsdp", "blk", "uly"), scatter_dimension=0, tiled=True),
        lax.psum_scatter(gate_grad, ("fsdp", "blk", "uly"), scatter_dimension=0, tiled=True),
        lax.psum_scatter(up_grad, ("fsdp", "blk", "uly"), scatter_dimension=0, tiled=True),
        lax.psum_scatter(down_grad, ("fsdp", "blk", "uly"), scatter_dimension=0, tiled=True),
    )
    fetched_again = fetch_attention(attn_gain, query_weight, key_matrix, value_matrix, out_weight)
    query_back, key_back, value_back, out_back = (
        fetched_again[1],
        fetched_again[2],
        fetched_again[3],
        fetched_again[4],
    )
    grad_middle_low = grad_middle.astype(jnp.bfloat16)
    out_grad = jnp.einsum(
        "ste,std->ed", attended_tok, grad_middle_low, preferred_element_type=jnp.float32
    )
    grad_att_tok = (
        jnp.einsum("std,ed->ste", grad_middle_low, out_back, preferred_element_type=jnp.float32)
        .astype(jnp.bfloat16)
        .reshape(seq_count, tok_count, query_heads, head_dim)
    )
    grad_att = lax.all_to_all(grad_att_tok, "uly", split_axis=2, concat_axis=1, tiled=True).reshape(
        seq_count, block_len, local_kv, heads_per_group, head_dim
    )
    delta = jnp.transpose(jnp.sum(grad_att.astype(jnp.float32) * attended, axis=-1), (0, 2, 3, 1))

    def block_grads(key_value, source):
        keys_in = key_value[0]
        values_in = key_value[1]
        probs = block_weights(keys_in, source) / row_totals[..., None]
        grad_probs = jnp.einsum(
            "sqhgd,skhd->shgqk", grad_att, values_in, preferred_element_type=jnp.float32
        )
        grad_scores = (probs * (grad_probs - delta[..., None])).astype(jnp.bfloat16)
        grad_query = (
            jnp.einsum(
                "shgqk,skhd->sqhgd", grad_scores, keys_in, preferred_element_type=jnp.float32
            )
            * scale
        )
        grad_keys = (
            jnp.einsum(
                "shgqk,sqhgd->skhd", grad_scores, query_group, preferred_element_type=jnp.float32
            )
            * scale
        )
        grad_values = jnp.einsum(
            "shgqk,sqhgd->skhd",
            probs.astype(jnp.bfloat16),
            grad_att,
            preferred_element_type=jnp.float32,
        )
        return (grad_query, jnp.stack([grad_keys, grad_values]))

    def pass_grads(moving):
        return from_behind(moving.astype(jnp.bfloat16), "blk", 1).astype(moving.dtype)

    query_start, pair_start = block_grads(own_pair, blk_index)

    def backward_turn(turn_index, carry):
        key_value, query_acc, pair_acc = carry
        key_value = passed_along(key_value, "blk", 1)
        pair_acc = pass_grads(pair_acc)

        def accumulate(holding):
            part_query, part_pair = block_grads(key_value, blk_index - turn_index)
            return (holding[0] + part_query, holding[1] + part_pair)

        query_acc, pair_acc = lax.cond(
            turn_index <= blk_index, accumulate, lambda holding: holding, (query_acc, pair_acc)
        )
        return (key_value, query_acc, pair_acc)

    spent_pair, query_total, pair_total = lax.fori_loop(
        1, blk_size, backward_turn, (own_pair, query_start, pair_start)
    )
    pair_total = pass_grads(pair_total)
    grad_query_low = query_total.reshape(
        seq_count, block_len, local_kv * heads_per_group, head_dim
    ).astype(jnp.bfloat16)
    grad_query_tok, grad_key_tok, grad_value_tok = (
        lax.all_to_all(grad_query_low, "uly", split_axis=1, concat_axis=2, tiled=True),
        lax.all_to_all(
            pair_total[0].astype(jnp.bfloat16), "uly", split_axis=1, concat_axis=2, tiled=True
        ),
        lax.all_to_all(
            pair_total[1].astype(jnp.bfloat16), "uly", split_axis=1, concat_axis=2, tiled=True
        ),
    )
    grad_query_pre, grad_key_pre, heads_grad = prep_pull(
        (grad_query_tok.astype(jnp.float32), grad_key_tok.astype(jnp.float32))
    )
    grad_query_flat = grad_query_pre.astype(jnp.bfloat16).reshape(
        seq_count, tok_count, query_heads * head_dim
    )
    grad_key_flat = grad_key_pre.astype(jnp.bfloat16).reshape(
        seq_count, tok_count, value_heads * head_dim
    )
    grad_value_flat = grad_value_tok.reshape(seq_count, tok_count, value_heads * head_dim)
    query_grad = jnp.einsum(
        "std,ste->de", normalized_input, grad_query_flat, preferred_element_type=jnp.float32
    )
    key_grad = jnp.einsum(
        "std,ste->de", normalized_input, grad_key_flat, preferred_element_type=jnp.float32
    )
    value_grad = jnp.einsum(
        "std,ste->de", normalized_input, grad_value_flat, preferred_element_type=jnp.float32
    )
    grad_normed = jnp.einsum(
        "ste,de->std", grad_query_flat, query_back, preferred_element_type=jnp.float32
    )
    grad_normed = grad_normed + jnp.einsum(
        "ste,de->std", grad_key_flat, key_back, preferred_element_type=jnp.float32
    )
    grad_normed = grad_normed + jnp.einsum(
        "ste,de->std", grad_value_flat, value_back, preferred_element_type=jnp.float32
    )
    input_part, gain_one_grad = norm_pull_one(grad_normed)
    input_grad = (grad_middle + input_part).astype(jnp.bfloat16)
    attn_shares = (
        lax.psum_scatter(gain_one_grad, ("fsdp", "blk", "uly"), scatter_dimension=0, tiled=True),
        lax.psum_scatter(heads_grad, ("fsdp", "blk", "uly"), scatter_dimension=1, tiled=True),
        lax.psum_scatter(query_grad, ("fsdp", "blk", "uly"), scatter_dimension=0, tiled=True),
        lax.psum_scatter(key_grad, ("fsdp", "blk", "uly"), scatter_dimension=0, tiled=True),
        lax.psum_scatter(value_grad, ("fsdp", "blk", "uly"), scatter_dimension=0, tiled=True),
        lax.psum_scatter(out_grad, ("fsdp", "blk", "uly"), scatter_dimension=0, tiled=True),
    )
    return (
        outputs,
        input_grad,
        attn_shares[0],
        attn_shares[1],
        attn_shares[2],
        attn_shares[3],
        attn_shares[4],
        attn_shares[5],
        ffn_shares[0],
        ffn_shares[1],
        ffn_shares[2],
        ffn_shares[3],
    )


MESH = pl.DeviceIdType.MESH
ANY = pl.BlockSpec(memory_space=pl.ANY)
VMEM = pl.BlockSpec(memory_space=pltpu.VMEM)
PLANE = [(dx, dy, dc) for dx in (0, 1) for dy in (0, 1) for dc in (0, 1)]
FAR = [(1, 1, 0), (1, 0, 0), (0, 1, 0)]
TURNS = (1, 2, 3)
SEM = pltpu.SemaphoreType.DMA


class Place:
    def __init__(self):
        self.x = lax.axis_index("fsdp")
        self.block = lax.axis_index("blk")
        self.z = lax.axis_index("uly")
        self.y, self.c = (self.block // 2, self.block % 2)
        self.head = 4 * self.x + self.block
        self.here = (self.x, self.block, self.z)

    def coords(self, dx, dy, dc):
        return ((self.x + dx) % 2, (self.y + dy) % 2, (self.c + dc) % 2)

    def peer(self, dx, dy, dc):
        x, y, c = self.coords(dx, dy, dc)
        return (x, 2 * y + c, self.z)

    def index(self, dx, dy, dc):
        x, y, c = self.coords(dx, dy, dc)
        return 4 * x + 2 * y + c

    def shard(self, ref, dx=0, dy=0, dc=0):
        x, y, c = self.coords(dx, dy, dc)
        return ref.at[2 * y + c, :, x]

    def behind(self, turn):
        return (self.z + 4 - turn) % 4

    def ahead(self, turn):
        return (self.z + turn) % 4

    def line(self, turn):
        return (self.x, self.block, self.ahead(turn))


def remote(src, dst, send_sem, recv_sem, device):
    return pltpu.make_async_remote_copy(
        src_ref=src,
        dst_ref=dst,
        send_sem=send_sem,
        recv_sem=recv_sem,
        device_id=device,
        device_id_type=MESH,
    )


def arrived(ref, sem):
    pltpu.make_async_copy(ref, ref, sem).wait()


def meet(peers):
    barrier = pltpu.get_barrier_semaphore()
    for peer in peers:
        pl.semaphore_signal(barrier, inc=1, device_id=peer, device_id_type=MESH)
    pl.semaphore_wait(barrier, len(peers))


class Sends:
    def __init__(self):
        self.pending = []

    def go(self, *args):
        copy = remote(*args)
        copy.start()
        self.pending.append((None, copy))

    def go_if(self, condition, *args):
        copy = remote(*args)
        pl.when(condition)(lambda: copy.start())
        self.pending.append((condition, copy))

    def drain(self):
        for condition, copy in self.pending:
            if condition is None:
                copy.wait_send()
            else:
                pl.when(condition)(lambda copy=copy: copy.wait_send())


def spread_start(me, sends, src, full, send_sems, recv_sems):
    for i, d in enumerate(FAR + [(0, 0, 1)]):
        sends.go(src, me.shard(full), send_sems.at[i], recv_sems.at[i], me.peer(*d))


def spread_forward(me, sends, full, send_sems, recv_sems):
    for i in (1, 2, 0):
        part = me.shard(full, *FAR[i])
        arrived(part, recv_sems.at[i])
        sends.go(part, part, send_sems.at[4 + i], recv_sems.at[4 + i], me.peer(0, 0, 1))


def spread_finish(me, full, recv_sems):
    for i, (dx, dy, _) in enumerate([(0, 0, 0)] + FAR):
        arrived(me.shard(full, dx, dy, 1), recv_sems.at[3 + i])


def full_shape(tokens, width):
    return (4, 4, 2, tokens // 32, width)


def half_start(me, sends, part, kept, sibling, keep_sems, send_sems, recv_sems):
    for i, (dx, dy, _) in enumerate(FAR + [(0, 0, 0)]):
        src = me.shard(part, dx, dy, 1)
        sends.go(src, sibling.at[i], send_sems.at[i], recv_sems.at[i], me.peer(0, 0, 1))
        pltpu.make_async_copy(me.shard(part, dx, dy, 0), kept.at[i], keep_sems.at[i]).start()


def half_send(me, sends, kept, sibling, out, came, keep_sems, send_sems, recv_sems):
    for i, d in enumerate(FAR):
        arrived(kept.at[i], keep_sems.at[i])
        arrived(sibling.at[i], recv_sems.at[i])
        out[i] = (
            kept[i].astype(jnp.float32) + sibling[i].astype(jnp.float32)
        ).astype(jnp.bfloat16)
        sends.go(out.at[i], came.at[i], send_sems.at[4 + i], recv_sems.at[4 + i], me.peer(*d))


def half_sum(kept, sibling, came, keep_sems, recv_sems):
    arrived(kept.at[3], keep_sems.at[3])
    arrived(sibling.at[3], recv_sems.at[3])
    total = kept[3].astype(jnp.float32) + sibling[3].astype(jnp.float32)
    for i in (1, 2, 0):
        arrived(came.at[i], recv_sems.at[4 + i])
        total = total + came[i].astype(jnp.float32)
    return total


def quarter_scratch(tokens, width):
    piece = (4, tokens // 32, width)
    return [
        pltpu.VMEM((4,) + piece, jnp.bfloat16),
        pltpu.VMEM((4,) + piece, jnp.bfloat16),
        pltpu.VMEM((3,) + piece, jnp.bfloat16),
        pltpu.VMEM((3,) + piece, jnp.bfloat16),
        SEM((4,)),
        SEM((7,)),
        SEM((7,)),
    ]


def near(me):
    return [me.peer(*d) for d in FAR + [(0, 0, 1)]]


def line_spread(me, sends, src, part, sems):
    for dz in (1, 2):
        sends.go_if(me.z < 4 - dz, src, part(me.z), sems.at[0, dz - 1], sems.at[1, dz - 1], me.line(dz))
        sends.go_if(me.z >= dz, src, part(me.z), sems.at[0, dz + 1], sems.at[1, dz + 1], me.line(4 - dz))


def line_forward(me, sends, part, sems):
    inner = jnp.logical_or(me.z == 1, me.z == 2)
    ref = part((me.z + 2) % 4)
    pl.when(me.z == 1)(lambda: arrived(ref, sems.at[1, 3]))
    pl.when(me.z == 2)(lambda: arrived(ref, sems.at[1, 1]))
    target = (me.x, me.block, (3 * me.z + 1) % 4)
    sends.go_if(inner, ref, ref, sems.at[0, 4], sems.at[1, 4], target)


def line_finish(me, part, sems):
    z = me.z
    pl.when(z > 0)(lambda: arrived(part((z + 3) % 4), sems.at[1, 0]))
    pl.when(z < 3)(lambda: arrived(part((z + 1) % 4), sems.at[1, 2]))

    @pl.when(z == 3)
    def _():
        arrived(part((z + 2) % 4), sems.at[1, 1])
        arrived(part((z + 1) % 4), sems.at[1, 4])

    @pl.when(z == 0)
    def _():
        arrived(part((z + 2) % 4), sems.at[1, 3])
        arrived(part((z + 3) % 4), sems.at[1, 4])


def lanes(shape):
    return lax.broadcasted_iota(jnp.int32, shape, len(shape) - 1)


def turned(vector):
    half = vector.shape[-1] // 2
    sign = jnp.where(lanes((1, 2 * half)) < half, -1.0, 1.0)
    return pltpu.roll(vector, half, 1) * sign


def head_scale(vector):
    return lax.rsqrt(jnp.mean(vector * vector, axis=-1, keepdims=True) + EPSILON)


def mat(a, b):
    return jnp.dot(a, b, preferred_element_type=jnp.float32)


def mat_right(a, b):
    return lax.dot_general(a, b, (((1,), (1,)), ((), ())), preferred_element_type=jnp.float32)


def mat_left(a, b):
    return lax.dot_general(a, b, (((0,), (0,)), ((), ())), preferred_element_type=jnp.float32)


def permute_in(me, src_ref, full_ref, send_sems, recv_sems, wait=False):
    half = src_ref.shape[1] // 2
    for j in (0, 1):
        for to in (0, 1):
            src = src_ref.at[j, pl.ds(half * to, half)]
            dst = full_ref.at[me.block, me.z, to]
            mine = jnp.logical_and(me.x == to, me.z == 2 * me.x + j)
            copy = remote(
                src, dst, send_sems.at[2 * j + to], recv_sems.at[me.z], (to, me.block, 2 * me.x + j)
            )
            if wait:
                pl.when(jnp.logical_not(mine))(lambda copy=copy: copy.wait_send())
                continue
            pl.when(jnp.logical_not(mine))(lambda copy=copy: copy.start())
            own = pltpu.make_async_copy(src, dst, recv_sems.at[me.z])
            pl.when(mine)(lambda own=own: own.start())


def permuted_in(me, full_ref, recv_sems):
    for k in range(4):
        arrived(full_ref.at[me.block, k, me.x], recv_sems.at[k])


def half_block(me, sends, part, sibling, send_sems, recv_sems, b):
    other = me.c != b % 2
    dy = (me.y + b // 2) % 2
    for to in (0, 1):
        slot = 3 - 2 * ((me.x + to) % 2) - dy
        sends.go_if(
            other, part.at[b, :, to], sibling.at[slot], send_sems.at[slot], recv_sems.at[slot],
            me.peer(0, 0, 1),
        )


def half_out(me, sends, part, sibling, out, came, send_sems, recv_sems):
    for i, d in enumerate(FAR):
        x, y, c = me.coords(*d)
        arrived(sibling.at[i], recv_sems.at[i])
        own = part[2 * y + c, :, x].astype(jnp.float32)
        out[i] = (own + sibling[i].astype(jnp.float32)).astype(jnp.bfloat16)
        sends.go(out.at[i], came.at[i], send_sems.at[4 + i], recv_sems.at[4 + i], me.peer(*d))


def half_in(me, part, sibling, came, recv_sems):
    arrived(sibling.at[3], recv_sems.at[3])
    total = part[me.block, :, me.x].astype(jnp.float32) + sibling[3].astype(jnp.float32)
    for i in (1, 2, 0):
        arrived(came.at[i], recv_sems.at[4 + i])
        total = total + came[i].astype(jnp.float32)
    return total


def half_scratch(tokens, width):
    piece = (4, tokens // 32, width)
    return [
        pltpu.VMEM((4,) + piece, jnp.bfloat16),
        pltpu.VMEM((3,) + piece, jnp.bfloat16),
        pltpu.VMEM((3,) + piece, jnp.bfloat16),
        SEM((7,)),
        SEM((7,)),
    ]


def gain_row(gains_ref, kind):
    rows = [jnp.sum(gains_ref[p, :, kind, :], axis=0, keepdims=True) for p in range(8)]
    return jnp.concatenate(rows, axis=1)


def allowed_keys(segcol, segrow, b, kb):
    same = segcol[b] == segrow[:, 256 * kb : 256 * kb + 256]
    if kb < b:
        return same
    rows = lax.broadcasted_iota(jnp.int32, (256, 256), 0)
    return jnp.logical_and(same, lanes((256, 256)) <= rows)


def forward_kernel(
    x_ref, cot_ref, seg_ref, q_ref, k_ref, v_ref, g_ref, u_ref, o_ref, d_ref, gain_ref, hg_ref,
    cf_ref, nf_ref, guf_ref, df_ref, segf_ref, wq_out, of_out, n1_out, xs_out, pre_out, qkv_out,
    att_out, cos_out, sin_out, mid_ref, grow_ref,
    xf, wf, of, segs, gains, n1, pre, qkv, segcol, cos_s, sin_s, att, attlow, part, n2,
    sibling, out, came, hs, hr, ps, pr, as_, ar, ws, wr, us, ur, gs, gr, zq, zo, zd, zg, ls,
):
    me = Place()
    x, z, p = (me.x, me.z, me.head)
    across = [((x + 1) % 2, me.block, me.ahead(turn)) for turn in TURNS]
    meet([me.peer(*d) for d in PLANE[1:]] + [me.line(turn) for turn in TURNS] + across)
    sends = Sends()

    def local(src, dst, sem):
        copy = pltpu.make_async_copy(src, dst, sem)
        copy.start()
        return copy

    own_gain = local(gain_ref, gains.at[p, z], ls.at[0])
    own_seg = local(seg_ref, segs.at[x], ls.at[1])
    sends.go(seg_ref, segs.at[x], ls.at[2], ls.at[3], me.peer(1, 0, 0))
    for turn in TURNS:
        sends.go(gain_ref, gains.at[p, z], gs.at[turn], gr.at[turn], me.line(turn))
    permute_in(me, x_ref, xf, ps.at[0], pr.at[0])
    own_o = local(o_ref, of.at[z], ls.at[4])
    own_d = local(d_ref, df_ref.at[z], ls.at[5])
    wide, narrow = (q_ref.shape[1] // 8, k_ref.shape[1] // 8)
    cuts = ((q_ref, wide, 0), (k_ref, narrow, wide), (v_ref, narrow, wide + narrow))
    for i, d in enumerate(PLANE):
        t = me.index(*d)
        for n, (ref, width, off) in enumerate(cuts):
            src = ref.at[:, pl.ds(pl.multiple_of(t * width, 128), width)]
            dst = wf.at[p, z, :, pl.ds(off, width)]
            if i == 0:
                local(src, dst, wr.at[n])
            else:
                sends.go(src, dst, ws.at[3 * i + n], wr.at[3 * i + n], me.peer(*d))
    permuted_in(me, xf, pr.at[0])
    spread_start(me, sends, me.shard(xf), xf, as_.at[0], ar.at[0])
    for i, d in enumerate(PLANE):
        t = me.index(*d)
        for n, (ref, width, off) in enumerate(cuts):
            arrived(wf.at[t, z, :, pl.ds(off, width)], wr.at[3 * i + n])
    qkv_part = lambda k: wf.at[:, k]
    o_part = lambda k: of.at[k]
    d_part = lambda k: df_ref.at[k]
    gu_part = lambda k: guf_ref.at[:, k]
    line_spread(me, sends, qkv_part(z), qkv_part, zq)
    permute_in(me, cot_ref, cf_ref, ps.at[1], pr.at[1])
    line_spread(me, sends, o_ref, o_part, zo)
    width = g_ref.shape[1] // 8
    for i, d in enumerate(PLANE):
        t = me.index(*d)
        for n, ref in enumerate((g_ref, u_ref)):
            src = ref.at[:, pl.ds(pl.multiple_of(t * width, 128), width)]
            dst = guf_ref.at[p, z, :, pl.ds(n * width, width)]
            if i == 0:
                local(src, dst, ur.at[n])
            else:
                sends.go(src, dst, us.at[2 * i + n], ur.at[2 * i + n], me.peer(*d))
    own_gain.wait()
    for turn in TURNS:
        arrived(gains.at[p, me.behind(turn)], gr.at[turn])
    for i, d in enumerate(PLANE[1:]):
        sends.go(gains.at[p], gains.at[p], gs.at[4 + i], gr.at[4 + i], me.peer(*d))
    own_seg.wait()
    arrived(segs.at[(x + 1) % 2], ls.at[3])
    local(segs, segf_ref, ls.at[6])
    head_dim = hg_ref.shape[1]
    segrow = segs[z // 2, pl.ds(z % 2, 1), :]
    tokens = segrow.shape[1]
    column = jnp.transpose(jnp.broadcast_to(segrow.astype(jnp.float32), (8, tokens)))[:, :1]
    segcol[...] = column.astype(jnp.int32).reshape(4, 256, 1)
    half_lane = (lanes((1, head_dim)) % (head_dim // 2)).astype(jnp.float32)
    inverse = jnp.exp(half_lane * (-2.0 * math.log(THETA) / head_dim))
    steps = lax.broadcasted_iota(jnp.int32, (32, head_dim), 0).astype(jnp.float32) * inverse
    cl, sl = (jnp.cos(steps), jnp.sin(steps))
    ch, sh = (jnp.cos(steps * 32.0), jnp.sin(steps * 32.0))
    doc_cos, doc_sin = ([], [])
    for doc in range(DOCS):
        start = jnp.sum((segrow < doc).astype(jnp.float32), axis=1, keepdims=True)
        doc_cos.append(jnp.cos(start * inverse))
        doc_sin.append(jnp.sin(start * inverse))
    for b in range(4):
        hi_c, hi_s = (ch[8 * b : 8 * b + 8][:, None, :], sh[8 * b : 8 * b + 8][:, None, :])
        cos_at = (hi_c * cl[None] - hi_s * sl[None]).reshape(256, head_dim)
        sin_at = (hi_s * cl[None] + hi_c * sl[None]).reshape(256, head_dim)
        column = segcol[b]
        cd, sd = (jnp.broadcast_to(v[0], (256, head_dim)) for v in (doc_cos, doc_sin))
        for doc in range(1, DOCS):
            cd = jnp.where(column == doc, doc_cos[doc], cd)
            sd = jnp.where(column == doc, doc_sin[doc], sd)
        cos_s[b] = cos_at * cd + sin_at * sd
        sin_s[b] = sin_at * cd - cos_at * sd
    local(cos_s, cos_out, ls.at[7])
    local(sin_s, sin_out, ls.at[8])
    for i, d in enumerate(PLANE[1:]):
        arrived(gains.at[me.index(*d)], gr.at[4 + i])
    gain_one, gain_two = (gain_row(gains, 0), gain_row(gains, 1))
    grow_ref[0:1] = gain_one
    grow_ref[1:2] = gain_two
    line_forward(me, sends, qkv_part, zq)
    spread_forward(me, sends, xf, as_.at[0], ar.at[0])
    spread_finish(me, xf, ar.at[0])
    xs_copy = local(me.shard(xf), xs_out, ls.at[9])

    def norm_block(b, carry):
        rows = xf[b].reshape(256, -1).astype(jnp.float32)
        n1[b] = (rows * head_scale(rows) * gain_one).astype(jnp.bfloat16)
        return carry

    lax.fori_loop(0, 4, norm_block, 0)
    local(n1, n1_out, ls.at[10])
    for i, d in enumerate(PLANE):
        t = me.index(*d)
        for n in (0, 1):
            arrived(guf_ref.at[t, z, :, pl.ds(n * width, width)], ur.at[2 * i + n])
    line_spread(me, sends, gu_part(z), gu_part, zg)
    line_spread(me, sends, d_ref, d_part, zd)
    line_finish(me, qkv_part, zq)
    local(wf, wq_out, ls.at[11])

    def qkv_block(b, carry):
        w = wf[...].reshape(-1, wf.shape[3])
        rows = mat(n1[b], w)
        pre[b] = rows
        cosine, sine = (cos_s[b], sin_s[b])
        for h in range(3):
            v = rows[:, head_dim * h : head_dim * (h + 1)]
            n = v * head_scale(v) * hg_ref[pl.ds(h // 2, 1), :]
            qkv[b, :, pl.ds(head_dim * h, head_dim)] = (n * cosine + turned(n) * sine).astype(jnp.bfloat16)
        qkv[b, :, pl.ds(3 * head_dim, head_dim)] = rows[:, 3 * head_dim :].astype(jnp.bfloat16)
        return carry

    lax.fori_loop(0, 4, qkv_block, 0)
    local(pre, pre_out, ls.at[12])
    local(qkv, qkv_out, ls.at[13])
    own_o.wait()
    line_forward(me, sends, o_part, zo)
    top = lambda r: jnp.max(jnp.abs(hg_ref[pl.ds(r, 1), :]), axis=1, keepdims=True)
    bound = math.sqrt(head_dim) * top(0) * top(1)
    scale = head_dim ** (-0.5)
    for b in range(4):
        for h in (0, 1):
            qb = qkv[b, :, pl.ds(head_dim * h, head_dim)]
            total, mixed = (None, None)
            for kb in range(b + 1):
                s = mat_right(qb, qkv[kb, :, pl.ds(2 * head_dim, head_dim)]) * scale
                w = jnp.where(allowed_keys(segcol, segrow, b, kb), jnp.exp(s - bound), 0.0)
                t = jnp.sum(w, axis=1, keepdims=True)
                m = mat(w.astype(jnp.bfloat16), qkv[kb, :, pl.ds(3 * head_dim, head_dim)])
                total = t if kb == 0 else total + t
                mixed = m if kb == 0 else mixed + m
            mixed = mixed / total
            att[b, :, pl.ds(head_dim * h, head_dim)] = mixed
            attlow[b, :, pl.ds(head_dim * h, head_dim)] = mixed.astype(jnp.bfloat16)
        if b == 2:
            permuted_in(me, cf_ref, pr.at[1])
            spread_start(me, sends, me.shard(cf_ref), cf_ref, as_.at[1], ar.at[1])
    local(att, att_out, ls.at[14])
    line_finish(me, o_part, zo)
    local(of, of_out, ls.at[15])
    for b in range(4):
        rows = mat(attlow[b], of[...].reshape(-1, of.shape[2])).astype(jnp.bfloat16)
        part[b] = rows.reshape(part.shape[1:])
        half_block(me, sends, part, sibling, hs, hr, b)
    half_out(me, sends, part, sibling, out, came, hs, hr)
    spread_forward(me, sends, cf_ref, as_.at[1], ar.at[1])
    middle = xf[me.block, :, x].astype(jnp.float32) + half_in(me, part, sibling, came, hr)
    mid_ref[...] = middle
    n2[...] = (middle * head_scale(middle) * gain_two).astype(jnp.bfloat16)
    own_n = local(n2, me.shard(nf_ref), ls.at[16])
    spread_start(me, sends, n2, nf_ref, as_.at[2], ar.at[2])
    line_forward(me, sends, gu_part, zg)
    line_forward(me, sends, d_part, zd)
    spread_forward(me, sends, nf_ref, as_.at[2], ar.at[2])
    spread_finish(me, nf_ref, ar.at[2])
    spread_finish(me, cf_ref, ar.at[1])
    own_d.wait()
    own_n.wait()
    line_finish(me, gu_part, zg)
    line_finish(me, d_part, zd)
    permute_in(me, x_ref, xf, ps.at[0], pr.at[0], wait=True)
    permute_in(me, cot_ref, cf_ref, ps.at[1], pr.at[1], wait=True)
    xs_copy.wait()
    for src, dst, i in (
        (segs, segf_ref, 6), (cos_s, cos_out, 7), (sin_s, sin_out, 8), (n1, n1_out, 10),
        (wf, wq_out, 11), (pre, pre_out, 12), (qkv, qkv_out, 13), (att, att_out, 14), (of, of_out, 15),
    ):
        pltpu.make_async_copy(src, dst, ls.at[i]).wait()
    sends.drain()


def forward_step(x, cot, seg, q, k, v, g, u, o, d, gain, head_gains):
    tokens, width = (16 * x.shape[1], x.shape[2])
    rows, low, wide = (q.shape[0], jnp.bfloat16, jnp.float32)
    cols = (q.shape[1] + 2 * k.shape[1]) // 8
    att_cols, head_dim = (q.shape[1] // 8, k.shape[1] // 8)
    full = full_shape(tokens, width)
    piece = (4, tokens // 32, width)
    quarter = tokens // 4
    S = jax.ShapeDtypeStruct
    return pl.pallas_call(
        forward_kernel,
        name="forward_step",
        out_shape=(
            S(full, low), S(full, low), S((8, 4, rows, g.shape[1] // 4), low), S((4,) + d.shape, low),
            S((2,) + seg.shape, seg.dtype), S((8, 4, rows, cols), low), S((4,) + o.shape, low),
            S((4, quarter, width), low), S(piece, low), S((4, quarter, cols), wide),
            S((4, quarter, cols), low), S((4, quarter, att_cols), wide),
            S((4, quarter, head_dim), wide), S((4, quarter, head_dim), wide),
            S(piece, wide), S((2, width), wide),
        ),
        in_specs=[ANY] * 11 + [VMEM],
        out_specs=(ANY,) * 14 + (VMEM,) * 2,
        scratch_shapes=[
            pltpu.VMEM(full, low), pltpu.VMEM((8, 4, rows, cols), low), pltpu.VMEM((4,) + o.shape, low),
            pltpu.VMEM((2,) + seg.shape, seg.dtype), pltpu.VMEM((8, 4, 8, 128), wide),
            pltpu.VMEM((4, quarter, width), low), pltpu.VMEM((4, quarter, cols), wide),
            pltpu.VMEM((4, quarter, cols), low), pltpu.VMEM((4, quarter, 1), jnp.int32),
            pltpu.VMEM((4, quarter, head_dim), wide), pltpu.VMEM((4, quarter, head_dim), wide),
            pltpu.VMEM((4, quarter, att_cols), wide), pltpu.VMEM((4, quarter, att_cols), low),
            pltpu.VMEM(full, low), pltpu.VMEM(piece, low),
        ]
        + half_scratch(tokens, width)
        + [SEM((2, 4)), SEM((2, 4)), SEM((3, 7)), SEM((3, 7)), SEM((24,)), SEM((24,)), SEM((16,)), SEM((16,))]
        + [SEM((11,)), SEM((11,))]
        + [SEM((2, 5))] * 4
        + [SEM((17,))],
        compiler_params=pltpu.CompilerParams(
            collective_id=0, has_side_effects=True, vmem_limit_bytes=60 * 1024 * 1024
        ),
    )(x, cot, seg, q, k, v, g, u, o, d, gain, head_gains)


def norm_back(grad, vector, gain, scale):
    weighted = grad * gain
    inner = jnp.mean(weighted * vector, axis=-1, keepdims=True)
    return scale * weighted - vector * (scale * scale * scale * inner)


def turn_kernel(
    part_ref, down_ref, cf_ref, mid_ref, gain_ref, gmid_ref, gf_ref, out_ref, gg_ref,
    kept, sibling, out, came, ks, ss, rs, kept2, sibling2, out2, came2, ks2, ss2, rs2,
    cs_ref, n_ref, as_, ar, ls,
):
    me = Place()
    meet(near(me))
    sends = Sends()
    half_start(me, sends, part_ref, kept, sibling, ks, ss, rs)
    own_c = pltpu.make_async_copy(me.shard(cf_ref), cs_ref, ls.at[0])
    own_c.start()
    half_start(me, sends, down_ref, kept2, sibling2, ks2, ss2, rs2)
    half_send(me, sends, kept, sibling, out, came, ks, ss, rs)
    half_send(me, sends, kept2, sibling2, out2, came2, ks2, ss2, rs2)
    own_c.wait()
    grad = half_sum(kept, sibling, came, ks, rs)
    middle = mid_ref[...]
    scale = lax.rsqrt(jnp.mean(middle * middle, axis=-1, keepdims=True) + EPSILON)
    total = cs_ref[...].astype(jnp.float32) + norm_back(grad, middle, gain_ref[...], scale)
    gmid_ref[...] = total
    n_ref[...] = total.astype(jnp.bfloat16)
    own_n = pltpu.make_async_copy(n_ref, me.shard(gf_ref), ls.at[1])
    own_n.start()
    spread_start(me, sends, n_ref, gf_ref, as_, ar)
    share = grad * middle * scale
    gg_ref[...] = jnp.sum(jnp.sum(share, axis=0), axis=0, keepdims=True)
    out_ref[...] = (middle + half_sum(kept2, sibling2, came2, ks2, rs2)).astype(jnp.bfloat16)
    spread_forward(me, sends, gf_ref, as_, ar)
    spread_finish(me, gf_ref, ar)
    own_n.wait()
    sends.drain()


def turn_step(part, down, cf, middle, gain):
    tokens, width = (part.shape[0], part.shape[1])
    piece = (4, tokens // 32, width)
    full = full_shape(tokens, width)
    return pl.pallas_call(
        turn_kernel,
        name="turn_step",
        out_shape=(
            jax.ShapeDtypeStruct(piece, jnp.float32),
            jax.ShapeDtypeStruct(full, jnp.bfloat16),
            jax.ShapeDtypeStruct(piece, jnp.bfloat16),
            jax.ShapeDtypeStruct((1, width), jnp.float32),
        ),
        in_specs=[ANY, ANY, ANY, VMEM, VMEM],
        out_specs=(VMEM, ANY, VMEM, VMEM),
        scratch_shapes=quarter_scratch(tokens, width) * 2
        + [pltpu.VMEM(piece, jnp.bfloat16)] * 2
        + [SEM((7,)), SEM((7,)), SEM((2,))],
        compiler_params=pltpu.CompilerParams(collective_id=2, has_side_effects=True),
    )(part.reshape(full), down.reshape(full), cf, middle, gain)


def last_kernel(
    part_ref, xf_ref, gmid_ref, out_ref, gain_ref, small_ref, dw_ref, dgu_ref,
    y_ref, gx_ref, q_ref, k_ref, v_ref, g_ref, u_ref, sums_ref,
    kept, sibling, out, came, ks, ss, rs, xs_ref, gi_ref, ps, pr, ls,
    wown, wcame, wsum, zs, zr, ws, wr, us, ur, pack, packs, lines, gs, gr,
):
    me = Place()
    x, z, p = (me.x, me.z, me.head)
    across = [((x + 1) % 2, me.block, me.ahead(turn)) for turn in TURNS]
    meet([me.peer(*d) for d in PLANE[1:]] + [me.line(turn) for turn in TURNS] + across)
    sends = Sends()
    half_start(me, sends, part_ref, kept, sibling, ks, ss, rs)
    for turn in TURNS:
        sends.go(
            dw_ref.at[:, me.ahead(turn)], wcame.at[turn - 1],
            zs.at[turn - 1], zr.at[turn - 1], me.line(turn),
        )
    own_w = pltpu.make_async_copy(dw_ref.at[:, z], wown, ls.at[2])
    own_w.start()
    own_x = pltpu.make_async_copy(xf_ref, xs_ref, ls.at[0])
    own_x.start()
    half_send(me, sends, kept, sibling, out, came, ks, ss, rs)
    half = y_ref.shape[1] // 2

    def permute(src_ref, dst_ref, o, wait=False):
        for k in range(4):
            dst = dst_ref.at[z % 2, pl.ds(half * x, half)]
            src = src_ref.at[k]
            mine = jnp.logical_and(x == z // 2, z == k)
            copy = remote(src, dst, ps.at[o + k], pr.at[o + 2 * (z % 2) + x], (z // 2, me.block, k))

            @pl.when(jnp.logical_not(mine))
            def _():
                if wait:
                    copy.wait_send()
                else:
                    copy.start()

            if not wait:

                @pl.when(mine)
                def _():
                    pltpu.make_async_copy(src, dst, pr.at[o + 2 * (z % 2) + x]).start()

    def permuted(dst_ref, o):
        for j in (0, 1):
            for to in (0, 1):
                arrived(dst_ref.at[j, pl.ds(half * to, half)], pr.at[o + 2 * j + to])

    permute(out_ref, y_ref, 0)
    width = g_ref.shape[1] // 8
    for i, d in enumerate(PLANE):
        t = me.index(*d)
        for n, ref in enumerate((g_ref, u_ref)):
            src = dgu_ref.at[t, :, pl.ds(n * width, width)]
            dst = ref.at[:, pl.ds(pl.multiple_of(p * width, 128), width)]
            if i == 0:
                pltpu.make_async_copy(src, dst, ur.at[n]).start()
            else:
                sends.go(src, dst, us.at[2 * i + n], ur.at[2 * i + n], me.peer(*d))
    own_x.wait()
    grad = half_sum(kept, sibling, came, ks, rs)
    rows = xs_ref[...].astype(jnp.float32)
    scale = lax.rsqrt(jnp.mean(rows * rows, axis=-1, keepdims=True) + EPSILON)
    gi_ref[...] = (gmid_ref[...] + norm_back(grad, rows, gain_ref[...], scale)).astype(jnp.bfloat16)
    permute(gi_ref, gx_ref, 4)
    share = jnp.sum(jnp.sum(grad * rows * scale, axis=0), axis=0, keepdims=True)
    for i in range(8):
        pack[pl.ds(i, 1)] = share[:, 128 * i : 128 * i + 128]
    pack[pl.ds(8, 16)] = small_ref[...]
    for i, d in enumerate(PLANE[1:]):
        sends.go(pack, packs.at[i], gs.at[i], gr.at[i], me.peer(*d))
    own_w.wait()
    for turn in TURNS:
        arrived(wcame.at[turn - 1], zr.at[turn - 1])
    wsum[...] = (
        wown[...].astype(jnp.float32)
        + wcame[0].astype(jnp.float32)
        + wcame[1].astype(jnp.float32)
        + wcame[2].astype(jnp.float32)
    ).astype(jnp.bfloat16)
    wide, narrow = (q_ref.shape[1] // 8, k_ref.shape[1] // 8)
    cuts = ((q_ref, wide, 0), (k_ref, narrow, wide), (v_ref, narrow, wide + narrow))
    for i, d in enumerate(PLANE):
        t = me.index(*d)
        for n, (ref, cols, off) in enumerate(cuts):
            src = wsum.at[t, :, pl.ds(off, cols)]
            dst = ref.at[:, pl.ds(pl.multiple_of(p * cols, 128), cols)]
            if i == 0:
                pltpu.make_async_copy(src, dst, wr.at[n]).start()
            else:
                sends.go(src, dst, ws.at[3 * i + n], wr.at[3 * i + n], me.peer(*d))
    total = pack[...]
    for i in range(7):
        arrived(packs.at[i], gr.at[i])
        total = total + packs[i]
    sums_ref[...] = total
    packs[7] = total
    for turn in TURNS:
        sends.go(packs.at[7], lines.at[turn - 1], gs.at[6 + turn], gr.at[6 + turn], me.line(turn))
    for turn in TURNS:
        arrived(lines.at[turn - 1], gr.at[6 + turn])
    sums_ref[...] = ((sums_ref[...] + lines[0]) + lines[1]) + lines[2]
    for i, d in enumerate(PLANE):
        t = me.index(*d)
        for n, ref in enumerate((g_ref, u_ref)):
            arrived(ref.at[:, pl.ds(pl.multiple_of(t * width, 128), width)], ur.at[2 * i + n])
        for n, (ref, cols, off) in enumerate(cuts):
            arrived(ref.at[:, pl.ds(pl.multiple_of(t * cols, 128), cols)], wr.at[3 * i + n])
    permuted(y_ref, 0)
    permuted(gx_ref, 4)
    permute(out_ref, y_ref, 0, wait=True)
    permute(gi_ref, gx_ref, 4, wait=True)
    sends.drain()


def last_step(part, xf, gmid, out, gain, small, dw, dgu, per_device):
    tokens, width = (part.shape[0], part.shape[1])
    piece = (4, tokens // 32, width)
    rows, cols = (dw.shape[2], dw.shape[3])
    token_shape, q_cols, k_cols, f_cols = per_device
    back = jax.ShapeDtypeStruct(token_shape, jnp.bfloat16)
    weights = [jax.ShapeDtypeStruct((rows, n), jnp.bfloat16) for n in (q_cols, k_cols, k_cols, f_cols, f_cols)]
    return pl.pallas_call(
        last_kernel,
        name="last_step",
        out_shape=(back, back, *weights, jax.ShapeDtypeStruct((24, 128), jnp.float32)),
        in_specs=[ANY, ANY, VMEM, ANY, VMEM, VMEM, ANY, ANY],
        out_specs=(ANY,) * 7 + (VMEM,),
        scratch_shapes=quarter_scratch(tokens, width)
        + [pltpu.VMEM(piece, jnp.bfloat16)] * 2
        + [SEM((8,)), SEM((8,)), SEM((3,))]
        + [
            pltpu.VMEM((8, rows, cols), jnp.bfloat16),
            pltpu.VMEM((3, 8, rows, cols), jnp.bfloat16),
            pltpu.VMEM((8, rows, cols), jnp.bfloat16),
            SEM((3,)), SEM((3,)), SEM((24,)), SEM((24,)), SEM((16,)), SEM((16,)),
            pltpu.VMEM((24, 128), jnp.float32),
            pltpu.VMEM((8, 24, 128), jnp.float32),
            pltpu.VMEM((3, 24, 128), jnp.float32),
            SEM((10,)), SEM((10,)),
        ],
        compiler_params=pltpu.CompilerParams(collective_id=3, has_side_effects=True),
    )(part.reshape(full_shape(tokens, width)), xf, gmid, out, gain, small, dw, dgu)


def dot(a, b, kind=jnp.float32):
    return jnp.dot(a, b, preferred_element_type=jnp.float32).astype(kind)


def dot_left(a, b, kind=jnp.float32):
    return lax.dot_general(
        a, b, (((0,), (0,)), ((), ())), preferred_element_type=jnp.float32
    ).astype(kind)


def dot_right(a, b, kind=jnp.float32):
    return lax.dot_general(
        a, b, (((1,), (1,)), ((), ())), preferred_element_type=jnp.float32
    ).astype(kind)


def plane_body(
    inputs, segments, attn_gain, head_gains, query_weight, key_matrix, value_matrix, out_weight,
    ffn_gain, gate_weight, up_weight, down_weight, cotangent,
):
    low = jnp.bfloat16
    width = inputs.shape[2]
    head_dim = head_gains.shape[1]
    z = lax.axis_index("uly")
    head = 4 * lax.axis_index("fsdp") + lax.axis_index("blk")
    piece = attn_gain.shape[0]
    pair = jnp.stack([attn_gain, ffn_gain]).astype(jnp.float32)
    spot = (jnp.arange(128, dtype=jnp.int32) // piece == z)[None]
    gains_own = jnp.where(spot, jnp.tile(pair, (1, 128 // piece)), 0.0)
    gains_own = jnp.concatenate([gains_own, jnp.zeros((6, 128), jnp.float32)], axis=0)
    head_float = head_gains.astype(jnp.float32)
    (
        cf, nf, gate_up, down_full, segf, w_qkv, out_full, normed, xs, pre, qkv, attended, cosine,
        sine, middle, gain_rows,
    ) = forward_step(
        inputs, cotangent, segments, query_weight, key_matrix, value_matrix, gate_weight, up_weight,
        out_weight, down_weight, gains_own, head_float,
    )
    gain_one, gain_two = (gain_rows[0:1], gain_rows[1:2])
    tokens = normed.shape[0] * normed.shape[1]
    normed = normed.reshape(tokens, width)
    w_qkv = w_qkv.reshape(width, -1)
    out_full = out_full.reshape(-1, width)
    down_full = down_full.reshape(-1, width)
    gate_up = gate_up.reshape(width, -1)
    cot_all = cf.reshape(tokens, width)
    segs = lax.dynamic_index_in_dim(segf.reshape(-1, tokens), z, 0, keepdims=False)
    groups = query_weight.shape[1] // 8 // head_dim
    pre = pre.reshape(tokens, -1, head_dim)
    qkv = qkv.reshape(tokens, -1, head_dim)
    query, key, value = (qkv[:, :groups], qkv[:, groups], qkv[:, groups + 1])
    cosine, sine = (cosine.reshape(tokens, head_dim), sine.reshape(tokens, head_dim))

    def prepare_local(query_arg, key_arg, gains_arg):
        return prepare(query_arg[None], key_arg[None], gains_arg, cosine[None], sine[None])

    _, prep_pull = jax.vjp(
        prepare_local, pre[:, :groups], pre[:, groups : groups + 1], head_float
    )
    bound = math.sqrt(head_dim) * jnp.max(jnp.abs(head_float[0])) * jnp.max(jnp.abs(head_float[1]))
    scale = head_dim ** (-0.5)
    index = jnp.arange(tokens, dtype=jnp.int32)
    allowed = (index[None, :] <= index[:, None]) & (segs[None, :] == segs[:, None])
    scores = jnp.einsum("qgd,kd->gqk", query, key, preferred_element_type=jnp.float32) * scale
    weights = jnp.where(allowed[None], jnp.exp(scores - bound), 0.0)
    totals = jnp.sum(weights, axis=-1)
    attended = attended.reshape(tokens, groups, head_dim)
    attended_low = attended.astype(low).reshape(tokens, groups * head_dim)
    normed_two = nf.reshape(tokens, width)
    hidden_width = gate_up.shape[1] // 2
    both = dot(normed_two, gate_up)
    gate_rows, up_rows = (both[:, :hidden_width], both[:, hidden_width:])
    hidden_float, swiglu_pull = jax.vjp(swiglu, gate_rows, up_rows)
    hidden = hidden_float.astype(low)
    down_part = dot(hidden, down_full, low)
    grad_hidden = dot_right(cot_all, down_full)
    grad_gate, grad_up = swiglu_pull(grad_hidden)
    grad_both = jnp.concatenate([grad_gate.astype(low), grad_up.astype(low)], axis=1)
    gmid, gf, out_own, gain_two_grad = turn_step(
        dot_right(grad_both, gate_up, low), down_part, cf, middle, gain_two
    )
    down_grad = lax.psum_scatter(
        dot_left(hidden, cot_all, low), "uly", scatter_dimension=0, tiled=True
    )
    both_grad = dot_left(normed_two, grad_both, low).reshape(8, 4, -1, 2 * hidden_width)
    both_grad = lax.psum_scatter(both_grad, "uly", scatter_dimension=1, tiled=False)
    grad_mid = gf.reshape(tokens, width)
    out_grad = lax.psum_scatter(
        dot_left(attended_low, grad_mid, low), "uly", scatter_dimension=0, tiled=True
    )
    grad_att = dot_right(grad_mid, out_full, low).reshape(tokens, groups, head_dim)
    delta = jnp.transpose(jnp.sum(grad_att.astype(jnp.float32) * attended, axis=-1))
    probs = weights / totals[..., None]
    grad_probs = jnp.einsum("qgd,kd->gqk", grad_att, value, preferred_element_type=jnp.float32)
    grad_scores = (probs * (grad_probs - delta[..., None])).astype(low)
    grad_query = (
        jnp.einsum("gqk,kd->qgd", grad_scores, key, preferred_element_type=jnp.float32) * scale
    )
    grad_key = (
        jnp.einsum("gqk,qgd->kd", grad_scores, query, preferred_element_type=jnp.float32) * scale
    )
    grad_value = jnp.einsum(
        "gqk,qgd->kd", probs.astype(low), grad_att, preferred_element_type=jnp.float32
    )
    grad_query_pre, grad_key_pre, heads_grad = prep_pull(
        (
            grad_query.astype(low).astype(jnp.float32)[None],
            grad_key.astype(low).astype(jnp.float32)[None, :, None],
        )
    )
    grad_pre = jnp.concatenate(
        [
            grad_query_pre.astype(low).reshape(tokens, groups * head_dim),
            grad_key_pre.astype(low).reshape(tokens, head_dim),
            grad_value.astype(low),
        ],
        axis=1,
    )
    dw = dot_left(normed, grad_pre, low).reshape(8, 4, -1, grad_pre.shape[1])
    small = jnp.concatenate(
        [gain_two_grad.reshape(8, 128), heads_grad, jnp.zeros((6, 128), jnp.float32)], axis=0
    )
    per_device = (inputs.shape, query_weight.shape[1], key_matrix.shape[1], gate_weight.shape[1])
    outputs, grad_inputs, q_grad, k_grad, v_grad, g_grad, u_grad, sums = last_step(
        dot_right(grad_pre, w_qkv, low), xs, gmid, out_own, gain_one, small, dw, both_grad, per_device
    )
    floats = lambda v: v.astype(jnp.float32)
    attn_gain_grad = lax.dynamic_slice(sums, (head, z * piece), (1, piece))[0]
    ffn_gain_grad = lax.dynamic_slice(sums, (8 + head, z * piece), (1, piece))[0]
    share = head_dim // 32
    head_gain_grad = lax.dynamic_slice(sums, (16, (4 * head + z) * share), (2, share))
    return (
        outputs, grad_inputs, attn_gain_grad, head_gain_grad, floats(q_grad), floats(k_grad),
        floats(v_grad), floats(out_grad), ffn_gain_grad, floats(g_grad), floats(u_grad),
        floats(down_grad),
    )


def fits_plane(mesh, seq_count, heads):
    shape = mesh.shape
    return (shape["fsdp"], shape["blk"], shape["uly"]) == (2, 4, 4) and seq_count == 4 and heads == 8


def solution(mesh):
    def step(*arrays):
        seq_count = arrays[0].shape[0]
        heads = arrays[5].shape[1] // arrays[3].shape[1]
        chosen = plane_body if fits_plane(mesh, seq_count, heads) else body
        return mapped(chosen)(*arrays)

    mapped = functools.partial(
        jax.shard_map,
        mesh=mesh,
        in_specs=(
            P("fsdp", ("blk", "uly"), None),
            P("fsdp", None),
            P(("fsdp", "blk", "uly")),
            P(),
            P(("fsdp", "blk", "uly"), None),
            P(("fsdp", "blk", "uly"), None),
            P(("fsdp", "blk", "uly"), None),
            P(("fsdp", "blk", "uly"), None),
            P(("fsdp", "blk", "uly")),
            P(("fsdp", "blk", "uly"), None),
            P(("fsdp", "blk", "uly"), None),
            P(("fsdp", "blk", "uly"), None),
            P("fsdp", ("blk", "uly"), None),
        ),
        out_specs=(
            P("fsdp", ("blk", "uly"), None),
            P("fsdp", ("blk", "uly"), None),
            P(("fsdp", "blk", "uly")),
            P(None, ("fsdp", "blk", "uly")),
            P(("fsdp", "blk", "uly"), None),
            P(("fsdp", "blk", "uly"), None),
            P(("fsdp", "blk", "uly"), None),
            P(("fsdp", "blk", "uly"), None),
            P(("fsdp", "blk", "uly")),
            P(("fsdp", "blk", "uly"), None),
            P(("fsdp", "blk", "uly"), None),
            P(("fsdp", "blk", "uly"), None),
        ),
        check_vma=False,
    )
    return step
```

```python
import functools
import math

import jax
import jax.numpy as jnp
from jax import lax
from jax.experimental import pallas as pl
from jax.experimental.pallas import tpu as pltpu
from jax.sharding import PartitionSpec as P

DOCS = 4


EPSILON = 1e-06
THETA = 1000000.0


def passed_along(value, axis, steps):
    count = lax.axis_size(axis)
    first, last = (max(0, -steps), min(count, count - steps))
    return lax.ppermute(value, axis, [(source, source + steps) for source in range(first, last)])


def from_behind(value, axis, steps):
    count = lax.axis_size(axis)
    pairs = [(source, (source + steps) % count) for source in range(count)]
    return lax.ppermute(value, axis, pairs)


def rms_norm(vector, weight):
    mean_square = jnp.mean(vector * vector, axis=-1, keepdims=True)
    return vector * lax.rsqrt(mean_square + EPSILON) * weight


def rotate(vector, cosine, sine_table):
    half_width = vector.shape[-1] // 2
    turned = jnp.concatenate([-vector[..., half_width:], vector[..., :half_width]], axis=-1)
    return vector * cosine + turned * sine_table


def prepare(query_pre, key_before_rotate, gains, cosine, sine_table):
    cos_heads = cosine[:, :, None, :]
    sin_heads = sine_table[:, :, None, :]
    query_rot = rotate(rms_norm(query_pre, gains[0]), cos_heads, sin_heads)
    key_rot = rotate(rms_norm(key_before_rotate, gains[1]), cos_heads, sin_heads)
    return (query_rot, key_rot)


def swiglu(gate_rows, up_rows):
    return jax.nn.silu(gate_rows) * up_rows


def fetch_attention(attn_gain, query_weight, key_matrix, value_matrix, out_weight):
    return (
        lax.all_gather(attn_gain, ("fsdp", "blk", "uly"), axis=0, tiled=True),
        lax.all_gather(query_weight, ("fsdp", "blk", "uly"), axis=0, tiled=True),
        lax.all_gather(key_matrix, ("fsdp", "blk", "uly"), axis=0, tiled=True),
        lax.all_gather(value_matrix, ("fsdp", "blk", "uly"), axis=0, tiled=True),
        lax.all_gather(out_weight, ("fsdp", "blk", "uly"), axis=0, tiled=True),
    )


def fetch_feedforward(ffn_gain, gate_weight, up_weight, down_weight):
    return (
        lax.all_gather(ffn_gain, ("fsdp", "blk", "uly"), axis=0, tiled=True),
        lax.all_gather(gate_weight, ("fsdp", "blk", "uly"), axis=0, tiled=True),
        lax.all_gather(up_weight, ("fsdp", "blk", "uly"), axis=0, tiled=True),
        lax.all_gather(down_weight, ("fsdp", "blk", "uly"), axis=0, tiled=True),
    )


def body(
    inputs,
    segments,
    attn_gain,
    head_gains,
    query_weight,
    key_matrix,
    value_matrix,
    out_weight,
    ffn_gain,
    gate_weight,
    up_weight,
    down_weight,
    cotangent,
):
    seq_count, tok_count, model_width = inputs.shape
    head_dim = head_gains.shape[1]
    query_heads = query_weight.shape[1] // head_dim
    value_heads = key_matrix.shape[1] // head_dim
    heads_per_group = query_heads // value_heads
    uly_size = lax.axis_size("uly")
    blk_size = lax.axis_size("blk")
    blk_index = lax.axis_index("blk")
    uly_index = lax.axis_index("uly")
    offset = (blk_index * uly_size + uly_index) * tok_count
    doc_ids = jnp.arange(DOCS, dtype=jnp.int32)
    starts = jnp.sum((segments[:, None, :] < doc_ids[None, :, None]).astype(jnp.int32), axis=2)
    local_segs = lax.dynamic_slice_in_dim(segments, offset, tok_count, 1)
    doc_start = jnp.sum(
        jnp.where(local_segs[:, :, None] == doc_ids[None, None, :], starts[:, None, :], 0), axis=2
    )
    token_place = (offset + jnp.arange(tok_count, dtype=jnp.int32)[None, :] - doc_start).astype(
        jnp.float32
    )
    inverse = jnp.exp(
        jnp.arange(head_dim // 2, dtype=jnp.float32) * (-2.0 * math.log(THETA) / head_dim)
    )
    angles = token_place[..., None] * inverse
    cosine = jnp.concatenate([jnp.cos(angles), jnp.cos(angles)], axis=-1)
    sine_table = jnp.concatenate([jnp.sin(angles), jnp.sin(angles)], axis=-1)
    floats = inputs.astype(jnp.float32)
    gain_one, query_full, key_full, value_full, out_full = fetch_attention(
        attn_gain, query_weight, key_matrix, value_matrix, out_weight
    )
    normed_float, norm_pull_one = jax.vjp(rms_norm, floats, gain_one.astype(jnp.float32))
    normalized_input = normed_float.astype(jnp.bfloat16)
    query_pre = jnp.einsum(
        "std,de->ste", normalized_input, query_full, preferred_element_type=jnp.float32
    ).reshape(seq_count, tok_count, query_heads, head_dim)
    key_before_rotate = jnp.einsum(
        "std,de->ste", normalized_input, key_full, preferred_element_type=jnp.float32
    ).reshape(seq_count, tok_count, value_heads, head_dim)
    rows_of_value = (
        jnp.einsum("std,de->ste", normalized_input, value_full, preferred_element_type=jnp.float32)
        .astype(jnp.bfloat16)
        .reshape(seq_count, tok_count, value_heads, head_dim)
    )
    head_float = head_gains.astype(jnp.float32)

    def prepare_local(query_arg, key_arg, gains_arg):
        return prepare(query_arg, key_arg, gains_arg, cosine, sine_table)

    (query_rot, key_rot), prep_pull = jax.vjp(
        prepare_local, query_pre, key_before_rotate, head_float
    )
    query_local, key_local, value_local = (
        lax.all_to_all(
            query_rot.astype(jnp.bfloat16), "uly", split_axis=2, concat_axis=1, tiled=True
        ),
        lax.all_to_all(
            key_rot.astype(jnp.bfloat16), "uly", split_axis=2, concat_axis=1, tiled=True
        ),
        lax.all_to_all(rows_of_value, "uly", split_axis=2, concat_axis=1, tiled=True),
    )
    block_len = query_local.shape[1]
    local_kv = key_local.shape[2]
    query_group = query_local.reshape(seq_count, block_len, local_kv, heads_per_group, head_dim)
    bound = math.sqrt(head_dim) * jnp.max(jnp.abs(head_float[0])) * jnp.max(jnp.abs(head_float[1]))
    scale = head_dim ** (-0.5)
    query_index = blk_index * block_len + jnp.arange(block_len, dtype=jnp.int32)
    query_segs = lax.dynamic_slice_in_dim(segments, blk_index * block_len, block_len, 1)

    def block_weights(keys_in, source):
        key_index = source * block_len + jnp.arange(block_len, dtype=jnp.int32)
        key_segs = lax.dynamic_slice_in_dim(segments, source * block_len, block_len, 1)
        allowed = (key_index[None, None, :] <= query_index[None, :, None]) & (
            key_segs[:, None, :] == query_segs[:, :, None]
        )
        scores = (
            jnp.einsum(
                "sqhgd,skhd->shgqk", query_group, keys_in, preferred_element_type=jnp.float32
            )
            * scale
        )
        return jnp.where(allowed[:, None, None], jnp.exp(scores - bound), 0.0)

    def absorb(stats, key_value, source):
        row_sums, summed = stats
        weights = block_weights(key_value[0], source)
        row_sums = row_sums + jnp.sum(weights, axis=-1)
        summed = summed + jnp.einsum(
            "shgqk,skhd->sqhgd",
            weights.astype(jnp.bfloat16),
            key_value[1],
            preferred_element_type=jnp.float32,
        )
        return (row_sums, summed)

    own_pair = jnp.stack([key_local, value_local])
    start_stats = (
        jnp.zeros((seq_count, local_kv, heads_per_group, block_len), jnp.float32),
        jnp.zeros((seq_count, block_len, local_kv, heads_per_group, head_dim), jnp.float32),
    )
    first_stats = absorb(start_stats, own_pair, blk_index)

    def forward_turn(turn_index, carry):
        key_value, stats_in = carry
        key_value = passed_along(key_value, "blk", 1)
        stats_in = lax.cond(
            turn_index <= blk_index,
            lambda holding: absorb(holding, key_value, blk_index - turn_index),
            lambda holding: holding,
            stats_in,
        )
        return (key_value, stats_in)

    moved_pair, (row_totals, summed_all) = lax.fori_loop(
        1, blk_size, forward_turn, (own_pair, first_stats)
    )
    attended = summed_all / jnp.transpose(row_totals, (0, 3, 1, 2))[..., None]
    attended_tok = lax.all_to_all(
        attended.reshape(seq_count, block_len, local_kv * heads_per_group, head_dim).astype(
            jnp.bfloat16
        ),
        "uly",
        split_axis=1,
        concat_axis=2,
        tiled=True,
    ).reshape(seq_count, tok_count, query_heads * head_dim)
    middle = floats + jnp.einsum(
        "ste,ed->std", attended_tok, out_full, preferred_element_type=jnp.float32
    )
    gain_two, gate_full, up_full, down_full = fetch_feedforward(
        ffn_gain, gate_weight, up_weight, down_weight
    )
    normed_two_float, norm_pull_two = jax.vjp(rms_norm, middle, gain_two.astype(jnp.float32))
    normed_two = normed_two_float.astype(jnp.bfloat16)
    gate_rows = jnp.einsum("std,df->stf", normed_two, gate_full, preferred_element_type=jnp.float32)
    up_rows = jnp.einsum("std,df->stf", normed_two, up_full, preferred_element_type=jnp.float32)
    hidden_float, swiglu_pull = jax.vjp(swiglu, gate_rows, up_rows)
    hidden = hidden_float.astype(jnp.bfloat16)
    outputs = (
        middle + jnp.einsum("stf,fd->std", hidden, down_full, preferred_element_type=jnp.float32)
    ).astype(jnp.bfloat16)
    refetched = fetch_feedforward(ffn_gain, gate_weight, up_weight, down_weight)
    gate_back, up_back, down_back = (refetched[1], refetched[2], refetched[3])
    grad_out = cotangent.astype(jnp.float32)
    down_grad = jnp.einsum("stf,std->fd", hidden, cotangent, preferred_element_type=jnp.float32)
    grad_hidden = jnp.einsum(
        "std,fd->stf", cotangent, down_back, preferred_element_type=jnp.float32
    )
    grad_gate, grad_up = swiglu_pull(grad_hidden)
    grad_gate = grad_gate.astype(jnp.bfloat16)
    grad_up = grad_up.astype(jnp.bfloat16)
    gate_grad = jnp.einsum("std,stf->df", normed_two, grad_gate, preferred_element_type=jnp.float32)
    up_grad = jnp.einsum("std,stf->df", normed_two, grad_up, preferred_element_type=jnp.float32)
    grad_normed_two = jnp.einsum(
        "stf,df->std", grad_gate, gate_back, preferred_element_type=jnp.float32
    ) + jnp.einsum("stf,df->std", grad_up, up_back, preferred_element_type=jnp.float32)
    middle_part, gain_two_grad = norm_pull_two(grad_normed_two)
    grad_middle = grad_out + middle_part
    ffn_shares = (
        lax.psum_scatter(gain_two_grad, ("fsdp", "blk", "uly"), scatter_dimension=0, tiled=True),
        lax.psum_scatter(gate_grad, ("fsdp", "blk", "uly"), scatter_dimension=0, tiled=True),
        lax.psum_scatter(up_grad, ("fsdp", "blk", "uly"), scatter_dimension=0, tiled=True),
        lax.psum_scatter(down_grad, ("fsdp", "blk", "uly"), scatter_dimension=0, tiled=True),
    )
    fetched_again = fetch_attention(attn_gain, query_weight, key_matrix, value_matrix, out_weight)
    query_back, key_back, value_back, out_back = (
        fetched_again[1],
        fetched_again[2],
        fetched_again[3],
        fetched_again[4],
    )
    grad_middle_low = grad_middle.astype(jnp.bfloat16)
    out_grad = jnp.einsum(
        "ste,std->ed", attended_tok, grad_middle_low, preferred_element_type=jnp.float32
    )
    grad_att_tok = (
        jnp.einsum("std,ed->ste", grad_middle_low, out_back, preferred_element_type=jnp.float32)
        .astype(jnp.bfloat16)
        .reshape(seq_count, tok_count, query_heads, head_dim)
    )
    grad_att = lax.all_to_all(grad_att_tok, "uly", split_axis=2, concat_axis=1, tiled=True).reshape(
        seq_count, block_len, local_kv, heads_per_group, head_dim
    )
    delta = jnp.transpose(jnp.sum(grad_att.astype(jnp.float32) * attended, axis=-1), (0, 2, 3, 1))

    def block_grads(key_value, source):
        keys_in = key_value[0]
        values_in = key_value[1]
        probs = block_weights(keys_in, source) / row_totals[..., None]
        grad_probs = jnp.einsum(
            "sqhgd,skhd->shgqk", grad_att, values_in, preferred_element_type=jnp.float32
        )
        grad_scores = (probs * (grad_probs - delta[..., None])).astype(jnp.bfloat16)
        grad_query = (
            jnp.einsum(
                "shgqk,skhd->sqhgd", grad_scores, keys_in, preferred_element_type=jnp.float32
            )
            * scale
        )
        grad_keys = (
            jnp.einsum(
                "shgqk,sqhgd->skhd", grad_scores, query_group, preferred_element_type=jnp.float32
            )
            * scale
        )
        grad_values = jnp.einsum(
            "shgqk,sqhgd->skhd",
            probs.astype(jnp.bfloat16),
            grad_att,
            preferred_element_type=jnp.float32,
        )
        return (grad_query, jnp.stack([grad_keys, grad_values]))

    def pass_grads(moving):
        return from_behind(moving.astype(jnp.bfloat16), "blk", 1).astype(moving.dtype)

    query_start, pair_start = block_grads(own_pair, blk_index)

    def backward_turn(turn_index, carry):
        key_value, query_acc, pair_acc = carry
        key_value = passed_along(key_value, "blk", 1)
        pair_acc = pass_grads(pair_acc)

        def accumulate(holding):
            part_query, part_pair = block_grads(key_value, blk_index - turn_index)
            return (holding[0] + part_query, holding[1] + part_pair)

        query_acc, pair_acc = lax.cond(
            turn_index <= blk_index, accumulate, lambda holding: holding, (query_acc, pair_acc)
        )
        return (key_value, query_acc, pair_acc)

    spent_pair, query_total, pair_total = lax.fori_loop(
        1, blk_size, backward_turn, (own_pair, query_start, pair_start)
    )
    pair_total = pass_grads(pair_total)
    grad_query_low = query_total.reshape(
        seq_count, block_len, local_kv * heads_per_group, head_dim
    ).astype(jnp.bfloat16)
    grad_query_tok, grad_key_tok, grad_value_tok = (
        lax.all_to_all(grad_query_low, "uly", split_axis=1, concat_axis=2, tiled=True),
        lax.all_to_all(
            pair_total[0].astype(jnp.bfloat16), "uly", split_axis=1, concat_axis=2, tiled=True
        ),
        lax.all_to_all(
            pair_total[1].astype(jnp.bfloat16), "uly", split_axis=1, concat_axis=2, tiled=True
        ),
    )
    grad_query_pre, grad_key_pre, heads_grad = prep_pull(
        (grad_query_tok.astype(jnp.float32), grad_key_tok.astype(jnp.float32))
    )
    grad_query_flat = grad_query_pre.astype(jnp.bfloat16).reshape(
        seq_count, tok_count, query_heads * head_dim
    )
    grad_key_flat = grad_key_pre.astype(jnp.bfloat16).reshape(
        seq_count, tok_count, value_heads * head_dim
    )
    grad_value_flat = grad_value_tok.reshape(seq_count, tok_count, value_heads * head_dim)
    query_grad = jnp.einsum(
        "std,ste->de", normalized_input, grad_query_flat, preferred_element_type=jnp.float32
    )
    key_grad = jnp.einsum(
        "std,ste->de", normalized_input, grad_key_flat, preferred_element_type=jnp.float32
    )
    value_grad = jnp.einsum(
        "std,ste->de", normalized_input, grad_value_flat, preferred_element_type=jnp.float32
    )
    grad_normed = jnp.einsum(
        "ste,de->std", grad_query_flat, query_back, preferred_element_type=jnp.float32
    )
    grad_normed = grad_normed + jnp.einsum(
        "ste,de->std", grad_key_flat, key_back, preferred_element_type=jnp.float32
    )
    grad_normed = grad_normed + jnp.einsum(
        "ste,de->std", grad_value_flat, value_back, preferred_element_type=jnp.float32
    )
    input_part, gain_one_grad = norm_pull_one(grad_normed)
    input_grad = (grad_middle + input_part).astype(jnp.bfloat16)
    attn_shares = (
        lax.psum_scatter(gain_one_grad, ("fsdp", "blk", "uly"), scatter_dimension=0, tiled=True),
        lax.psum_scatter(heads_grad, ("fsdp", "blk", "uly"), scatter_dimension=1, tiled=True),
        lax.psum_scatter(query_grad, ("fsdp", "blk", "uly"), scatter_dimension=0, tiled=True),
        lax.psum_scatter(key_grad, ("fsdp", "blk", "uly"), scatter_dimension=0, tiled=True),
        lax.psum_scatter(value_grad, ("fsdp", "blk", "uly"), scatter_dimension=0, tiled=True),
        lax.psum_scatter(out_grad, ("fsdp", "blk", "uly"), scatter_dimension=0, tiled=True),
    )
    return (
        outputs,
        input_grad,
        attn_shares[0],
        attn_shares[1],
        attn_shares[2],
        attn_shares[3],
        attn_shares[4],
        attn_shares[5],
        ffn_shares[0],
        ffn_shares[1],
        ffn_shares[2],
        ffn_shares[3],
    )


MESH = pl.DeviceIdType.MESH
ANY = pl.BlockSpec(memory_space=pl.ANY)
VMEM = pl.BlockSpec(memory_space=pltpu.VMEM)
PLANE = [(dx, dy, dc) for dx in (0, 1) for dy in (0, 1) for dc in (0, 1)]
FAR = [(1, 1, 0), (1, 0, 0), (0, 1, 0)]
TURNS = (1, 2, 3)
SEM = pltpu.SemaphoreType.DMA


class Place:
    def __init__(self):
        self.x = lax.axis_index("fsdp")
        self.block = lax.axis_index("blk")
        self.z = lax.axis_index("uly")
        self.y, self.c = (self.block // 2, self.block % 2)
        self.head = 4 * self.x + self.block
        self.here = (self.x, self.block, self.z)

    def coords(self, dx, dy, dc):
        return ((self.x + dx) % 2, (self.y + dy) % 2, (self.c + dc) % 2)

    def peer(self, dx, dy, dc):
        x, y, c = self.coords(dx, dy, dc)
        return (x, 2 * y + c, self.z)

    def index(self, dx, dy, dc):
        x, y, c = self.coords(dx, dy, dc)
        return 4 * x + 2 * y + c

    def shard(self, ref, dx=0, dy=0, dc=0):
        x, y, c = self.coords(dx, dy, dc)
        return ref.at[2 * y + c, :, x]

    def behind(self, turn):
        return (self.z + 4 - turn) % 4

    def ahead(self, turn):
        return (self.z + turn) % 4

    def line(self, turn):
        return (self.x, self.block, self.ahead(turn))


def remote(src, dst, send_sem, recv_sem, device):
    return pltpu.make_async_remote_copy(
        src_ref=src,
        dst_ref=dst,
        send_sem=send_sem,
        recv_sem=recv_sem,
        device_id=device,
        device_id_type=MESH,
    )


def arrived(ref, sem):
    pltpu.make_async_copy(ref, ref, sem).wait()


def meet(peers):
    barrier = pltpu.get_barrier_semaphore()
    for peer in peers:
        pl.semaphore_signal(barrier, inc=1, device_id=peer, device_id_type=MESH)
    pl.semaphore_wait(barrier, len(peers))


class Sends:
    def __init__(self):
        self.pending = []

    def go(self, *args):
        copy = remote(*args)
        copy.start()
        self.pending.append((None, copy))

    def go_if(self, condition, *args):
        copy = remote(*args)
        pl.when(condition)(lambda: copy.start())
        self.pending.append((condition, copy))

    def drain(self):
        for condition, copy in self.pending:
            if condition is None:
                copy.wait_send()
            else:
                pl.when(condition)(lambda copy=copy: copy.wait_send())


def spread_start(me, sends, src, full, send_sems, recv_sems):
    for i, d in enumerate(FAR + [(0, 0, 1)]):
        sends.go(src, me.shard(full), send_sems.at[i], recv_sems.at[i], me.peer(*d))


def spread_forward(me, sends, full, send_sems, recv_sems):
    for i in (1, 2, 0):
        part = me.shard(full, *FAR[i])
        arrived(part, recv_sems.at[i])
        sends.go(part, part, send_sems.at[4 + i], recv_sems.at[4 + i], me.peer(0, 0, 1))


def spread_finish(me, full, recv_sems):
    for i, (dx, dy, _) in enumerate([(0, 0, 0)] + FAR):
        arrived(me.shard(full, dx, dy, 1), recv_sems.at[3 + i])


def full_shape(tokens, width):
    return (4, 4, 2, tokens // 32, width)


def line_spread(me, sends, src, part, sems):
    for dz in (1, 2):
        sends.go_if(me.z < 4 - dz, src, part(me.z), sems.at[0, dz - 1], sems.at[1, dz - 1], me.line(dz))
        sends.go_if(me.z >= dz, src, part(me.z), sems.at[0, dz + 1], sems.at[1, dz + 1], me.line(4 - dz))


def line_forward(me, sends, part, sems):
    inner = jnp.logical_or(me.z == 1, me.z == 2)
    ref = part((me.z + 2) % 4)
    pl.when(me.z == 1)(lambda: arrived(ref, sems.at[1, 3]))
    pl.when(me.z == 2)(lambda: arrived(ref, sems.at[1, 1]))
    target = (me.x, me.block, (3 * me.z + 1) % 4)
    sends.go_if(inner, ref, ref, sems.at[0, 4], sems.at[1, 4], target)


def line_finish(me, part, sems):
    z = me.z
    pl.when(z > 0)(lambda: arrived(part((z + 3) % 4), sems.at[1, 0]))
    pl.when(z < 3)(lambda: arrived(part((z + 1) % 4), sems.at[1, 2]))

    @pl.when(z == 3)
    def _():
        arrived(part((z + 2) % 4), sems.at[1, 1])
        arrived(part((z + 1) % 4), sems.at[1, 4])

    @pl.when(z == 0)
    def _():
        arrived(part((z + 2) % 4), sems.at[1, 3])
        arrived(part((z + 3) % 4), sems.at[1, 4])


def line_to(me, z):
    return (me.x, me.block, z)


def outer_inner(me):
    outer = jnp.logical_or(me.z == 0, me.z == 3)
    return (outer, jnp.logical_not(outer))


def reduce_start(me, sends, own, came, sems):
    z = me.z
    outer, _ = outer_inner(me)
    sends.go_if(z < 3, own((z + 1) % 4), came.at[0], sems.at[0, 0], sems.at[1, 0], me.line(1))
    sends.go_if(z > 0, own((z + 3) % 4), came.at[1], sems.at[0, 1], sems.at[1, 1], me.line(3))
    nearer = line_to(me, 1 + z // 3)
    sends.go_if(outer, own((7 - z) % 4), came.at[3], sems.at[0, 3], sems.at[1, 3], nearer)
    far = (z + 2) % 4
    sends.go_if(outer, own(far), came.at[2], sems.at[0, 2], sems.at[1, 2], line_to(me, far))


def reduce_join(me, sends, own, came, buf, sems):
    _, inner = outer_inner(me)
    far = (me.z + 2) % 4

    @pl.when(inner)
    def _():
        arrived(came.at[3], sems.at[1, 3])
        buf[...] = (own(far)[...].astype(jnp.float32) + came[3].astype(jnp.float32)).astype(buf.dtype)

    sends.go_if(inner, buf, came.at[2], sems.at[0, 2], sems.at[1, 2], line_to(me, far))


def reduce_total(me, own, came, total, sems):
    arrived(came.at[2], sems.at[1, 2])
    total[...] = own(me.z)[...].astype(jnp.float32) + came[2].astype(jnp.float32)

    @pl.when(me.z > 0)
    def _():
        arrived(came.at[0], sems.at[1, 0])
        total[...] = total[...] + came[0].astype(jnp.float32)

    @pl.when(me.z < 3)
    def _():
        arrived(came.at[1], sems.at[1, 1])
        total[...] = total[...] + came[1].astype(jnp.float32)


def lanes(shape):
    return lax.broadcasted_iota(jnp.int32, shape, len(shape) - 1)


def turned(vector):
    half = vector.shape[-1] // 2
    sign = jnp.where(lanes((1, 2 * half)) < half, -1.0, 1.0)
    return pltpu.roll(vector, half, 1) * sign


def head_scale(vector):
    return lax.rsqrt(jnp.mean(vector * vector, axis=-1, keepdims=True) + EPSILON)


def mat(a, b):
    return jnp.dot(a, b, preferred_element_type=jnp.float32)


def mat_right(a, b):
    return lax.dot_general(a, b, (((1,), (1,)), ((), ())), preferred_element_type=jnp.float32)


def mat_left(a, b):
    return lax.dot_general(a, b, (((0,), (0,)), ((), ())), preferred_element_type=jnp.float32)


def permute_in(me, src_ref, full_ref, send_sems, recv_sems, wait=False):
    half = src_ref.shape[1] // 2
    for j in (0, 1):
        for to in (0, 1):
            src = src_ref.at[j, pl.ds(half * to, half)]
            dst = full_ref.at[me.block, me.z, to]
            mine = jnp.logical_and(me.x == to, me.z == 2 * me.x + j)
            copy = remote(
                src, dst, send_sems.at[2 * j + to], recv_sems.at[me.z], (to, me.block, 2 * me.x + j)
            )
            if wait:
                pl.when(jnp.logical_not(mine))(lambda copy=copy: copy.wait_send())
                continue
            pl.when(jnp.logical_not(mine))(lambda copy=copy: copy.start())
            own = pltpu.make_async_copy(src, dst, recv_sems.at[me.z])
            pl.when(mine)(lambda own=own: own.start())


def permuted_in(me, full_ref, recv_sems):
    for k in range(4):
        arrived(full_ref.at[me.block, k, me.x], recv_sems.at[k])


def half_block(me, part, sibling, send_sems, recv_sems, b, sends=None):
    other = me.c != b % 2
    dy = (me.y + b // 2) % 2
    for to in (0, 1):
        slot = 3 - 2 * ((me.x + to) % 2) - dy
        copy = remote(
            part.at[b, :, to], sibling.at[slot], send_sems.at[slot], recv_sems.at[slot],
            me.peer(0, 0, 1),
        )
        if sends is None:
            pl.when(other)(lambda copy=copy: copy.start())
        else:
            sends.pending.append((other, copy))


def half_out(me, sends, part, sibling, out, came, send_sems, recv_sems):
    for i, d in enumerate(FAR):
        x, y, c = me.coords(*d)
        arrived(sibling.at[i], recv_sems.at[i])
        own = part[2 * y + c, :, x].astype(jnp.float32)
        out[i] = (own + sibling[i].astype(jnp.float32)).astype(jnp.bfloat16)
        sends.go(out.at[i], came.at[i], send_sems.at[4 + i], recv_sems.at[4 + i], me.peer(*d))


def half_in(me, part, sibling, came, recv_sems):
    arrived(sibling.at[3], recv_sems.at[3])
    total = part[me.block, :, me.x].astype(jnp.float32) + sibling[3].astype(jnp.float32)
    for i in (1, 2, 0):
        arrived(came.at[i], recv_sems.at[4 + i])
        total = total + came[i].astype(jnp.float32)
    return total


def half_scratch(tokens, width):
    piece = (4, tokens // 32, width)
    return [
        pltpu.VMEM((4,) + piece, jnp.bfloat16),
        pltpu.VMEM((3,) + piece, jnp.bfloat16),
        pltpu.VMEM((3,) + piece, jnp.bfloat16),
        SEM((7,)),
        SEM((7,)),
    ]


def gain_row(gains_ref, kind):
    rows = [jnp.sum(gains_ref[p, :, kind, :], axis=0, keepdims=True) for p in range(8)]
    return jnp.concatenate(rows, axis=1)


def allowed_keys(segcol, segrow, b, kb):
    same = segcol[b] == segrow[:, 256 * kb : 256 * kb + 256]
    if kb < b:
        return same
    rows = lax.broadcasted_iota(jnp.int32, (256, 256), 0)
    return jnp.logical_and(same, lanes((256, 256)) <= rows)


def norm_back(grad, vector, gain, scale):
    weighted = grad * gain
    inner = jnp.mean(weighted * vector, axis=-1, keepdims=True)
    return scale * weighted - vector * (scale * scale * scale * inner)


def permute_out(me, src_ref, dst_ref, send_sems, recv_sems, wait=False):
    half = dst_ref.shape[1] // 2
    for k in range(4):
        src = src_ref.at[k]
        dst = dst_ref.at[me.z % 2, pl.ds(half * me.x, half)]
        mine = jnp.logical_and(me.x == me.z // 2, me.z == k)
        spot = 2 * (me.z % 2) + me.x
        copy = remote(src, dst, send_sems.at[k], recv_sems.at[spot], (me.z // 2, me.block, k))
        if wait:
            pl.when(jnp.logical_not(mine))(lambda copy=copy: copy.wait_send())
            continue
        pl.when(jnp.logical_not(mine))(lambda copy=copy: copy.start())
        own = pltpu.make_async_copy(src, dst, recv_sems.at[spot])
        pl.when(mine)(lambda own=own: own.start())


def permuted_out(dst_ref, recv_sems):
    half = dst_ref.shape[1] // 2
    for j in (0, 1):
        for to in (0, 1):
            arrived(dst_ref.at[j, pl.ds(half * to, half)], recv_sems.at[2 * j + to])


def total_row(share):
    return jnp.sum(jnp.sum(share, axis=0), axis=0, keepdims=True)


def layer_kernel(
    x_ref, cot_ref, seg_ref, q_ref, k_ref, v_ref, g_ref, u_ref, o_ref, d_ref, gain_ref, hg_ref,
    y_ref, gx_ref, dq_ref, dk_ref, dv_ref, dg_ref, du_ref, sums_ref, osum_ref, dsum_ref,
    xf, cf, wf, of, df, guf, segs, gains, n1, nf, gf, pre, qkv, segcol, cos_s, sin_s, att, attlow,
    totals, part, part2, part3, down, n2, gm, y_s, gi_s, mid, gmid,
    hid, gboth, ga, gq, gk, gv, gpre, dd, dgu, do, dw,
    d_came, d_buf, gu_came, gu_buf, gu_total, gu_sum, o_came, o_buf, w_came, w_buf, w_total, w_sum,
    pack, packs, linep,
    sib1, out1, came1, hs1, hr1, sib2, out2, came2, hs2, hr2, sib3, out3, came3, hs3, hr3,
    sib4, out4, came4, hs4, hr4,
    ps, pr, as_, ar, ws, wr, us, ur, gs, gr, zq, zo, zd, zg, rg, rd, ro, rw, cs, cr, ds, dr, ls,
):
    me = Place()
    x, z, p = (me.x, me.z, me.head)
    low, wide_t = (jnp.bfloat16, jnp.float32)
    across = [((x + 1) % 2, me.block, me.ahead(turn)) for turn in TURNS]
    meet([me.peer(*d) for d in PLANE[1:]] + [me.line(turn) for turn in TURNS] + across)
    sends = Sends()

    def local(src, dst, sem):
        copy = pltpu.make_async_copy(src, dst, sem)
        copy.start()
        return copy

    own_gain = local(gain_ref, gains.at[p, z], ls.at[0])
    own_seg = local(seg_ref, segs.at[x], ls.at[1])
    sends.go(seg_ref, segs.at[x], ls.at[2], ls.at[3], me.peer(1, 0, 0))
    for turn in TURNS:
        sends.go(gain_ref, gains.at[p, z], gs.at[turn], gr.at[turn], me.line(turn))
    permute_in(me, x_ref, xf, ps.at[0], pr.at[0])
    own_o = local(o_ref, of.at[z], ls.at[4])
    own_d = local(d_ref, df.at[z], ls.at[5])
    wide, narrow = (q_ref.shape[1] // 8, k_ref.shape[1] // 8)
    cuts = ((q_ref, wide, 0), (k_ref, narrow, wide), (v_ref, narrow, wide + narrow))
    for i, d in enumerate(PLANE):
        t = me.index(*d)
        for n, (ref, width, off) in enumerate(cuts):
            src = ref.at[:, pl.ds(pl.multiple_of(t * width, 128), width)]
            dst = wf.at[p, z, :, pl.ds(off, width)]
            if i == 0:
                local(src, dst, wr.at[n])
            else:
                sends.go(src, dst, ws.at[3 * i + n], wr.at[3 * i + n], me.peer(*d))
    permuted_in(me, xf, pr.at[0])
    spread_start(me, sends, me.shard(xf), xf, as_.at[0], ar.at[0])
    for i, d in enumerate(PLANE):
        t = me.index(*d)
        for n, (ref, width, off) in enumerate(cuts):
            arrived(wf.at[t, z, :, pl.ds(off, width)], wr.at[3 * i + n])
    qkv_part = lambda k: wf.at[:, k]
    o_part = lambda k: of.at[k]
    d_part = lambda k: df.at[k]
    gu_part = lambda k: guf.at[:, k]
    line_spread(me, sends, qkv_part(z), qkv_part, zq)
    permute_in(me, cot_ref, cf, ps.at[1], pr.at[1])
    line_spread(me, sends, o_ref, o_part, zo)
    ff = g_ref.shape[1] // 8
    for i, d in enumerate(PLANE):
        t = me.index(*d)
        for n, ref in enumerate((g_ref, u_ref)):
            src = ref.at[:, pl.ds(pl.multiple_of(t * ff, 128), ff)]
            dst = guf.at[p, z, :, pl.ds(n * ff, ff)]
            if i == 0:
                local(src, dst, ur.at[n])
            else:
                sends.go(src, dst, us.at[2 * i + n], ur.at[2 * i + n], me.peer(*d))
    own_gain.wait()
    for turn in TURNS:
        arrived(gains.at[p, me.behind(turn)], gr.at[turn])
    for i, d in enumerate(PLANE[1:]):
        sends.go(gains.at[p], gains.at[p], gs.at[4 + i], gr.at[4 + i], me.peer(*d))
    own_seg.wait()
    arrived(segs.at[(x + 1) % 2], ls.at[3])
    head_dim = hg_ref.shape[1]
    segrow = segs[z // 2, pl.ds(z % 2, 1), :]
    tokens = segrow.shape[1]
    column = jnp.transpose(jnp.broadcast_to(segrow.astype(wide_t), (8, tokens)))[:, :1]
    segcol[...] = column.astype(jnp.int32).reshape(4, 256, 1)
    half_lane = (lanes((1, head_dim)) % (head_dim // 2)).astype(wide_t)
    inverse = jnp.exp(half_lane * (-2.0 * math.log(THETA) / head_dim))
    steps = lax.broadcasted_iota(jnp.int32, (32, head_dim), 0).astype(wide_t) * inverse
    cl, sl = (jnp.cos(steps), jnp.sin(steps))
    ch, sh = (jnp.cos(steps * 32.0), jnp.sin(steps * 32.0))
    doc_cos, doc_sin = ([], [])
    for doc in range(DOCS):
        start = jnp.sum((segrow < doc).astype(wide_t), axis=1, keepdims=True)
        doc_cos.append(jnp.cos(start * inverse))
        doc_sin.append(jnp.sin(start * inverse))
    for b in range(4):
        hi_c, hi_s = (ch[8 * b : 8 * b + 8][:, None, :], sh[8 * b : 8 * b + 8][:, None, :])
        cos_at = (hi_c * cl[None] - hi_s * sl[None]).reshape(256, head_dim)
        sin_at = (hi_s * cl[None] + hi_c * sl[None]).reshape(256, head_dim)
        column = segcol[b]
        cd, sd = (jnp.broadcast_to(v[0], (256, head_dim)) for v in (doc_cos, doc_sin))
        for doc in range(1, DOCS):
            cd = jnp.where(column == doc, doc_cos[doc], cd)
            sd = jnp.where(column == doc, doc_sin[doc], sd)
        cos_s[b] = cos_at * cd + sin_at * sd
        sin_s[b] = sin_at * cd - cos_at * sd
    for i, d in enumerate(PLANE[1:]):
        arrived(gains.at[me.index(*d)], gr.at[4 + i])
    gain_one, gain_two = (gain_row(gains, 0), gain_row(gains, 1))
    line_forward(me, sends, qkv_part, zq)
    spread_forward(me, sends, xf, as_.at[0], ar.at[0])
    spread_finish(me, xf, ar.at[0])

    @pl.loop(0, 4)
    def _(b):
        rows = xf[b].reshape(256, -1).astype(wide_t)
        n1[b] = (rows * head_scale(rows) * gain_one).astype(low)

    for i, d in enumerate(PLANE):
        t = me.index(*d)
        for n in (0, 1):
            arrived(guf.at[t, z, :, pl.ds(n * ff, ff)], ur.at[2 * i + n])
    line_spread(me, sends, gu_part(z), gu_part, zg)
    line_spread(me, sends, d_ref, d_part, zd)
    line_finish(me, qkv_part, zq)

    @pl.loop(0, 4)
    def _(b):
        rows = mat(n1[b], wf[...].reshape(-1, wf.shape[3]))
        pre[b] = rows
        cosine, sine = (cos_s[b], sin_s[b])
        for h in range(3):
            v = rows[:, head_dim * h : head_dim * (h + 1)]
            n = v * head_scale(v) * hg_ref[pl.ds(h // 2, 1), :]
            qkv[b, :, pl.ds(head_dim * h, head_dim)] = (n * cosine + turned(n) * sine).astype(low)
        qkv[b, :, pl.ds(3 * head_dim, head_dim)] = rows[:, 3 * head_dim :].astype(low)

    own_o.wait()
    line_forward(me, sends, o_part, zo)
    top = lambda r: jnp.max(jnp.abs(hg_ref[pl.ds(r, 1), :]), axis=1, keepdims=True)
    bound = math.sqrt(head_dim) * top(0) * top(1)
    scale = head_dim ** (-0.5)
    key_at, value_at = (pl.ds(2 * head_dim, head_dim), pl.ds(3 * head_dim, head_dim))

    def weights_of(b, kb, query):
        s = mat_right(query, qkv[kb, :, key_at]) * scale
        return jnp.where(allowed_keys(segcol, segrow, b, kb), jnp.exp(s - bound), 0.0)

    for b in range(4):

        @pl.loop(0, 2)
        def _(h, b=b):
            at = pl.ds(pl.multiple_of(head_dim * h, head_dim), head_dim)
            query = qkv[b, :, at]
            total, mixed = (None, None)
            for kb in range(b + 1):
                w = weights_of(b, kb, query)
                t = jnp.sum(w, axis=1, keepdims=True)
                m = mat(w.astype(low), qkv[kb, :, value_at])
                total = t if kb == 0 else total + t
                mixed = m if kb == 0 else mixed + m
            mixed = mixed / total
            totals[b, h] = total
            att[b, :, at] = mixed
            attlow[b, :, at] = mixed.astype(low)

        if b == 2:
            permuted_in(me, cf, pr.at[1])
            spread_start(me, sends, me.shard(cf), cf, as_.at[1], ar.at[1])
    line_finish(me, o_part, zo)

    @pl.loop(0, 4)
    def _(b):
        rows = mat(attlow[b], of[...].reshape(-1, of.shape[2])).astype(low)
        part[b] = rows.reshape(part.shape[1:])
        half_block(me, part, sib1, hs1, hr1, b)

    for b in range(4):
        half_block(me, part, sib1, hs1, hr1, b, sends)
    half_out(me, sends, part, sib1, out1, came1, hs1, hr1)
    spread_forward(me, sends, cf, as_.at[1], ar.at[1])
    middle = xf[me.block, :, x].astype(wide_t) + half_in(me, part, sib1, came1, hr1)
    mid[...] = middle
    n2[...] = (middle * head_scale(middle) * gain_two).astype(low)
    own_n = local(n2, me.shard(nf), ls.at[6])
    spread_start(me, sends, n2, nf, as_.at[2], ar.at[2])
    line_forward(me, sends, gu_part, zg)
    line_forward(me, sends, d_part, zd)
    spread_forward(me, sends, nf, as_.at[2], ar.at[2])
    spread_finish(me, nf, ar.at[2])
    own_n.wait()
    spread_finish(me, cf, ar.at[1])
    own_d.wait()
    line_finish(me, gu_part, zg)
    line_finish(me, d_part, zd)

    @pl.loop(0, 4)
    def _(b):
        both = mat(nf[b].reshape(256, -1), guf[...].reshape(-1, 2 * ff))
        gate, up = (both[:, :ff], both[:, ff:])
        sig = 1.0 / (1.0 + jnp.exp(-gate))
        silu = gate * sig
        hidden = (silu * up).astype(low)
        hid[b] = hidden
        w_down = df[...].reshape(ff, -1)
        grad = mat_right(cf[b].reshape(256, -1), w_down)
        gboth[b, :, pl.ds(0, ff)] = (grad * up * sig * (1.0 + gate * (1.0 - sig))).astype(low)
        gboth[b, :, pl.ds(ff, ff)] = (grad * silu).astype(low)
        rows = mat_right(gboth[b], guf[...].reshape(-1, 2 * ff)).astype(low)
        part2[b] = rows.reshape(part2.shape[1:])
        half_block(me, part2, sib2, hs2, hr2, b)

    for b in range(4):
        half_block(me, part2, sib2, hs2, hr2, b, sends)
    half_out(me, sends, part2, sib2, out2, came2, hs2, hr2)

    @pl.loop(0, 4)
    def _(b):
        rows = nf[:, :, :, :, pl.ds(pl.multiple_of(256 * b, 256), 256)].reshape(-1, 256)
        grad = mat_left(rows, gboth[...].reshape(-1, 2 * ff)).astype(low)
        dgu[pl.ds(2 * b, 2)] = grad.reshape((2,) + dgu.shape[1:])

    own_gu = lambda k: dgu.at[:, k]
    reduce_start(me, sends, own_gu, gu_came, rg)
    grad = half_in(me, part2, sib2, came2, hr2)
    middle = mid[...]
    r = head_scale(middle)
    total = cf[me.block, :, x].astype(wide_t) + norm_back(grad, middle, gain_two, r)
    gmid[...] = total
    gm[...] = total.astype(low)
    own_gm = local(gm, me.shard(gf), ls.at[7])
    spread_start(me, sends, gm, gf, as_.at[3], ar.at[3])
    share = total_row(grad * middle * r)
    for i in range(8):
        pack[pl.ds(8 + i, 1)] = share[:, 128 * i : 128 * i + 128]

    @pl.loop(0, 4)
    def _(b):
        rows = mat(hid[b], df[...].reshape(ff, -1)).astype(low)
        down[b] = rows.reshape(down.shape[1:])
        half_block(me, down, sib3, hs3, hr3, b)

    for b in range(4):
        half_block(me, down, sib3, hs3, hr3, b, sends)
    dd[...] = mat_left(hid[...].reshape(-1, ff), cf[...].reshape(tokens, -1)).astype(low).reshape(dd.shape)
    own_dd = lambda k: dd.at[k]
    reduce_start(me, sends, own_dd, d_came, rd)
    half_out(me, sends, down, sib3, out3, came3, hs3, hr3)
    reduce_join(me, sends, own_gu, gu_came, gu_buf, rg)
    spread_forward(me, sends, gf, as_.at[3], ar.at[3])
    spread_finish(me, gf, ar.at[3])
    own_gm.wait()

    gk[...] = jnp.zeros_like(gk)
    gv[...] = jnp.zeros_like(gv)
    for b in range(4):
        ga[b] = mat_right(gf[b].reshape(256, -1), of[...].reshape(-1, of.shape[2])).astype(low)

        @pl.loop(0, 2)
        def _(h, b=b):
            at = pl.ds(pl.multiple_of(head_dim * h, head_dim), head_dim)
            query, grad = (qkv[b, :, at], ga[b, :, at])
            delta = jnp.sum(grad.astype(wide_t) * att[b, :, at], axis=1, keepdims=True)
            inv = 1.0 / totals[b, h]
            grad_query = None
            for kb in range(b + 1):
                probs = weights_of(b, kb, query) * inv
                gp = mat_right(grad, qkv[kb, :, value_at])
                gsc = (probs * (gp - delta)).astype(low)
                m = mat(gsc, qkv[kb, :, key_at])
                grad_query = m if kb == 0 else grad_query + m
                gk[kb] += mat_left(gsc, query)
                gv[kb] += mat_left(probs.astype(low), grad)
            gq[b, :, at] = grad_query

        if b == 0:
            reduce_join(me, sends, own_dd, d_came, d_buf, rd)
        if b == 1:
            y_s[...] = (mid[...] + half_in(me, down, sib3, came3, hr3)).astype(low)
            permute_out(me, y_s, y_ref, cs.at[0], cr.at[0])
    do[...] = mat_left(attlow[...].reshape(tokens, -1), gf[...].reshape(tokens, -1)).astype(low).reshape(do.shape)
    own_do = lambda k: do.at[k]
    reduce_start(me, sends, own_do, o_came, ro)
    pack[pl.ds(16, 8)] = jnp.zeros((8, 128), wide_t)

    @pl.loop(0, 4)
    def _(b):
        cosine, sine = (cos_s[b], sin_s[b])
        for h in range(3):
            at = pl.ds(head_dim * h, head_dim)
            source = gq[b, :, at] if h < 2 else gk[b]
            go = (source * scale).astype(low).astype(wide_t)
            gh = go * cosine - turned(go * sine)
            v = pre[b, :, at]
            r = head_scale(v)
            n = v * r
            pack[pl.ds(16 + h // 2, 1)] += jnp.sum(gh * n, axis=0, keepdims=True)
            gn = gh * hg_ref[pl.ds(h // 2, 1), :]
            gpre[b, :, at] = (r * (gn - n * jnp.mean(gn * n, axis=-1, keepdims=True))).astype(low)
        gpre[b, :, value_at] = gv[b].astype(low)
        rows = mat_right(gpre[b], wf[...].reshape(-1, wf.shape[3])).astype(low)
        part3[b] = rows.reshape(part3.shape[1:])
        half_block(me, part3, sib4, hs4, hr4, b)

    for b in range(4):
        half_block(me, part3, sib4, hs4, hr4, b, sends)
    half_out(me, sends, part3, sib4, out4, came4, hs4, hr4)

    @pl.loop(0, 4)
    def _(b):
        rows = n1[:, :, pl.ds(pl.multiple_of(256 * b, 256), 256)].reshape(-1, 256)
        grad = mat_left(rows, gpre[...].reshape(tokens, -1)).astype(low)
        dw[pl.ds(2 * b, 2)] = grad.reshape((2,) + dw.shape[1:])

    own_dw = lambda k: dw.at[:, k]
    reduce_start(me, sends, own_dw, w_came, rw)
    reduce_join(me, sends, own_do, o_came, o_buf, ro)
    reduce_total(me, own_gu, gu_came, gu_total, rg)
    gu_sum[...] = gu_total[...].astype(low)
    for i, d in enumerate(PLANE):
        t = me.index(*d)
        for n, ref in enumerate((dg_ref, du_ref)):
            src = gu_sum.at[t, :, pl.ds(n * ff, ff)]
            dst = ref.at[:, pl.ds(pl.multiple_of(p * ff, 128), ff)]
            if i == 0:
                local(src, dst, dr.at[n])
            else:
                sends.go(src, dst, ds.at[2 * i + n], dr.at[2 * i + n], me.peer(*d))
    reduce_total(me, own_dd, d_came, dsum_ref, rd)
    grad = half_in(me, part3, sib4, came4, hr4)
    rows = xf[me.block, :, x].astype(wide_t)
    r = head_scale(rows)
    gi_s[...] = (gmid[...] + norm_back(grad, rows, gain_one, r)).astype(low)
    permute_out(me, gi_s, gx_ref, cs.at[1], cr.at[1])
    share = total_row(grad * rows * r)
    for i in range(8):
        pack[pl.ds(i, 1)] = share[:, 128 * i : 128 * i + 128]
    for i, d in enumerate(PLANE[1:]):
        sends.go(pack, packs.at[i], gs.at[11 + i], gr.at[11 + i], me.peer(*d))
    reduce_join(me, sends, own_dw, w_came, w_buf, rw)
    reduce_total(me, own_do, o_came, osum_ref, ro)
    total = pack[...]
    for i in range(7):
        arrived(packs.at[i], gr.at[11 + i])
        total = total + packs[i]
    packs[7] = total
    for turn in TURNS:
        sends.go(packs.at[7], linep.at[turn - 1], gs.at[17 + turn], gr.at[17 + turn], me.line(turn))
    reduce_total(me, own_dw, w_came, w_total, rw)
    w_sum[...] = w_total[...].astype(low)
    backs = ((dq_ref, wide, 0), (dk_ref, narrow, wide), (dv_ref, narrow, wide + narrow))
    for i, d in enumerate(PLANE):
        t = me.index(*d)
        for n, (ref, cols, off) in enumerate(backs):
            src = w_sum.at[t, :, pl.ds(off, cols)]
            dst = ref.at[:, pl.ds(pl.multiple_of(p * cols, 128), cols)]
            if i == 0:
                local(src, dst, dr.at[16 + n])
            else:
                s = 16 + 3 * i + n
                sends.go(src, dst, ds.at[s], dr.at[s], me.peer(*d))
    for turn in TURNS:
        arrived(linep.at[turn - 1], gr.at[17 + turn])
    sums_ref[...] = ((total + linep[0]) + linep[1]) + linep[2]
    for i, d in enumerate(PLANE):
        t = me.index(*d)
        for n, ref in enumerate((dg_ref, du_ref)):
            arrived(ref.at[:, pl.ds(pl.multiple_of(t * ff, 128), ff)], dr.at[2 * i + n])
        for n, (ref, cols, off) in enumerate(backs):
            arrived(ref.at[:, pl.ds(pl.multiple_of(t * cols, 128), cols)], dr.at[16 + 3 * i + n])
    permuted_out(y_ref, cr.at[0])
    permuted_out(gx_ref, cr.at[1])
    permute_in(me, x_ref, xf, ps.at[0], pr.at[0], wait=True)
    permute_in(me, cot_ref, cf, ps.at[1], pr.at[1], wait=True)
    permute_out(me, y_s, y_ref, cs.at[0], cr.at[0], wait=True)
    permute_out(me, gi_s, gx_ref, cs.at[1], cr.at[1], wait=True)
    sends.drain()


def layer_step(x, cot, seg, q, k, v, g, u, o, d, gain, head_gains):
    tokens, width = (16 * x.shape[1], x.shape[2])
    rows, low, wide = (q.shape[0], jnp.bfloat16, jnp.float32)
    cols = (q.shape[1] + 2 * k.shape[1]) // 8
    att_cols, head_dim = (q.shape[1] // 8, k.shape[1] // 8)
    ff = g.shape[1] // 8
    full = full_shape(tokens, width)
    piece = (4, tokens // 32, width)
    quarter = tokens // 4
    shape, buf = (jax.ShapeDtypeStruct, pltpu.VMEM)
    blocks = lambda n, kind: buf((4, quarter, n), kind)
    return pl.pallas_call(
        layer_kernel,
        name="layer_step",
        out_shape=(
            shape(x.shape, low), shape(x.shape, low), shape(q.shape, low), shape(k.shape, low),
            shape(v.shape, low), shape(g.shape, low), shape(u.shape, low), shape((24, 128), wide),
            shape(o.shape, wide), shape(d.shape, wide),
        ),
        in_specs=[ANY] * 11 + [VMEM],
        out_specs=(ANY,) * 7 + (VMEM,) * 3,
        scratch_shapes=[
            buf(full, low), buf(full, low), buf((8, 4, rows, cols), low), buf((4,) + o.shape, low),
            buf((4,) + d.shape, low), buf((8, 4, rows, 2 * ff), low), buf((2,) + seg.shape, seg.dtype),
            buf((8, 4, 8, 128), wide), blocks(width, low), buf(full, low), buf(full, low),
            blocks(cols, wide), blocks(cols, low), blocks(1, jnp.int32), blocks(head_dim, wide),
            blocks(head_dim, wide), blocks(att_cols, wide), blocks(att_cols, low),
            buf((4, 2, quarter, 1), wide), buf(full, low), buf(full, low), buf(full, low), buf(full, low),
            buf(piece, low), buf(piece, low), buf(piece, low), buf(piece, low), buf(piece, wide),
            buf(piece, wide),
            blocks(ff, low), blocks(2 * ff, low), blocks(att_cols, low), blocks(att_cols, wide),
            blocks(head_dim, wide), blocks(head_dim, wide), blocks(cols, low),
            buf((4,) + d.shape, low), buf((8, 4, rows, 2 * ff), low), buf((4,) + o.shape, low),
            buf((8, 4, rows, cols), low),
            buf((4,) + d.shape, low), buf(d.shape, low),
            buf((4, 8, rows, 2 * ff), low), buf((8, rows, 2 * ff), low), buf((8, rows, 2 * ff), wide),
            buf((8, rows, 2 * ff), low),
            buf((4,) + o.shape, low), buf(o.shape, low),
            buf((4, 8, rows, cols), low), buf((8, rows, cols), low), buf((8, rows, cols), wide),
            buf((8, rows, cols), low),
            buf((24, 128), wide), buf((8, 24, 128), wide), buf((3, 24, 128), wide),
        ]
        + half_scratch(tokens, width) * 4
        + [SEM((2, 4)), SEM((2, 4)), SEM((4, 7)), SEM((4, 7)), SEM((24,)), SEM((24,)), SEM((16,)), SEM((16,))]
        + [SEM((21,)), SEM((21,))]
        + [SEM((2, 5))] * 4
        + [SEM((2, 4))] * 4
        + [SEM((2, 4)), SEM((2, 4)), SEM((40,)), SEM((40,)), SEM((8,))],
        compiler_params=pltpu.CompilerParams(
            collective_id=0, has_side_effects=True, vmem_limit_bytes=67043328
        ),
    )(x, cot, seg, q, k, v, g, u, o, d, gain, head_gains)


def finish_kernel(*refs):
    half = len(refs) // 2
    for src, dst in zip(refs[:half], refs[half:]):
        dst[...] = src[...].astype(dst.dtype)


def finish_step(*arrays):
    return pl.pallas_call(
        finish_kernel,
        name="finish_step",
        out_shape=tuple(
            jax.ShapeDtypeStruct(v.shape, v.dtype if i < 2 else jnp.float32) for i, v in enumerate(arrays)
        ),
        in_specs=[VMEM] * len(arrays),
        out_specs=(VMEM,) * len(arrays),
    )(*arrays)


def plane_body(
    inputs, segments, attn_gain, head_gains, query_weight, key_matrix, value_matrix, out_weight,
    ffn_gain, gate_weight, up_weight, down_weight, cotangent,
):
    head_dim = head_gains.shape[1]
    z = lax.axis_index("uly")
    head = 4 * lax.axis_index("fsdp") + lax.axis_index("blk")
    piece = attn_gain.shape[0]
    pair = jnp.stack([attn_gain, ffn_gain]).astype(jnp.float32)
    spot = (jnp.arange(128, dtype=jnp.int32) // piece == z)[None]
    gains_own = jnp.where(spot, jnp.tile(pair, (1, 128 // piece)), 0.0)
    gains_own = jnp.concatenate([gains_own, jnp.zeros((6, 128), jnp.float32)], axis=0)
    outputs, grad_inputs, q_grad, k_grad, v_grad, g_grad, u_grad, sums, out_grad, down_grad = layer_step(
        inputs, cotangent, segments, query_weight, key_matrix, value_matrix, gate_weight, up_weight,
        out_weight, down_weight, gains_own, head_gains.astype(jnp.float32),
    )
    attn_gain_grad = lax.dynamic_slice(sums, (head, z * piece), (1, piece))[0]
    ffn_gain_grad = lax.dynamic_slice(sums, (8 + head, z * piece), (1, piece))[0]
    share = head_dim // 32
    head_gain_grad = lax.dynamic_slice(sums, (16, (4 * head + z) * share), (2, share))
    outputs, grad_inputs, q_grad, k_grad, v_grad, out_grad, g_grad, u_grad, down_grad = finish_step(
        outputs, grad_inputs, q_grad, k_grad, v_grad, out_grad, g_grad, u_grad, down_grad
    )
    return (
        outputs, grad_inputs, attn_gain_grad, head_gain_grad, q_grad, k_grad, v_grad, out_grad,
        ffn_gain_grad, g_grad, u_grad, down_grad,
    )


def fits_plane(mesh, seq_count, heads):
    shape = mesh.shape
    return (shape["fsdp"], shape["blk"], shape["uly"]) == (2, 4, 4) and seq_count == 4 and heads == 8


def solution(mesh):
    def step(*arrays):
        seq_count = arrays[0].shape[0]
        heads = arrays[5].shape[1] // arrays[3].shape[1]
        chosen = plane_body if fits_plane(mesh, seq_count, heads) else body
        return mapped(chosen)(*arrays)

    mapped = functools.partial(
        jax.shard_map,
        mesh=mesh,
        in_specs=(
            P("fsdp", ("blk", "uly"), None),
            P("fsdp", None),
            P(("fsdp", "blk", "uly")),
            P(),
            P(("fsdp", "blk", "uly"), None),
            P(("fsdp", "blk", "uly"), None),
            P(("fsdp", "blk", "uly"), None),
            P(("fsdp", "blk", "uly"), None),
            P(("fsdp", "blk", "uly")),
            P(("fsdp", "blk", "uly"), None),
            P(("fsdp", "blk", "uly"), None),
            P(("fsdp", "blk", "uly"), None),
            P("fsdp", ("blk", "uly"), None),
        ),
        out_specs=(
            P("fsdp", ("blk", "uly"), None),
            P("fsdp", ("blk", "uly"), None),
            P(("fsdp", "blk", "uly")),
            P(None, ("fsdp", "blk", "uly")),
            P(("fsdp", "blk", "uly"), None),
            P(("fsdp", "blk", "uly"), None),
            P(("fsdp", "blk", "uly"), None),
            P(("fsdp", "blk", "uly"), None),
            P(("fsdp", "blk", "uly")),
            P(("fsdp", "blk", "uly"), None),
            P(("fsdp", "blk", "uly"), None),
            P(("fsdp", "blk", "uly"), None),
        ),
        check_vma=False,
    )
    return step
```

```python
import functools
import math

import jax
import jax.numpy as jnp
from jax import lax
from jax.experimental import pallas as pl
from jax.experimental.pallas import tpu as pltpu
from jax.sharding import PartitionSpec as P

DOCS = 4


EPSILON = 1e-06
THETA = 1000000.0


def passed_along(value, axis, steps):
    count = lax.axis_size(axis)
    first, last = (max(0, -steps), min(count, count - steps))
    return lax.ppermute(value, axis, [(source, source + steps) for source in range(first, last)])


def from_behind(value, axis, steps):
    count = lax.axis_size(axis)
    pairs = [(source, (source + steps) % count) for source in range(count)]
    return lax.ppermute(value, axis, pairs)


def rms_norm(vector, weight):
    mean_square = jnp.mean(vector * vector, axis=-1, keepdims=True)
    return vector * lax.rsqrt(mean_square + EPSILON) * weight


def rotate(vector, cosine, sine_table):
    half_width = vector.shape[-1] // 2
    turned = jnp.concatenate([-vector[..., half_width:], vector[..., :half_width]], axis=-1)
    return vector * cosine + turned * sine_table


def prepare(query_pre, key_before_rotate, gains, cosine, sine_table):
    cos_heads = cosine[:, :, None, :]
    sin_heads = sine_table[:, :, None, :]
    query_rot = rotate(rms_norm(query_pre, gains[0]), cos_heads, sin_heads)
    key_rot = rotate(rms_norm(key_before_rotate, gains[1]), cos_heads, sin_heads)
    return (query_rot, key_rot)


def swiglu(gate_rows, up_rows):
    return jax.nn.silu(gate_rows) * up_rows


def fetch_attention(attn_gain, query_weight, key_matrix, value_matrix, out_weight):
    return (
        lax.all_gather(attn_gain, ("fsdp", "blk", "uly"), axis=0, tiled=True),
        lax.all_gather(query_weight, ("fsdp", "blk", "uly"), axis=0, tiled=True),
        lax.all_gather(key_matrix, ("fsdp", "blk", "uly"), axis=0, tiled=True),
        lax.all_gather(value_matrix, ("fsdp", "blk", "uly"), axis=0, tiled=True),
        lax.all_gather(out_weight, ("fsdp", "blk", "uly"), axis=0, tiled=True),
    )


def fetch_feedforward(ffn_gain, gate_weight, up_weight, down_weight):
    return (
        lax.all_gather(ffn_gain, ("fsdp", "blk", "uly"), axis=0, tiled=True),
        lax.all_gather(gate_weight, ("fsdp", "blk", "uly"), axis=0, tiled=True),
        lax.all_gather(up_weight, ("fsdp", "blk", "uly"), axis=0, tiled=True),
        lax.all_gather(down_weight, ("fsdp", "blk", "uly"), axis=0, tiled=True),
    )


def body(
    inputs,
    segments,
    attn_gain,
    head_gains,
    query_weight,
    key_matrix,
    value_matrix,
    out_weight,
    ffn_gain,
    gate_weight,
    up_weight,
    down_weight,
    cotangent,
):
    seq_count, tok_count, model_width = inputs.shape
    head_dim = head_gains.shape[1]
    query_heads = query_weight.shape[1] // head_dim
    value_heads = key_matrix.shape[1] // head_dim
    heads_per_group = query_heads // value_heads
    uly_size = lax.axis_size("uly")
    blk_size = lax.axis_size("blk")
    blk_index = lax.axis_index("blk")
    uly_index = lax.axis_index("uly")
    offset = (blk_index * uly_size + uly_index) * tok_count
    doc_ids = jnp.arange(DOCS, dtype=jnp.int32)
    starts = jnp.sum((segments[:, None, :] < doc_ids[None, :, None]).astype(jnp.int32), axis=2)
    local_segs = lax.dynamic_slice_in_dim(segments, offset, tok_count, 1)
    doc_start = jnp.sum(
        jnp.where(local_segs[:, :, None] == doc_ids[None, None, :], starts[:, None, :], 0), axis=2
    )
    token_place = (offset + jnp.arange(tok_count, dtype=jnp.int32)[None, :] - doc_start).astype(
        jnp.float32
    )
    inverse = jnp.exp(
        jnp.arange(head_dim // 2, dtype=jnp.float32) * (-2.0 * math.log(THETA) / head_dim)
    )
    angles = token_place[..., None] * inverse
    cosine = jnp.concatenate([jnp.cos(angles), jnp.cos(angles)], axis=-1)
    sine_table = jnp.concatenate([jnp.sin(angles), jnp.sin(angles)], axis=-1)
    floats = inputs.astype(jnp.float32)
    gain_one, query_full, key_full, value_full, out_full = fetch_attention(
        attn_gain, query_weight, key_matrix, value_matrix, out_weight
    )
    normed_float, norm_pull_one = jax.vjp(rms_norm, floats, gain_one.astype(jnp.float32))
    normalized_input = normed_float.astype(jnp.bfloat16)
    query_pre = jnp.einsum(
        "std,de->ste", normalized_input, query_full, preferred_element_type=jnp.float32
    ).reshape(seq_count, tok_count, query_heads, head_dim)
    key_before_rotate = jnp.einsum(
        "std,de->ste", normalized_input, key_full, preferred_element_type=jnp.float32
    ).reshape(seq_count, tok_count, value_heads, head_dim)
    rows_of_value = (
        jnp.einsum("std,de->ste", normalized_input, value_full, preferred_element_type=jnp.float32)
        .astype(jnp.bfloat16)
        .reshape(seq_count, tok_count, value_heads, head_dim)
    )
    head_float = head_gains.astype(jnp.float32)

    def prepare_local(query_arg, key_arg, gains_arg):
        return prepare(query_arg, key_arg, gains_arg, cosine, sine_table)

    (query_rot, key_rot), prep_pull = jax.vjp(
        prepare_local, query_pre, key_before_rotate, head_float
    )
    query_local, key_local, value_local = (
        lax.all_to_all(
            query_rot.astype(jnp.bfloat16), "uly", split_axis=2, concat_axis=1, tiled=True
        ),
        lax.all_to_all(
            key_rot.astype(jnp.bfloat16), "uly", split_axis=2, concat_axis=1, tiled=True
        ),
        lax.all_to_all(rows_of_value, "uly", split_axis=2, concat_axis=1, tiled=True),
    )
    block_len = query_local.shape[1]
    local_kv = key_local.shape[2]
    query_group = query_local.reshape(seq_count, block_len, local_kv, heads_per_group, head_dim)
    bound = math.sqrt(head_dim) * jnp.max(jnp.abs(head_float[0])) * jnp.max(jnp.abs(head_float[1]))
    scale = head_dim ** (-0.5)
    query_index = blk_index * block_len + jnp.arange(block_len, dtype=jnp.int32)
    query_segs = lax.dynamic_slice_in_dim(segments, blk_index * block_len, block_len, 1)

    def block_weights(keys_in, source):
        key_index = source * block_len + jnp.arange(block_len, dtype=jnp.int32)
        key_segs = lax.dynamic_slice_in_dim(segments, source * block_len, block_len, 1)
        allowed = (key_index[None, None, :] <= query_index[None, :, None]) & (
            key_segs[:, None, :] == query_segs[:, :, None]
        )
        scores = (
            jnp.einsum(
                "sqhgd,skhd->shgqk", query_group, keys_in, preferred_element_type=jnp.float32
            )
            * scale
        )
        return jnp.where(allowed[:, None, None], jnp.exp(scores - bound), 0.0)

    def absorb(stats, key_value, source):
        row_sums, summed = stats
        weights = block_weights(key_value[0], source)
        row_sums = row_sums + jnp.sum(weights, axis=-1)
        summed = summed + jnp.einsum(
            "shgqk,skhd->sqhgd",
            weights.astype(jnp.bfloat16),
            key_value[1],
            preferred_element_type=jnp.float32,
        )
        return (row_sums, summed)

    own_pair = jnp.stack([key_local, value_local])
    start_stats = (
        jnp.zeros((seq_count, local_kv, heads_per_group, block_len), jnp.float32),
        jnp.zeros((seq_count, block_len, local_kv, heads_per_group, head_dim), jnp.float32),
    )
    first_stats = absorb(start_stats, own_pair, blk_index)

    def forward_turn(turn_index, carry):
        key_value, stats_in = carry
        key_value = passed_along(key_value, "blk", 1)
        stats_in = lax.cond(
            turn_index <= blk_index,
            lambda holding: absorb(holding, key_value, blk_index - turn_index),
            lambda holding: holding,
            stats_in,
        )
        return (key_value, stats_in)

    moved_pair, (row_totals, summed_all) = lax.fori_loop(
        1, blk_size, forward_turn, (own_pair, first_stats)
    )
    attended = summed_all / jnp.transpose(row_totals, (0, 3, 1, 2))[..., None]
    attended_tok = lax.all_to_all(
        attended.reshape(seq_count, block_len, local_kv * heads_per_group, head_dim).astype(
            jnp.bfloat16
        ),
        "uly",
        split_axis=1,
        concat_axis=2,
        tiled=True,
    ).reshape(seq_count, tok_count, query_heads * head_dim)
    middle = floats + jnp.einsum(
        "ste,ed->std", attended_tok, out_full, preferred_element_type=jnp.float32
    )
    gain_two, gate_full, up_full, down_full = fetch_feedforward(
        ffn_gain, gate_weight, up_weight, down_weight
    )
    normed_two_float, norm_pull_two = jax.vjp(rms_norm, middle, gain_two.astype(jnp.float32))
    normed_two = normed_two_float.astype(jnp.bfloat16)
    gate_rows = jnp.einsum("std,df->stf", normed_two, gate_full, preferred_element_type=jnp.float32)
    up_rows = jnp.einsum("std,df->stf", normed_two, up_full, preferred_element_type=jnp.float32)
    hidden_float, swiglu_pull = jax.vjp(swiglu, gate_rows, up_rows)
    hidden = hidden_float.astype(jnp.bfloat16)
    outputs = (
        middle + jnp.einsum("stf,fd->std", hidden, down_full, preferred_element_type=jnp.float32)
    ).astype(jnp.bfloat16)
    refetched = fetch_feedforward(ffn_gain, gate_weight, up_weight, down_weight)
    gate_back, up_back, down_back = (refetched[1], refetched[2], refetched[3])
    grad_out = cotangent.astype(jnp.float32)
    down_grad = jnp.einsum("stf,std->fd", hidden, cotangent, preferred_element_type=jnp.float32)
    grad_hidden = jnp.einsum(
        "std,fd->stf", cotangent, down_back, preferred_element_type=jnp.float32
    )
    grad_gate, grad_up = swiglu_pull(grad_hidden)
    grad_gate = grad_gate.astype(jnp.bfloat16)
    grad_up = grad_up.astype(jnp.bfloat16)
    gate_grad = jnp.einsum("std,stf->df", normed_two, grad_gate, preferred_element_type=jnp.float32)
    up_grad = jnp.einsum("std,stf->df", normed_two, grad_up, preferred_element_type=jnp.float32)
    grad_normed_two = jnp.einsum(
        "stf,df->std", grad_gate, gate_back, preferred_element_type=jnp.float32
    ) + jnp.einsum("stf,df->std", grad_up, up_back, preferred_element_type=jnp.float32)
    middle_part, gain_two_grad = norm_pull_two(grad_normed_two)
    grad_middle = grad_out + middle_part
    ffn_shares = (
        lax.psum_scatter(gain_two_grad, ("fsdp", "blk", "uly"), scatter_dimension=0, tiled=True),
        lax.psum_scatter(gate_grad, ("fsdp", "blk", "uly"), scatter_dimension=0, tiled=True),
        lax.psum_scatter(up_grad, ("fsdp", "blk", "uly"), scatter_dimension=0, tiled=True),
        lax.psum_scatter(down_grad, ("fsdp", "blk", "uly"), scatter_dimension=0, tiled=True),
    )
    fetched_again = fetch_attention(attn_gain, query_weight, key_matrix, value_matrix, out_weight)
    query_back, key_back, value_back, out_back = (
        fetched_again[1],
        fetched_again[2],
        fetched_again[3],
        fetched_again[4],
    )
    grad_middle_low = grad_middle.astype(jnp.bfloat16)
    out_grad = jnp.einsum(
        "ste,std->ed", attended_tok, grad_middle_low, preferred_element_type=jnp.float32
    )
    grad_att_tok = (
        jnp.einsum("std,ed->ste", grad_middle_low, out_back, preferred_element_type=jnp.float32)
        .astype(jnp.bfloat16)
        .reshape(seq_count, tok_count, query_heads, head_dim)
    )
    grad_att = lax.all_to_all(grad_att_tok, "uly", split_axis=2, concat_axis=1, tiled=True).reshape(
        seq_count, block_len, local_kv, heads_per_group, head_dim
    )
    delta = jnp.transpose(jnp.sum(grad_att.astype(jnp.float32) * attended, axis=-1), (0, 2, 3, 1))

    def block_grads(key_value, source):
        keys_in = key_value[0]
        values_in = key_value[1]
        probs = block_weights(keys_in, source) / row_totals[..., None]
        grad_probs = jnp.einsum(
            "sqhgd,skhd->shgqk", grad_att, values_in, preferred_element_type=jnp.float32
        )
        grad_scores = (probs * (grad_probs - delta[..., None])).astype(jnp.bfloat16)
        grad_query = (
            jnp.einsum(
                "shgqk,skhd->sqhgd", grad_scores, keys_in, preferred_element_type=jnp.float32
            )
            * scale
        )
        grad_keys = (
            jnp.einsum(
                "shgqk,sqhgd->skhd", grad_scores, query_group, preferred_element_type=jnp.float32
            )
            * scale
        )
        grad_values = jnp.einsum(
            "shgqk,sqhgd->skhd",
            probs.astype(jnp.bfloat16),
            grad_att,
            preferred_element_type=jnp.float32,
        )
        return (grad_query, jnp.stack([grad_keys, grad_values]))

    def pass_grads(moving):
        return from_behind(moving.astype(jnp.bfloat16), "blk", 1).astype(moving.dtype)

    query_start, pair_start = block_grads(own_pair, blk_index)

    def backward_turn(turn_index, carry):
        key_value, query_acc, pair_acc = carry
        key_value = passed_along(key_value, "blk", 1)
        pair_acc = pass_grads(pair_acc)

        def accumulate(holding):
            part_query, part_pair = block_grads(key_value, blk_index - turn_index)
            return (holding[0] + part_query, holding[1] + part_pair)

        query_acc, pair_acc = lax.cond(
            turn_index <= blk_index, accumulate, lambda holding: holding, (query_acc, pair_acc)
        )
        return (key_value, query_acc, pair_acc)

    spent_pair, query_total, pair_total = lax.fori_loop(
        1, blk_size, backward_turn, (own_pair, query_start, pair_start)
    )
    pair_total = pass_grads(pair_total)
    grad_query_low = query_total.reshape(
        seq_count, block_len, local_kv * heads_per_group, head_dim
    ).astype(jnp.bfloat16)
    grad_query_tok, grad_key_tok, grad_value_tok = (
        lax.all_to_all(grad_query_low, "uly", split_axis=1, concat_axis=2, tiled=True),
        lax.all_to_all(
            pair_total[0].astype(jnp.bfloat16), "uly", split_axis=1, concat_axis=2, tiled=True
        ),
        lax.all_to_all(
            pair_total[1].astype(jnp.bfloat16), "uly", split_axis=1, concat_axis=2, tiled=True
        ),
    )
    grad_query_pre, grad_key_pre, heads_grad = prep_pull(
        (grad_query_tok.astype(jnp.float32), grad_key_tok.astype(jnp.float32))
    )
    grad_query_flat = grad_query_pre.astype(jnp.bfloat16).reshape(
        seq_count, tok_count, query_heads * head_dim
    )
    grad_key_flat = grad_key_pre.astype(jnp.bfloat16).reshape(
        seq_count, tok_count, value_heads * head_dim
    )
    grad_value_flat = grad_value_tok.reshape(seq_count, tok_count, value_heads * head_dim)
    query_grad = jnp.einsum(
        "std,ste->de", normalized_input, grad_query_flat, preferred_element_type=jnp.float32
    )
    key_grad = jnp.einsum(
        "std,ste->de", normalized_input, grad_key_flat, preferred_element_type=jnp.float32
    )
    value_grad = jnp.einsum(
        "std,ste->de", normalized_input, grad_value_flat, preferred_element_type=jnp.float32
    )
    grad_normed = jnp.einsum(
        "ste,de->std", grad_query_flat, query_back, preferred_element_type=jnp.float32
    )
    grad_normed = grad_normed + jnp.einsum(
        "ste,de->std", grad_key_flat, key_back, preferred_element_type=jnp.float32
    )
    grad_normed = grad_normed + jnp.einsum(
        "ste,de->std", grad_value_flat, value_back, preferred_element_type=jnp.float32
    )
    input_part, gain_one_grad = norm_pull_one(grad_normed)
    input_grad = (grad_middle + input_part).astype(jnp.bfloat16)
    attn_shares = (
        lax.psum_scatter(gain_one_grad, ("fsdp", "blk", "uly"), scatter_dimension=0, tiled=True),
        lax.psum_scatter(heads_grad, ("fsdp", "blk", "uly"), scatter_dimension=1, tiled=True),
        lax.psum_scatter(query_grad, ("fsdp", "blk", "uly"), scatter_dimension=0, tiled=True),
        lax.psum_scatter(key_grad, ("fsdp", "blk", "uly"), scatter_dimension=0, tiled=True),
        lax.psum_scatter(value_grad, ("fsdp", "blk", "uly"), scatter_dimension=0, tiled=True),
        lax.psum_scatter(out_grad, ("fsdp", "blk", "uly"), scatter_dimension=0, tiled=True),
    )
    return (
        outputs,
        input_grad,
        attn_shares[0],
        attn_shares[1],
        attn_shares[2],
        attn_shares[3],
        attn_shares[4],
        attn_shares[5],
        ffn_shares[0],
        ffn_shares[1],
        ffn_shares[2],
        ffn_shares[3],
    )


MESH = pl.DeviceIdType.MESH
ANY = pl.BlockSpec(memory_space=pl.ANY)
VMEM = pl.BlockSpec(memory_space=pltpu.VMEM)
PLANE = [(dx, dy, dc) for dx in (0, 1) for dy in (0, 1) for dc in (0, 1)]
FAR = [(1, 1, 0), (1, 0, 0), (0, 1, 0)]
TURNS = (1, 2, 3)
SEM = pltpu.SemaphoreType.DMA


class Place:
    def __init__(self):
        self.x = lax.axis_index("fsdp")
        self.block = lax.axis_index("blk")
        self.z = lax.axis_index("uly")
        self.y, self.c = (self.block // 2, self.block % 2)
        self.head = 4 * self.x + self.block
        self.here = (self.x, self.block, self.z)

    def coords(self, dx, dy, dc):
        return ((self.x + dx) % 2, (self.y + dy) % 2, (self.c + dc) % 2)

    def peer(self, dx, dy, dc):
        x, y, c = self.coords(dx, dy, dc)
        return (x, 2 * y + c, self.z)

    def index(self, dx, dy, dc):
        x, y, c = self.coords(dx, dy, dc)
        return 4 * x + 2 * y + c

    def shard(self, ref, dx=0, dy=0, dc=0):
        x, y, c = self.coords(dx, dy, dc)
        return ref.at[2 * y + c, :, x]

    def behind(self, turn):
        return (self.z + 4 - turn) % 4

    def ahead(self, turn):
        return (self.z + turn) % 4

    def line(self, turn):
        return (self.x, self.block, self.ahead(turn))


def remote(src, dst, send_sem, recv_sem, device):
    return pltpu.make_async_remote_copy(
        src_ref=src,
        dst_ref=dst,
        send_sem=send_sem,
        recv_sem=recv_sem,
        device_id=device,
        device_id_type=MESH,
    )


def arrived(ref, sem):
    pltpu.make_async_copy(ref, ref, sem).wait()


def meet(peers):
    barrier = pltpu.get_barrier_semaphore()
    for peer in peers:
        pl.semaphore_signal(barrier, inc=1, device_id=peer, device_id_type=MESH)
    pl.semaphore_wait(barrier, len(peers))


class Sends:
    def __init__(self):
        self.pending = []

    def go(self, *args):
        copy = remote(*args)
        copy.start()
        self.pending.append((None, copy))

    def go_if(self, condition, *args):
        copy = remote(*args)
        pl.when(condition)(lambda: copy.start())
        self.pending.append((condition, copy))

    def drain(self):
        for condition, copy in self.pending:
            if condition is None:
                copy.wait_send()
            else:
                pl.when(condition)(lambda copy=copy: copy.wait_send())


def spread_start(me, sends, src, full, send_sems, recv_sems):
    for i, d in enumerate(FAR + [(0, 0, 1)]):
        sends.go(src, me.shard(full), send_sems.at[i], recv_sems.at[i], me.peer(*d))


def spread_piece(me, full, k, send_sems, recv_sems):
    part = full.at[me.block, k, me.x]
    for i, d in enumerate(FAR + [(0, 0, 1)]):
        remote(part, part, send_sems.at[i], recv_sems.at[i], me.peer(*d)).start()


def spread_pieces_sent(me, sends, full, send_sems, recv_sems):
    part = me.shard(full)
    for i, d in enumerate(FAR + [(0, 0, 1)]):
        sends.pending.append((None, remote(part, part, send_sems.at[i], recv_sems.at[i], me.peer(*d))))


def spread_forward(me, sends, full, send_sems, recv_sems, which=(1, 2, 0)):
    for i in which:
        part = me.shard(full, *FAR[i])
        arrived(part, recv_sems.at[i])
        sends.go(part, part, send_sems.at[4 + i], recv_sems.at[4 + i], me.peer(0, 0, 1))


def spread_finish(me, full, recv_sems):
    for i, (dx, dy, _) in enumerate([(0, 0, 0)] + FAR):
        arrived(me.shard(full, dx, dy, 1), recv_sems.at[3 + i])


def full_shape(tokens, width):
    return (4, 4, 2, tokens // 32, width)


def line_spread(me, sends, src, part, sems):
    for dz in (2, 1):
        sends.go_if(me.z < 4 - dz, src, part(me.z), sems.at[0, dz - 1], sems.at[1, dz - 1], me.line(dz))
        sends.go_if(me.z >= dz, src, part(me.z), sems.at[0, dz + 1], sems.at[1, dz + 1], me.line(4 - dz))


def line_forward(me, sends, part, sems):
    inner = jnp.logical_or(me.z == 1, me.z == 2)
    ref = part((me.z + 2) % 4)
    pl.when(me.z == 1)(lambda: arrived(ref, sems.at[1, 3]))
    pl.when(me.z == 2)(lambda: arrived(ref, sems.at[1, 1]))
    target = (me.x, me.block, (3 * me.z + 1) % 4)
    sends.go_if(inner, ref, ref, sems.at[0, 4], sems.at[1, 4], target)


def line_finish(me, part, sems):
    z = me.z
    pl.when(z > 0)(lambda: arrived(part((z + 3) % 4), sems.at[1, 0]))
    pl.when(z < 3)(lambda: arrived(part((z + 1) % 4), sems.at[1, 2]))

    @pl.when(z == 3)
    def _():
        arrived(part((z + 2) % 4), sems.at[1, 1])
        arrived(part((z + 1) % 4), sems.at[1, 4])

    @pl.when(z == 0)
    def _():
        arrived(part((z + 2) % 4), sems.at[1, 3])
        arrived(part((z + 3) % 4), sems.at[1, 4])


def line_to(me, z):
    return (me.x, me.block, z)


def outer_inner(me):
    outer = jnp.logical_or(me.z == 0, me.z == 3)
    return (outer, jnp.logical_not(outer))


def reduce_start(me, sends, own, came, sems):
    z = me.z
    outer, _ = outer_inner(me)
    nearer = line_to(me, 1 + z // 3)
    sends.go_if(outer, own((7 - z) % 4), came.at[3], sems.at[0, 3], sems.at[1, 3], nearer)
    far = (z + 2) % 4
    sends.go_if(outer, own(far), came.at[2], sems.at[0, 2], sems.at[1, 2], line_to(me, far))
    sends.go_if(z < 3, own((z + 1) % 4), came.at[0], sems.at[0, 0], sems.at[1, 0], me.line(1))
    sends.go_if(z > 0, own((z + 3) % 4), came.at[1], sems.at[0, 1], sems.at[1, 1], me.line(3))


def reduce_join(me, sends, own, came, buf, sems):
    _, inner = outer_inner(me)
    far = (me.z + 2) % 4

    @pl.when(inner)
    def _():
        arrived(came.at[3], sems.at[1, 3])
        buf[...] = (own(far)[...].astype(jnp.float32) + came[3].astype(jnp.float32)).astype(buf.dtype)

    sends.go_if(inner, buf, came.at[2], sems.at[0, 2], sems.at[1, 2], line_to(me, far))


def reduce_total(me, own, came, total, sems):
    arrived(came.at[2], sems.at[1, 2])
    total[...] = own(me.z)[...].astype(jnp.float32) + came[2].astype(jnp.float32)

    @pl.when(me.z > 0)
    def _():
        arrived(came.at[0], sems.at[1, 0])
        total[...] = total[...] + came[0].astype(jnp.float32)

    @pl.when(me.z < 3)
    def _():
        arrived(came.at[1], sems.at[1, 1])
        total[...] = total[...] + came[1].astype(jnp.float32)


def lanes(shape):
    return lax.broadcasted_iota(jnp.int32, shape, len(shape) - 1)


def turned(vector):
    half = vector.shape[-1] // 2
    sign = jnp.where(lanes((1, 2 * half)) < half, -1.0, 1.0)
    return pltpu.roll(vector, half, 1) * sign


def head_scale(vector):
    return lax.rsqrt(jnp.mean(vector * vector, axis=-1, keepdims=True) + EPSILON)


def mat(a, b):
    return jnp.dot(a, b, preferred_element_type=jnp.float32)


def mat_right(a, b):
    return lax.dot_general(a, b, (((1,), (1,)), ((), ())), preferred_element_type=jnp.float32)


def mat_left(a, b):
    return lax.dot_general(a, b, (((0,), (0,)), ((), ())), preferred_element_type=jnp.float32)


def permute_in(me, src_ref, full_ref, send_sems, recv_sems, wait=False):
    half = src_ref.shape[1] // 2
    for j in (0, 1):
        for to in (0, 1):
            src = src_ref.at[j, pl.ds(half * to, half)]
            dst = full_ref.at[me.block, me.z, to]
            mine = jnp.logical_and(me.x == to, me.z == 2 * j + me.x)
            copy = remote(
                src, dst, send_sems.at[2 * j + to], recv_sems.at[me.z], (to, me.block, 2 * j + me.x)
            )
            if wait:
                pl.when(jnp.logical_not(mine))(lambda copy=copy: copy.wait_send())
                continue
            pl.when(jnp.logical_not(mine))(lambda copy=copy: copy.start())
            own = pltpu.make_async_copy(src, dst, recv_sems.at[me.z])
            pl.when(mine)(lambda own=own: own.start())


def permuted_in(me, full_ref, recv_sems):
    for k in range(4):
        arrived(full_ref.at[me.block, k, me.x], recv_sems.at[k])


def half_block(me, part, sibling, send_sems, recv_sems, b, sends=None):
    other = me.c != b % 2
    dy = (me.y + b // 2) % 2
    for to in (0, 1):
        slot = 3 - 2 * ((me.x + to) % 2) - dy
        copy = remote(
            part.at[b, :, to], sibling.at[slot], send_sems.at[slot], recv_sems.at[slot],
            me.peer(0, 0, 1),
        )
        if sends is None:
            pl.when(other)(lambda copy=copy: copy.start())
        else:
            sends.pending.append((other, copy))


def half_out(me, sends, part, sibling, out, came, send_sems, recv_sems):
    for i, d in enumerate(FAR):
        x, y, c = me.coords(*d)
        arrived(sibling.at[i], recv_sems.at[i])
        own = part[2 * y + c, :, x].astype(jnp.float32)
        out[i] = (own + sibling[i].astype(jnp.float32)).astype(jnp.bfloat16)
        sends.go(out.at[i], came.at[i], send_sems.at[4 + i], recv_sems.at[4 + i], me.peer(*d))


def half_in(me, part, sibling, came, recv_sems):
    arrived(sibling.at[3], recv_sems.at[3])
    total = part[me.block, :, me.x].astype(jnp.float32) + sibling[3].astype(jnp.float32)
    for i in (1, 2, 0):
        arrived(came.at[i], recv_sems.at[4 + i])
        total = total + came[i].astype(jnp.float32)
    return total


def half_scratch(tokens, width):
    piece = (4, tokens // 32, width)
    return [
        pltpu.VMEM((4,) + piece, jnp.bfloat16),
        pltpu.VMEM((3,) + piece, jnp.bfloat16),
        pltpu.VMEM((3,) + piece, jnp.bfloat16),
        SEM((7,)),
        SEM((7,)),
    ]


def gain_row(gains_ref, kind):
    rows = [jnp.sum(gains_ref[p, :, kind, :], axis=0, keepdims=True) for p in range(8)]
    return jnp.concatenate(rows, axis=1)


def allowed_keys(segcol, segrow, b, kb):
    same = segcol[b] == segrow[:, 256 * kb : 256 * kb + 256]
    if kb < b:
        return same
    rows = lax.broadcasted_iota(jnp.int32, (256, 256), 0)
    return jnp.logical_and(same, lanes((256, 256)) <= rows)


def norm_back(grad, vector, gain, scale):
    weighted = grad * gain
    inner = jnp.mean(weighted * vector, axis=-1, keepdims=True)
    return scale * weighted - vector * (scale * scale * scale * inner)


def permute_out(me, src_ref, dst_ref, send_sems, recv_sems, wait=False):
    half = dst_ref.shape[1] // 2
    for k in range(4):
        src = src_ref.at[k]
        dst = dst_ref.at[me.z // 2, pl.ds(half * me.x, half)]
        mine = jnp.logical_and(me.x == me.z % 2, me.z == k)
        spot = 2 * (me.z // 2) + me.x
        copy = remote(src, dst, send_sems.at[k], recv_sems.at[spot], (me.z % 2, me.block, k))
        if wait:
            pl.when(jnp.logical_not(mine))(lambda copy=copy: copy.wait_send())
            continue
        pl.when(jnp.logical_not(mine))(lambda copy=copy: copy.start())
        own = pltpu.make_async_copy(src, dst, recv_sems.at[spot])
        pl.when(mine)(lambda own=own: own.start())


def permuted_out(dst_ref, recv_sems):
    half = dst_ref.shape[1] // 2
    for j in (0, 1):
        for to in (0, 1):
            arrived(dst_ref.at[j, pl.ds(half * to, half)], recv_sems.at[2 * j + to])


def total_row(share):
    return jnp.sum(jnp.sum(share, axis=0), axis=0, keepdims=True)


def layer_kernel(
    x_ref, cot_ref, seg_ref, q_ref, k_ref, v_ref, g_ref, u_ref, o_ref, d_ref, gain_ref, hg_ref,
    y_ref, gx_ref, dq_ref, dk_ref, dv_ref, dg_ref, du_ref, sums_ref, osum_ref, dsum_ref,
    xf, cf, wf, of, df, guf, segs, gains, n1, nf, gf, pre, qkv, segcol, cos_s, sin_s, att, attlow,
    totals, part, part2, part3, down, n2, gm, y_s, gi_s, mid, gmid,
    gates, hid, gboth, ga, gq, gk, gv, gpre, dd, dgu, do, dw,
    d_came, d_buf, gu_came, gu_buf, gu_total, gu_sum, o_came, o_buf, w_came, w_buf, w_total, w_sum,
    pack, packs, linep,
    sib1, out1, came1, hs1, hr1, sib2, out2, came2, hs2, hr2, sib3, out3, came3, hs3, hr3,
    sib4, out4, came4, hs4, hr4,
    ps, pr, as_, ar, ws, wr, us, ur, gs, gr, zq, zo, zd, zg, rg, rd, ro, rw, cs, cr, ds, dr, ls,
):
    me = Place()
    x, z, p = (me.x, me.z, me.head)
    low, wide_t = (jnp.bfloat16, jnp.float32)
    across = [((x + 1) % 2, me.block, me.ahead(turn)) for turn in TURNS]
    meet([me.peer(*d) for d in PLANE[1:]] + [me.line(turn) for turn in TURNS] + across)
    sends = Sends()

    def local(src, dst, sem):
        copy = pltpu.make_async_copy(src, dst, sem)
        copy.start()
        return copy

    own_gain = local(gain_ref, gains.at[p, z], ls.at[0])
    own_seg = local(seg_ref, segs.at[x], ls.at[1])
    sends.go(seg_ref, segs.at[x], ls.at[2], ls.at[3], me.peer(1, 0, 0))
    for turn in TURNS:
        sends.go(gain_ref, gains.at[p, z], gs.at[turn], gr.at[turn], me.line(turn))
    permute_in(me, x_ref, xf, ps.at[0], pr.at[0])
    own_o = local(o_ref, of.at[z], ls.at[4])
    own_d = local(d_ref, df.at[z], ls.at[5])
    wide, narrow = (q_ref.shape[1] // 8, k_ref.shape[1] // 8)
    cuts = ((q_ref, wide, 0), (k_ref, narrow, wide), (v_ref, narrow, wide + narrow))
    for i, d in enumerate(PLANE):
        t = me.index(*d)
        for n, (ref, width, off) in enumerate(cuts):
            src = ref.at[:, pl.ds(pl.multiple_of(t * width, 128), width)]
            dst = wf.at[p, z, :, pl.ds(off, width)]
            if i == 0:
                local(src, dst, wr.at[n])
            else:
                sends.go(src, dst, ws.at[3 * i + n], wr.at[3 * i + n], me.peer(*d))
    arrived(xf.at[me.block, z, x], pr.at[0, z])
    spread_piece(me, xf, z, as_.at[0], ar.at[0])
    for i, d in enumerate(PLANE):
        t = me.index(*d)
        for n, (ref, width, off) in enumerate(cuts):
            arrived(wf.at[t, z, :, pl.ds(off, width)], wr.at[3 * i + n])
    qkv_part = lambda k: wf.at[:, k]
    o_part = lambda k: of.at[k]
    d_part = lambda k: df.at[k]
    gu_part = lambda k: guf.at[:, k]
    line_spread(me, sends, qkv_part(z), qkv_part, zq)
    for turn in (1, 3, 2):
        k = (z + turn) % 4
        arrived(xf.at[me.block, k, x], pr.at[0, k])
        spread_piece(me, xf, k, as_.at[0], ar.at[0])
    spread_pieces_sent(me, sends, xf, as_.at[0], ar.at[0])
    own_gain.wait()
    for turn in TURNS:
        arrived(gains.at[p, me.behind(turn)], gr.at[turn])
    for i, d in enumerate(PLANE[1:]):
        sends.go(gains.at[p], gains.at[p], gs.at[4 + i], gr.at[4 + i], me.peer(*d))
    line_forward(me, sends, qkv_part, zq)
    permute_in(me, cot_ref, cf, ps.at[1], pr.at[1])
    line_spread(me, sends, o_ref, o_part, zo)
    ff = g_ref.shape[1] // 8
    for i, d in enumerate(PLANE):
        t = me.index(*d)
        for n, ref in enumerate((g_ref, u_ref)):
            src = ref.at[:, pl.ds(pl.multiple_of(t * ff, 128), ff)]
            dst = guf.at[p, z, :, pl.ds(n * ff, ff)]
            if i == 0:
                local(src, dst, ur.at[n])
            else:
                sends.go(src, dst, us.at[2 * i + n], ur.at[2 * i + n], me.peer(*d))
    own_seg.wait()
    arrived(segs.at[(x + 1) % 2], ls.at[3])
    head_dim = hg_ref.shape[1]
    segrow = segs[z % 2, pl.ds(z // 2, 1), :]
    tokens = segrow.shape[1]
    column = jnp.transpose(jnp.broadcast_to(segrow.astype(wide_t), (8, tokens)))[:, :1]
    segcol[...] = column.astype(jnp.int32).reshape(4, 256, 1)
    half_lane = (lanes((1, head_dim)) % (head_dim // 2)).astype(wide_t)
    inverse = jnp.exp(half_lane * (-2.0 * math.log(THETA) / head_dim))
    steps = lax.broadcasted_iota(jnp.int32, (32, head_dim), 0).astype(wide_t) * inverse
    cl, sl = (jnp.cos(steps), jnp.sin(steps))
    ch, sh = (jnp.cos(steps * 32.0), jnp.sin(steps * 32.0))
    doc_cos, doc_sin = ([], [])
    for doc in range(DOCS):
        start = jnp.sum((segrow < doc).astype(wide_t), axis=1, keepdims=True)
        doc_cos.append(jnp.cos(start * inverse))
        doc_sin.append(jnp.sin(start * inverse))
    for b in range(4):
        hi_c, hi_s = (ch[8 * b : 8 * b + 8][:, None, :], sh[8 * b : 8 * b + 8][:, None, :])
        cos_at = (hi_c * cl[None] - hi_s * sl[None]).reshape(256, head_dim)
        sin_at = (hi_s * cl[None] + hi_c * sl[None]).reshape(256, head_dim)
        column = segcol[b]
        cd, sd = (jnp.broadcast_to(v[0], (256, head_dim)) for v in (doc_cos, doc_sin))
        for doc in range(1, DOCS):
            cd = jnp.where(column == doc, doc_cos[doc], cd)
            sd = jnp.where(column == doc, doc_sin[doc], sd)
        cos_s[b] = cos_at * cd + sin_at * sd
        sin_s[b] = sin_at * cd - cos_at * sd
    for i, d in enumerate(PLANE[1:]):
        arrived(gains.at[me.index(*d)], gr.at[4 + i])
    gain_one, gain_two = (gain_row(gains, 0), gain_row(gains, 1))
    spread_forward(me, sends, xf, as_.at[0], ar.at[0])
    spread_finish(me, xf, ar.at[0])

    @pl.loop(0, 4)
    def _(b):
        rows = xf[b].reshape(256, -1).astype(wide_t)
        n1[b] = (rows * head_scale(rows) * gain_one).astype(low)

    line_finish(me, qkv_part, zq)

    @pl.loop(0, 4)
    def _(b):
        rows = mat(n1[b], wf[...].reshape(-1, wf.shape[3]))
        pre[b] = rows
        cosine, sine = (cos_s[b], sin_s[b])
        for h in range(3):
            v = rows[:, head_dim * h : head_dim * (h + 1)]
            n = v * head_scale(v) * hg_ref[pl.ds(h // 2, 1), :]
            qkv[b, :, pl.ds(head_dim * h, head_dim)] = (n * cosine + turned(n) * sine).astype(low)
        qkv[b, :, pl.ds(3 * head_dim, head_dim)] = rows[:, 3 * head_dim :].astype(low)

    permuted_in(me, cf, pr.at[1])
    spread_start(me, sends, me.shard(cf), cf, as_.at[1], ar.at[1])
    own_o.wait()
    line_forward(me, sends, o_part, zo)
    for i, d in enumerate(PLANE):
        t = me.index(*d)
        for n in (0, 1):
            arrived(guf.at[t, z, :, pl.ds(n * ff, ff)], ur.at[2 * i + n])
    line_spread(me, sends, gu_part(z), gu_part, zg)
    line_spread(me, sends, d_ref, d_part, zd)
    top = lambda r: jnp.max(jnp.abs(hg_ref[pl.ds(r, 1), :]), axis=1, keepdims=True)
    bound = math.sqrt(head_dim) * top(0) * top(1)
    scale = head_dim ** (-0.5)
    key_at, value_at = (pl.ds(2 * head_dim, head_dim), pl.ds(3 * head_dim, head_dim))

    def weights_of(b, kb, query):
        s = mat_right(query, qkv[kb, :, key_at]) * scale
        return jnp.where(allowed_keys(segcol, segrow, b, kb), jnp.exp(s - bound), 0.0)

    for b in range(4):

        @pl.loop(0, 2)
        def _(h, b=b):
            at = pl.ds(pl.multiple_of(head_dim * h, head_dim), head_dim)
            query = qkv[b, :, at]
            total, mixed = (None, None)
            for kb in range(b + 1):
                w = weights_of(b, kb, query)
                t = jnp.sum(w, axis=1, keepdims=True)
                m = mat(w.astype(low), qkv[kb, :, value_at])
                total = t if kb == 0 else total + t
                mixed = m if kb == 0 else mixed + m
            mixed = mixed / total
            totals[b, h] = total
            att[b, :, at] = mixed
            attlow[b, :, at] = mixed.astype(low)

    line_finish(me, o_part, zo)

    @pl.loop(0, 4)
    def _(b):
        rows = mat(attlow[b], of[...].reshape(-1, of.shape[2])).astype(low)
        part[b] = rows.reshape(part.shape[1:])
        half_block(me, part, sib1, hs1, hr1, b)

    for b in range(4):
        half_block(me, part, sib1, hs1, hr1, b, sends)
    half_out(me, sends, part, sib1, out1, came1, hs1, hr1)
    spread_forward(me, sends, cf, as_.at[1], ar.at[1])
    middle = xf[me.block, :, x].astype(wide_t) + half_in(me, part, sib1, came1, hr1)
    mid[...] = middle
    n2[...] = (middle * head_scale(middle) * gain_two).astype(low)
    own_n = local(n2, me.shard(nf), ls.at[6])
    spread_start(me, sends, n2, nf, as_.at[2], ar.at[2])
    line_forward(me, sends, gu_part, zg)
    spread_forward(me, sends, nf, as_.at[2], ar.at[2], (1, 2))
    line_forward(me, sends, d_part, zd)
    spread_forward(me, sends, nf, as_.at[2], ar.at[2], (0,))
    spread_finish(me, nf, ar.at[2])
    own_n.wait()
    line_finish(me, gu_part, zg)

    @pl.loop(0, 4)
    def _(b):
        both = mat(nf[b].reshape(256, -1), guf[...].reshape(-1, 2 * ff))
        gates[b] = both
        gate, up = (both[:, :ff], both[:, ff:])
        hid[b] = (gate / (1.0 + jnp.exp(-gate)) * up).astype(low)

    spread_finish(me, cf, ar.at[1])
    own_d.wait()
    dd[...] = mat_left(hid[...].reshape(-1, ff), cf[...].reshape(tokens, -1)).astype(low).reshape(dd.shape)
    own_dd = lambda k: dd.at[k]
    reduce_start(me, sends, own_dd, d_came, rd)
    line_finish(me, d_part, zd)

    @pl.loop(0, 4)
    def _(b):
        both = gates[b]
        gate, up = (both[:, :ff], both[:, ff:])
        sig = 1.0 / (1.0 + jnp.exp(-gate))
        grad = mat_right(cf[b].reshape(256, -1), df[...].reshape(ff, -1))
        gboth[b, :, pl.ds(0, ff)] = (grad * up * sig * (1.0 + gate * (1.0 - sig))).astype(low)
        gboth[b, :, pl.ds(ff, ff)] = (grad * (gate * sig)).astype(low)
        rows = mat_right(gboth[b], guf[...].reshape(-1, 2 * ff)).astype(low)
        part2[b] = rows.reshape(part2.shape[1:])
        half_block(me, part2, sib2, hs2, hr2, b)

    for b in range(4):
        half_block(me, part2, sib2, hs2, hr2, b, sends)
    half_out(me, sends, part2, sib2, out2, came2, hs2, hr2)

    @pl.loop(0, 4)
    def _(b):
        rows = nf[:, :, :, :, pl.ds(pl.multiple_of(256 * b, 256), 256)].reshape(-1, 256)
        grad = mat_left(rows, gboth[...].reshape(-1, 2 * ff)).astype(low)
        dgu[pl.ds(2 * b, 2)] = grad.reshape((2,) + dgu.shape[1:])

    own_gu = lambda k: dgu.at[:, k]
    reduce_start(me, sends, own_gu, gu_came, rg)
    reduce_join(me, sends, own_dd, d_came, d_buf, rd)
    grad = half_in(me, part2, sib2, came2, hr2)
    middle = mid[...]
    r = head_scale(middle)
    total = cf[me.block, :, x].astype(wide_t) + norm_back(grad, middle, gain_two, r)
    gmid[...] = total
    gm[...] = total.astype(low)
    own_gm = local(gm, me.shard(gf), ls.at[7])
    spread_start(me, sends, gm, gf, as_.at[3], ar.at[3])
    share = total_row(grad * middle * r)
    for i in range(8):
        pack[pl.ds(8 + i, 1)] = share[:, 128 * i : 128 * i + 128]

    @pl.loop(0, 4)
    def _(b):
        rows = mat(hid[b], df[...].reshape(ff, -1)).astype(low)
        down[b] = rows.reshape(down.shape[1:])
        half_block(me, down, sib3, hs3, hr3, b)

    for b in range(4):
        half_block(me, down, sib3, hs3, hr3, b, sends)
    half_out(me, sends, down, sib3, out3, came3, hs3, hr3)
    spread_forward(me, sends, gf, as_.at[3], ar.at[3], (1, 2))
    reduce_join(me, sends, own_gu, gu_came, gu_buf, rg)
    spread_forward(me, sends, gf, as_.at[3], ar.at[3], (0,))
    spread_finish(me, gf, ar.at[3])
    own_gm.wait()

    gk[...] = jnp.zeros_like(gk)
    gv[...] = jnp.zeros_like(gv)
    for b in range(4):
        ga[b] = mat_right(gf[b].reshape(256, -1), of[...].reshape(-1, of.shape[2])).astype(low)

        @pl.loop(0, 2)
        def _(h, b=b):
            at = pl.ds(pl.multiple_of(head_dim * h, head_dim), head_dim)
            query, grad = (qkv[b, :, at], ga[b, :, at])
            delta = jnp.sum(grad.astype(wide_t) * att[b, :, at], axis=1, keepdims=True)
            inv = 1.0 / totals[b, h]
            grad_query = None
            for kb in range(b + 1):
                probs = weights_of(b, kb, query) * inv
                gp = mat_right(grad, qkv[kb, :, value_at])
                gsc = (probs * (gp - delta)).astype(low)
                m = mat(gsc, qkv[kb, :, key_at])
                grad_query = m if kb == 0 else grad_query + m
                gk[kb] += mat_left(gsc, query)
                gv[kb] += mat_left(probs.astype(low), grad)
            gq[b, :, at] = grad_query

        if b == 2:
            y_s[...] = (mid[...] + half_in(me, down, sib3, came3, hr3)).astype(low)
            permute_out(me, y_s, y_ref, cs.at[0], cr.at[0])
    do[...] = mat_left(attlow[...].reshape(tokens, -1), gf[...].reshape(tokens, -1)).astype(low).reshape(do.shape)
    own_do = lambda k: do.at[k]
    reduce_start(me, sends, own_do, o_came, ro)
    pack[pl.ds(16, 8)] = jnp.zeros((8, 128), wide_t)

    @pl.loop(0, 4)
    def _(b):
        cosine, sine = (cos_s[b], sin_s[b])
        for h in range(3):
            at = pl.ds(head_dim * h, head_dim)
            source = gq[b, :, at] if h < 2 else gk[b]
            go = (source * scale).astype(low).astype(wide_t)
            gh = go * cosine - turned(go * sine)
            v = pre[b, :, at]
            r = head_scale(v)
            n = v * r
            pack[pl.ds(16 + h // 2, 1)] += jnp.sum(gh * n, axis=0, keepdims=True)
            gn = gh * hg_ref[pl.ds(h // 2, 1), :]
            gpre[b, :, at] = (r * (gn - n * jnp.mean(gn * n, axis=-1, keepdims=True))).astype(low)
        gpre[b, :, value_at] = gv[b].astype(low)

    @pl.loop(0, 4)
    def _(b):
        rows = n1[:, :, pl.ds(pl.multiple_of(256 * b, 256), 256)].reshape(-1, 256)
        grad = mat_left(rows, gpre[...].reshape(tokens, -1)).astype(low)
        dw[pl.ds(2 * b, 2)] = grad.reshape((2,) + dw.shape[1:])

    own_dw = lambda k: dw.at[:, k]
    reduce_start(me, sends, own_dw, w_came, rw)

    @pl.loop(0, 4)
    def _(b):
        rows = mat_right(gpre[b], wf[...].reshape(-1, wf.shape[3])).astype(low)
        part3[b] = rows.reshape(part3.shape[1:])
        half_block(me, part3, sib4, hs4, hr4, b)

    for b in range(4):
        half_block(me, part3, sib4, hs4, hr4, b, sends)
    half_out(me, sends, part3, sib4, out4, came4, hs4, hr4)
    reduce_join(me, sends, own_do, o_came, o_buf, ro)
    reduce_total(me, own_gu, gu_came, gu_total, rg)
    gu_sum[...] = gu_total[...].astype(low)
    for i, d in enumerate(PLANE):
        t = me.index(*d)
        for n, ref in enumerate((dg_ref, du_ref)):
            src = gu_sum.at[t, :, pl.ds(n * ff, ff)]
            dst = ref.at[:, pl.ds(pl.multiple_of(p * ff, 128), ff)]
            if i == 0:
                local(src, dst, dr.at[n])
            else:
                sends.go(src, dst, ds.at[2 * i + n], dr.at[2 * i + n], me.peer(*d))
    reduce_total(me, own_dd, d_came, dsum_ref, rd)
    reduce_join(me, sends, own_dw, w_came, w_buf, rw)
    grad = half_in(me, part3, sib4, came4, hr4)
    rows = xf[me.block, :, x].astype(wide_t)
    r = head_scale(rows)
    share = total_row(grad * rows * r)
    for i in range(8):
        pack[pl.ds(i, 1)] = share[:, 128 * i : 128 * i + 128]
    for turn in TURNS:
        sends.go(pack, linep.at[turn - 1], gs.at[17 + turn], gr.at[17 + turn], me.line(turn))
    gi_s[...] = (gmid[...] + norm_back(grad, rows, gain_one, r)).astype(low)
    permute_out(me, gi_s, gx_ref, cs.at[1], cr.at[1])
    reduce_total(me, own_dw, w_came, w_total, rw)
    w_sum[...] = w_total[...].astype(low)
    backs = ((dq_ref, wide, 0), (dk_ref, narrow, wide), (dv_ref, narrow, wide + narrow))
    for i, d in enumerate(PLANE):
        t = me.index(*d)
        for n, (ref, cols, off) in enumerate(backs):
            src = w_sum.at[t, :, pl.ds(off, cols)]
            dst = ref.at[:, pl.ds(pl.multiple_of(p * cols, 128), cols)]
            if i == 0:
                local(src, dst, dr.at[16 + n])
            else:
                s = 16 + 3 * i + n
                sends.go(src, dst, ds.at[s], dr.at[s], me.peer(*d))
    total = pack[...]
    for turn in TURNS:
        arrived(linep.at[turn - 1], gr.at[17 + turn])
        total = total + linep[turn - 1]
    packs[7] = total
    for i, d in enumerate(PLANE[1:]):
        sends.go(packs.at[7], packs.at[i], gs.at[11 + i], gr.at[11 + i], me.peer(*d))
    reduce_total(me, own_do, o_came, osum_ref, ro)
    for i in range(7):
        arrived(packs.at[i], gr.at[11 + i])
        total = total + packs[i]
    sums_ref[...] = total
    for i, d in enumerate(PLANE):
        t = me.index(*d)
        for n, ref in enumerate((dg_ref, du_ref)):
            arrived(ref.at[:, pl.ds(pl.multiple_of(t * ff, 128), ff)], dr.at[2 * i + n])
        for n, (ref, cols, off) in enumerate(backs):
            arrived(ref.at[:, pl.ds(pl.multiple_of(t * cols, 128), cols)], dr.at[16 + 3 * i + n])
    permuted_out(y_ref, cr.at[0])
    permuted_out(gx_ref, cr.at[1])
    permute_in(me, x_ref, xf, ps.at[0], pr.at[0], wait=True)
    permute_in(me, cot_ref, cf, ps.at[1], pr.at[1], wait=True)
    permute_out(me, y_s, y_ref, cs.at[0], cr.at[0], wait=True)
    permute_out(me, gi_s, gx_ref, cs.at[1], cr.at[1], wait=True)
    sends.drain()


def layer_step(x, cot, seg, q, k, v, g, u, o, d, gain, head_gains):
    tokens, width = (16 * x.shape[1], x.shape[2])
    rows, low, wide = (q.shape[0], jnp.bfloat16, jnp.float32)
    cols = (q.shape[1] + 2 * k.shape[1]) // 8
    att_cols, head_dim = (q.shape[1] // 8, k.shape[1] // 8)
    ff = g.shape[1] // 8
    full = full_shape(tokens, width)
    piece = (4, tokens // 32, width)
    quarter = tokens // 4
    shape, buf = (jax.ShapeDtypeStruct, pltpu.VMEM)
    blocks = lambda n, kind: buf((4, quarter, n), kind)
    return pl.pallas_call(
        layer_kernel,
        name="layer_step",
        out_shape=(
            shape(x.shape, low), shape(x.shape, low), shape(q.shape, low), shape(k.shape, low),
            shape(v.shape, low), shape(g.shape, low), shape(u.shape, low), shape((24, 128), wide),
            shape(o.shape, wide), shape(d.shape, wide),
        ),
        in_specs=[ANY] * 11 + [VMEM],
        out_specs=(ANY,) * 7 + (VMEM,) * 3,
        scratch_shapes=[
            buf(full, low), buf(full, low), buf((8, 4, rows, cols), low), buf((4,) + o.shape, low),
            buf((4,) + d.shape, low), buf((8, 4, rows, 2 * ff), low), buf((2,) + seg.shape, seg.dtype),
            buf((8, 4, 8, 128), wide), blocks(width, low), buf(full, low), buf(full, low),
            blocks(cols, wide), blocks(cols, low), blocks(1, jnp.int32), blocks(head_dim, wide),
            blocks(head_dim, wide), blocks(att_cols, wide), blocks(att_cols, low),
            buf((4, 2, quarter, 1), wide), buf(full, low), buf(full, low), buf(full, low), buf(full, low),
            buf(piece, low), buf(piece, low), buf(piece, low), buf(piece, low), buf(piece, wide),
            buf(piece, wide),
            blocks(2 * ff, wide), blocks(ff, low), blocks(2 * ff, low), blocks(att_cols, low), blocks(att_cols, wide),
            blocks(head_dim, wide), blocks(head_dim, wide), blocks(cols, low),
            buf((4,) + d.shape, low), buf((8, 4, rows, 2 * ff), low), buf((4,) + o.shape, low),
            buf((8, 4, rows, cols), low),
            buf((4,) + d.shape, low), buf(d.shape, low),
            buf((4, 8, rows, 2 * ff), low), buf((8, rows, 2 * ff), low), buf((8, rows, 2 * ff), wide),
            buf((8, rows, 2 * ff), low),
            buf((4,) + o.shape, low), buf(o.shape, low),
            buf((4, 8, rows, cols), low), buf((8, rows, cols), low), buf((8, rows, cols), wide),
            buf((8, rows, cols), low),
            buf((24, 128), wide), buf((8, 24, 128), wide), buf((3, 24, 128), wide),
        ]
        + half_scratch(tokens, width) * 4
        + [SEM((2, 4)), SEM((2, 4)), SEM((4, 7)), SEM((4, 7)), SEM((24,)), SEM((24,)), SEM((16,)), SEM((16,))]
        + [SEM((21,)), SEM((21,))]
        + [SEM((2, 6))] * 4
        + [SEM((2, 4))] * 4
        + [SEM((2, 4)), SEM((2, 4)), SEM((40,)), SEM((40,)), SEM((8,))],
        compiler_params=pltpu.CompilerParams(
            collective_id=0, has_side_effects=True, vmem_limit_bytes=67043328
        ),
    )(x, cot, seg, q, k, v, g, u, o, d, gain, head_gains)


def finish_kernel(sums_ref, *refs):
    half = len(refs) // 2
    for src, dst in zip(refs[:half], refs[half : 2 * half]):
        dst[...] = src[...].astype(dst.dtype)
    cut_ref = refs[2 * half]
    z = lax.axis_index("uly")
    head = 4 * lax.axis_index("fsdp") + lax.axis_index("blk")
    share = sums_ref.shape[1] // 4
    gain_rows = [sums_ref[pl.ds(head, 1), :], sums_ref[pl.ds(8 + head, 1), :]]
    gain_rows = pltpu.roll(jnp.concatenate(gain_rows + [jnp.zeros((6, 128), jnp.float32)], axis=0), 128 - share * z, 1)
    head_rows = pltpu.roll(sums_ref[16:24, :], 128 - (4 * head + z) * (share // 8), 1)
    cut_ref[0:8] = gain_rows
    cut_ref[8:16] = head_rows


def finish_step(sums, *arrays):
    return pl.pallas_call(
        finish_kernel,
        name="finish_step",
        out_shape=tuple(
            jax.ShapeDtypeStruct(v.shape, v.dtype if i < 2 else jnp.float32) for i, v in enumerate(arrays)
        )
        + (jax.ShapeDtypeStruct((16, 128), jnp.float32),),
        in_specs=[VMEM] * (1 + len(arrays)),
        out_specs=(VMEM,) * (1 + len(arrays)),
    )(sums, *arrays)


def plane_body(
    inputs, segments, attn_gain, head_gains, query_weight, key_matrix, value_matrix, out_weight,
    ffn_gain, gate_weight, up_weight, down_weight, cotangent,
):
    head_dim = head_gains.shape[1]
    z = lax.axis_index("uly")
    piece = attn_gain.shape[0]
    pair = jnp.stack([attn_gain, ffn_gain]).astype(jnp.float32)
    spot = (jnp.arange(128, dtype=jnp.int32) // piece == z)[None]
    gains_own = jnp.where(spot, jnp.tile(pair, (1, 128 // piece)), 0.0)
    gains_own = jnp.concatenate([gains_own, jnp.zeros((6, 128), jnp.float32)], axis=0)
    outputs, grad_inputs, q_grad, k_grad, v_grad, g_grad, u_grad, sums, out_grad, down_grad = layer_step(
        inputs, cotangent, segments, query_weight, key_matrix, value_matrix, gate_weight, up_weight, out_weight, down_weight, gains_own, head_gains.astype(jnp.float32),
    )
    outputs, grad_inputs, q_grad, k_grad, v_grad, out_grad, g_grad, u_grad, down_grad, cut = finish_step(
        sums, outputs, grad_inputs, q_grad, k_grad, v_grad, out_grad, g_grad, u_grad, down_grad
    )
    attn_gain_grad, ffn_gain_grad = (cut[0, :piece], cut[1, :piece])
    head_gain_grad = cut[8:10, : head_dim // 32]
    return (
        outputs, grad_inputs, attn_gain_grad, head_gain_grad, q_grad, k_grad, v_grad, out_grad,
        ffn_gain_grad, g_grad, u_grad, down_grad,
    )


def fits_plane(mesh, seq_count, heads):
    shape = mesh.shape
    return (shape["fsdp"], shape["blk"], shape["uly"]) == (2, 4, 4) and seq_count == 4 and heads == 8


def solution(mesh):
    def step(*arrays):
        seq_count = arrays[0].shape[0]
        heads = arrays[5].shape[1] // arrays[3].shape[1]
        chosen = plane_body if fits_plane(mesh, seq_count, heads) else body
        return mapped(chosen)(*arrays)

    mapped = functools.partial(
        jax.shard_map,
        mesh=mesh,
        in_specs=(
            P("fsdp", ("blk", "uly"), None),
            P("fsdp", None),
            P(("fsdp", "blk", "uly")),
            P(),
            P(("fsdp", "blk", "uly"), None),
            P(("fsdp", "blk", "uly"), None),
            P(("fsdp", "blk", "uly"), None),
            P(("fsdp", "blk", "uly"), None),
            P(("fsdp", "blk", "uly")),
            P(("fsdp", "blk", "uly"), None),
            P(("fsdp", "blk", "uly"), None),
            P(("fsdp", "blk", "uly"), None),
            P("fsdp", ("blk", "uly"), None),
        ),
        out_specs=(
            P("fsdp", ("blk", "uly"), None),
            P("fsdp", ("blk", "uly"), None),
            P(("fsdp", "blk", "uly")),
            P(None, ("fsdp", "blk", "uly")),
            P(("fsdp", "blk", "uly"), None),
            P(("fsdp", "blk", "uly"), None),
            P(("fsdp", "blk", "uly"), None),
            P(("fsdp", "blk", "uly"), None),
            P(("fsdp", "blk", "uly")),
            P(("fsdp", "blk", "uly"), None),
            P(("fsdp", "blk", "uly"), None),
            P(("fsdp", "blk", "uly"), None),
        ),
        check_vma=False,
    )
    return step
```

```python
import functools
import math

import jax
import jax.numpy as jnp
from jax import lax
from jax.experimental import pallas as pl
from jax.experimental.pallas import tpu as pltpu
from jax.sharding import PartitionSpec as P

DOCS = 4


EPSILON = 1e-06
THETA = 1000000.0


def passed_along(value, axis, steps):
    count = lax.axis_size(axis)
    first, last = (max(0, -steps), min(count, count - steps))
    return lax.ppermute(value, axis, [(source, source + steps) for source in range(first, last)])


def from_behind(value, axis, steps):
    count = lax.axis_size(axis)
    pairs = [(source, (source + steps) % count) for source in range(count)]
    return lax.ppermute(value, axis, pairs)


def rms_norm(vector, weight):
    mean_square = jnp.mean(vector * vector, axis=-1, keepdims=True)
    return vector * lax.rsqrt(mean_square + EPSILON) * weight


def rotate(vector, cosine, sine_table):
    half_width = vector.shape[-1] // 2
    turned = jnp.concatenate([-vector[..., half_width:], vector[..., :half_width]], axis=-1)
    return vector * cosine + turned * sine_table


def prepare(query_pre, key_before_rotate, gains, cosine, sine_table):
    cos_heads = cosine[:, :, None, :]
    sin_heads = sine_table[:, :, None, :]
    query_rot = rotate(rms_norm(query_pre, gains[0]), cos_heads, sin_heads)
    key_rot = rotate(rms_norm(key_before_rotate, gains[1]), cos_heads, sin_heads)
    return (query_rot, key_rot)


def swiglu(gate_rows, up_rows):
    return jax.nn.silu(gate_rows) * up_rows


def fetch_attention(attn_gain, query_weight, key_matrix, value_matrix, out_weight):
    return (
        lax.all_gather(attn_gain, ("fsdp", "blk", "uly"), axis=0, tiled=True),
        lax.all_gather(query_weight, ("fsdp", "blk", "uly"), axis=0, tiled=True),
        lax.all_gather(key_matrix, ("fsdp", "blk", "uly"), axis=0, tiled=True),
        lax.all_gather(value_matrix, ("fsdp", "blk", "uly"), axis=0, tiled=True),
        lax.all_gather(out_weight, ("fsdp", "blk", "uly"), axis=0, tiled=True),
    )


def fetch_feedforward(ffn_gain, gate_weight, up_weight, down_weight):
    return (
        lax.all_gather(ffn_gain, ("fsdp", "blk", "uly"), axis=0, tiled=True),
        lax.all_gather(gate_weight, ("fsdp", "blk", "uly"), axis=0, tiled=True),
        lax.all_gather(up_weight, ("fsdp", "blk", "uly"), axis=0, tiled=True),
        lax.all_gather(down_weight, ("fsdp", "blk", "uly"), axis=0, tiled=True),
    )


def body(
    inputs,
    segments,
    attn_gain,
    head_gains,
    query_weight,
    key_matrix,
    value_matrix,
    out_weight,
    ffn_gain,
    gate_weight,
    up_weight,
    down_weight,
    cotangent,
):
    seq_count, tok_count, model_width = inputs.shape
    head_dim = head_gains.shape[1]
    query_heads = query_weight.shape[1] // head_dim
    value_heads = key_matrix.shape[1] // head_dim
    heads_per_group = query_heads // value_heads
    uly_size = lax.axis_size("uly")
    blk_size = lax.axis_size("blk")
    blk_index = lax.axis_index("blk")
    uly_index = lax.axis_index("uly")
    offset = (blk_index * uly_size + uly_index) * tok_count
    doc_ids = jnp.arange(DOCS, dtype=jnp.int32)
    starts = jnp.sum((segments[:, None, :] < doc_ids[None, :, None]).astype(jnp.int32), axis=2)
    local_segs = lax.dynamic_slice_in_dim(segments, offset, tok_count, 1)
    doc_start = jnp.sum(
        jnp.where(local_segs[:, :, None] == doc_ids[None, None, :], starts[:, None, :], 0), axis=2
    )
    token_place = (offset + jnp.arange(tok_count, dtype=jnp.int32)[None, :] - doc_start).astype(
        jnp.float32
    )
    inverse = jnp.exp(
        jnp.arange(head_dim // 2, dtype=jnp.float32) * (-2.0 * math.log(THETA) / head_dim)
    )
    angles = token_place[..., None] * inverse
    cosine = jnp.concatenate([jnp.cos(angles), jnp.cos(angles)], axis=-1)
    sine_table = jnp.concatenate([jnp.sin(angles), jnp.sin(angles)], axis=-1)
    floats = inputs.astype(jnp.float32)
    gain_one, query_full, key_full, value_full, out_full = fetch_attention(
        attn_gain, query_weight, key_matrix, value_matrix, out_weight
    )
    normed_float, norm_pull_one = jax.vjp(rms_norm, floats, gain_one.astype(jnp.float32))
    normalized_input = normed_float.astype(jnp.bfloat16)
    query_pre = jnp.einsum(
        "std,de->ste", normalized_input, query_full, preferred_element_type=jnp.float32
    ).reshape(seq_count, tok_count, query_heads, head_dim)
    key_before_rotate = jnp.einsum(
        "std,de->ste", normalized_input, key_full, preferred_element_type=jnp.float32
    ).reshape(seq_count, tok_count, value_heads, head_dim)
    rows_of_value = (
        jnp.einsum("std,de->ste", normalized_input, value_full, preferred_element_type=jnp.float32)
        .astype(jnp.bfloat16)
        .reshape(seq_count, tok_count, value_heads, head_dim)
    )
    head_float = head_gains.astype(jnp.float32)

    def prepare_local(query_arg, key_arg, gains_arg):
        return prepare(query_arg, key_arg, gains_arg, cosine, sine_table)

    (query_rot, key_rot), prep_pull = jax.vjp(
        prepare_local, query_pre, key_before_rotate, head_float
    )
    query_local, key_local, value_local = (
        lax.all_to_all(
            query_rot.astype(jnp.bfloat16), "uly", split_axis=2, concat_axis=1, tiled=True
        ),
        lax.all_to_all(
            key_rot.astype(jnp.bfloat16), "uly", split_axis=2, concat_axis=1, tiled=True
        ),
        lax.all_to_all(rows_of_value, "uly", split_axis=2, concat_axis=1, tiled=True),
    )
    block_len = query_local.shape[1]
    local_kv = key_local.shape[2]
    query_group = query_local.reshape(seq_count, block_len, local_kv, heads_per_group, head_dim)
    bound = math.sqrt(head_dim) * jnp.max(jnp.abs(head_float[0])) * jnp.max(jnp.abs(head_float[1]))
    scale = head_dim ** (-0.5)
    query_index = blk_index * block_len + jnp.arange(block_len, dtype=jnp.int32)
    query_segs = lax.dynamic_slice_in_dim(segments, blk_index * block_len, block_len, 1)

    def block_weights(keys_in, source):
        key_index = source * block_len + jnp.arange(block_len, dtype=jnp.int32)
        key_segs = lax.dynamic_slice_in_dim(segments, source * block_len, block_len, 1)
        allowed = (key_index[None, None, :] <= query_index[None, :, None]) & (
            key_segs[:, None, :] == query_segs[:, :, None]
        )
        scores = (
            jnp.einsum(
                "sqhgd,skhd->shgqk", query_group, keys_in, preferred_element_type=jnp.float32
            )
            * scale
        )
        return jnp.where(allowed[:, None, None], jnp.exp(scores - bound), 0.0)

    def absorb(stats, key_value, source):
        row_sums, summed = stats
        weights = block_weights(key_value[0], source)
        row_sums = row_sums + jnp.sum(weights, axis=-1)
        summed = summed + jnp.einsum(
            "shgqk,skhd->sqhgd",
            weights.astype(jnp.bfloat16),
            key_value[1],
            preferred_element_type=jnp.float32,
        )
        return (row_sums, summed)

    own_pair = jnp.stack([key_local, value_local])
    start_stats = (
        jnp.zeros((seq_count, local_kv, heads_per_group, block_len), jnp.float32),
        jnp.zeros((seq_count, block_len, local_kv, heads_per_group, head_dim), jnp.float32),
    )
    first_stats = absorb(start_stats, own_pair, blk_index)

    def forward_turn(turn_index, carry):
        key_value, stats_in = carry
        key_value = passed_along(key_value, "blk", 1)
        stats_in = lax.cond(
            turn_index <= blk_index,
            lambda holding: absorb(holding, key_value, blk_index - turn_index),
            lambda holding: holding,
            stats_in,
        )
        return (key_value, stats_in)

    moved_pair, (row_totals, summed_all) = lax.fori_loop(
        1, blk_size, forward_turn, (own_pair, first_stats)
    )
    attended = summed_all / jnp.transpose(row_totals, (0, 3, 1, 2))[..., None]
    attended_tok = lax.all_to_all(
        attended.reshape(seq_count, block_len, local_kv * heads_per_group, head_dim).astype(
            jnp.bfloat16
        ),
        "uly",
        split_axis=1,
        concat_axis=2,
        tiled=True,
    ).reshape(seq_count, tok_count, query_heads * head_dim)
    middle = floats + jnp.einsum(
        "ste,ed->std", attended_tok, out_full, preferred_element_type=jnp.float32
    )
    gain_two, gate_full, up_full, down_full = fetch_feedforward(
        ffn_gain, gate_weight, up_weight, down_weight
    )
    normed_two_float, norm_pull_two = jax.vjp(rms_norm, middle, gain_two.astype(jnp.float32))
    normed_two = normed_two_float.astype(jnp.bfloat16)
    gate_rows = jnp.einsum("std,df->stf", normed_two, gate_full, preferred_element_type=jnp.float32)
    up_rows = jnp.einsum("std,df->stf", normed_two, up_full, preferred_element_type=jnp.float32)
    hidden_float, swiglu_pull = jax.vjp(swiglu, gate_rows, up_rows)
    hidden = hidden_float.astype(jnp.bfloat16)
    outputs = (
        middle + jnp.einsum("stf,fd->std", hidden, down_full, preferred_element_type=jnp.float32)
    ).astype(jnp.bfloat16)
    refetched = fetch_feedforward(ffn_gain, gate_weight, up_weight, down_weight)
    gate_back, up_back, down_back = (refetched[1], refetched[2], refetched[3])
    grad_out = cotangent.astype(jnp.float32)
    down_grad = jnp.einsum("stf,std->fd", hidden, cotangent, preferred_element_type=jnp.float32)
    grad_hidden = jnp.einsum(
        "std,fd->stf", cotangent, down_back, preferred_element_type=jnp.float32
    )
    grad_gate, grad_up = swiglu_pull(grad_hidden)
    grad_gate = grad_gate.astype(jnp.bfloat16)
    grad_up = grad_up.astype(jnp.bfloat16)
    gate_grad = jnp.einsum("std,stf->df", normed_two, grad_gate, preferred_element_type=jnp.float32)
    up_grad = jnp.einsum("std,stf->df", normed_two, grad_up, preferred_element_type=jnp.float32)
    grad_normed_two = jnp.einsum(
        "stf,df->std", grad_gate, gate_back, preferred_element_type=jnp.float32
    ) + jnp.einsum("stf,df->std", grad_up, up_back, preferred_element_type=jnp.float32)
    middle_part, gain_two_grad = norm_pull_two(grad_normed_two)
    grad_middle = grad_out + middle_part
    ffn_shares = (
        lax.psum_scatter(gain_two_grad, ("fsdp", "blk", "uly"), scatter_dimension=0, tiled=True),
        lax.psum_scatter(gate_grad, ("fsdp", "blk", "uly"), scatter_dimension=0, tiled=True),
        lax.psum_scatter(up_grad, ("fsdp", "blk", "uly"), scatter_dimension=0, tiled=True),
        lax.psum_scatter(down_grad, ("fsdp", "blk", "uly"), scatter_dimension=0, tiled=True),
    )
    fetched_again = fetch_attention(attn_gain, query_weight, key_matrix, value_matrix, out_weight)
    query_back, key_back, value_back, out_back = (
        fetched_again[1],
        fetched_again[2],
        fetched_again[3],
        fetched_again[4],
    )
    grad_middle_low = grad_middle.astype(jnp.bfloat16)
    out_grad = jnp.einsum(
        "ste,std->ed", attended_tok, grad_middle_low, preferred_element_type=jnp.float32
    )
    grad_att_tok = (
        jnp.einsum("std,ed->ste", grad_middle_low, out_back, preferred_element_type=jnp.float32)
        .astype(jnp.bfloat16)
        .reshape(seq_count, tok_count, query_heads, head_dim)
    )
    grad_att = lax.all_to_all(grad_att_tok, "uly", split_axis=2, concat_axis=1, tiled=True).reshape(
        seq_count, block_len, local_kv, heads_per_group, head_dim
    )
    delta = jnp.transpose(jnp.sum(grad_att.astype(jnp.float32) * attended, axis=-1), (0, 2, 3, 1))

    def block_grads(key_value, source):
        keys_in = key_value[0]
        values_in = key_value[1]
        probs = block_weights(keys_in, source) / row_totals[..., None]
        grad_probs = jnp.einsum(
            "sqhgd,skhd->shgqk", grad_att, values_in, preferred_element_type=jnp.float32
        )
        grad_scores = (probs * (grad_probs - delta[..., None])).astype(jnp.bfloat16)
        grad_query = (
            jnp.einsum(
                "shgqk,skhd->sqhgd", grad_scores, keys_in, preferred_element_type=jnp.float32
            )
            * scale
        )
        grad_keys = (
            jnp.einsum(
                "shgqk,sqhgd->skhd", grad_scores, query_group, preferred_element_type=jnp.float32
            )
            * scale
        )
        grad_values = jnp.einsum(
            "shgqk,sqhgd->skhd",
            probs.astype(jnp.bfloat16),
            grad_att,
            preferred_element_type=jnp.float32,
        )
        return (grad_query, jnp.stack([grad_keys, grad_values]))

    def pass_grads(moving):
        return from_behind(moving.astype(jnp.bfloat16), "blk", 1).astype(moving.dtype)

    query_start, pair_start = block_grads(own_pair, blk_index)

    def backward_turn(turn_index, carry):
        key_value, query_acc, pair_acc = carry
        key_value = passed_along(key_value, "blk", 1)
        pair_acc = pass_grads(pair_acc)

        def accumulate(holding):
            part_query, part_pair = block_grads(key_value, blk_index - turn_index)
            return (holding[0] + part_query, holding[1] + part_pair)

        query_acc, pair_acc = lax.cond(
            turn_index <= blk_index, accumulate, lambda holding: holding, (query_acc, pair_acc)
        )
        return (key_value, query_acc, pair_acc)

    spent_pair, query_total, pair_total = lax.fori_loop(
        1, blk_size, backward_turn, (own_pair, query_start, pair_start)
    )
    pair_total = pass_grads(pair_total)
    grad_query_low = query_total.reshape(
        seq_count, block_len, local_kv * heads_per_group, head_dim
    ).astype(jnp.bfloat16)
    grad_query_tok, grad_key_tok, grad_value_tok = (
        lax.all_to_all(grad_query_low, "uly", split_axis=1, concat_axis=2, tiled=True),
        lax.all_to_all(
            pair_total[0].astype(jnp.bfloat16), "uly", split_axis=1, concat_axis=2, tiled=True
        ),
        lax.all_to_all(
            pair_total[1].astype(jnp.bfloat16), "uly", split_axis=1, concat_axis=2, tiled=True
        ),
    )
    grad_query_pre, grad_key_pre, heads_grad = prep_pull(
        (grad_query_tok.astype(jnp.float32), grad_key_tok.astype(jnp.float32))
    )
    grad_query_flat = grad_query_pre.astype(jnp.bfloat16).reshape(
        seq_count, tok_count, query_heads * head_dim
    )
    grad_key_flat = grad_key_pre.astype(jnp.bfloat16).reshape(
        seq_count, tok_count, value_heads * head_dim
    )
    grad_value_flat = grad_value_tok.reshape(seq_count, tok_count, value_heads * head_dim)
    query_grad = jnp.einsum(
        "std,ste->de", normalized_input, grad_query_flat, preferred_element_type=jnp.float32
    )
    key_grad = jnp.einsum(
        "std,ste->de", normalized_input, grad_key_flat, preferred_element_type=jnp.float32
    )
    value_grad = jnp.einsum(
        "std,ste->de", normalized_input, grad_value_flat, preferred_element_type=jnp.float32
    )
    grad_normed = jnp.einsum(
        "ste,de->std", grad_query_flat, query_back, preferred_element_type=jnp.float32
    )
    grad_normed = grad_normed + jnp.einsum(
        "ste,de->std", grad_key_flat, key_back, preferred_element_type=jnp.float32
    )
    grad_normed = grad_normed + jnp.einsum(
        "ste,de->std", grad_value_flat, value_back, preferred_element_type=jnp.float32
    )
    input_part, gain_one_grad = norm_pull_one(grad_normed)
    input_grad = (grad_middle + input_part).astype(jnp.bfloat16)
    attn_shares = (
        lax.psum_scatter(gain_one_grad, ("fsdp", "blk", "uly"), scatter_dimension=0, tiled=True),
        lax.psum_scatter(heads_grad, ("fsdp", "blk", "uly"), scatter_dimension=1, tiled=True),
        lax.psum_scatter(query_grad, ("fsdp", "blk", "uly"), scatter_dimension=0, tiled=True),
        lax.psum_scatter(key_grad, ("fsdp", "blk", "uly"), scatter_dimension=0, tiled=True),
        lax.psum_scatter(value_grad, ("fsdp", "blk", "uly"), scatter_dimension=0, tiled=True),
        lax.psum_scatter(out_grad, ("fsdp", "blk", "uly"), scatter_dimension=0, tiled=True),
    )
    return (
        outputs,
        input_grad,
        attn_shares[0],
        attn_shares[1],
        attn_shares[2],
        attn_shares[3],
        attn_shares[4],
        attn_shares[5],
        ffn_shares[0],
        ffn_shares[1],
        ffn_shares[2],
        ffn_shares[3],
    )


MESH = pl.DeviceIdType.MESH
ANY = pl.BlockSpec(memory_space=pl.ANY)
VMEM = pl.BlockSpec(memory_space=pltpu.VMEM)
PLANE = [(dx, dy, dc) for dx in (0, 1) for dy in (0, 1) for dc in (0, 1)]
FAR = [(1, 1, 0), (1, 0, 0), (0, 1, 0)]
TURNS = (1, 2, 3)
SEM = pltpu.SemaphoreType.DMA


class Place:
    def __init__(self):
        self.x = lax.axis_index("fsdp")
        self.block = lax.axis_index("blk")
        self.z = lax.axis_index("uly")
        self.y, self.c = (self.block // 2, self.block % 2)
        self.head = 4 * self.x + self.block
        self.here = (self.x, self.block, self.z)

    def coords(self, dx, dy, dc):
        return ((self.x + dx) % 2, (self.y + dy) % 2, (self.c + dc) % 2)

    def peer(self, dx, dy, dc):
        x, y, c = self.coords(dx, dy, dc)
        return (x, 2 * y + c, self.z)

    def index(self, dx, dy, dc):
        x, y, c = self.coords(dx, dy, dc)
        return 4 * x + 2 * y + c

    def shard(self, ref, dx=0, dy=0, dc=0):
        x, y, c = self.coords(dx, dy, dc)
        return ref.at[2 * y + c, :, x]

    def behind(self, turn):
        return (self.z + 4 - turn) % 4

    def ahead(self, turn):
        return (self.z + turn) % 4

    def line(self, turn):
        return (self.x, self.block, self.ahead(turn))


def remote(src, dst, send_sem, recv_sem, device):
    return pltpu.make_async_remote_copy(
        src_ref=src,
        dst_ref=dst,
        send_sem=send_sem,
        recv_sem=recv_sem,
        device_id=device,
        device_id_type=MESH,
    )


def arrived(ref, sem):
    pltpu.make_async_copy(ref, ref, sem).wait()


def meet(peers):
    barrier = pltpu.get_barrier_semaphore()
    for peer in peers:
        pl.semaphore_signal(barrier, inc=1, device_id=peer, device_id_type=MESH)
    pl.semaphore_wait(barrier, len(peers))


class Sends:
    def __init__(self):
        self.pending = []

    def go(self, *args):
        copy = remote(*args)
        copy.start()
        self.pending.append((None, copy))

    def go_if(self, condition, *args):
        copy = remote(*args)
        pl.when(condition)(lambda: copy.start())
        self.pending.append((condition, copy))

    def drain(self):
        for condition, copy in self.pending:
            if condition is None:
                copy.wait_send()
            else:
                pl.when(condition)(lambda copy=copy: copy.wait_send())


WAYS = [(1, 0, 0), (0, 1, 0)]


def spread_start(me, sends, src, full, send_sems, recv_sems):
    for n, d, half in ((0, WAYS[0], 0), (1, WAYS[1], 1), (0, WAYS[0], 1), (1, WAYS[1], 0)):
        rows, k = (pl.ds(2 * half, 2), 2 * n + half)
        dst = me.shard(full).at[rows]
        sends.go(src.at[rows], dst, send_sems.at[k], recv_sems.at[k], me.peer(*d))
    sends.go(src, me.shard(full), send_sems.at[4], recv_sems.at[4], me.peer(0, 0, 1))


def spread_relay(me, sends, full, send_sems, recv_sems):
    for n in (0, 1):
        rows = pl.ds(2 * n, 2)
        part = me.shard(full, *WAYS[n]).at[rows]
        arrived(part, recv_sems.at[3 * n])
        sends.go(part, part, send_sems.at[5 + n], recv_sems.at[5 + n], me.peer(*WAYS[1 - n]))
    for n in (0, 1):
        rows = pl.ds(2 * (1 - n), 2)
        part = me.shard(full, *WAYS[n])
        arrived(part.at[rows], recv_sems.at[n + 1])
        sends.go(part, part, send_sems.at[7 + n], recv_sems.at[7 + n], me.peer(0, 0, 1))


def spread_far(me, sends, full, send_sems, recv_sems):
    for n in (0, 1):
        part = me.shard(full, 1, 1, 0).at[pl.ds(2 * n, 2)]
        arrived(part, recv_sems.at[5 + n])
        sends.go(part, part, send_sems.at[9 + n], recv_sems.at[9 + n], me.peer(0, 0, 1))


def spread_finish(me, full, recv_sems):
    arrived(me.shard(full, 0, 0, 1), recv_sems.at[4])
    for n in (0, 1):
        arrived(me.shard(full, *WAYS[n][:2], 1), recv_sems.at[7 + n])
        arrived(me.shard(full, 1, 1, 1).at[pl.ds(2 * n, 2)], recv_sems.at[9 + n])


PIECES = (0, 1, 3, 2)


def piece_start(me, sends, full, turn, send_sems, recv_sems):
    part = full.at[me.block, (me.z + turn) % 4, me.x]
    for n, d in enumerate(WAYS + [(0, 0, 1)]):
        k = 4 * n + turn
        sends.go(part, part, send_sems.at[k], recv_sems.at[k], me.peer(*d))


def piece_relay(me, sends, full, send_sems, recv_sems):
    for turn in PIECES:
        n = int(turn > 1)
        for way in (n, 1 - n):
            x, y, c = me.coords(*WAYS[way])
            part = full.at[2 * y + c, (me.z + turn) % 4, x]
            k = 4 * way + turn
            arrived(part, recv_sems.at[k])
            if way == n:
                sends.go(part, part, send_sems.at[12 + turn], recv_sems.at[12 + turn], me.peer(*WAYS[1 - n]))
            sends.go(part, part, send_sems.at[16 + k], recv_sems.at[16 + k], me.peer(0, 0, 1))


def piece_far(me, sends, full, send_sems, recv_sems):
    for turn in PIECES:
        x, y, c = me.coords(1, 1, 0)
        part = full.at[2 * y + c, (me.z + turn) % 4, x]
        arrived(part, recv_sems.at[12 + turn])
        sends.go(part, part, send_sems.at[24 + turn], recv_sems.at[24 + turn], me.peer(0, 0, 1))


def piece_finish(me, full, recv_sems):
    for n, (dx, dy) in enumerate(((0, 0), (1, 0), (0, 1), (1, 1))):
        x, y, c = me.coords(dx, dy, 1)
        for turn in PIECES:
            arrived(full.at[2 * y + c, (me.z + turn) % 4, x], recv_sems.at[(8, 16, 20, 24)[n] + turn])


def full_shape(tokens, width):
    return (4, 4, 2, tokens // 32, width)


def line_spread(me, sends, src, part, sems):
    for dz in (2, 1):
        sends.go_if(me.z < 4 - dz, src, part(me.z), sems.at[0, dz - 1], sems.at[1, dz - 1], me.line(dz))
        sends.go_if(me.z >= dz, src, part(me.z), sems.at[0, dz + 1], sems.at[1, dz + 1], me.line(4 - dz))


def line_spread_first(me, sends, src, part, sems, second=False):
    outer, inner = outer_inner(me)
    for dz in (2, 1):
        for up in (True, False):
            fits = me.z < 4 - dz if up else me.z >= dz
            outward = me.z == 2 if up else me.z == 1
            early = jnp.logical_or(outer, outward) if dz == 1 else outer
            now = jnp.logical_not(early) if second else early
            k = dz - 1 if up else dz + 1
            target = me.line(dz) if up else me.line(4 - dz)
            sends.go_if(jnp.logical_and(fits, now), src, part(me.z), sems.at[0, k], sems.at[1, k], target)


def line_forward(me, sends, part, sems):
    inner = jnp.logical_or(me.z == 1, me.z == 2)
    ref = part((me.z + 2) % 4)
    pl.when(me.z == 1)(lambda: arrived(ref, sems.at[1, 3]))
    pl.when(me.z == 2)(lambda: arrived(ref, sems.at[1, 1]))
    target = (me.x, me.block, (3 * me.z + 1) % 4)
    sends.go_if(inner, ref, ref, sems.at[0, 4], sems.at[1, 4], target)


def line_finish(me, part, sems):
    z = me.z
    pl.when(z > 0)(lambda: arrived(part((z + 3) % 4), sems.at[1, 0]))
    pl.when(z < 3)(lambda: arrived(part((z + 1) % 4), sems.at[1, 2]))

    @pl.when(z == 3)
    def _():
        arrived(part((z + 2) % 4), sems.at[1, 1])
        arrived(part((z + 1) % 4), sems.at[1, 4])

    @pl.when(z == 0)
    def _():
        arrived(part((z + 2) % 4), sems.at[1, 3])
        arrived(part((z + 3) % 4), sems.at[1, 4])


def line_to(me, z):
    return (me.x, me.block, z)


def outer_inner(me):
    outer = jnp.logical_or(me.z == 0, me.z == 3)
    return (outer, jnp.logical_not(outer))


def reduce_start(me, sends, own, came, sems):
    z = me.z
    outer, _ = outer_inner(me)
    nearer = line_to(me, 1 + z // 3)
    sends.go_if(outer, own((7 - z) % 4), came.at[3], sems.at[0, 3], sems.at[1, 3], nearer)
    far = (z + 2) % 4
    sends.go_if(outer, own(far), came.at[2], sems.at[0, 2], sems.at[1, 2], line_to(me, far))
    sends.go_if(z < 3, own((z + 1) % 4), came.at[0], sems.at[0, 0], sems.at[1, 0], me.line(1))
    sends.go_if(z > 0, own((z + 3) % 4), came.at[1], sems.at[0, 1], sems.at[1, 1], me.line(3))


def reduce_join(me, sends, own, came, buf, sems):
    _, inner = outer_inner(me)
    far = (me.z + 2) % 4

    @pl.when(inner)
    def _():
        arrived(came.at[3], sems.at[1, 3])
        buf[...] = (own(far)[...].astype(jnp.float32) + came[3].astype(jnp.float32)).astype(buf.dtype)

    sends.go_if(inner, buf, came.at[2], sems.at[0, 2], sems.at[1, 2], line_to(me, far))


def reduce_total(me, own, came, total, sems):
    arrived(came.at[2], sems.at[1, 2])
    total[...] = own(me.z)[...].astype(jnp.float32) + came[2].astype(jnp.float32)

    @pl.when(me.z > 0)
    def _():
        arrived(came.at[0], sems.at[1, 0])
        total[...] = total[...] + came[0].astype(jnp.float32)

    @pl.when(me.z < 3)
    def _():
        arrived(came.at[1], sems.at[1, 1])
        total[...] = total[...] + came[1].astype(jnp.float32)


def lanes(shape):
    return lax.broadcasted_iota(jnp.int32, shape, len(shape) - 1)


def turned(vector):
    half = vector.shape[-1] // 2
    sign = jnp.where(lanes((1, 2 * half)) < half, -1.0, 1.0)
    return pltpu.roll(vector, half, 1) * sign


def head_scale(vector):
    return lax.rsqrt(jnp.mean(vector * vector, axis=-1, keepdims=True) + EPSILON)


def mat(a, b):
    return jnp.dot(a, b, preferred_element_type=jnp.float32)


def mat_right(a, b):
    return lax.dot_general(a, b, (((1,), (1,)), ((), ())), preferred_element_type=jnp.float32)


def mat_left(a, b):
    return lax.dot_general(a, b, (((0,), (0,)), ((), ())), preferred_element_type=jnp.float32)


def permute_in(me, src_ref, full_ref, send_sems, recv_sems, wait=False):
    half = src_ref.shape[1] // 2
    for j in (0, 1):
        for to in (0, 1):
            src = src_ref.at[j, pl.ds(half * to, half)]
            dst = full_ref.at[me.block, me.z, to]
            mine = jnp.logical_and(me.x == to, me.z == 2 * j + me.x)
            copy = remote(
                src, dst, send_sems.at[2 * j + to], recv_sems.at[me.z], (to, me.block, 2 * j + me.x)
            )
            if wait:
                pl.when(jnp.logical_not(mine))(lambda copy=copy: copy.wait_send())
                continue
            pl.when(jnp.logical_not(mine))(lambda copy=copy: copy.start())
            own = pltpu.make_async_copy(src, dst, recv_sems.at[me.z])
            pl.when(mine)(lambda own=own: own.start())


def permuted_in(me, full_ref, recv_sems):
    for k in range(4):
        arrived(full_ref.at[me.block, k, me.x], recv_sems.at[k])


def half_block(me, part, sibling, send_sems, recv_sems, b, sends=None):
    other = me.c != b % 2
    dy = (me.y + b // 2) % 2
    for to in (0, 1):
        slot = 3 - 2 * ((me.x + to) % 2) - dy
        copy = remote(
            part.at[b, :, to], sibling.at[slot], send_sems.at[slot], recv_sems.at[slot],
            me.peer(0, 0, 1),
        )
        if sends is None:
            pl.when(other)(lambda copy=copy: copy.start())
        else:
            sends.pending.append((other, copy))


HALVES = (slice(0, 2), slice(2, 4))


def half_own(me, part, i, dims):
    x, y, c = me.coords(*(FAR + [(0, 0, 0)])[i])
    ref, sibling = part
    return ref[2 * y + c, dims, x].astype(jnp.float32) + sibling[i, dims].astype(jnp.float32)


def half_out(me, sends, part, sibling, out, came, send_sems, recv_sems):
    low, both = (out.dtype, (part, sibling))
    near = (me.peer(1, 0, 0), me.peer(0, 1, 0))
    arrived(sibling.at[0], recv_sems.at[0])
    out[0] = half_own(me, both, 0, slice(None)).astype(low)
    for n, dims in enumerate(HALVES):
        half = pl.ds(2 * n, 2)
        sends.go(out.at[0, half], came.at[0, half], send_sems.at[4 + n], recv_sems.at[4 + n], near[n])
    for n, dims in enumerate(HALVES):
        arrived(sibling.at[1 + n], recv_sems.at[1 + n])
        out[1 + n, dims] = half_own(me, both, 1 + n, dims).astype(low)
        half = pl.ds(2 * n, 2)
        k = 6 + 2 * n
        sends.go(out.at[1 + n, half], came.at[1 + n, half], send_sems.at[k], recv_sems.at[k], near[n])


def half_relay(me, sends, part, sibling, out, came, send_sems, recv_sems):
    low, both = (out.dtype, (part, sibling))
    near = (me.peer(1, 0, 0), me.peer(0, 1, 0))
    for n in (0, 1):
        dims, half, k = (HALVES[1 - n], pl.ds(2 * (1 - n), 2), 7 + 2 * n)
        arrived(came.at[0, half], recv_sems.at[5 - n])
        total = half_own(me, both, 1 + n, dims) + came[0, dims].astype(jnp.float32)
        out[1 + n, dims] = total.astype(low)
        sends.go(out.at[1 + n, half], came.at[1 + n, half], send_sems.at[k], recv_sems.at[k], near[n])


def half_in(me, part, sibling, came, recv_sems):
    arrived(sibling.at[3], recv_sems.at[3])
    for n, half in ((0, 0), (1, 1), (0, 1), (1, 0)):
        k = 6 + 2 * n + (half != n)
        arrived(came.at[1 + n, pl.ds(2 * half, 2)], recv_sems.at[k])
    total = half_own(me, (part, sibling), 3, slice(None))
    return total + came[1].astype(jnp.float32) + came[2].astype(jnp.float32)


def half_scratch(tokens, width):
    piece = (4, tokens // 32, width)
    return [
        pltpu.VMEM((4,) + piece, jnp.bfloat16),
        pltpu.VMEM((3,) + piece, jnp.bfloat16),
        pltpu.VMEM((3,) + piece, jnp.bfloat16),
        SEM((10,)),
        SEM((10,)),
    ]


def gain_row(gains_ref, kind):
    rows = [jnp.sum(gains_ref[p, :, kind, :], axis=0, keepdims=True) for p in range(8)]
    return jnp.concatenate(rows, axis=1)


def allowed_keys(segcol, segrow, b, kb):
    same = segcol[b] == segrow[:, 256 * kb : 256 * kb + 256]
    if kb < b:
        return same
    rows = lax.broadcasted_iota(jnp.int32, (256, 256), 0)
    return jnp.logical_and(same, lanes((256, 256)) <= rows)


def norm_back(grad, vector, gain, scale):
    weighted = grad * gain
    inner = jnp.mean(weighted * vector, axis=-1, keepdims=True)
    return scale * weighted - vector * (scale * scale * scale * inner)


def permute_out(me, src_ref, dst_ref, send_sems, recv_sems, wait=False):
    half = dst_ref.shape[1] // 2
    for k in range(4):
        src = src_ref.at[k]
        dst = dst_ref.at[me.z // 2, pl.ds(half * me.x, half)]
        mine = jnp.logical_and(me.x == me.z % 2, me.z == k)
        spot = 2 * (me.z // 2) + me.x
        copy = remote(src, dst, send_sems.at[k], recv_sems.at[spot], (me.z % 2, me.block, k))
        if wait:
            pl.when(jnp.logical_not(mine))(lambda copy=copy: copy.wait_send())
            continue
        pl.when(jnp.logical_not(mine))(lambda copy=copy: copy.start())
        own = pltpu.make_async_copy(src, dst, recv_sems.at[spot])
        pl.when(mine)(lambda own=own: own.start())


def permuted_out(dst_ref, recv_sems):
    half = dst_ref.shape[1] // 2
    for j in (0, 1):
        for to in (0, 1):
            arrived(dst_ref.at[j, pl.ds(half * to, half)], recv_sems.at[2 * j + to])


def total_row(share):
    return jnp.sum(jnp.sum(share, axis=0), axis=0, keepdims=True)


def layer_kernel(
    x_ref, cot_ref, seg_ref, q_ref, k_ref, v_ref, g_ref, u_ref, o_ref, d_ref, gain_ref, hg_ref,
    y_ref, gx_ref, dq_ref, dk_ref, dv_ref, dg_ref, du_ref, sums_ref, osum_ref, dsum_ref,
    xf, cf, wf, of, df, guf, segs, gains, n1, nf, gf, pre, qkv, segcol, cos_s, sin_s, att, attlow,
    totals, kept, part, part2, down, n2, gm, y_s, gi_s, mid, gmid,
    gates, hid, gboth, ga, gq, gk, gv, gpre, dd, dgu, do, dw,
    d_came, d_buf, gu_came, gu_buf, gu_total, gu_sum, o_came, o_buf, w_came, w_buf, w_total, w_sum,
    pack, packs, linep,
    sib1, out1, came1, hs1, hr1, sib2, out2, came2, hs2, hr2, sib3, out3, came3, hs3, hr3,
    ps, pr, as_, ar, xas, xar, ws, wr, us, ur, gs, gr, zq, zo, zd, zg, zu, rg, rd, ro, rw, cs, cr, ds, dr, ls,
):
    me = Place()
    x, z, p = (me.x, me.z, me.head)
    low, wide_t = (jnp.bfloat16, jnp.float32)
    across = [((x + 1) % 2, me.block, me.ahead(turn)) for turn in TURNS]
    meet([me.peer(*d) for d in PLANE[1:]] + [me.line(turn) for turn in TURNS] + across)
    sends, early = (Sends(), Sends())

    def local(src, dst, sem):
        copy = pltpu.make_async_copy(src, dst, sem)
        copy.start()
        return copy

    own_gain = local(gain_ref, gains.at[p, z], ls.at[0])
    own_seg = local(seg_ref, segs.at[x], ls.at[1])
    sends.go(seg_ref, segs.at[x], ls.at[2], ls.at[3], me.peer(1, 0, 0))
    for turn in TURNS:
        sends.go(gain_ref, gains.at[p, z], gs.at[turn], gr.at[turn], me.line(turn))
    permute_in(me, x_ref, xf, ps.at[0], pr.at[0])
    own_o = local(o_ref, of.at[z], ls.at[4])
    own_d = local(d_ref, df.at[z], ls.at[5])
    wide, narrow = (q_ref.shape[1] // 8, k_ref.shape[1] // 8)
    cuts = ((q_ref, wide, 0), (k_ref, narrow, wide), (v_ref, narrow, wide + narrow))
    for i, d in enumerate(PLANE):
        t = me.index(*d)
        for n, (ref, width, off) in enumerate(cuts):
            src = ref.at[:, pl.ds(pl.multiple_of(t * width, 128), width)]
            dst = wf.at[p, z, :, pl.ds(off, width)]
            if i == 0:
                local(src, dst, wr.at[n])
            else:
                sends.go(src, dst, ws.at[3 * i + n], wr.at[3 * i + n], me.peer(*d))
    ff = g_ref.shape[1] // 8
    arrived(xf.at[me.block, z, x], pr.at[0, z])
    piece_start(me, sends, xf, 0, xas, xar)
    for i, d in enumerate(PLANE):
        t = me.index(*d)
        for n, (ref, width, off) in enumerate(cuts):
            arrived(wf.at[t, z, :, pl.ds(off, width)], wr.at[3 * i + n])
    qkv_part = lambda k: wf.at[:, k]
    o_part = lambda k: of.at[k]
    d_part = lambda k: df.at[k]
    gate_part = lambda k: guf.at[:, k, :, pl.ds(0, ff)]
    up_part = lambda k: guf.at[:, k, :, pl.ds(ff, ff)]
    line_spread_first(me, sends, qkv_part(z), qkv_part, zq)
    for turn in (1, 3, 2):
        k = (z + turn) % 4
        arrived(xf.at[me.block, k, x], pr.at[0, k])
        piece_start(me, sends, xf, turn, xas, xar)
    line_spread_first(me, sends, qkv_part(z), qkv_part, zq, second=True)
    piece_relay(me, sends, xf, xas, xar)
    own_gain.wait()
    for turn in TURNS:
        arrived(gains.at[p, me.behind(turn)], gr.at[turn])
    for i, d in enumerate(PLANE[1:]):
        sends.go(gains.at[p], gains.at[p], gs.at[4 + i], gr.at[4 + i], me.peer(*d))
    line_forward(me, sends, qkv_part, zq)
    permute_in(me, cot_ref, cf, ps.at[1], pr.at[1])
    line_spread(me, sends, o_ref, o_part, zo)
    for i, d in enumerate(PLANE):
        t = me.index(*d)
        for n, ref in enumerate((g_ref, u_ref)):
            src = ref.at[:, pl.ds(pl.multiple_of(t * ff, 128), ff)]
            dst = guf.at[p, z, :, pl.ds(n * ff, ff)]
            if i == 0:
                local(src, dst, ur.at[n])
            else:
                sends.go(src, dst, us.at[2 * i + n], ur.at[2 * i + n], me.peer(*d))
    own_seg.wait()
    arrived(segs.at[(x + 1) % 2], ls.at[3])
    head_dim = hg_ref.shape[1]
    segrow = segs[z % 2, pl.ds(z // 2, 1), :]
    tokens = segrow.shape[1]
    column = jnp.transpose(jnp.broadcast_to(segrow.astype(wide_t), (8, tokens)))[:, :1]
    segcol[...] = column.astype(jnp.int32).reshape(4, 256, 1)
    half_lane = (lanes((1, head_dim)) % (head_dim // 2)).astype(wide_t)
    inverse = jnp.exp(half_lane * (-2.0 * math.log(THETA) / head_dim))
    steps = lax.broadcasted_iota(jnp.int32, (32, head_dim), 0).astype(wide_t) * inverse
    cl, sl = (jnp.cos(steps), jnp.sin(steps))
    ch, sh = (jnp.cos(steps * 32.0), jnp.sin(steps * 32.0))
    doc_cos, doc_sin = ([], [])
    for doc in range(DOCS):
        start = jnp.sum((segrow < doc).astype(wide_t), axis=1, keepdims=True)
        doc_cos.append(jnp.cos(start * inverse))
        doc_sin.append(jnp.sin(start * inverse))
    for b in range(4):
        hi_c, hi_s = (ch[8 * b : 8 * b + 8][:, None, :], sh[8 * b : 8 * b + 8][:, None, :])
        cos_at = (hi_c * cl[None] - hi_s * sl[None]).reshape(256, head_dim)
        sin_at = (hi_s * cl[None] + hi_c * sl[None]).reshape(256, head_dim)
        column = segcol[b]
        cd, sd = (jnp.broadcast_to(v[0], (256, head_dim)) for v in (doc_cos, doc_sin))
        for doc in range(1, DOCS):
            cd = jnp.where(column == doc, doc_cos[doc], cd)
            sd = jnp.where(column == doc, doc_sin[doc], sd)
        cos_s[b] = cos_at * cd + sin_at * sd
        sin_s[b] = sin_at * cd - cos_at * sd
    piece_far(me, sends, xf, xas, xar)
    for i, d in enumerate(PLANE[1:]):
        arrived(gains.at[me.index(*d)], gr.at[4 + i])
    gain_one, gain_two = (gain_row(gains, 0), gain_row(gains, 1))
    piece_finish(me, xf, xar)

    @pl.loop(0, 4)
    def _(b):
        rows = xf[b].reshape(256, -1).astype(wide_t)
        n1[b] = (rows * head_scale(rows) * gain_one).astype(low)

    line_finish(me, qkv_part, zq)

    own_o.wait()
    line_forward(me, sends, o_part, zo)
    for i, d in enumerate(PLANE):
        t = me.index(*d)
        for n in (0, 1):
            arrived(guf.at[t, z, :, pl.ds(n * ff, ff)], ur.at[2 * i + n])
    line_spread(me, sends, gate_part(z), gate_part, zg)
    line_spread(me, sends, up_part(z), up_part, zu)
    @pl.loop(0, 4)
    def _(b):
        rows = mat(n1[b], wf[...].reshape(-1, wf.shape[3]))
        pre[b] = rows
        cosine, sine = (cos_s[b], sin_s[b])
        for h in range(3):
            v = rows[:, head_dim * h : head_dim * (h + 1)]
            n = v * head_scale(v) * hg_ref[pl.ds(h // 2, 1), :]
            qkv[b, :, pl.ds(head_dim * h, head_dim)] = (n * cosine + turned(n) * sine).astype(low)
        qkv[b, :, pl.ds(3 * head_dim, head_dim)] = rows[:, 3 * head_dim :].astype(low)

    permuted_in(me, cf, pr.at[1])
    spread_start(me, sends, me.shard(cf), cf, as_.at[1], ar.at[1])
    top = lambda r: jnp.max(jnp.abs(hg_ref[pl.ds(r, 1), :]), axis=1, keepdims=True)
    bound = math.sqrt(head_dim) * top(0) * top(1)
    scale = head_dim ** (-0.5)
    key_at, value_at = (pl.ds(2 * head_dim, head_dim), pl.ds(3 * head_dim, head_dim))

    def weights_of(b, kb, query):
        s = mat_right(query, qkv[kb, :, key_at]) * scale
        return jnp.where(allowed_keys(segcol, segrow, b, kb), jnp.exp(s - bound), 0.0)

    for b in range(4):

        @pl.loop(0, 2)
        def _(h, b=b):
            at = pl.ds(pl.multiple_of(head_dim * h, head_dim), head_dim)
            query = qkv[b, :, at]
            total, mixed = (None, None)
            for kb in range(b + 1):
                w = weights_of(b, kb, query)
                t = jnp.sum(w, axis=1, keepdims=True)
                kept[h, b * (b + 1) // 2 + kb] = w.astype(low)
                m = mat(w.astype(low), qkv[kb, :, value_at])
                total = t if kb == 0 else total + t
                mixed = m if kb == 0 else mixed + m
            mixed = mixed / total
            totals[b, h] = total
            att[b, :, at] = mixed
            attlow[b, :, at] = mixed.astype(low)

    line_finish(me, o_part, zo)

    @pl.loop(0, 4)
    def _(b):
        rows = mat(attlow[b], of[...].reshape(-1, of.shape[2])).astype(low)
        part[b] = rows.reshape(part.shape[1:])
        half_block(me, part, sib1, hs1, hr1, b)

    for b in range(4):
        half_block(me, part, sib1, hs1, hr1, b, early)
    half_out(me, early, part, sib1, out1, came1, hs1, hr1)
    line_forward(me, sends, gate_part, zg)
    half_relay(me, early, part, sib1, out1, came1, hs1, hr1)
    spread_relay(me, sends, cf, as_.at[1], ar.at[1])
    middle = xf[me.block, :, x].astype(wide_t) + half_in(me, part, sib1, came1, hr1)
    mid[...] = middle
    n2[...] = (middle * head_scale(middle) * gain_two).astype(low)
    own_n = local(n2, me.shard(nf), ls.at[6])
    spread_start(me, sends, n2, nf, as_.at[2], ar.at[2])
    line_forward(me, sends, up_part, zu)
    line_spread(me, sends, d_ref, d_part, zd)
    spread_relay(me, sends, nf, as_.at[2], ar.at[2])
    line_forward(me, sends, d_part, zd)
    spread_far(me, sends, nf, as_.at[2], ar.at[2])
    spread_finish(me, nf, ar.at[2])
    own_n.wait()
    line_finish(me, gate_part, zg)
    line_finish(me, up_part, zu)

    @pl.loop(0, 4)
    def _(b):
        both = mat(nf[b].reshape(256, -1), guf[...].reshape(-1, 2 * ff))
        gates[b] = both
        gate, up = (both[:, :ff], both[:, ff:])
        hid[b] = (gate / (1.0 + jnp.exp(-gate)) * up).astype(low)

    spread_far(me, sends, cf, as_.at[1], ar.at[1])
    spread_finish(me, cf, ar.at[1])
    own_d.wait()
    dd[...] = mat_left(hid[...].reshape(-1, ff), cf[...].reshape(tokens, -1)).astype(low).reshape(dd.shape)
    own_dd = lambda k: dd.at[k]
    reduce_start(me, sends, own_dd, d_came, rd)
    line_finish(me, d_part, zd)

    @pl.loop(0, 4)
    def _(b):
        both = gates[b]
        gate, up = (both[:, :ff], both[:, ff:])
        sig = 1.0 / (1.0 + jnp.exp(-gate))
        grad = mat_right(cf[b].reshape(256, -1), df[...].reshape(ff, -1))
        gboth[b, :, pl.ds(0, ff)] = (grad * up * sig * (1.0 + gate * (1.0 - sig))).astype(low)
        gboth[b, :, pl.ds(ff, ff)] = (grad * (gate * sig)).astype(low)
        rows = mat_right(gboth[b], guf[...].reshape(-1, 2 * ff)).astype(low)
        part2[b] = rows.reshape(part2.shape[1:])
        half_block(me, part2, sib2, hs2, hr2, b)

    for b in range(4):
        half_block(me, part2, sib2, hs2, hr2, b, sends)
    half_out(me, sends, part2, sib2, out2, came2, hs2, hr2)

    @pl.loop(0, 4)
    def _(b):
        rows = nf[:, :, :, :, pl.ds(pl.multiple_of(256 * b, 256), 256)].reshape(-1, 256)
        grad = mat_left(rows, gboth[...].reshape(-1, 2 * ff)).astype(low)
        dgu[pl.ds(2 * b, 2)] = grad.reshape((2,) + dgu.shape[1:])

    own_gu = lambda k: dgu.at[:, k]
    reduce_start(me, sends, own_gu, gu_came, rg)
    half_relay(me, sends, part2, sib2, out2, came2, hs2, hr2)
    reduce_join(me, sends, own_dd, d_came, d_buf, rd)
    grad = half_in(me, part2, sib2, came2, hr2)
    middle = mid[...]
    r = head_scale(middle)
    total = cf[me.block, :, x].astype(wide_t) + norm_back(grad, middle, gain_two, r)
    gmid[...] = total
    gm[...] = total.astype(low)
    own_gm = local(gm, me.shard(gf), ls.at[7])
    spread_start(me, sends, gm, gf, as_.at[3], ar.at[3])
    share = total_row(grad * middle * r)
    for i in range(8):
        pack[pl.ds(8 + i, 1)] = share[:, 128 * i : 128 * i + 128]

    @pl.loop(0, 4)
    def _(b):
        rows = mat(hid[b], df[...].reshape(ff, -1)).astype(low)
        down[b] = rows.reshape(down.shape[1:])
        half_block(me, down, sib3, hs3, hr3, b)

    for b in range(4):
        half_block(me, down, sib3, hs3, hr3, b, sends)
    spread_relay(me, sends, gf, as_.at[3], ar.at[3])
    half_out(me, sends, down, sib3, out3, came3, hs3, hr3)
    reduce_join(me, sends, own_gu, gu_came, gu_buf, rg)
    spread_far(me, sends, gf, as_.at[3], ar.at[3])
    spread_finish(me, gf, ar.at[3])
    own_gm.wait()

    half_relay(me, sends, down, sib3, out3, came3, hs3, hr3)
    gk[...] = jnp.zeros_like(gk)
    gv[...] = jnp.zeros_like(gv)
    for b in range(4):
        ga[b] = mat_right(gf[b].reshape(256, -1), of[...].reshape(-1, of.shape[2])).astype(low)

        @pl.loop(0, 2)
        def _(h, b=b):
            at = pl.ds(pl.multiple_of(head_dim * h, head_dim), head_dim)
            query, grad = (qkv[b, :, at], ga[b, :, at])
            inv = 1.0 / totals[b, h]
            scaled = grad.astype(wide_t) * inv
            delta = jnp.sum(scaled * att[b, :, at], axis=1, keepdims=True)
            scaled = scaled.astype(low)
            grad_query = None
            for kb in range(b + 1):
                w = kept[h, b * (b + 1) // 2 + kb]
                gp = mat_right(scaled, qkv[kb, :, value_at])
                gsc = (w.astype(wide_t) * (gp - delta)).astype(low)
                m = mat(gsc, qkv[kb, :, key_at])
                grad_query = m if kb == 0 else grad_query + m
                gk[kb] += mat_left(gsc, query)
                gv[kb] += mat_left(w, scaled)
            gq[b, :, at] = grad_query

        if b == 2:
            y_s[...] = (mid[...] + half_in(me, down, sib3, came3, hr3)).astype(low)
            permute_out(me, y_s, y_ref, cs.at[0], cr.at[0])
    do[...] = mat_left(attlow[...].reshape(tokens, -1), gf[...].reshape(tokens, -1)).astype(low).reshape(do.shape)
    own_do = lambda k: do.at[k]
    reduce_start(me, sends, own_do, o_came, ro)
    pack[pl.ds(16, 8)] = jnp.zeros((8, 128), wide_t)

    @pl.loop(0, 4)
    def _(b):
        cosine, sine = (cos_s[b], sin_s[b])
        for h in range(3):
            at = pl.ds(head_dim * h, head_dim)
            source = gq[b, :, at] if h < 2 else gk[b]
            go = (source * scale).astype(low).astype(wide_t)
            gh = go * cosine - turned(go * sine)
            v = pre[b, :, at]
            r = head_scale(v)
            n = v * r
            pack[pl.ds(16 + h // 2, 1)] += jnp.sum(gh * n, axis=0, keepdims=True)
            gn = gh * hg_ref[pl.ds(h // 2, 1), :]
            gpre[b, :, at] = (r * (gn - n * jnp.mean(gn * n, axis=-1, keepdims=True))).astype(low)
        gpre[b, :, value_at] = gv[b].astype(low)

    early.drain()

    @pl.loop(0, 4)
    def _(b):
        rows = mat_right(gpre[b], wf[...].reshape(-1, wf.shape[3])).astype(low)
        part[b] = rows.reshape(part.shape[1:])
        half_block(me, part, sib1, hs1, hr1, b)

    for b in range(4):
        half_block(me, part, sib1, hs1, hr1, b, sends)
    half_out(me, sends, part, sib1, out1, came1, hs1, hr1)
    @pl.loop(0, 4)
    def _(b):
        rows = n1[:, :, pl.ds(pl.multiple_of(256 * b, 256), 256)].reshape(-1, 256)
        grad = mat_left(rows, gpre[...].reshape(tokens, -1)).astype(low)
        dw[pl.ds(2 * b, 2)] = grad.reshape((2,) + dw.shape[1:])

    own_dw = lambda k: dw.at[:, k]
    reduce_start(me, sends, own_dw, w_came, rw)
    half_relay(me, sends, part, sib1, out1, came1, hs1, hr1)
    reduce_join(me, sends, own_do, o_came, o_buf, ro)
    reduce_total(me, own_gu, gu_came, gu_total, rg)
    gu_sum[...] = gu_total[...].astype(low)
    for i, d in enumerate(PLANE):
        t = me.index(*d)
        for n, ref in enumerate((dg_ref, du_ref)):
            src = gu_sum.at[t, :, pl.ds(n * ff, ff)]
            dst = ref.at[:, pl.ds(pl.multiple_of(p * ff, 128), ff)]
            if i == 0:
                local(src, dst, dr.at[n])
            else:
                sends.go(src, dst, ds.at[2 * i + n], dr.at[2 * i + n], me.peer(*d))
    reduce_total(me, own_dd, d_came, dsum_ref, rd)
    reduce_join(me, sends, own_dw, w_came, w_buf, rw)
    grad = half_in(me, part, sib1, came1, hr1)
    rows = xf[me.block, :, x].astype(wide_t)
    r = head_scale(rows)
    share = total_row(grad * rows * r)
    for i in range(8):
        pack[pl.ds(i, 1)] = share[:, 128 * i : 128 * i + 128]
    for i, d in enumerate(PLANE[1:]):
        sends.go(pack, packs.at[i], gs.at[11 + i], gr.at[11 + i], me.peer(*d))
    gi_s[...] = (gmid[...] + norm_back(grad, rows, gain_one, r)).astype(low)
    total = pack[...]
    for i in range(7):
        arrived(packs.at[i], gr.at[11 + i])
        total = total + packs[i]
    packs[7] = total
    for turn in TURNS:
        sends.go(packs.at[7], linep.at[turn - 1], gs.at[17 + turn], gr.at[17 + turn], me.line(turn))
    permute_out(me, gi_s, gx_ref, cs.at[1], cr.at[1])
    reduce_total(me, own_dw, w_came, w_total, rw)
    w_sum[...] = w_total[...].astype(low)
    backs = ((dq_ref, wide, 0), (dk_ref, narrow, wide), (dv_ref, narrow, wide + narrow))
    for i, d in enumerate(PLANE):
        t = me.index(*d)
        for n, (ref, cols, off) in enumerate(backs):
            src = w_sum.at[t, :, pl.ds(off, cols)]
            dst = ref.at[:, pl.ds(pl.multiple_of(p * cols, 128), cols)]
            if i == 0:
                local(src, dst, dr.at[16 + n])
            else:
                s = 16 + 3 * i + n
                sends.go(src, dst, ds.at[s], dr.at[s], me.peer(*d))
    reduce_total(me, own_do, o_came, osum_ref, ro)
    for turn in TURNS:
        arrived(linep.at[turn - 1], gr.at[17 + turn])
        total = total + linep[turn - 1]
    sums_ref[...] = total
    for i, d in enumerate(PLANE):
        t = me.index(*d)
        for n, ref in enumerate((dg_ref, du_ref)):
            arrived(ref.at[:, pl.ds(pl.multiple_of(t * ff, 128), ff)], dr.at[2 * i + n])
        for n, (ref, cols, off) in enumerate(backs):
            arrived(ref.at[:, pl.ds(pl.multiple_of(t * cols, 128), cols)], dr.at[16 + 3 * i + n])
    permuted_out(y_ref, cr.at[0])
    permuted_out(gx_ref, cr.at[1])
    permute_in(me, x_ref, xf, ps.at[0], pr.at[0], wait=True)
    permute_in(me, cot_ref, cf, ps.at[1], pr.at[1], wait=True)
    permute_out(me, y_s, y_ref, cs.at[0], cr.at[0], wait=True)
    permute_out(me, gi_s, gx_ref, cs.at[1], cr.at[1], wait=True)
    sends.drain()


def layer_step(x, cot, seg, q, k, v, g, u, o, d, gain, head_gains):
    tokens, width = (16 * x.shape[1], x.shape[2])
    rows, low, wide = (q.shape[0], jnp.bfloat16, jnp.float32)
    cols = (q.shape[1] + 2 * k.shape[1]) // 8
    att_cols, head_dim = (q.shape[1] // 8, k.shape[1] // 8)
    ff = g.shape[1] // 8
    full = full_shape(tokens, width)
    piece = (4, tokens // 32, width)
    quarter = tokens // 4
    shape, buf = (jax.ShapeDtypeStruct, pltpu.VMEM)
    blocks = lambda n, kind: buf((4, quarter, n), kind)
    return pl.pallas_call(
        layer_kernel,
        name="layer_step",
        out_shape=(
            shape(x.shape, low), shape(x.shape, low), shape(q.shape, low), shape(k.shape, low),
            shape(v.shape, low), shape(g.shape, low), shape(u.shape, low), shape((24, 128), wide),
            shape(o.shape, wide), shape(d.shape, wide),
        ),
        in_specs=[ANY] * 11 + [VMEM],
        out_specs=(ANY,) * 7 + (VMEM,) * 3,
        scratch_shapes=[
            buf(full, low), buf(full, low), buf((8, 4, rows, cols), low), buf((4,) + o.shape, low),
            buf((4,) + d.shape, low), buf((8, 4, rows, 2 * ff), low), buf((2,) + seg.shape, seg.dtype),
            buf((8, 4, 8, 128), wide), blocks(width, low), buf(full, low), buf(full, low),
            blocks(cols, wide), blocks(cols, low), blocks(1, jnp.int32), blocks(head_dim, wide),
            blocks(head_dim, wide), blocks(att_cols, wide), blocks(att_cols, low),
            buf((4, 2, quarter, 1), wide), buf((2, 10, quarter, quarter), low), buf(full, low), buf(full, low), buf(full, low),
            buf(piece, low), buf(piece, low), buf(piece, low), buf(piece, low), buf(piece, wide),
            buf(piece, wide),
            blocks(2 * ff, wide), blocks(ff, low), blocks(2 * ff, low), blocks(att_cols, low), blocks(att_cols, wide),
            blocks(head_dim, wide), blocks(head_dim, wide), blocks(cols, low),
            buf((4,) + d.shape, low), buf((8, 4, rows, 2 * ff), low), buf((4,) + o.shape, low),
            buf((8, 4, rows, cols), low),
            buf((4,) + d.shape, low), buf(d.shape, low),
            buf((4, 8, rows, 2 * ff), low), buf((8, rows, 2 * ff), low), buf((8, rows, 2 * ff), wide),
            buf((8, rows, 2 * ff), low),
            buf((4,) + o.shape, low), buf(o.shape, low),
            buf((4, 8, rows, cols), low), buf((8, rows, cols), low), buf((8, rows, cols), wide),
            buf((8, rows, cols), low),
            buf((24, 128), wide), buf((8, 24, 128), wide), buf((3, 24, 128), wide),
        ]
        + half_scratch(tokens, width) * 3
        + [SEM((2, 4)), SEM((2, 4)), SEM((4, 11)), SEM((4, 11)), SEM((28,)), SEM((28,)), SEM((24,)), SEM((24,)), SEM((16,)), SEM((16,))]
        + [SEM((21,)), SEM((21,))]
        + [SEM((2, 5))] * 5
        + [SEM((2, 4))] * 4
        + [SEM((2, 4)), SEM((2, 4)), SEM((40,)), SEM((40,)), SEM((8,))],
        compiler_params=pltpu.CompilerParams(
            collective_id=0, has_side_effects=True, vmem_limit_bytes=67043328
        ),
    )(x, cot, seg, q, k, v, g, u, o, d, gain, head_gains)


def finish_kernel(sums_ref, *refs):
    half = len(refs) // 2
    for src, dst in zip(refs[:half], refs[half : 2 * half]):
        dst[...] = src[...].astype(dst.dtype)
    cut_ref = refs[2 * half]
    z = lax.axis_index("uly")
    head = 4 * lax.axis_index("fsdp") + lax.axis_index("blk")
    share = sums_ref.shape[1] // 4
    gain_rows = [sums_ref[pl.ds(head, 1), :], sums_ref[pl.ds(8 + head, 1), :]]
    gain_rows = pltpu.roll(jnp.concatenate(gain_rows + [jnp.zeros((6, 128), jnp.float32)], axis=0), 128 - share * z, 1)
    head_rows = pltpu.roll(sums_ref[16:24, :], 128 - (4 * head + z) * (share // 8), 1)
    cut_ref[0:8] = gain_rows
    cut_ref[8:16] = head_rows


def finish_step(sums, *arrays):
    return pl.pallas_call(
        finish_kernel,
        name="finish_step",
        out_shape=tuple(
            jax.ShapeDtypeStruct(v.shape, v.dtype if i < 2 else jnp.float32) for i, v in enumerate(arrays)
        )
        + (jax.ShapeDtypeStruct((16, 128), jnp.float32),),
        in_specs=[VMEM] * (1 + len(arrays)),
        out_specs=(VMEM,) * (1 + len(arrays)),
    )(sums, *arrays)


def plane_body(
    inputs, segments, attn_gain, head_gains, query_weight, key_matrix, value_matrix, out_weight,
    ffn_gain, gate_weight, up_weight, down_weight, cotangent,
):
    head_dim = head_gains.shape[1]
    z = lax.axis_index("uly")
    piece = attn_gain.shape[0]
    pair = jnp.stack([attn_gain, ffn_gain]).astype(jnp.float32)
    spot = (jnp.arange(128, dtype=jnp.int32) // piece == z)[None]
    gains_own = jnp.where(spot, jnp.tile(pair, (1, 128 // piece)), 0.0)
    gains_own = jnp.concatenate([gains_own, jnp.zeros((6, 128), jnp.float32)], axis=0)
    outputs, grad_inputs, q_grad, k_grad, v_grad, g_grad, u_grad, sums, out_grad, down_grad = layer_step(
        inputs, cotangent, segments, query_weight, key_matrix, value_matrix, gate_weight, up_weight, out_weight, down_weight, gains_own, head_gains.astype(jnp.float32),
    )
    outputs, grad_inputs, q_grad, k_grad, v_grad, out_grad, g_grad, u_grad, down_grad, cut = finish_step(
        sums, outputs, grad_inputs, q_grad, k_grad, v_grad, out_grad, g_grad, u_grad, down_grad
    )
    attn_gain_grad, ffn_gain_grad = (cut[0, :piece], cut[1, :piece])
    head_gain_grad = cut[8:10, : head_dim // 32]
    return (
        outputs, grad_inputs, attn_gain_grad, head_gain_grad, q_grad, k_grad, v_grad, out_grad,
        ffn_gain_grad, g_grad, u_grad, down_grad,
    )


def fits_plane(mesh, seq_count, heads):
    shape = mesh.shape
    return (shape["fsdp"], shape["blk"], shape["uly"]) == (2, 4, 4) and seq_count == 4 and heads == 8


def solution(mesh):
    def step(*arrays):
        seq_count = arrays[0].shape[0]
        heads = arrays[5].shape[1] // arrays[3].shape[1]
        chosen = plane_body if fits_plane(mesh, seq_count, heads) else body
        return mapped(chosen)(*arrays)

    mapped = functools.partial(
        jax.shard_map,
        mesh=mesh,
        in_specs=(
            P("fsdp", ("blk", "uly"), None),
            P("fsdp", None),
            P(("fsdp", "blk", "uly")),
            P(),
            P(("fsdp", "blk", "uly"), None),
            P(("fsdp", "blk", "uly"), None),
            P(("fsdp", "blk", "uly"), None),
            P(("fsdp", "blk", "uly"), None),
            P(("fsdp", "blk", "uly")),
            P(("fsdp", "blk", "uly"), None),
            P(("fsdp", "blk", "uly"), None),
            P(("fsdp", "blk", "uly"), None),
            P("fsdp", ("blk", "uly"), None),
        ),
        out_specs=(
            P("fsdp", ("blk", "uly"), None),
            P("fsdp", ("blk", "uly"), None),
            P(("fsdp", "blk", "uly")),
            P(None, ("fsdp", "blk", "uly")),
            P(("fsdp", "blk", "uly"), None),
            P(("fsdp", "blk", "uly"), None),
            P(("fsdp", "blk", "uly"), None),
            P(("fsdp", "blk", "uly"), None),
            P(("fsdp", "blk", "uly")),
            P(("fsdp", "blk", "uly"), None),
            P(("fsdp", "blk", "uly"), None),
            P(("fsdp", "blk", "uly"), None),
        ),
        check_vma=False,
    )
    return step
```

```python
import functools
import math

import jax
import jax.numpy as jnp
from jax import lax
from jax.experimental import pallas as pl
from jax.experimental.pallas import tpu as pltpu
from jax.sharding import PartitionSpec as P

DOCS = 4


EPSILON = 1e-06
THETA = 1000000.0


def passed_along(value, axis, steps):
    count = lax.axis_size(axis)
    first, last = (max(0, -steps), min(count, count - steps))
    return lax.ppermute(value, axis, [(source, source + steps) for source in range(first, last)])


def from_behind(value, axis, steps):
    count = lax.axis_size(axis)
    pairs = [(source, (source + steps) % count) for source in range(count)]
    return lax.ppermute(value, axis, pairs)


def rms_norm(vector, weight):
    mean_square = jnp.mean(vector * vector, axis=-1, keepdims=True)
    return vector * lax.rsqrt(mean_square + EPSILON) * weight


def rotate(vector, cosine, sine_table):
    half_width = vector.shape[-1] // 2
    turned = jnp.concatenate([-vector[..., half_width:], vector[..., :half_width]], axis=-1)
    return vector * cosine + turned * sine_table


def prepare(query_pre, key_before_rotate, gains, cosine, sine_table):
    cos_heads = cosine[:, :, None, :]
    sin_heads = sine_table[:, :, None, :]
    query_rot = rotate(rms_norm(query_pre, gains[0]), cos_heads, sin_heads)
    key_rot = rotate(rms_norm(key_before_rotate, gains[1]), cos_heads, sin_heads)
    return (query_rot, key_rot)


def swiglu(gate_rows, up_rows):
    return jax.nn.silu(gate_rows) * up_rows


def fetch_attention(attn_gain, query_weight, key_matrix, value_matrix, out_weight):
    return (
        lax.all_gather(attn_gain, ("fsdp", "blk", "uly"), axis=0, tiled=True),
        lax.all_gather(query_weight, ("fsdp", "blk", "uly"), axis=0, tiled=True),
        lax.all_gather(key_matrix, ("fsdp", "blk", "uly"), axis=0, tiled=True),
        lax.all_gather(value_matrix, ("fsdp", "blk", "uly"), axis=0, tiled=True),
        lax.all_gather(out_weight, ("fsdp", "blk", "uly"), axis=0, tiled=True),
    )


def fetch_feedforward(ffn_gain, gate_weight, up_weight, down_weight):
    return (
        lax.all_gather(ffn_gain, ("fsdp", "blk", "uly"), axis=0, tiled=True),
        lax.all_gather(gate_weight, ("fsdp", "blk", "uly"), axis=0, tiled=True),
        lax.all_gather(up_weight, ("fsdp", "blk", "uly"), axis=0, tiled=True),
        lax.all_gather(down_weight, ("fsdp", "blk", "uly"), axis=0, tiled=True),
    )


def body(
    inputs,
    segments,
    attn_gain,
    head_gains,
    query_weight,
    key_matrix,
    value_matrix,
    out_weight,
    ffn_gain,
    gate_weight,
    up_weight,
    down_weight,
    cotangent,
):
    seq_count, tok_count, model_width = inputs.shape
    head_dim = head_gains.shape[1]
    query_heads = query_weight.shape[1] // head_dim
    value_heads = key_matrix.shape[1] // head_dim
    heads_per_group = query_heads // value_heads
    uly_size = lax.axis_size("uly")
    blk_size = lax.axis_size("blk")
    blk_index = lax.axis_index("blk")
    uly_index = lax.axis_index("uly")
    offset = (blk_index * uly_size + uly_index) * tok_count
    doc_ids = jnp.arange(DOCS, dtype=jnp.int32)
    starts = jnp.sum((segments[:, None, :] < doc_ids[None, :, None]).astype(jnp.int32), axis=2)
    local_segs = lax.dynamic_slice_in_dim(segments, offset, tok_count, 1)
    doc_start = jnp.sum(
        jnp.where(local_segs[:, :, None] == doc_ids[None, None, :], starts[:, None, :], 0), axis=2
    )
    token_place = (offset + jnp.arange(tok_count, dtype=jnp.int32)[None, :] - doc_start).astype(
        jnp.float32
    )
    inverse = jnp.exp(
        jnp.arange(head_dim // 2, dtype=jnp.float32) * (-2.0 * math.log(THETA) / head_dim)
    )
    angles = token_place[..., None] * inverse
    cosine = jnp.concatenate([jnp.cos(angles), jnp.cos(angles)], axis=-1)
    sine_table = jnp.concatenate([jnp.sin(angles), jnp.sin(angles)], axis=-1)
    floats = inputs.astype(jnp.float32)
    gain_one, query_full, key_full, value_full, out_full = fetch_attention(
        attn_gain, query_weight, key_matrix, value_matrix, out_weight
    )
    normed_float, norm_pull_one = jax.vjp(rms_norm, floats, gain_one.astype(jnp.float32))
    normalized_input = normed_float.astype(jnp.bfloat16)
    query_pre = jnp.einsum(
        "std,de->ste", normalized_input, query_full, preferred_element_type=jnp.float32
    ).reshape(seq_count, tok_count, query_heads, head_dim)
    key_before_rotate = jnp.einsum(
        "std,de->ste", normalized_input, key_full, preferred_element_type=jnp.float32
    ).reshape(seq_count, tok_count, value_heads, head_dim)
    rows_of_value = (
        jnp.einsum("std,de->ste", normalized_input, value_full, preferred_element_type=jnp.float32)
        .astype(jnp.bfloat16)
        .reshape(seq_count, tok_count, value_heads, head_dim)
    )
    head_float = head_gains.astype(jnp.float32)

    def prepare_local(query_arg, key_arg, gains_arg):
        return prepare(query_arg, key_arg, gains_arg, cosine, sine_table)

    (query_rot, key_rot), prep_pull = jax.vjp(
        prepare_local, query_pre, key_before_rotate, head_float
    )
    query_local, key_local, value_local = (
        lax.all_to_all(
            query_rot.astype(jnp.bfloat16), "uly", split_axis=2, concat_axis=1, tiled=True
        ),
        lax.all_to_all(
            key_rot.astype(jnp.bfloat16), "uly", split_axis=2, concat_axis=1, tiled=True
        ),
        lax.all_to_all(rows_of_value, "uly", split_axis=2, concat_axis=1, tiled=True),
    )
    block_len = query_local.shape[1]
    local_kv = key_local.shape[2]
    query_group = query_local.reshape(seq_count, block_len, local_kv, heads_per_group, head_dim)
    bound = math.sqrt(head_dim) * jnp.max(jnp.abs(head_float[0])) * jnp.max(jnp.abs(head_float[1]))
    scale = head_dim ** (-0.5)
    query_index = blk_index * block_len + jnp.arange(block_len, dtype=jnp.int32)
    query_segs = lax.dynamic_slice_in_dim(segments, blk_index * block_len, block_len, 1)

    def block_weights(keys_in, source):
        key_index = source * block_len + jnp.arange(block_len, dtype=jnp.int32)
        key_segs = lax.dynamic_slice_in_dim(segments, source * block_len, block_len, 1)
        allowed = (key_index[None, None, :] <= query_index[None, :, None]) & (
            key_segs[:, None, :] == query_segs[:, :, None]
        )
        scores = (
            jnp.einsum(
                "sqhgd,skhd->shgqk", query_group, keys_in, preferred_element_type=jnp.float32
            )
            * scale
        )
        return jnp.where(allowed[:, None, None], jnp.exp(scores - bound), 0.0)

    def absorb(stats, key_value, source):
        row_sums, summed = stats
        weights = block_weights(key_value[0], source)
        row_sums = row_sums + jnp.sum(weights, axis=-1)
        summed = summed + jnp.einsum(
            "shgqk,skhd->sqhgd",
            weights.astype(jnp.bfloat16),
            key_value[1],
            preferred_element_type=jnp.float32,
        )
        return (row_sums, summed)

    own_pair = jnp.stack([key_local, value_local])
    start_stats = (
        jnp.zeros((seq_count, local_kv, heads_per_group, block_len), jnp.float32),
        jnp.zeros((seq_count, block_len, local_kv, heads_per_group, head_dim), jnp.float32),
    )
    first_stats = absorb(start_stats, own_pair, blk_index)

    def forward_turn(turn_index, carry):
        key_value, stats_in = carry
        key_value = passed_along(key_value, "blk", 1)
        stats_in = lax.cond(
            turn_index <= blk_index,
            lambda holding: absorb(holding, key_value, blk_index - turn_index),
            lambda holding: holding,
            stats_in,
        )
        return (key_value, stats_in)

    moved_pair, (row_totals, summed_all) = lax.fori_loop(
        1, blk_size, forward_turn, (own_pair, first_stats)
    )
    attended = summed_all / jnp.transpose(row_totals, (0, 3, 1, 2))[..., None]
    attended_tok = lax.all_to_all(
        attended.reshape(seq_count, block_len, local_kv * heads_per_group, head_dim).astype(
            jnp.bfloat16
        ),
        "uly",
        split_axis=1,
        concat_axis=2,
        tiled=True,
    ).reshape(seq_count, tok_count, query_heads * head_dim)
    middle = floats + jnp.einsum(
        "ste,ed->std", attended_tok, out_full, preferred_element_type=jnp.float32
    )
    gain_two, gate_full, up_full, down_full = fetch_feedforward(
        ffn_gain, gate_weight, up_weight, down_weight
    )
    normed_two_float, norm_pull_two = jax.vjp(rms_norm, middle, gain_two.astype(jnp.float32))
    normed_two = normed_two_float.astype(jnp.bfloat16)
    gate_rows = jnp.einsum("std,df->stf", normed_two, gate_full, preferred_element_type=jnp.float32)
    up_rows = jnp.einsum("std,df->stf", normed_two, up_full, preferred_element_type=jnp.float32)
    hidden_float, swiglu_pull = jax.vjp(swiglu, gate_rows, up_rows)
    hidden = hidden_float.astype(jnp.bfloat16)
    outputs = (
        middle + jnp.einsum("stf,fd->std", hidden, down_full, preferred_element_type=jnp.float32)
    ).astype(jnp.bfloat16)
    refetched = fetch_feedforward(ffn_gain, gate_weight, up_weight, down_weight)
    gate_back, up_back, down_back = (refetched[1], refetched[2], refetched[3])
    grad_out = cotangent.astype(jnp.float32)
    down_grad = jnp.einsum("stf,std->fd", hidden, cotangent, preferred_element_type=jnp.float32)
    grad_hidden = jnp.einsum(
        "std,fd->stf", cotangent, down_back, preferred_element_type=jnp.float32
    )
    grad_gate, grad_up = swiglu_pull(grad_hidden)
    grad_gate = grad_gate.astype(jnp.bfloat16)
    grad_up = grad_up.astype(jnp.bfloat16)
    gate_grad = jnp.einsum("std,stf->df", normed_two, grad_gate, preferred_element_type=jnp.float32)
    up_grad = jnp.einsum("std,stf->df", normed_two, grad_up, preferred_element_type=jnp.float32)
    grad_normed_two = jnp.einsum(
        "stf,df->std", grad_gate, gate_back, preferred_element_type=jnp.float32
    ) + jnp.einsum("stf,df->std", grad_up, up_back, preferred_element_type=jnp.float32)
    middle_part, gain_two_grad = norm_pull_two(grad_normed_two)
    grad_middle = grad_out + middle_part
    ffn_shares = (
        lax.psum_scatter(gain_two_grad, ("fsdp", "blk", "uly"), scatter_dimension=0, tiled=True),
        lax.psum_scatter(gate_grad, ("fsdp", "blk", "uly"), scatter_dimension=0, tiled=True),
        lax.psum_scatter(up_grad, ("fsdp", "blk", "uly"), scatter_dimension=0, tiled=True),
        lax.psum_scatter(down_grad, ("fsdp", "blk", "uly"), scatter_dimension=0, tiled=True),
    )
    fetched_again = fetch_attention(attn_gain, query_weight, key_matrix, value_matrix, out_weight)
    query_back, key_back, value_back, out_back = (
        fetched_again[1],
        fetched_again[2],
        fetched_again[3],
        fetched_again[4],
    )
    grad_middle_low = grad_middle.astype(jnp.bfloat16)
    out_grad = jnp.einsum(
        "ste,std->ed", attended_tok, grad_middle_low, preferred_element_type=jnp.float32
    )
    grad_att_tok = (
        jnp.einsum("std,ed->ste", grad_middle_low, out_back, preferred_element_type=jnp.float32)
        .astype(jnp.bfloat16)
        .reshape(seq_count, tok_count, query_heads, head_dim)
    )
    grad_att = lax.all_to_all(grad_att_tok, "uly", split_axis=2, concat_axis=1, tiled=True).reshape(
        seq_count, block_len, local_kv, heads_per_group, head_dim
    )
    delta = jnp.transpose(jnp.sum(grad_att.astype(jnp.float32) * attended, axis=-1), (0, 2, 3, 1))

    def block_grads(key_value, source):
        keys_in = key_value[0]
        values_in = key_value[1]
        probs = block_weights(keys_in, source) / row_totals[..., None]
        grad_probs = jnp.einsum(
            "sqhgd,skhd->shgqk", grad_att, values_in, preferred_element_type=jnp.float32
        )
        grad_scores = (probs * (grad_probs - delta[..., None])).astype(jnp.bfloat16)
        grad_query = (
            jnp.einsum(
                "shgqk,skhd->sqhgd", grad_scores, keys_in, preferred_element_type=jnp.float32
            )
            * scale
        )
        grad_keys = (
            jnp.einsum(
                "shgqk,sqhgd->skhd", grad_scores, query_group, preferred_element_type=jnp.float32
            )
            * scale
        )
        grad_values = jnp.einsum(
            "shgqk,sqhgd->skhd",
            probs.astype(jnp.bfloat16),
            grad_att,
            preferred_element_type=jnp.float32,
        )
        return (grad_query, jnp.stack([grad_keys, grad_values]))

    def pass_grads(moving):
        return from_behind(moving.astype(jnp.bfloat16), "blk", 1).astype(moving.dtype)

    query_start, pair_start = block_grads(own_pair, blk_index)

    def backward_turn(turn_index, carry):
        key_value, query_acc, pair_acc = carry
        key_value = passed_along(key_value, "blk", 1)
        pair_acc = pass_grads(pair_acc)

        def accumulate(holding):
            part_query, part_pair = block_grads(key_value, blk_index - turn_index)
            return (holding[0] + part_query, holding[1] + part_pair)

        query_acc, pair_acc = lax.cond(
            turn_index <= blk_index, accumulate, lambda holding: holding, (query_acc, pair_acc)
        )
        return (key_value, query_acc, pair_acc)

    spent_pair, query_total, pair_total = lax.fori_loop(
        1, blk_size, backward_turn, (own_pair, query_start, pair_start)
    )
    pair_total = pass_grads(pair_total)
    grad_query_low = query_total.reshape(
        seq_count, block_len, local_kv * heads_per_group, head_dim
    ).astype(jnp.bfloat16)
    grad_query_tok, grad_key_tok, grad_value_tok = (
        lax.all_to_all(grad_query_low, "uly", split_axis=1, concat_axis=2, tiled=True),
        lax.all_to_all(
            pair_total[0].astype(jnp.bfloat16), "uly", split_axis=1, concat_axis=2, tiled=True
        ),
        lax.all_to_all(
            pair_total[1].astype(jnp.bfloat16), "uly", split_axis=1, concat_axis=2, tiled=True
        ),
    )
    grad_query_pre, grad_key_pre, heads_grad = prep_pull(
        (grad_query_tok.astype(jnp.float32), grad_key_tok.astype(jnp.float32))
    )
    grad_query_flat = grad_query_pre.astype(jnp.bfloat16).reshape(
        seq_count, tok_count, query_heads * head_dim
    )
    grad_key_flat = grad_key_pre.astype(jnp.bfloat16).reshape(
        seq_count, tok_count, value_heads * head_dim
    )
    grad_value_flat = grad_value_tok.reshape(seq_count, tok_count, value_heads * head_dim)
    query_grad = jnp.einsum(
        "std,ste->de", normalized_input, grad_query_flat, preferred_element_type=jnp.float32
    )
    key_grad = jnp.einsum(
        "std,ste->de", normalized_input, grad_key_flat, preferred_element_type=jnp.float32
    )
    value_grad = jnp.einsum(
        "std,ste->de", normalized_input, grad_value_flat, preferred_element_type=jnp.float32
    )
    grad_normed = jnp.einsum(
        "ste,de->std", grad_query_flat, query_back, preferred_element_type=jnp.float32
    )
    grad_normed = grad_normed + jnp.einsum(
        "ste,de->std", grad_key_flat, key_back, preferred_element_type=jnp.float32
    )
    grad_normed = grad_normed + jnp.einsum(
        "ste,de->std", grad_value_flat, value_back, preferred_element_type=jnp.float32
    )
    input_part, gain_one_grad = norm_pull_one(grad_normed)
    input_grad = (grad_middle + input_part).astype(jnp.bfloat16)
    attn_shares = (
        lax.psum_scatter(gain_one_grad, ("fsdp", "blk", "uly"), scatter_dimension=0, tiled=True),
        lax.psum_scatter(heads_grad, ("fsdp", "blk", "uly"), scatter_dimension=1, tiled=True),
        lax.psum_scatter(query_grad, ("fsdp", "blk", "uly"), scatter_dimension=0, tiled=True),
        lax.psum_scatter(key_grad, ("fsdp", "blk", "uly"), scatter_dimension=0, tiled=True),
        lax.psum_scatter(value_grad, ("fsdp", "blk", "uly"), scatter_dimension=0, tiled=True),
        lax.psum_scatter(out_grad, ("fsdp", "blk", "uly"), scatter_dimension=0, tiled=True),
    )
    return (
        outputs,
        input_grad,
        attn_shares[0],
        attn_shares[1],
        attn_shares[2],
        attn_shares[3],
        attn_shares[4],
        attn_shares[5],
        ffn_shares[0],
        ffn_shares[1],
        ffn_shares[2],
        ffn_shares[3],
    )


MESH = pl.DeviceIdType.MESH
ANY = pl.BlockSpec(memory_space=pl.ANY)
VMEM = pl.BlockSpec(memory_space=pltpu.VMEM)
PLANE = [(dx, dy, dc) for dx in (0, 1) for dy in (0, 1) for dc in (0, 1)]
FAR = [(1, 1, 0), (1, 0, 0), (0, 1, 0)]
TURNS = (1, 2, 3)
SEM = pltpu.SemaphoreType.DMA


class Place:
    def __init__(self):
        self.x = lax.axis_index("fsdp")
        self.block = lax.axis_index("blk")
        self.z = lax.axis_index("uly")
        self.y, self.c = (self.block // 2, self.block % 2)
        self.head = 4 * self.x + self.block
        self.here = (self.x, self.block, self.z)

    def coords(self, dx, dy, dc):
        return ((self.x + dx) % 2, (self.y + dy) % 2, (self.c + dc) % 2)

    def peer(self, dx, dy, dc):
        x, y, c = self.coords(dx, dy, dc)
        return (x, 2 * y + c, self.z)

    def index(self, dx, dy, dc):
        x, y, c = self.coords(dx, dy, dc)
        return 4 * x + 2 * y + c

    def shard(self, ref, dx=0, dy=0, dc=0):
        x, y, c = self.coords(dx, dy, dc)
        return ref.at[2 * y + c, :, x]

    def behind(self, turn):
        return (self.z + 4 - turn) % 4

    def ahead(self, turn):
        return (self.z + turn) % 4

    def line(self, turn):
        return (self.x, self.block, self.ahead(turn))


def remote(src, dst, send_sem, recv_sem, device):
    return pltpu.make_async_remote_copy(
        src_ref=src,
        dst_ref=dst,
        send_sem=send_sem,
        recv_sem=recv_sem,
        device_id=device,
        device_id_type=MESH,
    )


def arrived(ref, sem):
    pltpu.make_async_copy(ref, ref, sem).wait()


def meet(peers):
    barrier = pltpu.get_barrier_semaphore()
    for peer in peers:
        pl.semaphore_signal(barrier, inc=1, device_id=peer, device_id_type=MESH)
    pl.semaphore_wait(barrier, len(peers))


class Sends:
    def __init__(self):
        self.pending = []

    def go(self, *args):
        copy = remote(*args)
        copy.start()
        self.pending.append((None, copy))

    def go_if(self, condition, *args):
        copy = remote(*args)
        pl.when(condition)(lambda: copy.start())
        self.pending.append((condition, copy))

    def drain(self):
        for condition, copy in self.pending:
            if condition is None:
                copy.wait_send()
            else:
                pl.when(condition)(lambda copy=copy: copy.wait_send())


WAYS = [(1, 0, 0), (0, 1, 0)]


def spread_start(me, sends, src, full, send_sems, recv_sems):
    for n, d, half in ((0, WAYS[0], 0), (1, WAYS[1], 1), (0, WAYS[0], 1), (1, WAYS[1], 0)):
        rows, k = (pl.ds(2 * half, 2), 2 * n + half)
        dst = me.shard(full).at[rows]
        sends.go(src.at[rows], dst, send_sems.at[k], recv_sems.at[k], me.peer(*d))
    sends.go(src, me.shard(full), send_sems.at[4], recv_sems.at[4], me.peer(0, 0, 1))


def spread_relay(me, sends, full, send_sems, recv_sems):
    for n in (0, 1):
        rows = pl.ds(2 * n, 2)
        part = me.shard(full, *WAYS[n]).at[rows]
        arrived(part, recv_sems.at[3 * n])
        sends.go(part, part, send_sems.at[5 + n], recv_sems.at[5 + n], me.peer(*WAYS[1 - n]))
    for n in (0, 1):
        rows = pl.ds(2 * (1 - n), 2)
        part = me.shard(full, *WAYS[n])
        arrived(part.at[rows], recv_sems.at[n + 1])
        sends.go(part, part, send_sems.at[7 + n], recv_sems.at[7 + n], me.peer(0, 0, 1))


def spread_far(me, sends, full, send_sems, recv_sems):
    for n in (0, 1):
        part = me.shard(full, 1, 1, 0).at[pl.ds(2 * n, 2)]
        arrived(part, recv_sems.at[5 + n])
        sends.go(part, part, send_sems.at[9 + n], recv_sems.at[9 + n], me.peer(0, 0, 1))


def spread_finish(me, full, recv_sems):
    arrived(me.shard(full, 0, 0, 1), recv_sems.at[4])
    for n in (0, 1):
        arrived(me.shard(full, *WAYS[n][:2], 1), recv_sems.at[7 + n])
        arrived(me.shard(full, 1, 1, 1).at[pl.ds(2 * n, 2)], recv_sems.at[9 + n])


PIECES = (0, 1, 3, 2)


def piece_start(me, sends, full, turn, send_sems, recv_sems):
    part = full.at[me.block, (me.z + turn) % 4, me.x]
    for n, d in enumerate(WAYS + [(0, 0, 1)]):
        k = 4 * n + turn
        sends.go(part, part, send_sems.at[k], recv_sems.at[k], me.peer(*d))


def piece_relay(me, sends, full, send_sems, recv_sems, turns):
    for turn in turns:
        n = int(turn > 1)
        for way in (n, 1 - n):
            x, y, c = me.coords(*WAYS[way])
            part = full.at[2 * y + c, (me.z + turn) % 4, x]
            k = 4 * way + turn
            arrived(part, recv_sems.at[k])
            if way == n:
                sends.go(part, part, send_sems.at[12 + turn], recv_sems.at[12 + turn], me.peer(*WAYS[1 - n]))
            sends.go(part, part, send_sems.at[16 + k], recv_sems.at[16 + k], me.peer(0, 0, 1))


def piece_far(me, sends, full, send_sems, recv_sems):
    for turn in PIECES:
        x, y, c = me.coords(1, 1, 0)
        part = full.at[2 * y + c, (me.z + turn) % 4, x]
        arrived(part, recv_sems.at[12 + turn])
        sends.go(part, part, send_sems.at[24 + turn], recv_sems.at[24 + turn], me.peer(0, 0, 1))


def piece_finish(me, full, recv_sems):
    for n, (dx, dy) in enumerate(((0, 0), (1, 0), (0, 1), (1, 1))):
        x, y, c = me.coords(dx, dy, 1)
        for turn in PIECES:
            arrived(full.at[2 * y + c, (me.z + turn) % 4, x], recv_sems.at[(8, 16, 20, 24)[n] + turn])


def full_shape(tokens, width):
    return (4, 4, 2, tokens // 32, width)


def line_spread(me, sends, src, part, sems):
    for dz in (2, 1):
        sends.go_if(me.z < 4 - dz, src, part(me.z), sems.at[0, dz - 1], sems.at[1, dz - 1], me.line(dz))
        sends.go_if(me.z >= dz, src, part(me.z), sems.at[0, dz + 1], sems.at[1, dz + 1], me.line(4 - dz))


def line_spread_first(me, sends, src, part, sems, second=False):
    outer, inner = outer_inner(me)
    for dz in (2, 1):
        for up in (True, False):
            fits = me.z < 4 - dz if up else me.z >= dz
            outward = me.z == 2 if up else me.z == 1
            early = jnp.logical_or(outer, outward) if dz == 1 else outer
            now = jnp.logical_not(early) if second else early
            k = dz - 1 if up else dz + 1
            target = me.line(dz) if up else me.line(4 - dz)
            sends.go_if(jnp.logical_and(fits, now), src, part(me.z), sems.at[0, k], sems.at[1, k], target)


def line_forward(me, sends, part, sems):
    inner = jnp.logical_or(me.z == 1, me.z == 2)
    ref = part((me.z + 2) % 4)
    pl.when(me.z == 1)(lambda: arrived(ref, sems.at[1, 3]))
    pl.when(me.z == 2)(lambda: arrived(ref, sems.at[1, 1]))
    target = (me.x, me.block, (3 * me.z + 1) % 4)
    sends.go_if(inner, ref, ref, sems.at[0, 4], sems.at[1, 4], target)


def line_finish(me, part, sems):
    z = me.z
    pl.when(z > 0)(lambda: arrived(part((z + 3) % 4), sems.at[1, 0]))
    pl.when(z < 3)(lambda: arrived(part((z + 1) % 4), sems.at[1, 2]))

    @pl.when(z == 3)
    def _():
        arrived(part((z + 2) % 4), sems.at[1, 1])
        arrived(part((z + 1) % 4), sems.at[1, 4])

    @pl.when(z == 0)
    def _():
        arrived(part((z + 2) % 4), sems.at[1, 3])
        arrived(part((z + 3) % 4), sems.at[1, 4])


def line_to(me, z):
    return (me.x, me.block, z)


def outer_inner(me):
    outer = jnp.logical_or(me.z == 0, me.z == 3)
    return (outer, jnp.logical_not(outer))


def reduce_start(me, sends, own, came, sems, joins=True, rest=True):
    z = me.z
    outer, _ = outer_inner(me)
    if joins:
        nearer = line_to(me, 1 + z // 3)
        sends.go_if(outer, own((7 - z) % 4), came.at[3], sems.at[0, 3], sems.at[1, 3], nearer)
    if rest:
        far = (z + 2) % 4
        sends.go_if(outer, own(far), came.at[2], sems.at[0, 2], sems.at[1, 2], line_to(me, far))
        sends.go_if(z < 3, own((z + 1) % 4), came.at[0], sems.at[0, 0], sems.at[1, 0], me.line(1))
        sends.go_if(z > 0, own((z + 3) % 4), came.at[1], sems.at[0, 1], sems.at[1, 1], me.line(3))


def reduce_join(me, sends, own, came, buf, sems):
    _, inner = outer_inner(me)
    far = (me.z + 2) % 4

    @pl.when(inner)
    def _():
        arrived(came.at[3], sems.at[1, 3])
        buf[...] = (own(far)[...].astype(jnp.float32) + came[3].astype(jnp.float32)).astype(buf.dtype)

    sends.go_if(inner, buf, came.at[2], sems.at[0, 2], sems.at[1, 2], line_to(me, far))


def reduce_total(me, own, came, total, sems):
    arrived(came.at[2], sems.at[1, 2])
    total[...] = own(me.z)[...].astype(jnp.float32) + came[2].astype(jnp.float32)

    @pl.when(me.z > 0)
    def _():
        arrived(came.at[0], sems.at[1, 0])
        total[...] = total[...] + came[0].astype(jnp.float32)

    @pl.when(me.z < 3)
    def _():
        arrived(came.at[1], sems.at[1, 1])
        total[...] = total[...] + came[1].astype(jnp.float32)


def lanes(shape):
    return lax.broadcasted_iota(jnp.int32, shape, len(shape) - 1)


def turned(vector):
    half = vector.shape[-1] // 2
    sign = jnp.where(lanes((1, 2 * half)) < half, -1.0, 1.0)
    return pltpu.roll(vector, half, 1) * sign


def head_scale(vector):
    return lax.rsqrt(jnp.mean(vector * vector, axis=-1, keepdims=True) + EPSILON)


def mat(a, b):
    return jnp.dot(a, b, preferred_element_type=jnp.float32)


def mat_right(a, b):
    return lax.dot_general(a, b, (((1,), (1,)), ((), ())), preferred_element_type=jnp.float32)


def mat_left(a, b):
    return lax.dot_general(a, b, (((0,), (0,)), ((), ())), preferred_element_type=jnp.float32)


def permute_in(me, src_ref, full_ref, send_sems, recv_sems, wait=False):
    half = src_ref.shape[1] // 2
    for j in (0, 1):
        for to in (0, 1):
            src = src_ref.at[j, pl.ds(half * to, half)]
            dst = full_ref.at[me.block, me.z, to]
            mine = jnp.logical_and(me.x == to, me.z == 2 * j + me.x)
            copy = remote(
                src, dst, send_sems.at[2 * j + to], recv_sems.at[me.z], (to, me.block, 2 * j + me.x)
            )
            if wait:
                pl.when(jnp.logical_not(mine))(lambda copy=copy: copy.wait_send())
                continue
            pl.when(jnp.logical_not(mine))(lambda copy=copy: copy.start())
            own = pltpu.make_async_copy(src, dst, recv_sems.at[me.z])
            pl.when(mine)(lambda own=own: own.start())


def permuted_in(me, full_ref, recv_sems):
    for k in range(4):
        arrived(full_ref.at[me.block, k, me.x], recv_sems.at[k])


def half_block(me, part, sibling, send_sems, recv_sems, b, sends=None):
    other = me.c != b % 2
    dy = (me.y + b // 2) % 2
    for to in (0, 1):
        slot = 3 - 2 * ((me.x + to) % 2) - dy
        copy = remote(
            part.at[b, :, to], sibling.at[slot], send_sems.at[slot], recv_sems.at[slot],
            me.peer(0, 0, 1),
        )
        if sends is None:
            pl.when(other)(lambda copy=copy: copy.start())
        else:
            sends.pending.append((other, copy))


HALVES = (slice(0, 2), slice(2, 4))


def half_own(me, part, i, dims):
    x, y, c = me.coords(*(FAR + [(0, 0, 0)])[i])
    ref, sibling = part
    return ref[2 * y + c, dims, x].astype(jnp.float32) + sibling[i, dims].astype(jnp.float32)


def half_out(me, sends, part, sibling, out, came, send_sems, recv_sems):
    low, both = (out.dtype, (part, sibling))
    near = (me.peer(1, 0, 0), me.peer(0, 1, 0))
    arrived(sibling.at[0], recv_sems.at[0])
    out[0] = half_own(me, both, 0, slice(None)).astype(low)
    for n, dims in enumerate(HALVES):
        half = pl.ds(2 * n, 2)
        sends.go(out.at[0, half], came.at[0, half], send_sems.at[4 + n], recv_sems.at[4 + n], near[n])
    for n, dims in enumerate(HALVES):
        arrived(sibling.at[1 + n], recv_sems.at[1 + n])
        out[1 + n, dims] = half_own(me, both, 1 + n, dims).astype(low)
        half = pl.ds(2 * n, 2)
        k = 6 + 2 * n
        sends.go(out.at[1 + n, half], came.at[1 + n, half], send_sems.at[k], recv_sems.at[k], near[n])


def half_relay(me, sends, part, sibling, out, came, send_sems, recv_sems):
    low, both = (out.dtype, (part, sibling))
    near = (me.peer(1, 0, 0), me.peer(0, 1, 0))
    for n in (0, 1):
        dims, half, k = (HALVES[1 - n], pl.ds(2 * (1 - n), 2), 7 + 2 * n)
        arrived(came.at[0, half], recv_sems.at[5 - n])
        total = half_own(me, both, 1 + n, dims) + came[0, dims].astype(jnp.float32)
        out[1 + n, dims] = total.astype(low)
        sends.go(out.at[1 + n, half], came.at[1 + n, half], send_sems.at[k], recv_sems.at[k], near[n])


def half_in(me, part, sibling, came, recv_sems):
    arrived(sibling.at[3], recv_sems.at[3])
    for n, half in ((0, 0), (1, 1), (0, 1), (1, 0)):
        k = 6 + 2 * n + (half != n)
        arrived(came.at[1 + n, pl.ds(2 * half, 2)], recv_sems.at[k])
    total = half_own(me, (part, sibling), 3, slice(None))
    return total + came[1].astype(jnp.float32) + came[2].astype(jnp.float32)


def half_scratch(tokens, width):
    piece = (4, tokens // 32, width)
    return [
        pltpu.VMEM((4,) + piece, jnp.bfloat16),
        pltpu.VMEM((3,) + piece, jnp.bfloat16),
        pltpu.VMEM((3,) + piece, jnp.bfloat16),
        SEM((10,)),
        SEM((10,)),
    ]


def gain_row(gains_ref, kind):
    rows = [jnp.sum(gains_ref[p, :, kind, :], axis=0, keepdims=True) for p in range(8)]
    return jnp.concatenate(rows, axis=1)


def allowed_keys(segcol, segrow, b, kb):
    same = segcol[b] == segrow[:, 256 * kb : 256 * kb + 256]
    if kb < b:
        return same
    rows = lax.broadcasted_iota(jnp.int32, (256, 256), 0)
    return jnp.logical_and(same, lanes((256, 256)) <= rows)


def norm_back(grad, vector, gain, scale):
    weighted = grad * gain
    inner = jnp.mean(weighted * vector, axis=-1, keepdims=True)
    return scale * weighted - vector * (scale * scale * scale * inner)


def permute_out(me, src_ref, dst_ref, send_sems, recv_sems, wait=False):
    half = dst_ref.shape[1] // 2
    for k in range(4):
        src = src_ref.at[k]
        dst = dst_ref.at[me.z // 2, pl.ds(half * me.x, half)]
        mine = jnp.logical_and(me.x == me.z % 2, me.z == k)
        spot = 2 * (me.z // 2) + me.x
        copy = remote(src, dst, send_sems.at[k], recv_sems.at[spot], (me.z % 2, me.block, k))
        if wait:
            pl.when(jnp.logical_not(mine))(lambda copy=copy: copy.wait_send())
            continue
        pl.when(jnp.logical_not(mine))(lambda copy=copy: copy.start())
        own = pltpu.make_async_copy(src, dst, recv_sems.at[spot])
        pl.when(mine)(lambda own=own: own.start())


def permuted_out(dst_ref, recv_sems):
    half = dst_ref.shape[1] // 2
    for j in (0, 1):
        for to in (0, 1):
            arrived(dst_ref.at[j, pl.ds(half * to, half)], recv_sems.at[2 * j + to])


def total_row(share):
    return jnp.sum(jnp.sum(share, axis=0), axis=0, keepdims=True)


def layer_kernel(
    x_ref, cot_ref, seg_ref, q_ref, k_ref, v_ref, g_ref, u_ref, o_ref, d_ref, ag_ref, fg_ref, hg_in,
    y_ref, gx_ref, dq_ref, dk_ref, dv_ref, dg_ref, du_ref, sums_ref, osum_out, dsum_out,
    xf, cf, wf, of, df, guf, segs, gains, n1, nf, gf, pre, qkv, segcol, cos_s, sin_s, att, attlow,
    totals, kept, part, part2, down, n2, gm, y_s, gi_s, mid, gmid,
    gates, hid, gboth, ga, gq, gk, gv, gpre, dd, dgu, do, dw,
    d_came, d_buf, gu_came, gu_buf, gu_total, gu_sum, o_came, o_buf, w_came, w_buf, w_total, w_sum,
    pack, packs, linep,
    sib1, out1, came1, hs1, hr1, sib2, out2, came2, hs2, hr2, sib3, out3, came3, hs3, hr3,
    ps, pr, as_, ar, xas, xar, ws, wr, us, ur, gs, gr, zq, zo, zd, zg, zu, rg, rd, ro, rw, cs, cr, ds, dr, ls, raw1, raw2, hg_low, hg_ref, osum_ref, dsum_ref,
):
    me = Place()
    x, z, p = (me.x, me.z, me.head)
    low, wide_t = (jnp.bfloat16, jnp.float32)
    across = [((x + 1) % 2, me.block, me.ahead(turn)) for turn in TURNS]
    meet([me.peer(*d) for d in PLANE[1:]] + [me.line(turn) for turn in TURNS] + across)
    sends, early = (Sends(), Sends())

    def local(src, dst, sem):
        copy = pltpu.make_async_copy(src, dst, sem)
        copy.start()
        return copy

    own_raw = [local(ref, dst, ls.at[6 + i]) for i, (ref, dst) in enumerate(((ag_ref, raw1), (fg_ref, raw2)))]
    own_head = local(hg_in, hg_low, ls.at[0])
    own_seg = local(seg_ref, segs.at[x], ls.at[1])
    sends.go(seg_ref, segs.at[x], ls.at[2], ls.at[3], me.peer(1, 0, 0))
    permute_in(me, x_ref, xf, ps.at[0], pr.at[0])
    permute_in(me, cot_ref, cf, ps.at[1], pr.at[1])
    own_o = local(o_ref, of.at[z], ls.at[4])
    own_d = local(d_ref, df.at[z], ls.at[5])
    wide, narrow = (q_ref.shape[1] // 8, k_ref.shape[1] // 8)
    cuts = ((q_ref, wide, 0), (k_ref, narrow, wide), (v_ref, narrow, wide + narrow))
    for i, d in enumerate(PLANE):
        t = me.index(*d)
        for n, (ref, width, off) in enumerate(cuts):
            src = ref.at[:, pl.ds(pl.multiple_of(t * width, 128), width)]
            dst = wf.at[p, z, :, pl.ds(off, width)]
            if i == 0:
                local(src, dst, wr.at[n])
            else:
                sends.go(src, dst, ws.at[3 * i + n], wr.at[3 * i + n], me.peer(*d))
    ff = g_ref.shape[1] // 8
    for copy in own_raw + [own_head]:
        copy.wait()
    hg_ref[...] = hg_low[...].astype(wide_t)
    piece = raw1.shape[1]
    rows = [raw1[...].astype(wide_t), raw2[...].astype(wide_t), jnp.zeros((6, piece), wide_t)]
    rows = [jnp.concatenate(rows, axis=0), jnp.zeros((8, 128 - piece), wide_t)]
    rows = jnp.concatenate(rows, axis=1)
    gains[p, z] = pltpu.roll(rows, piece * z, 1)
    arrived(xf.at[me.block, z, x], pr.at[0, z])
    piece_start(me, sends, xf, 0, xas, xar)
    for turn in TURNS:
        sends.go(gains.at[p, z], gains.at[p, z], gs.at[turn], gr.at[turn], me.line(turn))
    for i, d in enumerate(PLANE):
        t = me.index(*d)
        for n, (ref, width, off) in enumerate(cuts):
            arrived(wf.at[t, z, :, pl.ds(off, width)], wr.at[3 * i + n])
    qkv_part = lambda k: wf.at[:, k]
    o_part = lambda k: of.at[k]
    d_part = lambda k: df.at[k]
    gate_part = lambda k: guf.at[:, k, :, pl.ds(0, ff)]
    up_part = lambda k: guf.at[:, k, :, pl.ds(ff, ff)]
    line_spread_first(me, sends, qkv_part(z), qkv_part, zq)
    for turn in (1, 3, 2):
        k = (z + turn) % 4
        arrived(xf.at[me.block, k, x], pr.at[0, k])
        piece_start(me, sends, xf, turn, xas, xar)
    line_spread_first(me, sends, qkv_part(z), qkv_part, zq, second=True)
    line_spread(me, sends, o_ref, o_part, zo)
    piece_relay(me, sends, xf, xas, xar, PIECES[:2])
    line_forward(me, sends, qkv_part, zq)
    piece_relay(me, sends, xf, xas, xar, PIECES[2:])
    for turn in TURNS:
        arrived(gains.at[p, me.behind(turn)], gr.at[turn])
    for i, d in enumerate(PLANE[1:]):
        sends.go(gains.at[p], gains.at[p], gs.at[4 + i], gr.at[4 + i], me.peer(*d))
    for i, d in enumerate(PLANE):
        t = me.index(*d)
        for n, ref in enumerate((g_ref, u_ref)):
            src = ref.at[:, pl.ds(pl.multiple_of(t * ff, 128), ff)]
            dst = guf.at[p, z, :, pl.ds(n * ff, ff)]
            if i == 0:
                local(src, dst, ur.at[n])
            else:
                sends.go(src, dst, us.at[2 * i + n], ur.at[2 * i + n], me.peer(*d))
    permuted_in(me, cf, pr.at[1])
    spread_start(me, sends, me.shard(cf), cf, as_.at[1], ar.at[1])
    own_seg.wait()
    arrived(segs.at[(x + 1) % 2], ls.at[3])
    head_dim = hg_ref.shape[1]
    segrow = segs[z % 2, pl.ds(z // 2, 1), :]
    tokens = segrow.shape[1]
    column = jnp.transpose(jnp.broadcast_to(segrow.astype(wide_t), (8, tokens)))[:, :1]
    segcol[...] = column.astype(jnp.int32).reshape(4, 256, 1)
    half_lane = (lanes((1, head_dim)) % (head_dim // 2)).astype(wide_t)
    inverse = jnp.exp(half_lane * (-2.0 * math.log(THETA) / head_dim))
    steps = lax.broadcasted_iota(jnp.int32, (32, head_dim), 0).astype(wide_t) * inverse
    cl, sl = (jnp.cos(steps), jnp.sin(steps))
    ch, sh = (jnp.cos(steps * 32.0), jnp.sin(steps * 32.0))
    doc_cos, doc_sin = ([], [])
    for doc in range(DOCS):
        start = jnp.sum((segrow < doc).astype(wide_t), axis=1, keepdims=True)
        doc_cos.append(jnp.cos(start * inverse))
        doc_sin.append(jnp.sin(start * inverse))
    for b in range(4):
        hi_c, hi_s = (ch[8 * b : 8 * b + 8][:, None, :], sh[8 * b : 8 * b + 8][:, None, :])
        cos_at = (hi_c * cl[None] - hi_s * sl[None]).reshape(256, head_dim)
        sin_at = (hi_s * cl[None] + hi_c * sl[None]).reshape(256, head_dim)
        column = segcol[b]
        cd, sd = (jnp.broadcast_to(v[0], (256, head_dim)) for v in (doc_cos, doc_sin))
        for doc in range(1, DOCS):
            cd = jnp.where(column == doc, doc_cos[doc], cd)
            sd = jnp.where(column == doc, doc_sin[doc], sd)
        cos_s[b] = cos_at * cd + sin_at * sd
        sin_s[b] = sin_at * cd - cos_at * sd
    piece_far(me, sends, xf, xas, xar)
    for i, d in enumerate(PLANE[1:]):
        arrived(gains.at[me.index(*d)], gr.at[4 + i])
    gain_one, gain_two = (gain_row(gains, 0), gain_row(gains, 1))
    piece_finish(me, xf, xar)

    @pl.loop(0, 4)
    def _(b):
        rows = xf[b].reshape(256, -1).astype(wide_t)
        n1[b] = (rows * head_scale(rows) * gain_one).astype(low)

    line_finish(me, qkv_part, zq)

    own_o.wait()
    line_forward(me, sends, o_part, zo)
    for i, d in enumerate(PLANE):
        t = me.index(*d)
        for n in (0, 1):
            arrived(guf.at[t, z, :, pl.ds(n * ff, ff)], ur.at[2 * i + n])
    line_spread(me, sends, gate_part(z), gate_part, zg)
    line_spread(me, sends, up_part(z), up_part, zu)
    spread_relay(me, sends, cf, as_.at[1], ar.at[1])
    @pl.loop(0, 4)
    def _(b):
        rows = mat(n1[b], wf[...].reshape(-1, wf.shape[3]))
        pre[b] = rows
        cosine, sine = (cos_s[b], sin_s[b])
        for h in range(3):
            v = rows[:, head_dim * h : head_dim * (h + 1)]
            n = v * head_scale(v) * hg_ref[pl.ds(h // 2, 1), :]
            qkv[b, :, pl.ds(head_dim * h, head_dim)] = (n * cosine + turned(n) * sine).astype(low)
        qkv[b, :, pl.ds(3 * head_dim, head_dim)] = rows[:, 3 * head_dim :].astype(low)

    top = lambda r: jnp.max(jnp.abs(hg_ref[pl.ds(r, 1), :]), axis=1, keepdims=True)
    bound = math.sqrt(head_dim) * top(0) * top(1)
    scale = head_dim ** (-0.5)
    key_at, value_at = (pl.ds(2 * head_dim, head_dim), pl.ds(3 * head_dim, head_dim))

    def weights_of(b, kb, query):
        s = mat_right(query, qkv[kb, :, key_at]) * scale
        return jnp.where(allowed_keys(segcol, segrow, b, kb), jnp.exp(s - bound), 0.0)

    for b in range(4):

        @pl.loop(0, 2)
        def _(h, b=b):
            at = pl.ds(pl.multiple_of(head_dim * h, head_dim), head_dim)
            query = qkv[b, :, at]
            total, mixed = (None, None)
            for kb in range(b + 1):
                w = weights_of(b, kb, query)
                t = jnp.sum(w, axis=1, keepdims=True)
                kept[h, b * (b + 1) // 2 + kb] = w.astype(low)
                m = mat(w.astype(low), qkv[kb, :, value_at])
                total = t if kb == 0 else total + t
                mixed = m if kb == 0 else mixed + m
            mixed = mixed / total
            totals[b, h] = total
            att[b, :, at] = mixed
            attlow[b, :, at] = mixed.astype(low)

    line_finish(me, o_part, zo)

    @pl.loop(0, 4)
    def _(b):
        rows = mat(attlow[b], of[...].reshape(-1, of.shape[2])).astype(low)
        part[b] = rows.reshape(part.shape[1:])
        half_block(me, part, sib1, hs1, hr1, b)

    for b in range(4):
        half_block(me, part, sib1, hs1, hr1, b, early)
    half_out(me, early, part, sib1, out1, came1, hs1, hr1)
    line_forward(me, sends, gate_part, zg)
    half_relay(me, early, part, sib1, out1, came1, hs1, hr1)
    middle = xf[me.block, :, x].astype(wide_t) + half_in(me, part, sib1, came1, hr1)
    mid[...] = middle
    n2[...] = (middle * head_scale(middle) * gain_two).astype(low)
    own_n = local(n2, me.shard(nf), ls.at[8])
    spread_start(me, sends, n2, nf, as_.at[2], ar.at[2])
    line_forward(me, sends, up_part, zu)
    line_spread(me, sends, d_ref, d_part, zd)
    spread_relay(me, sends, nf, as_.at[2], ar.at[2])
    line_forward(me, sends, d_part, zd)
    spread_far(me, sends, nf, as_.at[2], ar.at[2])
    spread_finish(me, nf, ar.at[2])
    own_n.wait()
    line_finish(me, gate_part, zg)
    line_finish(me, up_part, zu)

    @pl.loop(0, 4)
    def _(b):
        both = mat(nf[b].reshape(256, -1), guf[...].reshape(-1, 2 * ff))
        gates[b] = both
        gate, up = (both[:, :ff], both[:, ff:])
        hid[b] = (gate / (1.0 + jnp.exp(-gate)) * up).astype(low)

    spread_far(me, sends, cf, as_.at[1], ar.at[1])
    spread_finish(me, cf, ar.at[1])
    own_d.wait()
    dd[...] = mat_left(hid[...].reshape(-1, ff), cf[...].reshape(tokens, -1)).astype(low).reshape(dd.shape)
    own_dd = lambda k: dd.at[k]
    reduce_start(me, sends, own_dd, d_came, rd)
    line_finish(me, d_part, zd)

    @pl.loop(0, 4)
    def _(b):
        both = gates[b]
        gate, up = (both[:, :ff], both[:, ff:])
        sig = 1.0 / (1.0 + jnp.exp(-gate))
        grad = mat_right(cf[b].reshape(256, -1), df[...].reshape(ff, -1))
        gboth[b, :, pl.ds(0, ff)] = (grad * up * sig * (1.0 + gate * (1.0 - sig))).astype(low)
        gboth[b, :, pl.ds(ff, ff)] = (grad * (gate * sig)).astype(low)
        rows = mat_right(gboth[b], guf[...].reshape(-1, 2 * ff)).astype(low)
        part2[b] = rows.reshape(part2.shape[1:])
        half_block(me, part2, sib2, hs2, hr2, b)

    for b in range(4):
        half_block(me, part2, sib2, hs2, hr2, b, sends)
    half_out(me, sends, part2, sib2, out2, came2, hs2, hr2)

    @pl.loop(0, 4)
    def _(b):
        rows = nf[:, :, :, :, pl.ds(pl.multiple_of(256 * b, 256), 256)].reshape(-1, 256)
        grad = mat_left(rows, gboth[...].reshape(-1, 2 * ff)).astype(low)
        dgu[pl.ds(2 * b, 2)] = grad.reshape((2,) + dgu.shape[1:])

    own_gu = lambda k: dgu.at[:, k]
    reduce_start(me, sends, own_gu, gu_came, rg)
    half_relay(me, sends, part2, sib2, out2, came2, hs2, hr2)
    reduce_join(me, sends, own_dd, d_came, d_buf, rd)
    grad = half_in(me, part2, sib2, came2, hr2)
    middle = mid[...]
    r = head_scale(middle)
    total = cf[me.block, :, x].astype(wide_t) + norm_back(grad, middle, gain_two, r)
    gmid[...] = total
    gm[...] = total.astype(low)
    own_gm = local(gm, me.shard(gf), ls.at[9])
    spread_start(me, sends, gm, gf, as_.at[3], ar.at[3])
    share = total_row(grad * middle * r)
    for i in range(8):
        pack[pl.ds(8 + i, 1)] = share[:, 128 * i : 128 * i + 128]

    @pl.loop(0, 4)
    def _(b):
        rows = mat(hid[b], df[...].reshape(ff, -1)).astype(low)
        down[b] = rows.reshape(down.shape[1:])
        half_block(me, down, sib3, hs3, hr3, b)

    for b in range(4):
        half_block(me, down, sib3, hs3, hr3, b, sends)
    spread_relay(me, sends, gf, as_.at[3], ar.at[3])
    half_out(me, sends, down, sib3, out3, came3, hs3, hr3)
    reduce_join(me, sends, own_gu, gu_came, gu_buf, rg)
    spread_far(me, sends, gf, as_.at[3], ar.at[3])
    spread_finish(me, gf, ar.at[3])
    own_gm.wait()

    half_relay(me, sends, down, sib3, out3, came3, hs3, hr3)
    gk[...] = jnp.zeros_like(gk)
    gv[...] = jnp.zeros_like(gv)
    for b in range(4):
        ga[b] = mat_right(gf[b].reshape(256, -1), of[...].reshape(-1, of.shape[2])).astype(low)

        @pl.loop(0, 2)
        def _(h, b=b):
            at = pl.ds(pl.multiple_of(head_dim * h, head_dim), head_dim)
            query, grad = (qkv[b, :, at], ga[b, :, at])
            inv = 1.0 / totals[b, h]
            scaled = grad.astype(wide_t) * inv
            delta = jnp.sum(scaled * att[b, :, at], axis=1, keepdims=True)
            scaled = scaled.astype(low)
            grad_query = None
            for kb in range(b + 1):
                w = kept[h, b * (b + 1) // 2 + kb]
                gp = mat_right(scaled, qkv[kb, :, value_at])
                gsc = (w.astype(wide_t) * (gp - delta)).astype(low)
                m = mat(gsc, qkv[kb, :, key_at])
                grad_query = m if kb == 0 else grad_query + m
                gk[kb] += mat_left(gsc, query)
                gv[kb] += mat_left(w, scaled)
            gq[b, :, at] = grad_query

        if b == 2:
            y_s[...] = (mid[...] + half_in(me, down, sib3, came3, hr3)).astype(low)
            permute_out(me, y_s, y_ref, cs.at[0], cr.at[0])
    do[...] = mat_left(attlow[...].reshape(tokens, -1), gf[...].reshape(tokens, -1)).astype(low).reshape(do.shape)
    own_do = lambda k: do.at[k]
    reduce_start(me, sends, own_do, o_came, ro)
    pack[pl.ds(16, 8)] = jnp.zeros((8, 128), wide_t)

    @pl.loop(0, 4)
    def _(b):
        cosine, sine = (cos_s[b], sin_s[b])
        for h in range(3):
            at = pl.ds(head_dim * h, head_dim)
            source = gq[b, :, at] if h < 2 else gk[b]
            go = (source * scale).astype(low).astype(wide_t)
            gh = go * cosine - turned(go * sine)
            v = pre[b, :, at]
            r = head_scale(v)
            n = v * r
            pack[pl.ds(16 + h // 2, 1)] += jnp.sum(gh * n, axis=0, keepdims=True)
            gn = gh * hg_ref[pl.ds(h // 2, 1), :]
            gpre[b, :, at] = (r * (gn - n * jnp.mean(gn * n, axis=-1, keepdims=True))).astype(low)
        gpre[b, :, value_at] = gv[b].astype(low)

    early.drain()

    @pl.loop(0, 4)
    def _(b):
        rows = mat_right(gpre[b], wf[...].reshape(-1, wf.shape[3])).astype(low)
        part[b] = rows.reshape(part.shape[1:])
        half_block(me, part, sib1, hs1, hr1, b)

    for b in range(4):
        half_block(me, part, sib1, hs1, hr1, b, sends)
    half_out(me, sends, part, sib1, out1, came1, hs1, hr1)
    @pl.loop(0, 4)
    def _(b):
        rows = n1[:, :, pl.ds(pl.multiple_of(256 * b, 256), 256)].reshape(-1, 256)
        grad = mat_left(rows, gpre[...].reshape(tokens, -1)).astype(low)
        grad = grad.reshape((2,) + dw.shape[2:-1] + (2 * dw.shape[-1],))
        for n in (0, 1):
            dw[n, pl.ds(2 * b, 2)] = grad[..., n * dw.shape[-1] : (n + 1) * dw.shape[-1]]

    own_dw = [lambda k, n=n: dw.at[n, :, k] for n in (0, 1)]
    for joins in (True, False):
        for n in (0, 1):
            reduce_start(me, sends, own_dw[n], w_came.at[n], rw.at[n], joins, not joins)
    half_relay(me, sends, part, sib1, out1, came1, hs1, hr1)
    reduce_join(me, sends, own_do, o_came, o_buf, ro)
    reduce_total(me, own_gu, gu_came, gu_total, rg)
    gu_sum[...] = gu_total[...].astype(low)
    for i, d in enumerate(PLANE):
        t = me.index(*d)
        for n, ref in enumerate((dg_ref, du_ref)):
            src = gu_sum.at[t, :, pl.ds(n * ff, ff)]
            dst = ref.at[:, pl.ds(pl.multiple_of(p * ff, 128), ff)]
            if i == 0:
                local(src, dst, dr.at[n])
            else:
                sends.go(src, dst, ds.at[2 * i + n], dr.at[2 * i + n], me.peer(*d))
    reduce_total(me, own_dd, d_came, dsum_ref, rd)
    dsum_copy = local(dsum_ref, dsum_out, ls.at[6])
    for n in (0, 1):
        reduce_join(me, sends, own_dw[n], w_came.at[n], w_buf.at[n], rw.at[n])
    grad = half_in(me, part, sib1, came1, hr1)
    rows = xf[me.block, :, x].astype(wide_t)
    r = head_scale(rows)
    share = total_row(grad * rows * r)
    for i in range(8):
        pack[pl.ds(i, 1)] = share[:, 128 * i : 128 * i + 128]
    for i, d in enumerate(PLANE[1:]):
        sends.go(pack, packs.at[i], gs.at[11 + i], gr.at[11 + i], me.peer(*d))
    gi_s[...] = (gmid[...] + norm_back(grad, rows, gain_one, r)).astype(low)
    total = pack[...]
    for i in range(7):
        arrived(packs.at[i], gr.at[11 + i])
        total = total + packs[i]
    packs[7] = total
    for turn in TURNS:
        sends.go(packs.at[7], linep.at[turn - 1], gs.at[17 + turn], gr.at[17 + turn], me.line(turn))
    permute_out(me, gi_s, gx_ref, cs.at[1], cr.at[1])
    backs = (((dq_ref, wide, 0),), ((dk_ref, narrow, 0), (dv_ref, narrow, narrow)))
    for block in (0, 1):
        reduce_total(me, own_dw[block], w_came.at[block], w_total, rw.at[block])
        w_sum[block] = w_total[...].astype(low)
        for i, d in enumerate(PLANE):
            t = me.index(*d)
            for n, (ref, cols, off) in enumerate(backs[block]):
                src = w_sum.at[block, t, :, pl.ds(off, cols)]
                dst = ref.at[:, pl.ds(pl.multiple_of(p * cols, 128), cols)]
                k = 16 + 3 * i + block + n
                if i == 0:
                    local(src, dst, dr.at[k])
                else:
                    sends.go(src, dst, ds.at[k], dr.at[k], me.peer(*d))
    reduce_total(me, own_do, o_came, osum_ref, ro)
    osum_copy = local(osum_ref, osum_out, ls.at[7])
    for turn in TURNS:
        arrived(linep.at[turn - 1], gr.at[17 + turn])
        total = total + linep[turn - 1]
    sums_ref[...] = total
    for i, d in enumerate(PLANE):
        t = me.index(*d)
        for n, ref in enumerate((dg_ref, du_ref)):
            arrived(ref.at[:, pl.ds(pl.multiple_of(t * ff, 128), ff)], dr.at[2 * i + n])
        for n, (ref, cols, off) in enumerate(backs[0] + backs[1]):
            arrived(ref.at[:, pl.ds(pl.multiple_of(t * cols, 128), cols)], dr.at[16 + 3 * i + n])
    dsum_copy.wait()
    osum_copy.wait()
    permuted_out(y_ref, cr.at[0])
    permuted_out(gx_ref, cr.at[1])
    permute_in(me, x_ref, xf, ps.at[0], pr.at[0], wait=True)
    permute_in(me, cot_ref, cf, ps.at[1], pr.at[1], wait=True)
    permute_out(me, y_s, y_ref, cs.at[0], cr.at[0], wait=True)
    permute_out(me, gi_s, gx_ref, cs.at[1], cr.at[1], wait=True)
    sends.drain()


def layer_step(x, cot, seg, q, k, v, g, u, o, d, gain, gain_two, head_gains):
    tokens, width = (16 * x.shape[1], x.shape[2])
    rows, low, wide = (q.shape[0], jnp.bfloat16, jnp.float32)
    cols = (q.shape[1] + 2 * k.shape[1]) // 8
    att_cols, head_dim = (q.shape[1] // 8, k.shape[1] // 8)
    ff = g.shape[1] // 8
    full = full_shape(tokens, width)
    piece = (4, tokens // 32, width)
    quarter = tokens // 4
    shape, buf = (jax.ShapeDtypeStruct, pltpu.VMEM)
    blocks = lambda n, kind: buf((4, quarter, n), kind)
    return pl.pallas_call(
        layer_kernel,
        name="layer_step",
        out_shape=(
            shape(x.shape, low), shape(x.shape, low), shape(q.shape, low), shape(k.shape, low),
            shape(v.shape, low), shape(g.shape, low), shape(u.shape, low), shape((24, 128), wide),
            shape(o.shape, wide), shape(d.shape, wide),
        ),
        in_specs=[ANY] * 13,
        out_specs=(ANY,) * 7 + (VMEM, ANY, ANY),
        scratch_shapes=[
            buf(full, low), buf(full, low), buf((8, 4, rows, cols), low), buf((4,) + o.shape, low),
            buf((4,) + d.shape, low), buf((8, 4, rows, 2 * ff), low), buf((2,) + seg.shape, seg.dtype),
            buf((8, 4, 8, 128), wide), blocks(width, low), buf(full, low), buf(full, low),
            blocks(cols, wide), blocks(cols, low), blocks(1, jnp.int32), blocks(head_dim, wide),
            blocks(head_dim, wide), blocks(att_cols, wide), blocks(att_cols, low),
            buf((4, 2, quarter, 1), wide), buf((2, 10, quarter, quarter), low), buf(full, low), buf(full, low), buf(full, low),
            buf(piece, low), buf(piece, low), buf(piece, low), buf(piece, low), buf(piece, wide),
            buf(piece, wide),
            blocks(2 * ff, wide), blocks(ff, low), blocks(2 * ff, low), blocks(att_cols, low), blocks(att_cols, wide),
            blocks(head_dim, wide), blocks(head_dim, wide), blocks(cols, low),
            buf((4,) + d.shape, low), buf((8, 4, rows, 2 * ff), low), buf((4,) + o.shape, low),
            buf((2, 8, 4, rows, cols // 2), low),
            buf((4,) + d.shape, low), buf(d.shape, low),
            buf((4, 8, rows, 2 * ff), low), buf((8, rows, 2 * ff), low), buf((8, rows, 2 * ff), wide),
            buf((8, rows, 2 * ff), low),
            buf((4,) + o.shape, low), buf(o.shape, low),
            buf((2, 4, 8, rows, cols // 2), low), buf((2, 8, rows, cols // 2), low),
            buf((8, rows, cols // 2), wide), buf((2, 8, rows, cols // 2), low),
            buf((24, 128), wide), buf((8, 24, 128), wide), buf((3, 24, 128), wide),
        ]
        + half_scratch(tokens, width) * 3
        + [SEM((2, 4)), SEM((2, 4)), SEM((4, 11)), SEM((4, 11)), SEM((28,)), SEM((28,)), SEM((24,)), SEM((24,)), SEM((16,)), SEM((16,))]
        + [SEM((21,)), SEM((21,))]
        + [SEM((2, 5))] * 5
        + [SEM((2, 4))] * 3
        + [SEM((2, 2, 4))]
        + [SEM((2, 4)), SEM((2, 4)), SEM((40,)), SEM((40,)), SEM((10,)),
            buf(gain.shape, low), buf(gain.shape, low), buf(head_gains.shape, low), buf(head_gains.shape, wide),
            buf(o.shape, wide), buf(d.shape, wide)],
        compiler_params=pltpu.CompilerParams(
            collective_id=0, has_side_effects=True, vmem_limit_bytes=67043328
        ),
    )(x, cot, seg, q, k, v, g, u, o, d, gain, gain_two, head_gains)


def finish_kernel(sums_ref, *refs):
    half = (len(refs) - 3) // 2
    for src, dst in zip(refs[:half], refs[half : 2 * half]):
        dst[...] = src[...].astype(dst.dtype)
    attn_ref, ffn_ref, head_ref = refs[2 * half :]
    z = lax.axis_index("uly")
    head = 4 * lax.axis_index("fsdp") + lax.axis_index("blk")
    piece, share = (attn_ref.shape[1], head_ref.shape[1])
    rows = [sums_ref[pl.ds(head, 1), :], sums_ref[pl.ds(8 + head, 1), :], jnp.zeros((6, 128), jnp.float32)]
    rows = pltpu.roll(jnp.concatenate(rows, axis=0), 128 - piece * z, 1)
    attn_ref[...] = rows[0:1, :piece]
    ffn_ref[...] = rows[1:2, :piece]
    head_ref[...] = pltpu.roll(sums_ref[16:24, :], 128 - (4 * head + z) * share, 1)[0:2, :share]


def finish_step(piece, share, sums, *arrays):
    return pl.pallas_call(
        finish_kernel,
        name="finish_step",
        out_shape=tuple(
            jax.ShapeDtypeStruct(v.shape, v.dtype if i < 2 else jnp.float32) for i, v in enumerate(arrays)
        )
        + tuple(jax.ShapeDtypeStruct(v, jnp.float32) for v in ((1, piece), (1, piece), (2, share))),
        in_specs=[VMEM] * (1 + len(arrays)),
        out_specs=(VMEM,) * (3 + len(arrays)),
    )(sums, *arrays)


def plane_body(
    inputs, segments, attn_gain, head_gains, query_weight, key_matrix, value_matrix, out_weight,
    ffn_gain, gate_weight, up_weight, down_weight, cotangent,
):
    outputs, grad_inputs, q_grad, k_grad, v_grad, g_grad, u_grad, sums, out_grad, down_grad = layer_step(
        inputs, cotangent, segments, query_weight, key_matrix, value_matrix, gate_weight, up_weight,
        out_weight, down_weight, attn_gain[None], ffn_gain[None], head_gains,
    )
    (
        outputs, grad_inputs, q_grad, k_grad, v_grad, out_grad, g_grad, u_grad, down_grad, attn_gain_grad,
        ffn_gain_grad, head_gain_grad,
    ) = finish_step(
        attn_gain.shape[0], head_gains.shape[1] // 32, sums, outputs, grad_inputs, q_grad, k_grad, v_grad,
        out_grad, g_grad, u_grad, down_grad,
    )
    return (
        outputs, grad_inputs, attn_gain_grad[0], head_gain_grad, q_grad, k_grad, v_grad, out_grad,
        ffn_gain_grad[0], g_grad, u_grad, down_grad,
    )


def fits_plane(mesh, seq_count, heads):
    shape = mesh.shape
    return (shape["fsdp"], shape["blk"], shape["uly"]) == (2, 4, 4) and seq_count == 4 and heads == 8


def solution(mesh):
    def step(*arrays):
        seq_count = arrays[0].shape[0]
        heads = arrays[5].shape[1] // arrays[3].shape[1]
        chosen = plane_body if fits_plane(mesh, seq_count, heads) else body
        return mapped(chosen)(*arrays)

    mapped = functools.partial(
        jax.shard_map,
        mesh=mesh,
        in_specs=(
            P("fsdp", ("blk", "uly"), None),
            P("fsdp", None),
            P(("fsdp", "blk", "uly")),
            P(),
            P(("fsdp", "blk", "uly"), None),
            P(("fsdp", "blk", "uly"), None),
            P(("fsdp", "blk", "uly"), None),
            P(("fsdp", "blk", "uly"), None),
            P(("fsdp", "blk", "uly")),
            P(("fsdp", "blk", "uly"), None),
            P(("fsdp", "blk", "uly"), None),
            P(("fsdp", "blk", "uly"), None),
            P("fsdp", ("blk", "uly"), None),
        ),
        out_specs=(
            P("fsdp", ("blk", "uly"), None),
            P("fsdp", ("blk", "uly"), None),
            P(("fsdp", "blk", "uly")),
            P(None, ("fsdp", "blk", "uly")),
            P(("fsdp", "blk", "uly"), None),
            P(("fsdp", "blk", "uly"), None),
            P(("fsdp", "blk", "uly"), None),
            P(("fsdp", "blk", "uly"), None),
            P(("fsdp", "blk", "uly")),
            P(("fsdp", "blk", "uly"), None),
            P(("fsdp", "blk", "uly"), None),
            P(("fsdp", "blk", "uly"), None),
        ),
        check_vma=False,
    )
    return step
```

```python
import functools
import math

import jax
import jax.numpy as jnp
from jax import lax
from jax.experimental import pallas as pl
from jax.experimental.pallas import tpu as pltpu
from jax.sharding import PartitionSpec as P

DOCS = 4


EPSILON = 1e-06
THETA = 1000000.0


def passed_along(value, axis, steps):
    count = lax.axis_size(axis)
    first, last = (max(0, -steps), min(count, count - steps))
    return lax.ppermute(value, axis, [(source, source + steps) for source in range(first, last)])


def from_behind(value, axis, steps):
    count = lax.axis_size(axis)
    pairs = [(source, (source + steps) % count) for source in range(count)]
    return lax.ppermute(value, axis, pairs)


def rms_norm(vector, weight):
    mean_square = jnp.mean(vector * vector, axis=-1, keepdims=True)
    return vector * lax.rsqrt(mean_square + EPSILON) * weight


def rotate(vector, cosine, sine_table):
    half_width = vector.shape[-1] // 2
    turned = jnp.concatenate([-vector[..., half_width:], vector[..., :half_width]], axis=-1)
    return vector * cosine + turned * sine_table


def prepare(query_pre, key_before_rotate, gains, cosine, sine_table):
    cos_heads = cosine[:, :, None, :]
    sin_heads = sine_table[:, :, None, :]
    query_rot = rotate(rms_norm(query_pre, gains[0]), cos_heads, sin_heads)
    key_rot = rotate(rms_norm(key_before_rotate, gains[1]), cos_heads, sin_heads)
    return (query_rot, key_rot)


def swiglu(gate_rows, up_rows):
    return jax.nn.silu(gate_rows) * up_rows


def fetch_attention(attn_gain, query_weight, key_matrix, value_matrix, out_weight):
    return (
        lax.all_gather(attn_gain, ("fsdp", "blk", "uly"), axis=0, tiled=True),
        lax.all_gather(query_weight, ("fsdp", "blk", "uly"), axis=0, tiled=True),
        lax.all_gather(key_matrix, ("fsdp", "blk", "uly"), axis=0, tiled=True),
        lax.all_gather(value_matrix, ("fsdp", "blk", "uly"), axis=0, tiled=True),
        lax.all_gather(out_weight, ("fsdp", "blk", "uly"), axis=0, tiled=True),
    )


def fetch_feedforward(ffn_gain, gate_weight, up_weight, down_weight):
    return (
        lax.all_gather(ffn_gain, ("fsdp", "blk", "uly"), axis=0, tiled=True),
        lax.all_gather(gate_weight, ("fsdp", "blk", "uly"), axis=0, tiled=True),
        lax.all_gather(up_weight, ("fsdp", "blk", "uly"), axis=0, tiled=True),
        lax.all_gather(down_weight, ("fsdp", "blk", "uly"), axis=0, tiled=True),
    )


def body(
    inputs,
    segments,
    attn_gain,
    head_gains,
    query_weight,
    key_matrix,
    value_matrix,
    out_weight,
    ffn_gain,
    gate_weight,
    up_weight,
    down_weight,
    cotangent,
):
    seq_count, tok_count, model_width = inputs.shape
    head_dim = head_gains.shape[1]
    query_heads = query_weight.shape[1] // head_dim
    value_heads = key_matrix.shape[1] // head_dim
    heads_per_group = query_heads // value_heads
    uly_size = lax.axis_size("uly")
    blk_size = lax.axis_size("blk")
    blk_index = lax.axis_index("blk")
    uly_index = lax.axis_index("uly")
    offset = (blk_index * uly_size + uly_index) * tok_count
    doc_ids = jnp.arange(DOCS, dtype=jnp.int32)
    starts = jnp.sum((segments[:, None, :] < doc_ids[None, :, None]).astype(jnp.int32), axis=2)
    local_segs = lax.dynamic_slice_in_dim(segments, offset, tok_count, 1)
    doc_start = jnp.sum(
        jnp.where(local_segs[:, :, None] == doc_ids[None, None, :], starts[:, None, :], 0), axis=2
    )
    token_place = (offset + jnp.arange(tok_count, dtype=jnp.int32)[None, :] - doc_start).astype(
        jnp.float32
    )
    inverse = jnp.exp(
        jnp.arange(head_dim // 2, dtype=jnp.float32) * (-2.0 * math.log(THETA) / head_dim)
    )
    angles = token_place[..., None] * inverse
    cosine = jnp.concatenate([jnp.cos(angles), jnp.cos(angles)], axis=-1)
    sine_table = jnp.concatenate([jnp.sin(angles), jnp.sin(angles)], axis=-1)
    floats = inputs.astype(jnp.float32)
    gain_one, query_full, key_full, value_full, out_full = fetch_attention(
        attn_gain, query_weight, key_matrix, value_matrix, out_weight
    )
    normed_float, norm_pull_one = jax.vjp(rms_norm, floats, gain_one.astype(jnp.float32))
    normalized_input = normed_float.astype(jnp.bfloat16)
    query_pre = jnp.einsum(
        "std,de->ste", normalized_input, query_full, preferred_element_type=jnp.float32
    ).reshape(seq_count, tok_count, query_heads, head_dim)
    key_before_rotate = jnp.einsum(
        "std,de->ste", normalized_input, key_full, preferred_element_type=jnp.float32
    ).reshape(seq_count, tok_count, value_heads, head_dim)
    rows_of_value = (
        jnp.einsum("std,de->ste", normalized_input, value_full, preferred_element_type=jnp.float32)
        .astype(jnp.bfloat16)
        .reshape(seq_count, tok_count, value_heads, head_dim)
    )
    head_float = head_gains.astype(jnp.float32)

    def prepare_local(query_arg, key_arg, gains_arg):
        return prepare(query_arg, key_arg, gains_arg, cosine, sine_table)

    (query_rot, key_rot), prep_pull = jax.vjp(
        prepare_local, query_pre, key_before_rotate, head_float
    )
    query_local, key_local, value_local = (
        lax.all_to_all(
            query_rot.astype(jnp.bfloat16), "uly", split_axis=2, concat_axis=1, tiled=True
        ),
        lax.all_to_all(
            key_rot.astype(jnp.bfloat16), "uly", split_axis=2, concat_axis=1, tiled=True
        ),
        lax.all_to_all(rows_of_value, "uly", split_axis=2, concat_axis=1, tiled=True),
    )
    block_len = query_local.shape[1]
    local_kv = key_local.shape[2]
    query_group = query_local.reshape(seq_count, block_len, local_kv, heads_per_group, head_dim)
    bound = math.sqrt(head_dim) * jnp.max(jnp.abs(head_float[0])) * jnp.max(jnp.abs(head_float[1]))
    scale = head_dim ** (-0.5)
    query_index = blk_index * block_len + jnp.arange(block_len, dtype=jnp.int32)
    query_segs = lax.dynamic_slice_in_dim(segments, blk_index * block_len, block_len, 1)

    def block_weights(keys_in, source):
        key_index = source * block_len + jnp.arange(block_len, dtype=jnp.int32)
        key_segs = lax.dynamic_slice_in_dim(segments, source * block_len, block_len, 1)
        allowed = (key_index[None, None, :] <= query_index[None, :, None]) & (
            key_segs[:, None, :] == query_segs[:, :, None]
        )
        scores = (
            jnp.einsum(
                "sqhgd,skhd->shgqk", query_group, keys_in, preferred_element_type=jnp.float32
            )
            * scale
        )
        return jnp.where(allowed[:, None, None], jnp.exp(scores - bound), 0.0)

    def absorb(stats, key_value, source):
        row_sums, summed = stats
        weights = block_weights(key_value[0], source)
        row_sums = row_sums + jnp.sum(weights, axis=-1)
        summed = summed + jnp.einsum(
            "shgqk,skhd->sqhgd",
            weights.astype(jnp.bfloat16),
            key_value[1],
            preferred_element_type=jnp.float32,
        )
        return (row_sums, summed)

    own_pair = jnp.stack([key_local, value_local])
    start_stats = (
        jnp.zeros((seq_count, local_kv, heads_per_group, block_len), jnp.float32),
        jnp.zeros((seq_count, block_len, local_kv, heads_per_group, head_dim), jnp.float32),
    )
    first_stats = absorb(start_stats, own_pair, blk_index)

    def forward_turn(turn_index, carry):
        key_value, stats_in = carry
        key_value = passed_along(key_value, "blk", 1)
        stats_in = lax.cond(
            turn_index <= blk_index,
            lambda holding: absorb(holding, key_value, blk_index - turn_index),
            lambda holding: holding,
            stats_in,
        )
        return (key_value, stats_in)

    moved_pair, (row_totals, summed_all) = lax.fori_loop(
        1, blk_size, forward_turn, (own_pair, first_stats)
    )
    attended = summed_all / jnp.transpose(row_totals, (0, 3, 1, 2))[..., None]
    attended_tok = lax.all_to_all(
        attended.reshape(seq_count, block_len, local_kv * heads_per_group, head_dim).astype(
            jnp.bfloat16
        ),
        "uly",
        split_axis=1,
        concat_axis=2,
        tiled=True,
    ).reshape(seq_count, tok_count, query_heads * head_dim)
    middle = floats + jnp.einsum(
        "ste,ed->std", attended_tok, out_full, preferred_element_type=jnp.float32
    )
    gain_two, gate_full, up_full, down_full = fetch_feedforward(
        ffn_gain, gate_weight, up_weight, down_weight
    )
    normed_two_float, norm_pull_two = jax.vjp(rms_norm, middle, gain_two.astype(jnp.float32))
    normed_two = normed_two_float.astype(jnp.bfloat16)
    gate_rows = jnp.einsum("std,df->stf", normed_two, gate_full, preferred_element_type=jnp.float32)
    up_rows = jnp.einsum("std,df->stf", normed_two, up_full, preferred_element_type=jnp.float32)
    hidden_float, swiglu_pull = jax.vjp(swiglu, gate_rows, up_rows)
    hidden = hidden_float.astype(jnp.bfloat16)
    outputs = (
        middle + jnp.einsum("stf,fd->std", hidden, down_full, preferred_element_type=jnp.float32)
    ).astype(jnp.bfloat16)
    refetched = fetch_feedforward(ffn_gain, gate_weight, up_weight, down_weight)
    gate_back, up_back, down_back = (refetched[1], refetched[2], refetched[3])
    grad_out = cotangent.astype(jnp.float32)
    down_grad = jnp.einsum("stf,std->fd", hidden, cotangent, preferred_element_type=jnp.float32)
    grad_hidden = jnp.einsum(
        "std,fd->stf", cotangent, down_back, preferred_element_type=jnp.float32
    )
    grad_gate, grad_up = swiglu_pull(grad_hidden)
    grad_gate = grad_gate.astype(jnp.bfloat16)
    grad_up = grad_up.astype(jnp.bfloat16)
    gate_grad = jnp.einsum("std,stf->df", normed_two, grad_gate, preferred_element_type=jnp.float32)
    up_grad = jnp.einsum("std,stf->df", normed_two, grad_up, preferred_element_type=jnp.float32)
    grad_normed_two = jnp.einsum(
        "stf,df->std", grad_gate, gate_back, preferred_element_type=jnp.float32
    ) + jnp.einsum("stf,df->std", grad_up, up_back, preferred_element_type=jnp.float32)
    middle_part, gain_two_grad = norm_pull_two(grad_normed_two)
    grad_middle = grad_out + middle_part
    ffn_shares = (
        lax.psum_scatter(gain_two_grad, ("fsdp", "blk", "uly"), scatter_dimension=0, tiled=True),
        lax.psum_scatter(gate_grad, ("fsdp", "blk", "uly"), scatter_dimension=0, tiled=True),
        lax.psum_scatter(up_grad, ("fsdp", "blk", "uly"), scatter_dimension=0, tiled=True),
        lax.psum_scatter(down_grad, ("fsdp", "blk", "uly"), scatter_dimension=0, tiled=True),
    )
    fetched_again = fetch_attention(attn_gain, query_weight, key_matrix, value_matrix, out_weight)
    query_back, key_back, value_back, out_back = (
        fetched_again[1],
        fetched_again[2],
        fetched_again[3],
        fetched_again[4],
    )
    grad_middle_low = grad_middle.astype(jnp.bfloat16)
    out_grad = jnp.einsum(
        "ste,std->ed", attended_tok, grad_middle_low, preferred_element_type=jnp.float32
    )
    grad_att_tok = (
        jnp.einsum("std,ed->ste", grad_middle_low, out_back, preferred_element_type=jnp.float32)
        .astype(jnp.bfloat16)
        .reshape(seq_count, tok_count, query_heads, head_dim)
    )
    grad_att = lax.all_to_all(grad_att_tok, "uly", split_axis=2, concat_axis=1, tiled=True).reshape(
        seq_count, block_len, local_kv, heads_per_group, head_dim
    )
    delta = jnp.transpose(jnp.sum(grad_att.astype(jnp.float32) * attended, axis=-1), (0, 2, 3, 1))

    def block_grads(key_value, source):
        keys_in = key_value[0]
        values_in = key_value[1]
        probs = block_weights(keys_in, source) / row_totals[..., None]
        grad_probs = jnp.einsum(
            "sqhgd,skhd->shgqk", grad_att, values_in, preferred_element_type=jnp.float32
        )
        grad_scores = (probs * (grad_probs - delta[..., None])).astype(jnp.bfloat16)
        grad_query = (
            jnp.einsum(
                "shgqk,skhd->sqhgd", grad_scores, keys_in, preferred_element_type=jnp.float32
            )
            * scale
        )
        grad_keys = (
            jnp.einsum(
                "shgqk,sqhgd->skhd", grad_scores, query_group, preferred_element_type=jnp.float32
            )
            * scale
        )
        grad_values = jnp.einsum(
            "shgqk,sqhgd->skhd",
            probs.astype(jnp.bfloat16),
            grad_att,
            preferred_element_type=jnp.float32,
        )
        return (grad_query, jnp.stack([grad_keys, grad_values]))

    def pass_grads(moving):
        return from_behind(moving.astype(jnp.bfloat16), "blk", 1).astype(moving.dtype)

    query_start, pair_start = block_grads(own_pair, blk_index)

    def backward_turn(turn_index, carry):
        key_value, query_acc, pair_acc = carry
        key_value = passed_along(key_value, "blk", 1)
        pair_acc = pass_grads(pair_acc)

        def accumulate(holding):
            part_query, part_pair = block_grads(key_value, blk_index - turn_index)
            return (holding[0] + part_query, holding[1] + part_pair)

        query_acc, pair_acc = lax.cond(
            turn_index <= blk_index, accumulate, lambda holding: holding, (query_acc, pair_acc)
        )
        return (key_value, query_acc, pair_acc)

    spent_pair, query_total, pair_total = lax.fori_loop(
        1, blk_size, backward_turn, (own_pair, query_start, pair_start)
    )
    pair_total = pass_grads(pair_total)
    grad_query_low = query_total.reshape(
        seq_count, block_len, local_kv * heads_per_group, head_dim
    ).astype(jnp.bfloat16)
    grad_query_tok, grad_key_tok, grad_value_tok = (
        lax.all_to_all(grad_query_low, "uly", split_axis=1, concat_axis=2, tiled=True),
        lax.all_to_all(
            pair_total[0].astype(jnp.bfloat16), "uly", split_axis=1, concat_axis=2, tiled=True
        ),
        lax.all_to_all(
            pair_total[1].astype(jnp.bfloat16), "uly", split_axis=1, concat_axis=2, tiled=True
        ),
    )
    grad_query_pre, grad_key_pre, heads_grad = prep_pull(
        (grad_query_tok.astype(jnp.float32), grad_key_tok.astype(jnp.float32))
    )
    grad_query_flat = grad_query_pre.astype(jnp.bfloat16).reshape(
        seq_count, tok_count, query_heads * head_dim
    )
    grad_key_flat = grad_key_pre.astype(jnp.bfloat16).reshape(
        seq_count, tok_count, value_heads * head_dim
    )
    grad_value_flat = grad_value_tok.reshape(seq_count, tok_count, value_heads * head_dim)
    query_grad = jnp.einsum(
        "std,ste->de", normalized_input, grad_query_flat, preferred_element_type=jnp.float32
    )
    key_grad = jnp.einsum(
        "std,ste->de", normalized_input, grad_key_flat, preferred_element_type=jnp.float32
    )
    value_grad = jnp.einsum(
        "std,ste->de", normalized_input, grad_value_flat, preferred_element_type=jnp.float32
    )
    grad_normed = jnp.einsum(
        "ste,de->std", grad_query_flat, query_back, preferred_element_type=jnp.float32
    )
    grad_normed = grad_normed + jnp.einsum(
        "ste,de->std", grad_key_flat, key_back, preferred_element_type=jnp.float32
    )
    grad_normed = grad_normed + jnp.einsum(
        "ste,de->std", grad_value_flat, value_back, preferred_element_type=jnp.float32
    )
    input_part, gain_one_grad = norm_pull_one(grad_normed)
    input_grad = (grad_middle + input_part).astype(jnp.bfloat16)
    attn_shares = (
        lax.psum_scatter(gain_one_grad, ("fsdp", "blk", "uly"), scatter_dimension=0, tiled=True),
        lax.psum_scatter(heads_grad, ("fsdp", "blk", "uly"), scatter_dimension=1, tiled=True),
        lax.psum_scatter(query_grad, ("fsdp", "blk", "uly"), scatter_dimension=0, tiled=True),
        lax.psum_scatter(key_grad, ("fsdp", "blk", "uly"), scatter_dimension=0, tiled=True),
        lax.psum_scatter(value_grad, ("fsdp", "blk", "uly"), scatter_dimension=0, tiled=True),
        lax.psum_scatter(out_grad, ("fsdp", "blk", "uly"), scatter_dimension=0, tiled=True),
    )
    return (
        outputs,
        input_grad,
        attn_shares[0],
        attn_shares[1],
        attn_shares[2],
        attn_shares[3],
        attn_shares[4],
        attn_shares[5],
        ffn_shares[0],
        ffn_shares[1],
        ffn_shares[2],
        ffn_shares[3],
    )


MESH = pl.DeviceIdType.MESH
ANY = pl.BlockSpec(memory_space=pl.ANY)
VMEM = pl.BlockSpec(memory_space=pltpu.VMEM)
PLANE = [(dx, dy, dc) for dx in (0, 1) for dy in (0, 1) for dc in (0, 1)]
FAR = [(1, 1, 0), (1, 0, 0), (0, 1, 0)]
TURNS = (1, 2, 3)
SEM = pltpu.SemaphoreType.DMA


class Place:
    def __init__(self):
        self.x = lax.axis_index("fsdp")
        self.block = lax.axis_index("blk")
        self.z = lax.axis_index("uly")
        self.y, self.c = (self.block // 2, self.block % 2)
        self.head = 4 * self.x + self.block
        self.here = (self.x, self.block, self.z)

    def coords(self, dx, dy, dc):
        return ((self.x + dx) % 2, (self.y + dy) % 2, (self.c + dc) % 2)

    def peer(self, dx, dy, dc):
        x, y, c = self.coords(dx, dy, dc)
        return (x, 2 * y + c, self.z)

    def index(self, dx, dy, dc):
        x, y, c = self.coords(dx, dy, dc)
        return 4 * x + 2 * y + c

    def shard(self, ref, dx=0, dy=0, dc=0):
        x, y, c = self.coords(dx, dy, dc)
        return ref.at[2 * y + c, :, x]

    def behind(self, turn):
        return (self.z + 4 - turn) % 4

    def ahead(self, turn):
        return (self.z + turn) % 4

    def line(self, turn):
        return (self.x, self.block, self.ahead(turn))


def remote(src, dst, send_sem, recv_sem, device):
    return pltpu.make_async_remote_copy(
        src_ref=src,
        dst_ref=dst,
        send_sem=send_sem,
        recv_sem=recv_sem,
        device_id=device,
        device_id_type=MESH,
    )


def arrived(ref, sem):
    pltpu.make_async_copy(ref, ref, sem).wait()


def meet(peers):
    barrier = pltpu.get_barrier_semaphore()
    for peer in peers:
        pl.semaphore_signal(barrier, inc=1, device_id=peer, device_id_type=MESH)
    pl.semaphore_wait(barrier, len(peers))


class Sends:
    def __init__(self):
        self.pending = []

    def go(self, *args):
        copy = remote(*args)
        copy.start()
        self.pending.append((None, copy))

    def go_if(self, condition, *args):
        copy = remote(*args)
        pl.when(condition)(lambda: copy.start())
        self.pending.append((condition, copy))

    def drain(self):
        for condition, copy in self.pending:
            if condition is None:
                copy.wait_send()
            else:
                pl.when(condition)(lambda copy=copy: copy.wait_send())


WAYS = [(1, 0, 0), (0, 1, 0)]


def spread_start(me, sends, src, full, send_sems, recv_sems):
    for n, d, half in ((0, WAYS[0], 0), (1, WAYS[1], 1), (0, WAYS[0], 1), (1, WAYS[1], 0)):
        rows, k = (pl.ds(2 * half, 2), 2 * n + half)
        dst = me.shard(full).at[rows]
        sends.go(src.at[rows], dst, send_sems.at[k], recv_sems.at[k], me.peer(*d))
    sends.go(src, me.shard(full), send_sems.at[4], recv_sems.at[4], me.peer(0, 0, 1))


def spread_relay(me, sends, full, send_sems, recv_sems):
    for n in (0, 1):
        rows = pl.ds(2 * n, 2)
        part = me.shard(full, *WAYS[n]).at[rows]
        arrived(part, recv_sems.at[3 * n])
        sends.go(part, part, send_sems.at[5 + n], recv_sems.at[5 + n], me.peer(*WAYS[1 - n]))
    for n in (0, 1):
        rows = pl.ds(2 * (1 - n), 2)
        part = me.shard(full, *WAYS[n])
        arrived(part.at[rows], recv_sems.at[n + 1])
        sends.go(part, part, send_sems.at[7 + n], recv_sems.at[7 + n], me.peer(0, 0, 1))


def spread_far(me, sends, full, send_sems, recv_sems):
    for n in (0, 1):
        part = me.shard(full, 1, 1, 0).at[pl.ds(2 * n, 2)]
        arrived(part, recv_sems.at[5 + n])
        sends.go(part, part, send_sems.at[9 + n], recv_sems.at[9 + n], me.peer(0, 0, 1))


def spread_finish(me, full, recv_sems):
    arrived(me.shard(full, 0, 0, 1), recv_sems.at[4])
    for n in (0, 1):
        arrived(me.shard(full, *WAYS[n][:2], 1), recv_sems.at[7 + n])
        arrived(me.shard(full, 1, 1, 1).at[pl.ds(2 * n, 2)], recv_sems.at[9 + n])


PIECES = (0, 1, 3, 2)


def piece_start(me, sends, full, turn, send_sems, recv_sems):
    part = full.at[me.block, (me.z + turn) % 4, me.x]
    for n, d in enumerate(WAYS + [(0, 0, 1)]):
        k = 4 * n + turn
        sends.go(part, part, send_sems.at[k], recv_sems.at[k], me.peer(*d))


def piece_relay(me, sends, full, send_sems, recv_sems, turns):
    for turn in turns:
        n = int(turn > 1)
        for way in (n, 1 - n):
            x, y, c = me.coords(*WAYS[way])
            part = full.at[2 * y + c, (me.z + turn) % 4, x]
            k = 4 * way + turn
            arrived(part, recv_sems.at[k])
            if way == n:
                sends.go(part, part, send_sems.at[12 + turn], recv_sems.at[12 + turn], me.peer(*WAYS[1 - n]))
            sends.go(part, part, send_sems.at[16 + k], recv_sems.at[16 + k], me.peer(0, 0, 1))


def piece_far(me, sends, full, send_sems, recv_sems):
    for turn in PIECES:
        x, y, c = me.coords(1, 1, 0)
        part = full.at[2 * y + c, (me.z + turn) % 4, x]
        arrived(part, recv_sems.at[12 + turn])
        sends.go(part, part, send_sems.at[24 + turn], recv_sems.at[24 + turn], me.peer(0, 0, 1))


def piece_finish(me, full, recv_sems):
    for n, (dx, dy) in enumerate(((0, 0), (1, 0), (0, 1), (1, 1))):
        x, y, c = me.coords(dx, dy, 1)
        for turn in PIECES:
            arrived(full.at[2 * y + c, (me.z + turn) % 4, x], recv_sems.at[(8, 16, 20, 24)[n] + turn])


def full_shape(tokens, width):
    return (4, 4, 2, tokens // 32, width)


def line_spread(me, sends, src, part, sems):
    for dz in (2, 1):
        sends.go_if(me.z < 4 - dz, src, part(me.z), sems.at[0, dz - 1], sems.at[1, dz - 1], me.line(dz))
        sends.go_if(me.z >= dz, src, part(me.z), sems.at[0, dz + 1], sems.at[1, dz + 1], me.line(4 - dz))


def relay_spread(me, sends, src, part, sems):
    outer, _ = outer_inner(me)
    mine = part(me.z)
    for up, far in ((True, me.z == 0), (False, me.z == 3)):
        k = 1 if up else 3
        sends.go_if(far, src, mine, sems.at[0, k], sems.at[1, k], me.line(2))
        near = me.z < 3 if up else me.z > 0
        k = 0 if up else 2
        sends.go_if(near, src, mine, sems.at[0, k], sems.at[1, k], me.line(1 if up else 3))


def relay_forward(me, sends, part, sems):
    _, inner = outer_inner(me)
    ref = part((7 - me.z) % 4)
    pl.when(me.z == 1)(lambda: arrived(ref, sems.at[1, 2]))
    pl.when(me.z == 2)(lambda: arrived(ref, sems.at[1, 0]))
    target = (me.x, me.block, (3 * me.z + 1) % 4)
    for z, k in ((1, 3), (2, 1)):
        sends.go_if(me.z == z, ref, ref, sems.at[0, k], sems.at[1, k], target)
    line_forward(me, sends, part, sems)


def relay_finish(me, part, sems):
    z = me.z
    low, high = (part((z + 3) % 4), part((z + 1) % 4))
    pl.when(jnp.logical_or(z == 1, z == 3))(lambda: arrived(low, sems.at[1, 0]))
    pl.when(jnp.logical_or(z == 0, z == 2))(lambda: arrived(high, sems.at[1, 2]))

    @pl.when(z == 3)
    def _():
        arrived(part((z + 2) % 4), sems.at[1, 1])
        arrived(high, sems.at[1, 4])

    @pl.when(z == 0)
    def _():
        arrived(part((z + 2) % 4), sems.at[1, 3])
        arrived(low, sems.at[1, 4])


def line_forward(me, sends, part, sems):
    inner = jnp.logical_or(me.z == 1, me.z == 2)
    ref = part((me.z + 2) % 4)
    pl.when(me.z == 1)(lambda: arrived(ref, sems.at[1, 3]))
    pl.when(me.z == 2)(lambda: arrived(ref, sems.at[1, 1]))
    target = (me.x, me.block, (3 * me.z + 1) % 4)
    sends.go_if(inner, ref, ref, sems.at[0, 4], sems.at[1, 4], target)


def line_finish(me, part, sems):
    z = me.z
    pl.when(z > 0)(lambda: arrived(part((z + 3) % 4), sems.at[1, 0]))
    pl.when(z < 3)(lambda: arrived(part((z + 1) % 4), sems.at[1, 2]))

    @pl.when(z == 3)
    def _():
        arrived(part((z + 2) % 4), sems.at[1, 1])
        arrived(part((z + 1) % 4), sems.at[1, 4])

    @pl.when(z == 0)
    def _():
        arrived(part((z + 2) % 4), sems.at[1, 3])
        arrived(part((z + 3) % 4), sems.at[1, 4])


def line_to(me, z):
    return (me.x, me.block, z)


def outer_inner(me):
    outer = jnp.logical_or(me.z == 0, me.z == 3)
    return (outer, jnp.logical_not(outer))


def reduce_start(me, sends, own, came, sems, joins=True, rest=True):
    z = me.z
    outer, _ = outer_inner(me)
    if joins:
        nearer = line_to(me, 1 + z // 3)
        sends.go_if(outer, own((7 - z) % 4), came.at[3], sems.at[0, 3], sems.at[1, 3], nearer)
    if rest:
        far = (z + 2) % 4
        sends.go_if(outer, own(far), came.at[2], sems.at[0, 2], sems.at[1, 2], line_to(me, far))
        sends.go_if(z < 3, own((z + 1) % 4), came.at[0], sems.at[0, 0], sems.at[1, 0], me.line(1))
        sends.go_if(z > 0, own((z + 3) % 4), came.at[1], sems.at[0, 1], sems.at[1, 1], me.line(3))


def reduce_join(me, sends, own, came, buf, sems):
    _, inner = outer_inner(me)
    far = (me.z + 2) % 4

    @pl.when(inner)
    def _():
        arrived(came.at[3], sems.at[1, 3])
        buf[...] = (own(far)[...].astype(jnp.float32) + came[3].astype(jnp.float32)).astype(buf.dtype)

    sends.go_if(inner, buf, came.at[2], sems.at[0, 2], sems.at[1, 2], line_to(me, far))


def reduce_total(me, own, came, total, sems):
    arrived(came.at[2], sems.at[1, 2])
    total[...] = own(me.z)[...].astype(jnp.float32) + came[2].astype(jnp.float32)

    @pl.when(me.z > 0)
    def _():
        arrived(came.at[0], sems.at[1, 0])
        total[...] = total[...] + came[0].astype(jnp.float32)

    @pl.when(me.z < 3)
    def _():
        arrived(came.at[1], sems.at[1, 1])
        total[...] = total[...] + came[1].astype(jnp.float32)


def lanes(shape):
    return lax.broadcasted_iota(jnp.int32, shape, len(shape) - 1)


def turned(vector):
    half = vector.shape[-1] // 2
    sign = jnp.where(lanes((1, 2 * half)) < half, -1.0, 1.0)
    return pltpu.roll(vector, half, 1) * sign


def head_scale(vector):
    return lax.rsqrt(jnp.mean(vector * vector, axis=-1, keepdims=True) + EPSILON)


def mat(a, b):
    return jnp.dot(a, b, preferred_element_type=jnp.float32)


def mat_right(a, b):
    return lax.dot_general(a, b, (((1,), (1,)), ((), ())), preferred_element_type=jnp.float32)


def mat_left(a, b):
    return lax.dot_general(a, b, (((0,), (0,)), ((), ())), preferred_element_type=jnp.float32)


def permute_in(me, src_ref, full_ref, send_sems, recv_sems, wait=False):
    half = src_ref.shape[1] // 2
    for j in (0, 1):
        for to in (0, 1):
            src = src_ref.at[j, pl.ds(half * to, half)]
            dst = full_ref.at[me.block, me.z, to]
            mine = jnp.logical_and(me.x == to, me.z == 2 * j + me.x)
            copy = remote(
                src, dst, send_sems.at[2 * j + to], recv_sems.at[me.z], (to, me.block, 2 * j + me.x)
            )
            if wait:
                pl.when(jnp.logical_not(mine))(lambda copy=copy: copy.wait_send())
                continue
            pl.when(jnp.logical_not(mine))(lambda copy=copy: copy.start())
            own = pltpu.make_async_copy(src, dst, recv_sems.at[me.z])
            pl.when(mine)(lambda own=own: own.start())


def permuted_in(me, full_ref, recv_sems):
    for k in range(4):
        arrived(full_ref.at[me.block, k, me.x], recv_sems.at[k])


def half_block(me, part, sibling, send_sems, recv_sems, b, sends=None):
    other = me.c != b % 2
    dy = (me.y + b // 2) % 2
    for to in (0, 1):
        slot = 3 - 2 * ((me.x + to) % 2) - dy
        copy = remote(
            part.at[b, :, to], sibling.at[slot], send_sems.at[slot], recv_sems.at[slot],
            me.peer(0, 0, 1),
        )
        if sends is None:
            pl.when(other)(lambda copy=copy: copy.start())
        else:
            sends.pending.append((other, copy))


HALVES = (slice(0, 2), slice(2, 4))


def half_own(me, part, i, dims):
    x, y, c = me.coords(*(FAR + [(0, 0, 0)])[i])
    ref, sibling = part
    return ref[2 * y + c, dims, x].astype(jnp.float32) + sibling[i, dims].astype(jnp.float32)


def half_out(me, sends, part, sibling, out, came, send_sems, recv_sems):
    low, both = (out.dtype, (part, sibling))
    near = (me.peer(1, 0, 0), me.peer(0, 1, 0))
    arrived(sibling.at[0], recv_sems.at[0])
    out[0] = half_own(me, both, 0, slice(None)).astype(low)
    for n, dims in enumerate(HALVES):
        half = pl.ds(2 * n, 2)
        sends.go(out.at[0, half], came.at[0, half], send_sems.at[4 + n], recv_sems.at[4 + n], near[n])
    for n, dims in enumerate(HALVES):
        arrived(sibling.at[1 + n], recv_sems.at[1 + n])
        out[1 + n, dims] = half_own(me, both, 1 + n, dims).astype(low)
        half = pl.ds(2 * n, 2)
        k = 6 + 2 * n
        sends.go(out.at[1 + n, half], came.at[1 + n, half], send_sems.at[k], recv_sems.at[k], near[n])


def half_relay(me, sends, part, sibling, out, came, send_sems, recv_sems):
    low, both = (out.dtype, (part, sibling))
    near = (me.peer(1, 0, 0), me.peer(0, 1, 0))
    for n in (0, 1):
        dims, half, k = (HALVES[1 - n], pl.ds(2 * (1 - n), 2), 7 + 2 * n)
        arrived(came.at[0, half], recv_sems.at[5 - n])
        total = half_own(me, both, 1 + n, dims) + came[0, dims].astype(jnp.float32)
        out[1 + n, dims] = total.astype(low)
        sends.go(out.at[1 + n, half], came.at[1 + n, half], send_sems.at[k], recv_sems.at[k], near[n])


def half_in(me, part, sibling, came, recv_sems):
    arrived(sibling.at[3], recv_sems.at[3])
    for n, half in ((0, 0), (1, 1), (0, 1), (1, 0)):
        k = 6 + 2 * n + (half != n)
        arrived(came.at[1 + n, pl.ds(2 * half, 2)], recv_sems.at[k])
    total = half_own(me, (part, sibling), 3, slice(None))
    return total + came[1].astype(jnp.float32) + came[2].astype(jnp.float32)


def half_scratch(tokens, width):
    piece = (4, tokens // 32, width)
    return [
        pltpu.VMEM((4,) + piece, jnp.bfloat16),
        pltpu.VMEM((3,) + piece, jnp.bfloat16),
        pltpu.VMEM((3,) + piece, jnp.bfloat16),
        SEM((10,)),
        SEM((10,)),
    ]


def gain_row(gains_ref, kind):
    rows = [jnp.sum(gains_ref[p, :, kind, :], axis=0, keepdims=True) for p in range(8)]
    return jnp.concatenate(rows, axis=1)


def allowed_keys(segcol, segrow, b, kb):
    same = segcol[b] == segrow[:, 256 * kb : 256 * kb + 256]
    if kb < b:
        return same
    rows = lax.broadcasted_iota(jnp.int32, (256, 256), 0)
    return jnp.logical_and(same, lanes((256, 256)) <= rows)


def norm_back(grad, vector, gain, scale):
    weighted = grad * gain
    inner = jnp.mean(weighted * vector, axis=-1, keepdims=True)
    return scale * weighted - vector * (scale * scale * scale * inner)


def permute_out(me, src_ref, dst_ref, send_sems, recv_sems, wait=False):
    half = dst_ref.shape[1] // 2
    for k in range(4):
        src = src_ref.at[k]
        dst = dst_ref.at[me.z // 2, pl.ds(half * me.x, half)]
        mine = jnp.logical_and(me.x == me.z % 2, me.z == k)
        spot = 2 * (me.z // 2) + me.x
        copy = remote(src, dst, send_sems.at[k], recv_sems.at[spot], (me.z % 2, me.block, k))
        if wait:
            pl.when(jnp.logical_not(mine))(lambda copy=copy: copy.wait_send())
            continue
        pl.when(jnp.logical_not(mine))(lambda copy=copy: copy.start())
        own = pltpu.make_async_copy(src, dst, recv_sems.at[spot])
        pl.when(mine)(lambda own=own: own.start())


def permuted_out(dst_ref, recv_sems):
    half = dst_ref.shape[1] // 2
    for j in (0, 1):
        for to in (0, 1):
            arrived(dst_ref.at[j, pl.ds(half * to, half)], recv_sems.at[2 * j + to])


def total_row(share):
    return jnp.sum(jnp.sum(share, axis=0), axis=0, keepdims=True)


def layer_kernel(
    x_ref, cot_ref, seg_ref, q_ref, k_ref, v_ref, g_ref, u_ref, o_ref, d_ref, ag_ref, fg_ref, hg_in,
    y_ref, gx_ref, dq_ref, dk_ref, dv_ref, dg_ref, du_ref, sums_ref, osum_out, dsum_out,
    xf, cf, wf, of, df, guf, segs, gains, n1, nf, gf, pre, qkv, segcol, cos_s, sin_s, att, attlow,
    totals, kept, part, part2, down, n2, gm, y_s, gi_s, mid, gmid,
    gates, hid, gboth, ga, gq, gk, gv, gpre, dd, dgu, do, dw,
    d_came, d_buf, gu_came, gu_buf, gu_total, gu_sum, o_came, o_buf, w_came, w_buf, w_total, w_sum,
    pack, packs, linep,
    sib1, out1, came1, hs1, hr1, sib2, out2, came2, hs2, hr2, sib3, out3, came3, hs3, hr3,
    ps, pr, as_, ar, xas, xar, ws, wr, us, ur, gs, gr, zq, zo, zd, zg, zu, rg, rd, ro, rw, cs, cr, ds, dr, ls, raw1, raw2, hg_low, hg_ref, osum_ref, dsum_ref,
):
    me = Place()
    x, z, p = (me.x, me.z, me.head)
    low, wide_t = (jnp.bfloat16, jnp.float32)
    across = [((x + 1) % 2, me.block, me.ahead(turn)) for turn in TURNS]
    meet([me.peer(*d) for d in PLANE[1:]] + [me.line(turn) for turn in TURNS] + across)
    sends, early = (Sends(), Sends())

    def local(src, dst, sem):
        copy = pltpu.make_async_copy(src, dst, sem)
        copy.start()
        return copy

    own_raw = [local(ref, dst, ls.at[6 + i]) for i, (ref, dst) in enumerate(((ag_ref, raw1), (fg_ref, raw2)))]
    own_head = local(hg_in, hg_low, ls.at[0])
    own_seg = local(seg_ref, segs.at[x], ls.at[1])
    sends.go(seg_ref, segs.at[x], ls.at[2], ls.at[3], me.peer(1, 0, 0))
    permute_in(me, x_ref, xf, ps.at[0], pr.at[0])
    permute_in(me, cot_ref, cf, ps.at[1], pr.at[1])
    own_o = local(o_ref, of.at[z], ls.at[4])
    own_d = local(d_ref, df.at[z], ls.at[5])
    wide, narrow = (q_ref.shape[1] // 8, k_ref.shape[1] // 8)
    cuts = ((q_ref, wide, 0), (k_ref, narrow, wide), (v_ref, narrow, wide + narrow))
    for i, d in enumerate(PLANE):
        t = me.index(*d)
        for n, (ref, width, off) in enumerate(cuts):
            src = ref.at[:, pl.ds(pl.multiple_of(t * width, 128), width)]
            dst = wf.at[p, z, :, pl.ds(off, width)]
            if i == 0:
                local(src, dst, wr.at[n])
            else:
                sends.go(src, dst, ws.at[3 * i + n], wr.at[3 * i + n], me.peer(*d))
    ff = g_ref.shape[1] // 8
    for copy in own_raw + [own_head]:
        copy.wait()
    hg_ref[...] = hg_low[...].astype(wide_t)
    piece = raw1.shape[1]
    rows = [raw1[...].astype(wide_t), raw2[...].astype(wide_t), jnp.zeros((6, piece), wide_t)]
    rows = [jnp.concatenate(rows, axis=0), jnp.zeros((8, 128 - piece), wide_t)]
    rows = jnp.concatenate(rows, axis=1)
    gains[p, z] = pltpu.roll(rows, piece * z, 1)
    arrived(xf.at[me.block, z, x], pr.at[0, z])
    piece_start(me, sends, xf, 0, xas, xar)
    for turn in TURNS:
        sends.go(gains.at[p, z], gains.at[p, z], gs.at[turn], gr.at[turn], me.line(turn))
    for i, d in enumerate(PLANE):
        t = me.index(*d)
        for n, (ref, width, off) in enumerate(cuts):
            arrived(wf.at[t, z, :, pl.ds(off, width)], wr.at[3 * i + n])
    qkv_part = lambda k: wf.at[:, k]
    o_part = lambda k: of.at[k]
    d_part = lambda k: df.at[k]
    gate_part = lambda k: guf.at[:, k, :, pl.ds(0, ff)]
    up_part = lambda k: guf.at[:, k, :, pl.ds(ff, ff)]
    line_spread(me, sends, qkv_part(z), qkv_part, zq)
    for turn in (1, 3, 2):
        k = (z + turn) % 4
        arrived(xf.at[me.block, k, x], pr.at[0, k])
        piece_start(me, sends, xf, turn, xas, xar)
    line_spread(me, sends, o_ref, o_part, zo)
    piece_relay(me, sends, xf, xas, xar, PIECES[:2])
    line_forward(me, sends, qkv_part, zq)
    piece_relay(me, sends, xf, xas, xar, PIECES[2:])
    for turn in TURNS:
        arrived(gains.at[p, me.behind(turn)], gr.at[turn])
    for i, d in enumerate(PLANE[1:]):
        sends.go(gains.at[p], gains.at[p], gs.at[4 + i], gr.at[4 + i], me.peer(*d))
    for i, d in enumerate(PLANE):
        t = me.index(*d)
        for n, ref in enumerate((g_ref, u_ref)):
            src = ref.at[:, pl.ds(pl.multiple_of(t * ff, 128), ff)]
            dst = guf.at[p, z, :, pl.ds(n * ff, ff)]
            if i == 0:
                local(src, dst, ur.at[n])
            else:
                sends.go(src, dst, us.at[2 * i + n], ur.at[2 * i + n], me.peer(*d))
    permuted_in(me, cf, pr.at[1])
    spread_start(me, sends, me.shard(cf), cf, as_.at[1], ar.at[1])
    own_seg.wait()
    arrived(segs.at[(x + 1) % 2], ls.at[3])
    head_dim = hg_ref.shape[1]
    segrow = segs[z % 2, pl.ds(z // 2, 1), :]
    tokens = segrow.shape[1]
    column = jnp.transpose(jnp.broadcast_to(segrow.astype(wide_t), (8, tokens)))[:, :1]
    segcol[...] = column.astype(jnp.int32).reshape(4, 256, 1)
    half_lane = (lanes((1, head_dim)) % (head_dim // 2)).astype(wide_t)
    inverse = jnp.exp(half_lane * (-2.0 * math.log(THETA) / head_dim))
    steps = lax.broadcasted_iota(jnp.int32, (32, head_dim), 0).astype(wide_t) * inverse
    cl, sl = (jnp.cos(steps), jnp.sin(steps))
    ch, sh = (jnp.cos(steps * 32.0), jnp.sin(steps * 32.0))
    doc_cos, doc_sin = ([], [])
    for doc in range(DOCS):
        start = jnp.sum((segrow < doc).astype(wide_t), axis=1, keepdims=True)
        doc_cos.append(jnp.cos(start * inverse))
        doc_sin.append(jnp.sin(start * inverse))
    for b in range(4):
        hi_c, hi_s = (ch[8 * b : 8 * b + 8][:, None, :], sh[8 * b : 8 * b + 8][:, None, :])
        cos_at = (hi_c * cl[None] - hi_s * sl[None]).reshape(256, head_dim)
        sin_at = (hi_s * cl[None] + hi_c * sl[None]).reshape(256, head_dim)
        column = segcol[b]
        cd, sd = (jnp.broadcast_to(v[0], (256, head_dim)) for v in (doc_cos, doc_sin))
        for doc in range(1, DOCS):
            cd = jnp.where(column == doc, doc_cos[doc], cd)
            sd = jnp.where(column == doc, doc_sin[doc], sd)
        cos_s[b] = cos_at * cd + sin_at * sd
        sin_s[b] = sin_at * cd - cos_at * sd
    piece_far(me, sends, xf, xas, xar)
    for i, d in enumerate(PLANE[1:]):
        arrived(gains.at[me.index(*d)], gr.at[4 + i])
    gain_one, gain_two = (gain_row(gains, 0), gain_row(gains, 1))
    piece_finish(me, xf, xar)

    @pl.loop(0, 4)
    def _(b):
        rows = xf[b].reshape(256, -1).astype(wide_t)
        n1[b] = (rows * head_scale(rows) * gain_one).astype(low)

    line_finish(me, qkv_part, zq)

    own_o.wait()
    line_forward(me, sends, o_part, zo)
    for i, d in enumerate(PLANE):
        t = me.index(*d)
        for n in (0, 1):
            arrived(guf.at[t, z, :, pl.ds(n * ff, ff)], ur.at[2 * i + n])
    relay_spread(me, sends, gate_part(z), gate_part, zg)
    line_spread(me, sends, up_part(z), up_part, zu)
    spread_relay(me, sends, cf, as_.at[1], ar.at[1])
    @pl.loop(0, 4)
    def _(b):
        rows = mat(n1[b], wf[...].reshape(-1, wf.shape[3]))
        pre[b] = rows
        cosine, sine = (cos_s[b], sin_s[b])
        for h in range(3):
            v = rows[:, head_dim * h : head_dim * (h + 1)]
            n = v * head_scale(v) * hg_ref[pl.ds(h // 2, 1), :]
            qkv[b, :, pl.ds(head_dim * h, head_dim)] = (n * cosine + turned(n) * sine).astype(low)
        qkv[b, :, pl.ds(3 * head_dim, head_dim)] = rows[:, 3 * head_dim :].astype(low)

    top = lambda r: jnp.max(jnp.abs(hg_ref[pl.ds(r, 1), :]), axis=1, keepdims=True)
    bound = math.sqrt(head_dim) * top(0) * top(1)
    scale = head_dim ** (-0.5)
    key_at, value_at = (pl.ds(2 * head_dim, head_dim), pl.ds(3 * head_dim, head_dim))

    def weights_of(b, kb, query):
        s = mat_right(query, qkv[kb, :, key_at]) * scale
        return jnp.where(allowed_keys(segcol, segrow, b, kb), jnp.exp(s - bound), 0.0)

    for b in range(4):

        @pl.loop(0, 2)
        def _(h, b=b):
            at = pl.ds(pl.multiple_of(head_dim * h, head_dim), head_dim)
            query = qkv[b, :, at]
            total, mixed = (None, None)
            for kb in range(b + 1):
                w = weights_of(b, kb, query)
                t = jnp.sum(w, axis=1, keepdims=True)
                kept[h, b * (b + 1) // 2 + kb] = w.astype(low)
                m = mat(w.astype(low), qkv[kb, :, value_at])
                total = t if kb == 0 else total + t
                mixed = m if kb == 0 else mixed + m
            mixed = mixed / total
            totals[b, h] = total
            att[b, :, at] = mixed
            attlow[b, :, at] = mixed.astype(low)

    line_finish(me, o_part, zo)

    @pl.loop(0, 4)
    def _(b):
        rows = mat(attlow[b], of[...].reshape(-1, of.shape[2])).astype(low)
        part[b] = rows.reshape(part.shape[1:])
        half_block(me, part, sib1, hs1, hr1, b)

    for b in range(4):
        half_block(me, part, sib1, hs1, hr1, b, early)
    half_out(me, early, part, sib1, out1, came1, hs1, hr1)
    relay_forward(me, sends, gate_part, zg)
    half_relay(me, early, part, sib1, out1, came1, hs1, hr1)
    middle = xf[me.block, :, x].astype(wide_t) + half_in(me, part, sib1, came1, hr1)
    mid[...] = middle
    n2[...] = (middle * head_scale(middle) * gain_two).astype(low)
    own_n = local(n2, me.shard(nf), ls.at[8])
    spread_start(me, sends, n2, nf, as_.at[2], ar.at[2])
    line_forward(me, sends, up_part, zu)
    line_spread(me, sends, d_ref, d_part, zd)
    spread_relay(me, sends, nf, as_.at[2], ar.at[2])
    line_forward(me, sends, d_part, zd)
    spread_far(me, sends, nf, as_.at[2], ar.at[2])
    spread_finish(me, nf, ar.at[2])
    own_n.wait()
    relay_finish(me, gate_part, zg)
    line_finish(me, up_part, zu)

    @pl.loop(0, 4)
    def _(b):
        both = mat(nf[b].reshape(256, -1), guf[...].reshape(-1, 2 * ff))
        gates[b] = both
        gate, up = (both[:, :ff], both[:, ff:])
        hid[b] = (gate / (1.0 + jnp.exp(-gate)) * up).astype(low)

    spread_far(me, sends, cf, as_.at[1], ar.at[1])
    spread_finish(me, cf, ar.at[1])
    own_d.wait()
    dd[...] = mat_left(hid[...].reshape(-1, ff), cf[...].reshape(tokens, -1)).astype(low).reshape(dd.shape)
    own_dd = lambda k: dd.at[k]
    reduce_start(me, sends, own_dd, d_came, rd)
    line_finish(me, d_part, zd)

    @pl.loop(0, 4)
    def _(b):
        both = gates[b]
        gate, up = (both[:, :ff], both[:, ff:])
        sig = 1.0 / (1.0 + jnp.exp(-gate))
        grad = mat_right(cf[b].reshape(256, -1), df[...].reshape(ff, -1))
        gboth[b, :, pl.ds(0, ff)] = (grad * up * sig * (1.0 + gate * (1.0 - sig))).astype(low)
        gboth[b, :, pl.ds(ff, ff)] = (grad * (gate * sig)).astype(low)
        rows = mat_right(gboth[b], guf[...].reshape(-1, 2 * ff)).astype(low)
        part2[b] = rows.reshape(part2.shape[1:])
        half_block(me, part2, sib2, hs2, hr2, b)

    for b in range(4):
        half_block(me, part2, sib2, hs2, hr2, b, sends)
    half_out(me, sends, part2, sib2, out2, came2, hs2, hr2)

    @pl.loop(0, 4)
    def _(b):
        rows = nf[:, :, :, :, pl.ds(pl.multiple_of(256 * b, 256), 256)].reshape(-1, 256)
        grad = mat_left(rows, gboth[...].reshape(-1, 2 * ff)).astype(low)
        dgu[pl.ds(2 * b, 2)] = grad.reshape((2,) + dgu.shape[1:])

    own_gu = lambda k: dgu.at[:, k]
    reduce_start(me, sends, own_gu, gu_came, rg)
    half_relay(me, sends, part2, sib2, out2, came2, hs2, hr2)
    reduce_join(me, sends, own_dd, d_came, d_buf, rd)
    grad = half_in(me, part2, sib2, came2, hr2)
    middle = mid[...]
    r = head_scale(middle)
    total = cf[me.block, :, x].astype(wide_t) + norm_back(grad, middle, gain_two, r)
    gmid[...] = total
    gm[...] = total.astype(low)
    own_gm = local(gm, me.shard(gf), ls.at[9])
    spread_start(me, sends, gm, gf, as_.at[3], ar.at[3])
    share = total_row(grad * middle * r)
    for i in range(8):
        pack[pl.ds(8 + i, 1)] = share[:, 128 * i : 128 * i + 128]

    @pl.loop(0, 4)
    def _(b):
        rows = mat(hid[b], df[...].reshape(ff, -1)).astype(low)
        down[b] = rows.reshape(down.shape[1:])
        half_block(me, down, sib3, hs3, hr3, b)

    for b in range(4):
        half_block(me, down, sib3, hs3, hr3, b, sends)
    spread_relay(me, sends, gf, as_.at[3], ar.at[3])
    half_out(me, sends, down, sib3, out3, came3, hs3, hr3)
    reduce_join(me, sends, own_gu, gu_came, gu_buf, rg)
    spread_far(me, sends, gf, as_.at[3], ar.at[3])
    spread_finish(me, gf, ar.at[3])
    own_gm.wait()

    half_relay(me, sends, down, sib3, out3, came3, hs3, hr3)
    gk[...] = jnp.zeros_like(gk)
    gv[...] = jnp.zeros_like(gv)
    for b in range(4):
        ga[b] = mat_right(gf[b].reshape(256, -1), of[...].reshape(-1, of.shape[2])).astype(low)

        @pl.loop(0, 2)
        def _(h, b=b):
            at = pl.ds(pl.multiple_of(head_dim * h, head_dim), head_dim)
            query, grad = (qkv[b, :, at], ga[b, :, at])
            inv = 1.0 / totals[b, h]
            scaled = grad.astype(wide_t) * inv
            delta = jnp.sum(scaled * att[b, :, at], axis=1, keepdims=True)
            scaled = scaled.astype(low)
            grad_query = None
            for kb in range(b + 1):
                w = kept[h, b * (b + 1) // 2 + kb]
                gp = mat_right(scaled, qkv[kb, :, value_at])
                gsc = (w.astype(wide_t) * (gp - delta)).astype(low)
                m = mat(gsc, qkv[kb, :, key_at])
                grad_query = m if kb == 0 else grad_query + m
                gk[kb] += mat_left(gsc, query)
                gv[kb] += mat_left(w, scaled)
            gq[b, :, at] = grad_query

        if b == 2:
            y_s[...] = (mid[...] + half_in(me, down, sib3, came3, hr3)).astype(low)
            permute_out(me, y_s, y_ref, cs.at[0], cr.at[0])
    do[...] = mat_left(attlow[...].reshape(tokens, -1), gf[...].reshape(tokens, -1)).astype(low).reshape(do.shape)
    own_do = lambda k: do.at[k]
    reduce_start(me, sends, own_do, o_came, ro)
    pack[pl.ds(16, 8)] = jnp.zeros((8, 128), wide_t)

    @pl.loop(0, 4)
    def _(b):
        cosine, sine = (cos_s[b], sin_s[b])
        for h in range(3):
            at = pl.ds(head_dim * h, head_dim)
            source = gq[b, :, at] if h < 2 else gk[b]
            go = (source * scale).astype(low).astype(wide_t)
            gh = go * cosine - turned(go * sine)
            v = pre[b, :, at]
            r = head_scale(v)
            n = v * r
            pack[pl.ds(16 + h // 2, 1)] += jnp.sum(gh * n, axis=0, keepdims=True)
            gn = gh * hg_ref[pl.ds(h // 2, 1), :]
            gpre[b, :, at] = (r * (gn - n * jnp.mean(gn * n, axis=-1, keepdims=True))).astype(low)
        gpre[b, :, value_at] = gv[b].astype(low)

    early.drain()

    @pl.loop(0, 4)
    def _(b):
        rows = mat_right(gpre[b], wf[...].reshape(-1, wf.shape[3])).astype(low)
        part[b] = rows.reshape(part.shape[1:])
        half_block(me, part, sib1, hs1, hr1, b)

    for b in range(4):
        half_block(me, part, sib1, hs1, hr1, b, sends)
    half_out(me, sends, part, sib1, out1, came1, hs1, hr1)
    @pl.loop(0, 4)
    def _(b):
        rows = n1[:, :, pl.ds(pl.multiple_of(256 * b, 256), 256)].reshape(-1, 256)
        grad = mat_left(rows, gpre[...].reshape(tokens, -1)).astype(low)
        grad = grad.reshape((2,) + dw.shape[2:-1] + (2 * dw.shape[-1],))
        for n in (0, 1):
            dw[n, pl.ds(2 * b, 2)] = grad[..., n * dw.shape[-1] : (n + 1) * dw.shape[-1]]

    own_dw = [lambda k, n=n: dw.at[n, :, k] for n in (0, 1)]
    for joins in (True, False):
        for n in (0, 1):
            reduce_start(me, sends, own_dw[n], w_came.at[n], rw.at[n], joins, not joins)
    half_relay(me, sends, part, sib1, out1, came1, hs1, hr1)
    reduce_join(me, sends, own_do, o_came, o_buf, ro)
    reduce_total(me, own_gu, gu_came, gu_total, rg)
    gu_sum[...] = gu_total[...].astype(low)
    for i, d in enumerate(PLANE):
        t = me.index(*d)
        for n, ref in enumerate((dg_ref, du_ref)):
            src = gu_sum.at[t, :, pl.ds(n * ff, ff)]
            dst = ref.at[:, pl.ds(pl.multiple_of(p * ff, 128), ff)]
            if i == 0:
                local(src, dst, dr.at[n])
            else:
                sends.go(src, dst, ds.at[2 * i + n], dr.at[2 * i + n], me.peer(*d))
    reduce_total(me, own_dd, d_came, dsum_ref, rd)
    dsum_copy = local(dsum_ref, dsum_out, ls.at[6])
    for n in (0, 1):
        reduce_join(me, sends, own_dw[n], w_came.at[n], w_buf.at[n], rw.at[n])
    grad = half_in(me, part, sib1, came1, hr1)
    rows = xf[me.block, :, x].astype(wide_t)
    r = head_scale(rows)
    share = total_row(grad * rows * r)
    for i in range(8):
        pack[pl.ds(i, 1)] = share[:, 128 * i : 128 * i + 128]
    for i, d in enumerate(PLANE[1:]):
        sends.go(pack, packs.at[i], gs.at[11 + i], gr.at[11 + i], me.peer(*d))
    gi_s[...] = (gmid[...] + norm_back(grad, rows, gain_one, r)).astype(low)
    total = pack[...]
    for i in range(7):
        arrived(packs.at[i], gr.at[11 + i])
        total = total + packs[i]
    packs[7] = total
    for turn in TURNS:
        sends.go(packs.at[7], linep.at[turn - 1], gs.at[17 + turn], gr.at[17 + turn], me.line(turn))
    permute_out(me, gi_s, gx_ref, cs.at[1], cr.at[1])
    backs = (((dq_ref, wide, 0),), ((dk_ref, narrow, 0), (dv_ref, narrow, narrow)))
    for block in (0, 1):
        reduce_total(me, own_dw[block], w_came.at[block], w_total, rw.at[block])
        w_sum[block] = w_total[...].astype(low)
        for i, d in enumerate(PLANE):
            t = me.index(*d)
            for n, (ref, cols, off) in enumerate(backs[block]):
                src = w_sum.at[block, t, :, pl.ds(off, cols)]
                dst = ref.at[:, pl.ds(pl.multiple_of(p * cols, 128), cols)]
                k = 16 + 3 * i + block + n
                if i == 0:
                    local(src, dst, dr.at[k])
                else:
                    sends.go(src, dst, ds.at[k], dr.at[k], me.peer(*d))
    reduce_total(me, own_do, o_came, osum_ref, ro)
    osum_copy = local(osum_ref, osum_out, ls.at[7])
    for turn in TURNS:
        arrived(linep.at[turn - 1], gr.at[17 + turn])
        total = total + linep[turn - 1]
    sums_ref[...] = total
    for i, d in enumerate(PLANE):
        t = me.index(*d)
        for n, ref in enumerate((dg_ref, du_ref)):
            arrived(ref.at[:, pl.ds(pl.multiple_of(t * ff, 128), ff)], dr.at[2 * i + n])
        for n, (ref, cols, off) in enumerate(backs[0] + backs[1]):
            arrived(ref.at[:, pl.ds(pl.multiple_of(t * cols, 128), cols)], dr.at[16 + 3 * i + n])
    dsum_copy.wait()
    osum_copy.wait()
    permuted_out(y_ref, cr.at[0])
    permuted_out(gx_ref, cr.at[1])
    permute_in(me, x_ref, xf, ps.at[0], pr.at[0], wait=True)
    permute_in(me, cot_ref, cf, ps.at[1], pr.at[1], wait=True)
    permute_out(me, y_s, y_ref, cs.at[0], cr.at[0], wait=True)
    permute_out(me, gi_s, gx_ref, cs.at[1], cr.at[1], wait=True)
    sends.drain()


def layer_step(x, cot, seg, q, k, v, g, u, o, d, gain, gain_two, head_gains):
    tokens, width = (16 * x.shape[1], x.shape[2])
    rows, low, wide = (q.shape[0], jnp.bfloat16, jnp.float32)
    cols = (q.shape[1] + 2 * k.shape[1]) // 8
    att_cols, head_dim = (q.shape[1] // 8, k.shape[1] // 8)
    ff = g.shape[1] // 8
    full = full_shape(tokens, width)
    piece = (4, tokens // 32, width)
    quarter = tokens // 4
    shape, buf = (jax.ShapeDtypeStruct, pltpu.VMEM)
    blocks = lambda n, kind: buf((4, quarter, n), kind)
    return pl.pallas_call(
        layer_kernel,
        name="layer_step",
        out_shape=(
            shape(x.shape, low), shape(x.shape, low), shape(q.shape, low), shape(k.shape, low),
            shape(v.shape, low), shape(g.shape, low), shape(u.shape, low), shape((24, 128), wide),
            shape(o.shape, wide), shape(d.shape, wide),
        ),
        in_specs=[ANY] * 13,
        out_specs=(ANY,) * 7 + (VMEM, ANY, ANY),
        scratch_shapes=[
            buf(full, low), buf(full, low), buf((8, 4, rows, cols), low), buf((4,) + o.shape, low),
            buf((4,) + d.shape, low), buf((8, 4, rows, 2 * ff), low), buf((2,) + seg.shape, seg.dtype),
            buf((8, 4, 8, 128), wide), blocks(width, low), buf(full, low), buf(full, low),
            blocks(cols, wide), blocks(cols, low), blocks(1, jnp.int32), blocks(head_dim, wide),
            blocks(head_dim, wide), blocks(att_cols, wide), blocks(att_cols, low),
            buf((4, 2, quarter, 1), wide), buf((2, 10, quarter, quarter), low), buf(full, low), buf(full, low), buf(full, low),
            buf(piece, low), buf(piece, low), buf(piece, low), buf(piece, low), buf(piece, wide),
            buf(piece, wide),
            blocks(2 * ff, wide), blocks(ff, low), blocks(2 * ff, low), blocks(att_cols, low), blocks(att_cols, wide),
            blocks(head_dim, wide), blocks(head_dim, wide), blocks(cols, low),
            buf((4,) + d.shape, low), buf((8, 4, rows, 2 * ff), low), buf((4,) + o.shape, low),
            buf((2, 8, 4, rows, cols // 2), low),
            buf((4,) + d.shape, low), buf(d.shape, low),
            buf((4, 8, rows, 2 * ff), low), buf((8, rows, 2 * ff), low), buf((8, rows, 2 * ff), wide),
            buf((8, rows, 2 * ff), low),
            buf((4,) + o.shape, low), buf(o.shape, low),
            buf((2, 4, 8, rows, cols // 2), low), buf((2, 8, rows, cols // 2), low),
            buf((8, rows, cols // 2), wide), buf((2, 8, rows, cols // 2), low),
            buf((24, 128), wide), buf((8, 24, 128), wide), buf((3, 24, 128), wide),
        ]
        + half_scratch(tokens, width) * 3
        + [SEM((2, 4)), SEM((2, 4)), SEM((4, 11)), SEM((4, 11)), SEM((28,)), SEM((28,)), SEM((24,)), SEM((24,)), SEM((16,)), SEM((16,))]
        + [SEM((21,)), SEM((21,))]
        + [SEM((2, 5))] * 5
        + [SEM((2, 4))] * 3
        + [SEM((2, 2, 4))]
        + [SEM((2, 4)), SEM((2, 4)), SEM((40,)), SEM((40,)), SEM((10,)),
            buf(gain.shape, low), buf(gain.shape, low), buf(head_gains.shape, low), buf(head_gains.shape, wide),
            buf(o.shape, wide), buf(d.shape, wide)],
        compiler_params=pltpu.CompilerParams(
            collective_id=0, has_side_effects=True, vmem_limit_bytes=67043328
        ),
    )(x, cot, seg, q, k, v, g, u, o, d, gain, gain_two, head_gains)


def finish_kernel(sums_ref, *refs):
    half = (len(refs) - 3) // 2
    for src, dst in zip(refs[:half], refs[half : 2 * half]):
        dst[...] = src[...].astype(dst.dtype)
    attn_ref, ffn_ref, head_ref = refs[2 * half :]
    z = lax.axis_index("uly")
    head = 4 * lax.axis_index("fsdp") + lax.axis_index("blk")
    piece, share = (attn_ref.shape[1], head_ref.shape[1])
    rows = [sums_ref[pl.ds(head, 1), :], sums_ref[pl.ds(8 + head, 1), :], jnp.zeros((6, 128), jnp.float32)]
    rows = pltpu.roll(jnp.concatenate(rows, axis=0), 128 - piece * z, 1)
    attn_ref[...] = rows[0:1, :piece]
    ffn_ref[...] = rows[1:2, :piece]
    head_ref[...] = pltpu.roll(sums_ref[16:24, :], 128 - (4 * head + z) * share, 1)[0:2, :share]


def finish_step(piece, share, sums, *arrays):
    return pl.pallas_call(
        finish_kernel,
        name="finish_step",
        out_shape=tuple(
            jax.ShapeDtypeStruct(v.shape, v.dtype if i < 2 else jnp.float32) for i, v in enumerate(arrays)
        )
        + tuple(jax.ShapeDtypeStruct(v, jnp.float32) for v in ((1, piece), (1, piece), (2, share))),
        in_specs=[VMEM] * (1 + len(arrays)),
        out_specs=(VMEM,) * (3 + len(arrays)),
    )(sums, *arrays)


def plane_body(
    inputs, segments, attn_gain, head_gains, query_weight, key_matrix, value_matrix, out_weight,
    ffn_gain, gate_weight, up_weight, down_weight, cotangent,
):
    outputs, grad_inputs, q_grad, k_grad, v_grad, g_grad, u_grad, sums, out_grad, down_grad = layer_step(
        inputs, cotangent, segments, query_weight, key_matrix, value_matrix, gate_weight, up_weight,
        out_weight, down_weight, attn_gain[None], ffn_gain[None], head_gains,
    )
    (
        outputs, grad_inputs, q_grad, k_grad, v_grad, out_grad, g_grad, u_grad, down_grad, attn_gain_grad,
        ffn_gain_grad, head_gain_grad,
    ) = finish_step(
        attn_gain.shape[0], head_gains.shape[1] // 32, sums, outputs, grad_inputs, q_grad, k_grad, v_grad,
        out_grad, g_grad, u_grad, down_grad,
    )
    return (
        outputs, grad_inputs, attn_gain_grad[0], head_gain_grad, q_grad, k_grad, v_grad, out_grad,
        ffn_gain_grad[0], g_grad, u_grad, down_grad,
    )


def fits_plane(mesh, seq_count, heads):
    shape = mesh.shape
    return (shape["fsdp"], shape["blk"], shape["uly"]) == (2, 4, 4) and seq_count == 4 and heads == 8


def solution(mesh):
    def step(*arrays):
        seq_count = arrays[0].shape[0]
        heads = arrays[5].shape[1] // arrays[3].shape[1]
        chosen = plane_body if fits_plane(mesh, seq_count, heads) else body
        return mapped(chosen)(*arrays)

    mapped = functools.partial(
        jax.shard_map,
        mesh=mesh,
        in_specs=(
            P("fsdp", ("blk", "uly"), None),
            P("fsdp", None),
            P(("fsdp", "blk", "uly")),
            P(),
            P(("fsdp", "blk", "uly"), None),
            P(("fsdp", "blk", "uly"), None),
            P(("fsdp", "blk", "uly"), None),
            P(("fsdp", "blk", "uly"), None),
            P(("fsdp", "blk", "uly")),
            P(("fsdp", "blk", "uly"), None),
            P(("fsdp", "blk", "uly"), None),
            P(("fsdp", "blk", "uly"), None),
            P("fsdp", ("blk", "uly"), None),
        ),
        out_specs=(
            P("fsdp", ("blk", "uly"), None),
            P("fsdp", ("blk", "uly"), None),
            P(("fsdp", "blk", "uly")),
            P(None, ("fsdp", "blk", "uly")),
            P(("fsdp", "blk", "uly"), None),
            P(("fsdp", "blk", "uly"), None),
            P(("fsdp", "blk", "uly"), None),
            P(("fsdp", "blk", "uly"), None),
            P(("fsdp", "blk", "uly")),
            P(("fsdp", "blk", "uly"), None),
            P(("fsdp", "blk", "uly"), None),
            P(("fsdp", "blk", "uly"), None),
        ),
        check_vma=False,
    )
    return step
```

```python
import functools
import math

import jax
import jax.numpy as jnp
from jax import lax
from jax.experimental import pallas as pl
from jax.experimental.pallas import tpu as pltpu
from jax.sharding import PartitionSpec as P

DOCS = 4


EPSILON = 1e-06
THETA = 1000000.0


def passed_along(value, axis, steps):
    count = lax.axis_size(axis)
    first, last = (max(0, -steps), min(count, count - steps))
    return lax.ppermute(value, axis, [(source, source + steps) for source in range(first, last)])


def from_behind(value, axis, steps):
    count = lax.axis_size(axis)
    pairs = [(source, (source + steps) % count) for source in range(count)]
    return lax.ppermute(value, axis, pairs)


def rms_norm(vector, weight):
    mean_square = jnp.mean(vector * vector, axis=-1, keepdims=True)
    return vector * lax.rsqrt(mean_square + EPSILON) * weight


def rotate(vector, cosine, sine_table):
    half_width = vector.shape[-1] // 2
    turned = jnp.concatenate([-vector[..., half_width:], vector[..., :half_width]], axis=-1)
    return vector * cosine + turned * sine_table


def prepare(query_pre, key_before_rotate, gains, cosine, sine_table):
    cos_heads = cosine[:, :, None, :]
    sin_heads = sine_table[:, :, None, :]
    query_rot = rotate(rms_norm(query_pre, gains[0]), cos_heads, sin_heads)
    key_rot = rotate(rms_norm(key_before_rotate, gains[1]), cos_heads, sin_heads)
    return (query_rot, key_rot)


def swiglu(gate_rows, up_rows):
    return jax.nn.silu(gate_rows) * up_rows


def fetch_attention(attn_gain, query_weight, key_matrix, value_matrix, out_weight):
    return (
        lax.all_gather(attn_gain, ("fsdp", "blk", "uly"), axis=0, tiled=True),
        lax.all_gather(query_weight, ("fsdp", "blk", "uly"), axis=0, tiled=True),
        lax.all_gather(key_matrix, ("fsdp", "blk", "uly"), axis=0, tiled=True),
        lax.all_gather(value_matrix, ("fsdp", "blk", "uly"), axis=0, tiled=True),
        lax.all_gather(out_weight, ("fsdp", "blk", "uly"), axis=0, tiled=True),
    )


def fetch_feedforward(ffn_gain, gate_weight, up_weight, down_weight):
    return (
        lax.all_gather(ffn_gain, ("fsdp", "blk", "uly"), axis=0, tiled=True),
        lax.all_gather(gate_weight, ("fsdp", "blk", "uly"), axis=0, tiled=True),
        lax.all_gather(up_weight, ("fsdp", "blk", "uly"), axis=0, tiled=True),
        lax.all_gather(down_weight, ("fsdp", "blk", "uly"), axis=0, tiled=True),
    )


def body(
    inputs,
    segments,
    attn_gain,
    head_gains,
    query_weight,
    key_matrix,
    value_matrix,
    out_weight,
    ffn_gain,
    gate_weight,
    up_weight,
    down_weight,
    cotangent,
):
    seq_count, tok_count, model_width = inputs.shape
    head_dim = head_gains.shape[1]
    query_heads = query_weight.shape[1] // head_dim
    value_heads = key_matrix.shape[1] // head_dim
    heads_per_group = query_heads // value_heads
    uly_size = lax.axis_size("uly")
    blk_size = lax.axis_size("blk")
    blk_index = lax.axis_index("blk")
    uly_index = lax.axis_index("uly")
    offset = (blk_index * uly_size + uly_index) * tok_count
    doc_ids = jnp.arange(DOCS, dtype=jnp.int32)
    starts = jnp.sum((segments[:, None, :] < doc_ids[None, :, None]).astype(jnp.int32), axis=2)
    local_segs = lax.dynamic_slice_in_dim(segments, offset, tok_count, 1)
    doc_start = jnp.sum(
        jnp.where(local_segs[:, :, None] == doc_ids[None, None, :], starts[:, None, :], 0), axis=2
    )
    token_place = (offset + jnp.arange(tok_count, dtype=jnp.int32)[None, :] - doc_start).astype(
        jnp.float32
    )
    inverse = jnp.exp(
        jnp.arange(head_dim // 2, dtype=jnp.float32) * (-2.0 * math.log(THETA) / head_dim)
    )
    angles = token_place[..., None] * inverse
    cosine = jnp.concatenate([jnp.cos(angles), jnp.cos(angles)], axis=-1)
    sine_table = jnp.concatenate([jnp.sin(angles), jnp.sin(angles)], axis=-1)
    floats = inputs.astype(jnp.float32)
    gain_one, query_full, key_full, value_full, out_full = fetch_attention(
        attn_gain, query_weight, key_matrix, value_matrix, out_weight
    )
    normed_float, norm_pull_one = jax.vjp(rms_norm, floats, gain_one.astype(jnp.float32))
    normalized_input = normed_float.astype(jnp.bfloat16)
    query_pre = jnp.einsum(
        "std,de->ste", normalized_input, query_full, preferred_element_type=jnp.float32
    ).reshape(seq_count, tok_count, query_heads, head_dim)
    key_before_rotate = jnp.einsum(
        "std,de->ste", normalized_input, key_full, preferred_element_type=jnp.float32
    ).reshape(seq_count, tok_count, value_heads, head_dim)
    rows_of_value = (
        jnp.einsum("std,de->ste", normalized_input, value_full, preferred_element_type=jnp.float32)
        .astype(jnp.bfloat16)
        .reshape(seq_count, tok_count, value_heads, head_dim)
    )
    head_float = head_gains.astype(jnp.float32)

    def prepare_local(query_arg, key_arg, gains_arg):
        return prepare(query_arg, key_arg, gains_arg, cosine, sine_table)

    (query_rot, key_rot), prep_pull = jax.vjp(
        prepare_local, query_pre, key_before_rotate, head_float
    )
    query_local, key_local, value_local = (
        lax.all_to_all(
            query_rot.astype(jnp.bfloat16), "uly", split_axis=2, concat_axis=1, tiled=True
        ),
        lax.all_to_all(
            key_rot.astype(jnp.bfloat16), "uly", split_axis=2, concat_axis=1, tiled=True
        ),
        lax.all_to_all(rows_of_value, "uly", split_axis=2, concat_axis=1, tiled=True),
    )
    block_len = query_local.shape[1]
    local_kv = key_local.shape[2]
    query_group = query_local.reshape(seq_count, block_len, local_kv, heads_per_group, head_dim)
    bound = math.sqrt(head_dim) * jnp.max(jnp.abs(head_float[0])) * jnp.max(jnp.abs(head_float[1]))
    scale = head_dim ** (-0.5)
    query_index = blk_index * block_len + jnp.arange(block_len, dtype=jnp.int32)
    query_segs = lax.dynamic_slice_in_dim(segments, blk_index * block_len, block_len, 1)

    def block_weights(keys_in, source):
        key_index = source * block_len + jnp.arange(block_len, dtype=jnp.int32)
        key_segs = lax.dynamic_slice_in_dim(segments, source * block_len, block_len, 1)
        allowed = (key_index[None, None, :] <= query_index[None, :, None]) & (
            key_segs[:, None, :] == query_segs[:, :, None]
        )
        scores = (
            jnp.einsum(
                "sqhgd,skhd->shgqk", query_group, keys_in, preferred_element_type=jnp.float32
            )
            * scale
        )
        return jnp.where(allowed[:, None, None], jnp.exp(scores - bound), 0.0)

    def absorb(stats, key_value, source):
        row_sums, summed = stats
        weights = block_weights(key_value[0], source)
        row_sums = row_sums + jnp.sum(weights, axis=-1)
        summed = summed + jnp.einsum(
            "shgqk,skhd->sqhgd",
            weights.astype(jnp.bfloat16),
            key_value[1],
            preferred_element_type=jnp.float32,
        )
        return (row_sums, summed)

    own_pair = jnp.stack([key_local, value_local])
    start_stats = (
        jnp.zeros((seq_count, local_kv, heads_per_group, block_len), jnp.float32),
        jnp.zeros((seq_count, block_len, local_kv, heads_per_group, head_dim), jnp.float32),
    )
    first_stats = absorb(start_stats, own_pair, blk_index)

    def forward_turn(turn_index, carry):
        key_value, stats_in = carry
        key_value = passed_along(key_value, "blk", 1)
        stats_in = lax.cond(
            turn_index <= blk_index,
            lambda holding: absorb(holding, key_value, blk_index - turn_index),
            lambda holding: holding,
            stats_in,
        )
        return (key_value, stats_in)

    moved_pair, (row_totals, summed_all) = lax.fori_loop(
        1, blk_size, forward_turn, (own_pair, first_stats)
    )
    attended = summed_all / jnp.transpose(row_totals, (0, 3, 1, 2))[..., None]
    attended_tok = lax.all_to_all(
        attended.reshape(seq_count, block_len, local_kv * heads_per_group, head_dim).astype(
            jnp.bfloat16
        ),
        "uly",
        split_axis=1,
        concat_axis=2,
        tiled=True,
    ).reshape(seq_count, tok_count, query_heads * head_dim)
    middle = floats + jnp.einsum(
        "ste,ed->std", attended_tok, out_full, preferred_element_type=jnp.float32
    )
    gain_two, gate_full, up_full, down_full = fetch_feedforward(
        ffn_gain, gate_weight, up_weight, down_weight
    )
    normed_two_float, norm_pull_two = jax.vjp(rms_norm, middle, gain_two.astype(jnp.float32))
    normed_two = normed_two_float.astype(jnp.bfloat16)
    gate_rows = jnp.einsum("std,df->stf", normed_two, gate_full, preferred_element_type=jnp.float32)
    up_rows = jnp.einsum("std,df->stf", normed_two, up_full, preferred_element_type=jnp.float32)
    hidden_float, swiglu_pull = jax.vjp(swiglu, gate_rows, up_rows)
    hidden = hidden_float.astype(jnp.bfloat16)
    outputs = (
        middle + jnp.einsum("stf,fd->std", hidden, down_full, preferred_element_type=jnp.float32)
    ).astype(jnp.bfloat16)
    refetched = fetch_feedforward(ffn_gain, gate_weight, up_weight, down_weight)
    gate_back, up_back, down_back = (refetched[1], refetched[2], refetched[3])
    grad_out = cotangent.astype(jnp.float32)
    down_grad = jnp.einsum("stf,std->fd", hidden, cotangent, preferred_element_type=jnp.float32)
    grad_hidden = jnp.einsum(
        "std,fd->stf", cotangent, down_back, preferred_element_type=jnp.float32
    )
    grad_gate, grad_up = swiglu_pull(grad_hidden)
    grad_gate = grad_gate.astype(jnp.bfloat16)
    grad_up = grad_up.astype(jnp.bfloat16)
    gate_grad = jnp.einsum("std,stf->df", normed_two, grad_gate, preferred_element_type=jnp.float32)
    up_grad = jnp.einsum("std,stf->df", normed_two, grad_up, preferred_element_type=jnp.float32)
    grad_normed_two = jnp.einsum(
        "stf,df->std", grad_gate, gate_back, preferred_element_type=jnp.float32
    ) + jnp.einsum("stf,df->std", grad_up, up_back, preferred_element_type=jnp.float32)
    middle_part, gain_two_grad = norm_pull_two(grad_normed_two)
    grad_middle = grad_out + middle_part
    ffn_shares = (
        lax.psum_scatter(gain_two_grad, ("fsdp", "blk", "uly"), scatter_dimension=0, tiled=True),
        lax.psum_scatter(gate_grad, ("fsdp", "blk", "uly"), scatter_dimension=0, tiled=True),
        lax.psum_scatter(up_grad, ("fsdp", "blk", "uly"), scatter_dimension=0, tiled=True),
        lax.psum_scatter(down_grad, ("fsdp", "blk", "uly"), scatter_dimension=0, tiled=True),
    )
    fetched_again = fetch_attention(attn_gain, query_weight, key_matrix, value_matrix, out_weight)
    query_back, key_back, value_back, out_back = (
        fetched_again[1],
        fetched_again[2],
        fetched_again[3],
        fetched_again[4],
    )
    grad_middle_low = grad_middle.astype(jnp.bfloat16)
    out_grad = jnp.einsum(
        "ste,std->ed", attended_tok, grad_middle_low, preferred_element_type=jnp.float32
    )
    grad_att_tok = (
        jnp.einsum("std,ed->ste", grad_middle_low, out_back, preferred_element_type=jnp.float32)
        .astype(jnp.bfloat16)
        .reshape(seq_count, tok_count, query_heads, head_dim)
    )
    grad_att = lax.all_to_all(grad_att_tok, "uly", split_axis=2, concat_axis=1, tiled=True).reshape(
        seq_count, block_len, local_kv, heads_per_group, head_dim
    )
    delta = jnp.transpose(jnp.sum(grad_att.astype(jnp.float32) * attended, axis=-1), (0, 2, 3, 1))

    def block_grads(key_value, source):
        keys_in = key_value[0]
        values_in = key_value[1]
        probs = block_weights(keys_in, source) / row_totals[..., None]
        grad_probs = jnp.einsum(
            "sqhgd,skhd->shgqk", grad_att, values_in, preferred_element_type=jnp.float32
        )
        grad_scores = (probs * (grad_probs - delta[..., None])).astype(jnp.bfloat16)
        grad_query = (
            jnp.einsum(
                "shgqk,skhd->sqhgd", grad_scores, keys_in, preferred_element_type=jnp.float32
            )
            * scale
        )
        grad_keys = (
            jnp.einsum(
                "shgqk,sqhgd->skhd", grad_scores, query_group, preferred_element_type=jnp.float32
            )
            * scale
        )
        grad_values = jnp.einsum(
            "shgqk,sqhgd->skhd",
            probs.astype(jnp.bfloat16),
            grad_att,
            preferred_element_type=jnp.float32,
        )
        return (grad_query, jnp.stack([grad_keys, grad_values]))

    def pass_grads(moving):
        return from_behind(moving.astype(jnp.bfloat16), "blk", 1).astype(moving.dtype)

    query_start, pair_start = block_grads(own_pair, blk_index)

    def backward_turn(turn_index, carry):
        key_value, query_acc, pair_acc = carry
        key_value = passed_along(key_value, "blk", 1)
        pair_acc = pass_grads(pair_acc)

        def accumulate(holding):
            part_query, part_pair = block_grads(key_value, blk_index - turn_index)
            return (holding[0] + part_query, holding[1] + part_pair)

        query_acc, pair_acc = lax.cond(
            turn_index <= blk_index, accumulate, lambda holding: holding, (query_acc, pair_acc)
        )
        return (key_value, query_acc, pair_acc)

    spent_pair, query_total, pair_total = lax.fori_loop(
        1, blk_size, backward_turn, (own_pair, query_start, pair_start)
    )
    pair_total = pass_grads(pair_total)
    grad_query_low = query_total.reshape(
        seq_count, block_len, local_kv * heads_per_group, head_dim
    ).astype(jnp.bfloat16)
    grad_query_tok, grad_key_tok, grad_value_tok = (
        lax.all_to_all(grad_query_low, "uly", split_axis=1, concat_axis=2, tiled=True),
        lax.all_to_all(
            pair_total[0].astype(jnp.bfloat16), "uly", split_axis=1, concat_axis=2, tiled=True
        ),
        lax.all_to_all(
            pair_total[1].astype(jnp.bfloat16), "uly", split_axis=1, concat_axis=2, tiled=True
        ),
    )
    grad_query_pre, grad_key_pre, heads_grad = prep_pull(
        (grad_query_tok.astype(jnp.float32), grad_key_tok.astype(jnp.float32))
    )
    grad_query_flat = grad_query_pre.astype(jnp.bfloat16).reshape(
        seq_count, tok_count, query_heads * head_dim
    )
    grad_key_flat = grad_key_pre.astype(jnp.bfloat16).reshape(
        seq_count, tok_count, value_heads * head_dim
    )
    grad_value_flat = grad_value_tok.reshape(seq_count, tok_count, value_heads * head_dim)
    query_grad = jnp.einsum(
        "std,ste->de", normalized_input, grad_query_flat, preferred_element_type=jnp.float32
    )
    key_grad = jnp.einsum(
        "std,ste->de", normalized_input, grad_key_flat, preferred_element_type=jnp.float32
    )
    value_grad = jnp.einsum(
        "std,ste->de", normalized_input, grad_value_flat, preferred_element_type=jnp.float32
    )
    grad_normed = jnp.einsum(
        "ste,de->std", grad_query_flat, query_back, preferred_element_type=jnp.float32
    )
    grad_normed = grad_normed + jnp.einsum(
        "ste,de->std", grad_key_flat, key_back, preferred_element_type=jnp.float32
    )
    grad_normed = grad_normed + jnp.einsum(
        "ste,de->std", grad_value_flat, value_back, preferred_element_type=jnp.float32
    )
    input_part, gain_one_grad = norm_pull_one(grad_normed)
    input_grad = (grad_middle + input_part).astype(jnp.bfloat16)
    attn_shares = (
        lax.psum_scatter(gain_one_grad, ("fsdp", "blk", "uly"), scatter_dimension=0, tiled=True),
        lax.psum_scatter(heads_grad, ("fsdp", "blk", "uly"), scatter_dimension=1, tiled=True),
        lax.psum_scatter(query_grad, ("fsdp", "blk", "uly"), scatter_dimension=0, tiled=True),
        lax.psum_scatter(key_grad, ("fsdp", "blk", "uly"), scatter_dimension=0, tiled=True),
        lax.psum_scatter(value_grad, ("fsdp", "blk", "uly"), scatter_dimension=0, tiled=True),
        lax.psum_scatter(out_grad, ("fsdp", "blk", "uly"), scatter_dimension=0, tiled=True),
    )
    return (
        outputs,
        input_grad,
        attn_shares[0],
        attn_shares[1],
        attn_shares[2],
        attn_shares[3],
        attn_shares[4],
        attn_shares[5],
        ffn_shares[0],
        ffn_shares[1],
        ffn_shares[2],
        ffn_shares[3],
    )


MESH = pl.DeviceIdType.MESH
ANY = pl.BlockSpec(memory_space=pl.ANY)
VMEM = pl.BlockSpec(memory_space=pltpu.VMEM)
PLANE = [(dx, dy, dc) for dx in (0, 1) for dy in (0, 1) for dc in (0, 1)]
FAR = [(1, 1, 0), (1, 0, 0), (0, 1, 0)]
TURNS = (1, 2, 3)
SEM = pltpu.SemaphoreType.DMA


class Place:
    def __init__(self):
        self.x = lax.axis_index("fsdp")
        self.block = lax.axis_index("blk")
        self.z = lax.axis_index("uly")
        self.y, self.c = (self.block // 2, self.block % 2)
        self.head = 4 * self.x + self.block
        self.here = (self.x, self.block, self.z)

    def coords(self, dx, dy, dc):
        return ((self.x + dx) % 2, (self.y + dy) % 2, (self.c + dc) % 2)

    def peer(self, dx, dy, dc):
        x, y, c = self.coords(dx, dy, dc)
        return (x, 2 * y + c, self.z)

    def index(self, dx, dy, dc):
        x, y, c = self.coords(dx, dy, dc)
        return 4 * x + 2 * y + c

    def shard(self, ref, dx=0, dy=0, dc=0):
        x, y, c = self.coords(dx, dy, dc)
        return ref.at[2 * y + c, :, x]

    def behind(self, turn):
        return (self.z + 4 - turn) % 4

    def ahead(self, turn):
        return (self.z + turn) % 4

    def line(self, turn):
        return (self.x, self.block, self.ahead(turn))


def remote(src, dst, send_sem, recv_sem, device):
    return pltpu.make_async_remote_copy(
        src_ref=src,
        dst_ref=dst,
        send_sem=send_sem,
        recv_sem=recv_sem,
        device_id=device,
        device_id_type=MESH,
    )


def arrived(ref, sem):
    pltpu.make_async_copy(ref, ref, sem).wait()


def meet(peers):
    barrier = pltpu.get_barrier_semaphore()
    for peer in peers:
        pl.semaphore_signal(barrier, inc=1, device_id=peer, device_id_type=MESH)
    pl.semaphore_wait(barrier, len(peers))


class Sends:
    def __init__(self):
        self.pending = []

    def go(self, *args):
        copy = remote(*args)
        copy.start()
        self.pending.append((None, copy))

    def go_if(self, condition, *args):
        copy = remote(*args)
        pl.when(condition)(lambda: copy.start())
        self.pending.append((condition, copy))

    def drain(self):
        for condition, copy in self.pending:
            if condition is None:
                copy.wait_send()
            else:
                pl.when(condition)(lambda copy=copy: copy.wait_send())


WAYS = [(1, 0, 0), (0, 1, 0)]


def spread_start(me, sends, src, full, send_sems, recv_sems):
    for n, d, half in ((0, WAYS[0], 0), (1, WAYS[1], 1), (0, WAYS[0], 1), (1, WAYS[1], 0)):
        rows, k = (pl.ds(2 * half, 2), 2 * n + half)
        dst = me.shard(full).at[rows]
        sends.go(src.at[rows], dst, send_sems.at[k], recv_sems.at[k], me.peer(*d))
    sends.go(src, me.shard(full), send_sems.at[4], recv_sems.at[4], me.peer(0, 0, 1))


def spread_relay(me, sends, full, send_sems, recv_sems):
    for n in (0, 1):
        rows = pl.ds(2 * n, 2)
        part = me.shard(full, *WAYS[n]).at[rows]
        arrived(part, recv_sems.at[3 * n])
        sends.go(part, part, send_sems.at[5 + n], recv_sems.at[5 + n], me.peer(*WAYS[1 - n]))
    for n in (0, 1):
        rows = pl.ds(2 * (1 - n), 2)
        part = me.shard(full, *WAYS[n])
        arrived(part.at[rows], recv_sems.at[n + 1])
        sends.go(part, part, send_sems.at[7 + n], recv_sems.at[7 + n], me.peer(0, 0, 1))


def spread_far(me, sends, full, send_sems, recv_sems):
    for n in (0, 1):
        part = me.shard(full, 1, 1, 0).at[pl.ds(2 * n, 2)]
        arrived(part, recv_sems.at[5 + n])
        sends.go(part, part, send_sems.at[9 + n], recv_sems.at[9 + n], me.peer(0, 0, 1))


def spread_finish(me, full, recv_sems):
    arrived(me.shard(full, 0, 0, 1), recv_sems.at[4])
    for n in (0, 1):
        arrived(me.shard(full, *WAYS[n][:2], 1), recv_sems.at[7 + n])
        arrived(me.shard(full, 1, 1, 1).at[pl.ds(2 * n, 2)], recv_sems.at[9 + n])


PIECES = (0, 1, 3, 2)


def piece_start(me, sends, full, turn, send_sems, recv_sems):
    part = full.at[me.block, (me.z + turn) % 4, me.x]
    for n, d in enumerate(WAYS + [(0, 0, 1)]):
        k = 4 * n + turn
        sends.go(part, part, send_sems.at[k], recv_sems.at[k], me.peer(*d))


def piece_relay(me, sends, full, send_sems, recv_sems, turns):
    for turn in turns:
        n = int(turn > 1)
        for way in (n, 1 - n):
            x, y, c = me.coords(*WAYS[way])
            part = full.at[2 * y + c, (me.z + turn) % 4, x]
            k = 4 * way + turn
            arrived(part, recv_sems.at[k])
            if way == n:
                sends.go(part, part, send_sems.at[12 + turn], recv_sems.at[12 + turn], me.peer(*WAYS[1 - n]))
            sends.go(part, part, send_sems.at[16 + k], recv_sems.at[16 + k], me.peer(0, 0, 1))


def piece_far(me, sends, full, send_sems, recv_sems):
    for turn in PIECES:
        x, y, c = me.coords(1, 1, 0)
        part = full.at[2 * y + c, (me.z + turn) % 4, x]
        arrived(part, recv_sems.at[12 + turn])
        sends.go(part, part, send_sems.at[24 + turn], recv_sems.at[24 + turn], me.peer(0, 0, 1))


def piece_finish(me, full, recv_sems):
    for n, (dx, dy) in enumerate(((0, 0), (1, 0), (0, 1), (1, 1))):
        x, y, c = me.coords(dx, dy, 1)
        for turn in PIECES:
            arrived(full.at[2 * y + c, (me.z + turn) % 4, x], recv_sems.at[(8, 16, 20, 24)[n] + turn])


def full_shape(tokens, width):
    return (4, 4, 2, tokens // 32, width)


def line_spread(me, sends, src, part, sems):
    for dz in (2, 1):
        sends.go_if(me.z < 4 - dz, src, part(me.z), sems.at[0, dz - 1], sems.at[1, dz - 1], me.line(dz))
        sends.go_if(me.z >= dz, src, part(me.z), sems.at[0, dz + 1], sems.at[1, dz + 1], me.line(4 - dz))


def relay_spread(me, sends, src, part, sems):
    outer, _ = outer_inner(me)
    mine = part(me.z)
    for up, far in ((True, me.z == 0), (False, me.z == 3)):
        k = 1 if up else 3
        sends.go_if(far, src, mine, sems.at[0, k], sems.at[1, k], me.line(2))
        near = me.z < 3 if up else me.z > 0
        k = 0 if up else 2
        sends.go_if(near, src, mine, sems.at[0, k], sems.at[1, k], me.line(1 if up else 3))


def relay_forward(me, sends, part, sems):
    _, inner = outer_inner(me)
    ref = part((7 - me.z) % 4)
    pl.when(me.z == 1)(lambda: arrived(ref, sems.at[1, 2]))
    pl.when(me.z == 2)(lambda: arrived(ref, sems.at[1, 0]))
    target = (me.x, me.block, (3 * me.z + 1) % 4)
    for z, k in ((1, 3), (2, 1)):
        sends.go_if(me.z == z, ref, ref, sems.at[0, k], sems.at[1, k], target)
    line_forward(me, sends, part, sems)


def relay_finish(me, part, sems):
    z = me.z
    low, high = (part((z + 3) % 4), part((z + 1) % 4))
    pl.when(jnp.logical_or(z == 1, z == 3))(lambda: arrived(low, sems.at[1, 0]))
    pl.when(jnp.logical_or(z == 0, z == 2))(lambda: arrived(high, sems.at[1, 2]))

    @pl.when(z == 3)
    def _():
        arrived(part((z + 2) % 4), sems.at[1, 1])
        arrived(high, sems.at[1, 4])

    @pl.when(z == 0)
    def _():
        arrived(part((z + 2) % 4), sems.at[1, 3])
        arrived(low, sems.at[1, 4])


def line_forward(me, sends, part, sems):
    inner = jnp.logical_or(me.z == 1, me.z == 2)
    ref = part((me.z + 2) % 4)
    pl.when(me.z == 1)(lambda: arrived(ref, sems.at[1, 3]))
    pl.when(me.z == 2)(lambda: arrived(ref, sems.at[1, 1]))
    target = (me.x, me.block, (3 * me.z + 1) % 4)
    sends.go_if(inner, ref, ref, sems.at[0, 4], sems.at[1, 4], target)


def line_finish(me, part, sems):
    z = me.z
    pl.when(z > 0)(lambda: arrived(part((z + 3) % 4), sems.at[1, 0]))
    pl.when(z < 3)(lambda: arrived(part((z + 1) % 4), sems.at[1, 2]))

    @pl.when(z == 3)
    def _():
        arrived(part((z + 2) % 4), sems.at[1, 1])
        arrived(part((z + 1) % 4), sems.at[1, 4])

    @pl.when(z == 0)
    def _():
        arrived(part((z + 2) % 4), sems.at[1, 3])
        arrived(part((z + 3) % 4), sems.at[1, 4])


def line_to(me, z):
    return (me.x, me.block, z)


def outer_inner(me):
    outer = jnp.logical_or(me.z == 0, me.z == 3)
    return (outer, jnp.logical_not(outer))


def reduce_start(me, sends, own, came, sems, joins=True, rest=True):
    z = me.z
    outer, _ = outer_inner(me)
    if joins:
        nearer = line_to(me, 1 + z // 3)
        sends.go_if(outer, own((7 - z) % 4), came.at[3], sems.at[0, 3], sems.at[1, 3], nearer)
    if rest:
        far = (z + 2) % 4
        sends.go_if(outer, own(far), came.at[2], sems.at[0, 2], sems.at[1, 2], line_to(me, far))
        sends.go_if(z < 3, own((z + 1) % 4), came.at[0], sems.at[0, 0], sems.at[1, 0], me.line(1))
        sends.go_if(z > 0, own((z + 3) % 4), came.at[1], sems.at[0, 1], sems.at[1, 1], me.line(3))


def reduce_join(me, sends, own, came, buf, sems):
    _, inner = outer_inner(me)
    far = (me.z + 2) % 4

    @pl.when(inner)
    def _():
        arrived(came.at[3], sems.at[1, 3])
        buf[...] = (own(far)[...].astype(jnp.float32) + came[3].astype(jnp.float32)).astype(buf.dtype)

    sends.go_if(inner, buf, came.at[2], sems.at[0, 2], sems.at[1, 2], line_to(me, far))


def reduce_total(me, own, came, total, sems):
    arrived(came.at[2], sems.at[1, 2])
    total[...] = own(me.z)[...].astype(jnp.float32) + came[2].astype(jnp.float32)

    @pl.when(me.z > 0)
    def _():
        arrived(came.at[0], sems.at[1, 0])
        total[...] = total[...] + came[0].astype(jnp.float32)

    @pl.when(me.z < 3)
    def _():
        arrived(came.at[1], sems.at[1, 1])
        total[...] = total[...] + came[1].astype(jnp.float32)


def lanes(shape):
    return lax.broadcasted_iota(jnp.int32, shape, len(shape) - 1)


def turned(vector):
    half = vector.shape[-1] // 2
    sign = jnp.where(lanes((1, 2 * half)) < half, -1.0, 1.0)
    return pltpu.roll(vector, half, 1) * sign


def head_scale(vector):
    return lax.rsqrt(jnp.mean(vector * vector, axis=-1, keepdims=True) + EPSILON)


def mat(a, b):
    return jnp.dot(a, b, preferred_element_type=jnp.float32)


def mat_right(a, b):
    return lax.dot_general(a, b, (((1,), (1,)), ((), ())), preferred_element_type=jnp.float32)


def mat_left(a, b):
    return lax.dot_general(a, b, (((0,), (0,)), ((), ())), preferred_element_type=jnp.float32)


def permute_in(me, src_ref, full_ref, send_sems, recv_sems, wait=False):
    half = src_ref.shape[1] // 2
    for j in (0, 1):
        for to in (0, 1):
            src = src_ref.at[j, pl.ds(half * to, half)]
            dst = full_ref.at[me.block, me.z, to]
            mine = jnp.logical_and(me.x == to, me.z == 2 * j + me.x)
            copy = remote(
                src, dst, send_sems.at[2 * j + to], recv_sems.at[me.z], (to, me.block, 2 * j + me.x)
            )
            if wait:
                pl.when(jnp.logical_not(mine))(lambda copy=copy: copy.wait_send())
                continue
            pl.when(jnp.logical_not(mine))(lambda copy=copy: copy.start())
            own = pltpu.make_async_copy(src, dst, recv_sems.at[me.z])
            pl.when(mine)(lambda own=own: own.start())


def permuted_in(me, full_ref, recv_sems):
    for k in range(4):
        arrived(full_ref.at[me.block, k, me.x], recv_sems.at[k])


def half_block(me, part, sibling, send_sems, recv_sems, b, sends=None):
    other = me.c != b % 2
    dy = (me.y + b // 2) % 2
    for to in (0, 1):
        slot = 3 - 2 * ((me.x + to) % 2) - dy
        copy = remote(
            part.at[b, :, to], sibling.at[slot], send_sems.at[slot], recv_sems.at[slot],
            me.peer(0, 0, 1),
        )
        if sends is None:
            pl.when(other)(lambda copy=copy: copy.start())
        else:
            sends.pending.append((other, copy))


HALVES = (slice(0, 2), slice(2, 4))


def half_own(me, part, i, dims):
    x, y, c = me.coords(*(FAR + [(0, 0, 0)])[i])
    ref, sibling = part
    return ref[2 * y + c, dims, x].astype(jnp.float32) + sibling[i, dims].astype(jnp.float32)


def half_out(me, sends, part, sibling, out, came, send_sems, recv_sems):
    low, both = (out.dtype, (part, sibling))
    near = (me.peer(1, 0, 0), me.peer(0, 1, 0))
    arrived(sibling.at[0], recv_sems.at[0])
    out[0] = half_own(me, both, 0, slice(None)).astype(low)
    for n, dims in enumerate(HALVES):
        half = pl.ds(2 * n, 2)
        sends.go(out.at[0, half], came.at[0, half], send_sems.at[4 + n], recv_sems.at[4 + n], near[n])
    for n, dims in enumerate(HALVES):
        arrived(sibling.at[1 + n], recv_sems.at[1 + n])
        out[1 + n, dims] = half_own(me, both, 1 + n, dims).astype(low)
        half = pl.ds(2 * n, 2)
        k = 6 + 2 * n
        sends.go(out.at[1 + n, half], came.at[1 + n, half], send_sems.at[k], recv_sems.at[k], near[n])


def half_relay(me, sends, part, sibling, out, came, send_sems, recv_sems):
    low, both = (out.dtype, (part, sibling))
    near = (me.peer(1, 0, 0), me.peer(0, 1, 0))
    for n in (0, 1):
        dims, half, k = (HALVES[1 - n], pl.ds(2 * (1 - n), 2), 7 + 2 * n)
        arrived(came.at[0, half], recv_sems.at[5 - n])
        total = half_own(me, both, 1 + n, dims) + came[0, dims].astype(jnp.float32)
        out[1 + n, dims] = total.astype(low)
        sends.go(out.at[1 + n, half], came.at[1 + n, half], send_sems.at[k], recv_sems.at[k], near[n])


def half_in(me, part, sibling, came, recv_sems):
    arrived(sibling.at[3], recv_sems.at[3])
    for n, half in ((0, 0), (1, 1), (0, 1), (1, 0)):
        k = 6 + 2 * n + (half != n)
        arrived(came.at[1 + n, pl.ds(2 * half, 2)], recv_sems.at[k])
    total = half_own(me, (part, sibling), 3, slice(None))
    return total + came[1].astype(jnp.float32) + came[2].astype(jnp.float32)


def half_scratch(tokens, width):
    piece = (4, tokens // 32, width)
    return [
        pltpu.VMEM((4,) + piece, jnp.bfloat16),
        pltpu.VMEM((3,) + piece, jnp.bfloat16),
        pltpu.VMEM((3,) + piece, jnp.bfloat16),
        SEM((10,)),
        SEM((10,)),
    ]


def gain_row(gains_ref, kind):
    rows = [jnp.sum(gains_ref[p, :, kind, :], axis=0, keepdims=True) for p in range(8)]
    return jnp.concatenate(rows, axis=1)


def allowed_keys(segcol, segrow, b, kb):
    same = segcol[b] == segrow[:, 256 * kb : 256 * kb + 256]
    if kb < b:
        return same
    rows = lax.broadcasted_iota(jnp.int32, (256, 256), 0)
    return jnp.logical_and(same, lanes((256, 256)) <= rows)


def norm_back(grad, vector, gain, scale):
    weighted = grad * gain
    inner = jnp.mean(weighted * vector, axis=-1, keepdims=True)
    return scale * weighted - vector * (scale * scale * scale * inner)


def permute_out(me, src_ref, dst_ref, send_sems, recv_sems, wait=False):
    half = dst_ref.shape[1] // 2
    for k in range(4):
        src = src_ref.at[k]
        dst = dst_ref.at[me.z // 2, pl.ds(half * me.x, half)]
        mine = jnp.logical_and(me.x == me.z % 2, me.z == k)
        spot = 2 * (me.z // 2) + me.x
        copy = remote(src, dst, send_sems.at[k], recv_sems.at[spot], (me.z % 2, me.block, k))
        if wait:
            pl.when(jnp.logical_not(mine))(lambda copy=copy: copy.wait_send())
            continue
        pl.when(jnp.logical_not(mine))(lambda copy=copy: copy.start())
        own = pltpu.make_async_copy(src, dst, recv_sems.at[spot])
        pl.when(mine)(lambda own=own: own.start())


def permuted_out(dst_ref, recv_sems):
    half = dst_ref.shape[1] // 2
    for j in (0, 1):
        for to in (0, 1):
            arrived(dst_ref.at[j, pl.ds(half * to, half)], recv_sems.at[2 * j + to])


def total_row(share):
    return jnp.sum(jnp.sum(share, axis=0), axis=0, keepdims=True)


def layer_kernel(
    x_ref, cot_ref, seg_ref, q_ref, k_ref, v_ref, g_ref, u_ref, o_ref, d_ref, ag_ref, fg_ref, hg_in,
    y_ref, gx_ref, dq_ref, dk_ref, dv_ref, dg_ref, du_ref, sums_ref, osum_out, dsum_out,
    xf, cf, wf, of, df, guf, segs, gains, n1, nf, gf, pre, qkv, segcol, cos_s, sin_s, att, attlow,
    totals, kept, part, part2, down, n2, gm, y_s, gi_s, mid, gmid,
    gates, hid, gboth, ga, gq, gk, gv, gpre, dd, dgu, do, dw,
    d_came, d_buf, gu_came, gu_buf, gu_total, gu_sum, o_came, o_buf, w_came, w_buf, w_total, w_sum,
    pack, packs, linep,
    sib1, out1, came1, hs1, hr1, sib2, out2, came2, hs2, hr2, sib3, out3, came3, hs3, hr3,
    ps, pr, as_, ar, xas, xar, ws, wr, us, ur, gs, gr, zq, zo, zd, zg, zu, rg, rd, ro, rw, cs, cr, ds, dr, ls, raw1, raw2, hg_low, hg_ref, osum_ref, dsum_ref,
):
    me = Place()
    x, z, p = (me.x, me.z, me.head)
    low, wide_t = (jnp.bfloat16, jnp.float32)
    across = [((x + 1) % 2, me.block, me.ahead(turn)) for turn in TURNS]
    meet([me.peer(*d) for d in PLANE[1:]] + [me.line(turn) for turn in TURNS] + across)
    sends, early = (Sends(), Sends())

    def local(src, dst, sem):
        copy = pltpu.make_async_copy(src, dst, sem)
        copy.start()
        return copy

    own_raw = [local(ref, dst, ls.at[6 + i]) for i, (ref, dst) in enumerate(((ag_ref, raw1), (fg_ref, raw2)))]
    own_head = local(hg_in, hg_low, ls.at[0])
    own_seg = local(seg_ref, segs.at[x], ls.at[1])
    sends.go(seg_ref, segs.at[x], ls.at[2], ls.at[3], me.peer(1, 0, 0))
    permute_in(me, x_ref, xf, ps.at[0], pr.at[0])
    permute_in(me, cot_ref, cf, ps.at[1], pr.at[1])
    own_o = local(o_ref, of.at[z], ls.at[4])
    own_d = local(d_ref, df.at[z], ls.at[5])
    wide, narrow = (q_ref.shape[1] // 8, k_ref.shape[1] // 8)
    cuts = ((q_ref, wide, 0), (k_ref, narrow, wide), (v_ref, narrow, wide + narrow))
    for i, d in enumerate(PLANE):
        t = me.index(*d)
        for n, (ref, width, off) in enumerate(cuts):
            src = ref.at[:, pl.ds(pl.multiple_of(t * width, 128), width)]
            dst = wf.at[p, z, :, pl.ds(off, width)]
            if i == 0:
                local(src, dst, wr.at[n])
            else:
                sends.go(src, dst, ws.at[3 * i + n], wr.at[3 * i + n], me.peer(*d))
    ff = g_ref.shape[1] // 8
    for copy in own_raw + [own_head]:
        copy.wait()
    hg_ref[...] = hg_low[...].astype(wide_t)
    piece = raw1.shape[1]
    rows = [raw1[...].astype(wide_t), raw2[...].astype(wide_t), jnp.zeros((6, piece), wide_t)]
    rows = [jnp.concatenate(rows, axis=0), jnp.zeros((8, 128 - piece), wide_t)]
    rows = jnp.concatenate(rows, axis=1)
    gains[p, z] = pltpu.roll(rows, piece * z, 1)
    arrived(xf.at[me.block, z, x], pr.at[0, z])
    piece_start(me, sends, xf, 0, xas, xar)
    for turn in TURNS:
        sends.go(gains.at[p, z], gains.at[p, z], gs.at[turn], gr.at[turn], me.line(turn))
    for i, d in enumerate(PLANE):
        t = me.index(*d)
        for n, (ref, width, off) in enumerate(cuts):
            arrived(wf.at[t, z, :, pl.ds(off, width)], wr.at[3 * i + n])
    qkv_part = lambda k: wf.at[:, k]
    o_part = lambda k: of.at[k]
    d_part = lambda k: df.at[k]
    gate_part = lambda k: guf.at[:, k, :, pl.ds(0, ff)]
    up_part = lambda k: guf.at[:, k, :, pl.ds(ff, ff)]
    line_spread(me, sends, qkv_part(z), qkv_part, zq)
    for turn in (1, 3, 2):
        k = (z + turn) % 4
        arrived(xf.at[me.block, k, x], pr.at[0, k])
        piece_start(me, sends, xf, turn, xas, xar)
    line_spread(me, sends, o_ref, o_part, zo)
    piece_relay(me, sends, xf, xas, xar, PIECES[:2])
    line_forward(me, sends, qkv_part, zq)
    piece_relay(me, sends, xf, xas, xar, PIECES[2:])
    for turn in TURNS:
        arrived(gains.at[p, me.behind(turn)], gr.at[turn])
    for i, d in enumerate(PLANE[1:]):
        sends.go(gains.at[p], gains.at[p], gs.at[4 + i], gr.at[4 + i], me.peer(*d))
    for i, d in enumerate(PLANE):
        t = me.index(*d)
        for n, ref in enumerate((g_ref, u_ref)):
            src = ref.at[:, pl.ds(pl.multiple_of(t * ff, 128), ff)]
            dst = guf.at[p, z, :, pl.ds(n * ff, ff)]
            if i == 0:
                local(src, dst, ur.at[n])
            else:
                sends.go(src, dst, us.at[2 * i + n], ur.at[2 * i + n], me.peer(*d))
    permuted_in(me, cf, pr.at[1])
    spread_start(me, sends, me.shard(cf), cf, as_.at[1], ar.at[1])
    own_seg.wait()
    arrived(segs.at[(x + 1) % 2], ls.at[3])
    head_dim = hg_ref.shape[1]
    segrow = segs[z % 2, pl.ds(z // 2, 1), :]
    tokens = segrow.shape[1]
    column = jnp.transpose(jnp.broadcast_to(segrow.astype(wide_t), (8, tokens)))[:, :1]
    segcol[...] = column.astype(jnp.int32).reshape(4, 256, 1)
    half_lane = (lanes((1, head_dim)) % (head_dim // 2)).astype(wide_t)
    inverse = jnp.exp(half_lane * (-2.0 * math.log(THETA) / head_dim))
    steps = lax.broadcasted_iota(jnp.int32, (32, head_dim), 0).astype(wide_t) * inverse
    cl, sl = (jnp.cos(steps), jnp.sin(steps))
    ch, sh = (jnp.cos(steps * 32.0), jnp.sin(steps * 32.0))
    doc_cos, doc_sin = ([], [])
    for doc in range(DOCS):
        start = jnp.sum((segrow < doc).astype(wide_t), axis=1, keepdims=True)
        doc_cos.append(jnp.cos(start * inverse))
        doc_sin.append(jnp.sin(start * inverse))
    for b in range(4):
        hi_c, hi_s = (ch[8 * b : 8 * b + 8][:, None, :], sh[8 * b : 8 * b + 8][:, None, :])
        cos_at = (hi_c * cl[None] - hi_s * sl[None]).reshape(256, head_dim)
        sin_at = (hi_s * cl[None] + hi_c * sl[None]).reshape(256, head_dim)
        column = segcol[b]
        cd, sd = (jnp.broadcast_to(v[0], (256, head_dim)) for v in (doc_cos, doc_sin))
        for doc in range(1, DOCS):
            cd = jnp.where(column == doc, doc_cos[doc], cd)
            sd = jnp.where(column == doc, doc_sin[doc], sd)
        cos_s[b] = cos_at * cd + sin_at * sd
        sin_s[b] = sin_at * cd - cos_at * sd
    piece_far(me, sends, xf, xas, xar)
    for i, d in enumerate(PLANE[1:]):
        arrived(gains.at[me.index(*d)], gr.at[4 + i])
    gain_one, gain_two = (gain_row(gains, 0), gain_row(gains, 1))
    piece_finish(me, xf, xar)

    @pl.loop(0, 4)
    def _(b):
        rows = xf[b].reshape(256, -1).astype(wide_t)
        n1[b] = (rows * head_scale(rows) * gain_one).astype(low)

    line_finish(me, qkv_part, zq)

    own_o.wait()
    line_forward(me, sends, o_part, zo)
    for i, d in enumerate(PLANE):
        t = me.index(*d)
        for n in (0, 1):
            arrived(guf.at[t, z, :, pl.ds(n * ff, ff)], ur.at[2 * i + n])
    relay_spread(me, sends, gate_part(z), gate_part, zg)
    line_spread(me, sends, up_part(z), up_part, zu)
    spread_relay(me, sends, cf, as_.at[1], ar.at[1])
    @pl.loop(0, 4)
    def _(b):
        rows = mat(n1[b], wf[...].reshape(-1, wf.shape[3]))
        pre[b] = rows
        cosine, sine = (cos_s[b], sin_s[b])
        for h in range(3):
            v = rows[:, head_dim * h : head_dim * (h + 1)]
            n = v * head_scale(v) * hg_ref[pl.ds(h // 2, 1), :]
            qkv[b, :, pl.ds(head_dim * h, head_dim)] = (n * cosine + turned(n) * sine).astype(low)
        qkv[b, :, pl.ds(3 * head_dim, head_dim)] = rows[:, 3 * head_dim :].astype(low)

    top = lambda r: jnp.max(jnp.abs(hg_ref[pl.ds(r, 1), :]), axis=1, keepdims=True)
    bound = math.sqrt(head_dim) * top(0) * top(1)
    scale = head_dim ** (-0.5)
    key_at, value_at = (pl.ds(2 * head_dim, head_dim), pl.ds(3 * head_dim, head_dim))

    def weights_of(b, kb, query):
        s = mat_right(query, qkv[kb, :, key_at]) * scale
        return jnp.where(allowed_keys(segcol, segrow, b, kb), jnp.exp(s - bound), 0.0)

    for b in range(4):

        @pl.loop(0, 2)
        def _(h, b=b):
            at = pl.ds(pl.multiple_of(head_dim * h, head_dim), head_dim)
            query = qkv[b, :, at]
            total, mixed = (None, None)
            for kb in range(b + 1):
                w = weights_of(b, kb, query)
                t = jnp.sum(w, axis=1, keepdims=True)
                kept[h, b * (b + 1) // 2 + kb] = w.astype(low)
                m = mat(w.astype(low), qkv[kb, :, value_at])
                total = t if kb == 0 else total + t
                mixed = m if kb == 0 else mixed + m
            mixed = mixed / total
            totals[b, h] = total
            att[b, :, at] = mixed
            attlow[b, :, at] = mixed.astype(low)

    line_finish(me, o_part, zo)

    @pl.loop(0, 4)
    def _(b):
        rows = mat(attlow[b], of[...].reshape(-1, of.shape[2])).astype(low)
        part[b] = rows.reshape(part.shape[1:])
        half_block(me, part, sib1, hs1, hr1, b)

    for b in range(4):
        half_block(me, part, sib1, hs1, hr1, b, early)
    half_out(me, early, part, sib1, out1, came1, hs1, hr1)
    relay_forward(me, sends, gate_part, zg)
    half_relay(me, early, part, sib1, out1, came1, hs1, hr1)
    middle = xf[me.block, :, x].astype(wide_t) + half_in(me, part, sib1, came1, hr1)
    mid[...] = middle
    n2[...] = (middle * head_scale(middle) * gain_two).astype(low)
    own_n = local(n2, me.shard(nf), ls.at[8])
    spread_start(me, sends, n2, nf, as_.at[2], ar.at[2])
    line_forward(me, sends, up_part, zu)
    line_spread(me, sends, d_ref, d_part, zd)
    spread_relay(me, sends, nf, as_.at[2], ar.at[2])
    line_forward(me, sends, d_part, zd)
    spread_far(me, sends, nf, as_.at[2], ar.at[2])
    spread_finish(me, nf, ar.at[2])
    own_n.wait()
    relay_finish(me, gate_part, zg)
    line_finish(me, up_part, zu)

    @pl.loop(0, 4)
    def _(b):
        both = mat(nf[b].reshape(256, -1), guf[...].reshape(-1, 2 * ff))
        gates[b] = both
        gate, up = (both[:, :ff], both[:, ff:])
        hid[b] = (gate / (1.0 + jnp.exp(-gate)) * up).astype(low)

    spread_far(me, sends, cf, as_.at[1], ar.at[1])
    spread_finish(me, cf, ar.at[1])
    own_d.wait()
    dd[...] = mat_left(hid[...].reshape(-1, ff), cf[...].reshape(tokens, -1)).astype(low).reshape(dd.shape)
    own_dd = lambda k: dd.at[k]
    reduce_start(me, sends, own_dd, d_came, rd)
    line_finish(me, d_part, zd)

    @pl.loop(0, 4)
    def _(b):
        both = gates[b]
        gate, up = (both[:, :ff], both[:, ff:])
        sig = 1.0 / (1.0 + jnp.exp(-gate))
        grad = mat_right(cf[b].reshape(256, -1), df[...].reshape(ff, -1))
        gboth[b, :, pl.ds(0, ff)] = (grad * up * sig * (1.0 + gate * (1.0 - sig))).astype(low)
        gboth[b, :, pl.ds(ff, ff)] = (grad * (gate * sig)).astype(low)
        rows = mat_right(gboth[b], guf[...].reshape(-1, 2 * ff)).astype(low)
        part2[b] = rows.reshape(part2.shape[1:])
        half_block(me, part2, sib2, hs2, hr2, b)

    for b in range(4):
        half_block(me, part2, sib2, hs2, hr2, b, sends)
    half_out(me, sends, part2, sib2, out2, came2, hs2, hr2)

    @pl.loop(0, 4)
    def _(b):
        rows = nf[:, :, :, :, pl.ds(pl.multiple_of(256 * b, 256), 256)].reshape(-1, 256)
        grad = mat_left(rows, gboth[...].reshape(-1, 2 * ff)).astype(low)
        dgu[pl.ds(2 * b, 2)] = grad.reshape((2,) + dgu.shape[1:])

    own_gu = lambda k: dgu.at[:, k]
    reduce_start(me, sends, own_gu, gu_came, rg)
    half_relay(me, sends, part2, sib2, out2, came2, hs2, hr2)
    reduce_join(me, sends, own_dd, d_came, d_buf, rd)
    grad = half_in(me, part2, sib2, came2, hr2)
    middle = mid[...]
    r = head_scale(middle)
    total = cf[me.block, :, x].astype(wide_t) + norm_back(grad, middle, gain_two, r)
    gmid[...] = total
    gm[...] = total.astype(low)
    own_gm = local(gm, me.shard(gf), ls.at[9])
    spread_start(me, sends, gm, gf, as_.at[3], ar.at[3])
    share = total_row(grad * middle * r)
    for i in range(8):
        pack[pl.ds(8 + i, 1)] = share[:, 128 * i : 128 * i + 128]

    @pl.loop(0, 4)
    def _(b):
        rows = mat(hid[b], df[...].reshape(ff, -1)).astype(low)
        down[b] = rows.reshape(down.shape[1:])
        half_block(me, down, sib3, hs3, hr3, b)

    for b in range(4):
        half_block(me, down, sib3, hs3, hr3, b, sends)
    spread_relay(me, sends, gf, as_.at[3], ar.at[3])
    half_out(me, sends, down, sib3, out3, came3, hs3, hr3)
    reduce_join(me, sends, own_gu, gu_came, gu_buf, rg)
    spread_far(me, sends, gf, as_.at[3], ar.at[3])
    spread_finish(me, gf, ar.at[3])
    own_gm.wait()

    half_relay(me, sends, down, sib3, out3, came3, hs3, hr3)
    gk[...] = jnp.zeros_like(gk)
    gv[...] = jnp.zeros_like(gv)
    for b in range(4):
        ga[b] = mat_right(gf[b].reshape(256, -1), of[...].reshape(-1, of.shape[2])).astype(low)

        @pl.loop(0, 2)
        def _(h, b=b):
            at = pl.ds(pl.multiple_of(head_dim * h, head_dim), head_dim)
            query, grad = (qkv[b, :, at], ga[b, :, at])
            inv = 1.0 / totals[b, h]
            scaled = grad.astype(wide_t) * inv
            delta = jnp.sum(scaled * att[b, :, at], axis=1, keepdims=True)
            scaled = scaled.astype(low)
            grad_query = None
            for kb in range(b + 1):
                w = kept[h, b * (b + 1) // 2 + kb]
                gp = mat_right(scaled, qkv[kb, :, value_at])
                gsc = (w.astype(wide_t) * (gp - delta)).astype(low)
                m = mat(gsc, qkv[kb, :, key_at])
                grad_query = m if kb == 0 else grad_query + m
                gk[kb] += mat_left(gsc, query)
                gv[kb] += mat_left(w, scaled)
            gq[b, :, at] = grad_query

        if b == 2:
            y_s[...] = (mid[...] + half_in(me, down, sib3, came3, hr3)).astype(low)
            permute_out(me, y_s, y_ref, cs.at[0], cr.at[0])
    do[...] = mat_left(attlow[...].reshape(tokens, -1), gf[...].reshape(tokens, -1)).astype(low).reshape(do.shape)
    own_do = lambda k: do.at[k]
    reduce_start(me, sends, own_do, o_came, ro)
    pack[pl.ds(16, 8)] = jnp.zeros((8, 128), wide_t)

    @pl.loop(0, 4)
    def _(b):
        cosine, sine = (cos_s[b], sin_s[b])
        for h in range(3):
            at = pl.ds(head_dim * h, head_dim)
            source = gq[b, :, at] if h < 2 else gk[b]
            go = (source * scale).astype(low).astype(wide_t)
            gh = go * cosine - turned(go * sine)
            v = pre[b, :, at]
            r = head_scale(v)
            n = v * r
            pack[pl.ds(16 + h // 2, 1)] += jnp.sum(gh * n, axis=0, keepdims=True)
            gn = gh * hg_ref[pl.ds(h // 2, 1), :]
            gpre[b, :, at] = (r * (gn - n * jnp.mean(gn * n, axis=-1, keepdims=True))).astype(low)
        gpre[b, :, value_at] = gv[b].astype(low)

    early.drain()

    @pl.loop(0, 4)
    def _(b):
        rows = mat_right(gpre[b], wf[...].reshape(-1, wf.shape[3])).astype(low)
        part[b] = rows.reshape(part.shape[1:])
        half_block(me, part, sib1, hs1, hr1, b)

    for b in range(4):
        half_block(me, part, sib1, hs1, hr1, b, sends)
    half_out(me, sends, part, sib1, out1, came1, hs1, hr1)
    @pl.loop(0, 4)
    def _(b):
        rows = n1[:, :, pl.ds(pl.multiple_of(256 * b, 256), 256)].reshape(-1, 256)
        grad = mat_left(rows, gpre[...].reshape(tokens, -1)).astype(low)
        grad = grad.reshape((2,) + dw.shape[2:-1] + (2 * dw.shape[-1],))
        for n in (0, 1):
            dw[n, pl.ds(2 * b, 2)] = grad[..., n * dw.shape[-1] : (n + 1) * dw.shape[-1]]

    own_dw = [lambda k, n=n: dw.at[n, :, k] for n in (0, 1)]
    for joins in (True, False):
        for n in (0, 1):
            reduce_start(me, sends, own_dw[n], w_came.at[n], rw.at[n], joins, not joins)
    half_relay(me, sends, part, sib1, out1, came1, hs1, hr1)
    reduce_join(me, sends, own_do, o_came, o_buf, ro)
    reduce_total(me, own_gu, gu_came, gu_total, rg)
    gu_sum[...] = gu_total[...].astype(low)
    for i, d in enumerate(PLANE):
        t = me.index(*d)
        for n, ref in enumerate((dg_ref, du_ref)):
            src = gu_sum.at[t, :, pl.ds(n * ff, ff)]
            dst = ref.at[:, pl.ds(pl.multiple_of(p * ff, 128), ff)]
            if i == 0:
                local(src, dst, dr.at[n])
            else:
                sends.go(src, dst, ds.at[2 * i + n], dr.at[2 * i + n], me.peer(*d))
    reduce_total(me, own_dd, d_came, dsum_ref, rd)
    dsum_copy = local(dsum_ref, dsum_out, ls.at[6])
    for n in (0, 1):
        reduce_join(me, sends, own_dw[n], w_came.at[n], w_buf.at[n], rw.at[n])
    grad = half_in(me, part, sib1, came1, hr1)
    rows = xf[me.block, :, x].astype(wide_t)
    r = head_scale(rows)
    share = total_row(grad * rows * r)
    for i in range(8):
        pack[pl.ds(i, 1)] = share[:, 128 * i : 128 * i + 128]
    for i, d in enumerate(PLANE[1:]):
        sends.go(pack, packs.at[i], gs.at[11 + i], gr.at[11 + i], me.peer(*d))
    gi_s[...] = (gmid[...] + norm_back(grad, rows, gain_one, r)).astype(low)
    permute_out(me, gi_s, gx_ref, cs.at[1], cr.at[1])
    total = pack[...]
    for i in range(7):
        arrived(packs.at[i], gr.at[11 + i])
        total = total + packs[i]
    packs[7] = total
    for turn in TURNS:
        sends.go(packs.at[7], linep.at[turn - 1], gs.at[17 + turn], gr.at[17 + turn], me.line(turn))
    backs = (((dq_ref, wide, 0),), ((dk_ref, narrow, 0), (dv_ref, narrow, narrow)))
    for block in (0, 1):
        reduce_total(me, own_dw[block], w_came.at[block], w_total, rw.at[block])
        w_sum[block] = w_total[...].astype(low)
        for i, d in enumerate(PLANE):
            t = me.index(*d)
            for n, (ref, cols, off) in enumerate(backs[block]):
                src = w_sum.at[block, t, :, pl.ds(off, cols)]
                dst = ref.at[:, pl.ds(pl.multiple_of(p * cols, 128), cols)]
                k = 16 + 3 * i + block + n
                if i == 0:
                    local(src, dst, dr.at[k])
                else:
                    sends.go(src, dst, ds.at[k], dr.at[k], me.peer(*d))
    reduce_total(me, own_do, o_came, osum_ref, ro)
    osum_copy = local(osum_ref, osum_out, ls.at[7])
    for turn in TURNS:
        arrived(linep.at[turn - 1], gr.at[17 + turn])
        total = total + linep[turn - 1]
    sums_ref[...] = total
    for i, d in enumerate(PLANE):
        t = me.index(*d)
        for n, ref in enumerate((dg_ref, du_ref)):
            arrived(ref.at[:, pl.ds(pl.multiple_of(t * ff, 128), ff)], dr.at[2 * i + n])
        for n, (ref, cols, off) in enumerate(backs[0] + backs[1]):
            arrived(ref.at[:, pl.ds(pl.multiple_of(t * cols, 128), cols)], dr.at[16 + 3 * i + n])
    dsum_copy.wait()
    osum_copy.wait()
    permuted_out(y_ref, cr.at[0])
    permuted_out(gx_ref, cr.at[1])
    permute_in(me, x_ref, xf, ps.at[0], pr.at[0], wait=True)
    permute_in(me, cot_ref, cf, ps.at[1], pr.at[1], wait=True)
    permute_out(me, y_s, y_ref, cs.at[0], cr.at[0], wait=True)
    permute_out(me, gi_s, gx_ref, cs.at[1], cr.at[1], wait=True)
    sends.drain()


def layer_step(x, cot, seg, q, k, v, g, u, o, d, gain, gain_two, head_gains):
    tokens, width = (16 * x.shape[1], x.shape[2])
    rows, low, wide = (q.shape[0], jnp.bfloat16, jnp.float32)
    cols = (q.shape[1] + 2 * k.shape[1]) // 8
    att_cols, head_dim = (q.shape[1] // 8, k.shape[1] // 8)
    ff = g.shape[1] // 8
    full = full_shape(tokens, width)
    piece = (4, tokens // 32, width)
    quarter = tokens // 4
    shape, buf = (jax.ShapeDtypeStruct, pltpu.VMEM)
    blocks = lambda n, kind: buf((4, quarter, n), kind)
    return pl.pallas_call(
        layer_kernel,
        name="layer_step",
        out_shape=(
            shape(x.shape, low), shape(x.shape, low), shape(q.shape, low), shape(k.shape, low),
            shape(v.shape, low), shape(g.shape, low), shape(u.shape, low), shape((24, 128), wide),
            shape(o.shape, wide), shape(d.shape, wide),
        ),
        in_specs=[ANY] * 13,
        out_specs=(ANY,) * 7 + (VMEM, ANY, ANY),
        scratch_shapes=[
            buf(full, low), buf(full, low), buf((8, 4, rows, cols), low), buf((4,) + o.shape, low),
            buf((4,) + d.shape, low), buf((8, 4, rows, 2 * ff), low), buf((2,) + seg.shape, seg.dtype),
            buf((8, 4, 8, 128), wide), blocks(width, low), buf(full, low), buf(full, low),
            blocks(cols, wide), blocks(cols, low), blocks(1, jnp.int32), blocks(head_dim, wide),
            blocks(head_dim, wide), blocks(att_cols, wide), blocks(att_cols, low),
            buf((4, 2, quarter, 1), wide), buf((2, 10, quarter, quarter), low), buf(full, low), buf(full, low), buf(full, low),
            buf(piece, low), buf(piece, low), buf(piece, low), buf(piece, low), buf(piece, wide),
            buf(piece, wide),
            blocks(2 * ff, wide), blocks(ff, low), blocks(2 * ff, low), blocks(att_cols, low), blocks(att_cols, wide),
            blocks(head_dim, wide), blocks(head_dim, wide), blocks(cols, low),
            buf((4,) + d.shape, low), buf((8, 4, rows, 2 * ff), low), buf((4,) + o.shape, low),
            buf((2, 8, 4, rows, cols // 2), low),
            buf((4,) + d.shape, low), buf(d.shape, low),
            buf((4, 8, rows, 2 * ff), low), buf((8, rows, 2 * ff), low), buf((8, rows, 2 * ff), wide),
            buf((8, rows, 2 * ff), low),
            buf((4,) + o.shape, low), buf(o.shape, low),
            buf((2, 4, 8, rows, cols // 2), low), buf((2, 8, rows, cols // 2), low),
            buf((8, rows, cols // 2), wide), buf((2, 8, rows, cols // 2), low),
            buf((24, 128), wide), buf((8, 24, 128), wide), buf((3, 24, 128), wide),
        ]
        + half_scratch(tokens, width) * 3
        + [SEM((2, 4)), SEM((2, 4)), SEM((4, 11)), SEM((4, 11)), SEM((28,)), SEM((28,)), SEM((24,)), SEM((24,)), SEM((16,)), SEM((16,))]
        + [SEM((21,)), SEM((21,))]
        + [SEM((2, 5))] * 5
        + [SEM((2, 4))] * 3
        + [SEM((2, 2, 4))]
        + [SEM((2, 4)), SEM((2, 4)), SEM((40,)), SEM((40,)), SEM((10,)),
            buf(gain.shape, low), buf(gain.shape, low), buf(head_gains.shape, low), buf(head_gains.shape, wide),
            buf(o.shape, wide), buf(d.shape, wide)],
        compiler_params=pltpu.CompilerParams(
            collective_id=0, has_side_effects=True, vmem_limit_bytes=67043328
        ),
    )(x, cot, seg, q, k, v, g, u, o, d, gain, gain_two, head_gains)


def finish_kernel(sums_ref, *refs):
    half = (len(refs) - 3) // 2
    for src, dst in zip(refs[:half], refs[half : 2 * half]):
        dst[...] = src[...].astype(dst.dtype)
    attn_ref, ffn_ref, head_ref = refs[2 * half :]
    z = lax.axis_index("uly")
    head = 4 * lax.axis_index("fsdp") + lax.axis_index("blk")
    piece, share = (attn_ref.shape[1], head_ref.shape[1])
    rows = [sums_ref[pl.ds(head, 1), :], sums_ref[pl.ds(8 + head, 1), :], jnp.zeros((6, 128), jnp.float32)]
    rows = pltpu.roll(jnp.concatenate(rows, axis=0), 128 - piece * z, 1)
    attn_ref[...] = rows[0:1, :piece]
    ffn_ref[...] = rows[1:2, :piece]
    head_ref[...] = pltpu.roll(sums_ref[16:24, :], 128 - (4 * head + z) * share, 1)[0:2, :share]


def finish_step(piece, share, sums, *arrays):
    return pl.pallas_call(
        finish_kernel,
        name="finish_step",
        out_shape=tuple(
            jax.ShapeDtypeStruct(v.shape, v.dtype if i < 2 else jnp.float32) for i, v in enumerate(arrays)
        )
        + tuple(jax.ShapeDtypeStruct(v, jnp.float32) for v in ((1, piece), (1, piece), (2, share))),
        in_specs=[VMEM] * (1 + len(arrays)),
        out_specs=(VMEM,) * (3 + len(arrays)),
    )(sums, *arrays)


def plane_body(
    inputs, segments, attn_gain, head_gains, query_weight, key_matrix, value_matrix, out_weight,
    ffn_gain, gate_weight, up_weight, down_weight, cotangent,
):
    outputs, grad_inputs, q_grad, k_grad, v_grad, g_grad, u_grad, sums, out_grad, down_grad = layer_step(
        inputs, cotangent, segments, query_weight, key_matrix, value_matrix, gate_weight, up_weight,
        out_weight, down_weight, attn_gain[None], ffn_gain[None], head_gains,
    )
    (
        outputs, grad_inputs, q_grad, k_grad, v_grad, out_grad, g_grad, u_grad, down_grad, attn_gain_grad,
        ffn_gain_grad, head_gain_grad,
    ) = finish_step(
        attn_gain.shape[0], head_gains.shape[1] // 32, sums, outputs, grad_inputs, q_grad, k_grad, v_grad,
        out_grad, g_grad, u_grad, down_grad,
    )
    return (
        outputs, grad_inputs, attn_gain_grad[0], head_gain_grad, q_grad, k_grad, v_grad, out_grad,
        ffn_gain_grad[0], g_grad, u_grad, down_grad,
    )


def fits_plane(mesh, seq_count, heads):
    shape = mesh.shape
    return (shape["fsdp"], shape["blk"], shape["uly"]) == (2, 4, 4) and seq_count == 4 and heads == 8


def solution(mesh):
    def step(*arrays):
        seq_count = arrays[0].shape[0]
        heads = arrays[5].shape[1] // arrays[3].shape[1]
        chosen = plane_body if fits_plane(mesh, seq_count, heads) else body
        return mapped(chosen)(*arrays)

    mapped = functools.partial(
        jax.shard_map,
        mesh=mesh,
        in_specs=(
            P("fsdp", ("blk", "uly"), None),
            P("fsdp", None),
            P(("fsdp", "blk", "uly")),
            P(),
            P(("fsdp", "blk", "uly"), None),
            P(("fsdp", "blk", "uly"), None),
            P(("fsdp", "blk", "uly"), None),
            P(("fsdp", "blk", "uly"), None),
            P(("fsdp", "blk", "uly")),
            P(("fsdp", "blk", "uly"), None),
            P(("fsdp", "blk", "uly"), None),
            P(("fsdp", "blk", "uly"), None),
            P("fsdp", ("blk", "uly"), None),
        ),
        out_specs=(
            P("fsdp", ("blk", "uly"), None),
            P("fsdp", ("blk", "uly"), None),
            P(("fsdp", "blk", "uly")),
            P(None, ("fsdp", "blk", "uly")),
            P(("fsdp", "blk", "uly"), None),
            P(("fsdp", "blk", "uly"), None),
            P(("fsdp", "blk", "uly"), None),
            P(("fsdp", "blk", "uly"), None),
            P(("fsdp", "blk", "uly")),
            P(("fsdp", "blk", "uly"), None),
            P(("fsdp", "blk", "uly"), None),
            P(("fsdp", "blk", "uly"), None),
        ),
        check_vma=False,
    )
    return step
```
